32 devices in a mesh: batch: 2 (over x), row: 4 (over z), col: 4 (over y, core).
Axes of the slice: x: 2, y: 2, z: 4, core: 2. Of those that a mesh axis runs over, the one named last changes fastest.
Arguments:
- a_mat: bfloat16 [2048, 32768], P(('batch', 'row'), 'col'), parts along dimension 0
Outputs:
- output: bfloat16 [2048, 1024], P(('batch', 'row'), 'col'), parts along dimension 0
There are 2 independent parts. The reference program is written for one: setup_inputs(seed, part) draws one part's arguments, and reference() takes and returns one part's arrays. A program takes and returns all parts, laid end to end along the dimension named above; each array names one.
All inputs are finite; a program needn't handle non-finite values.
Results may differ from the reference program's by a relative error of at most 0.001.
Values are sent between devices in bfloat16 or wider.
A program may use at most 1 GiB of HBM per device.

```python
import jax
import jax.numpy as jnp
from jax import lax

N = 1024
BLOCK = 256
M_COLS = 32768
ROW_GROUPS = 4
COL_GROUPS = 4


def setup_inputs(seed: int = 0, part: int = 0) -> dict:
    base_key = jax.random.fold_in(jax.random.key(seed), part)
    values = jax.random.normal(base_key, (N, M_COLS), jnp.float32) * (M_COLS ** -0.25)
    return {"a_mat": values.astype(jnp.bfloat16)}


def global_index(size, groups):
    stored = jnp.arange(size)
    per_group = size // groups
    group_id = stored // per_group
    within = stored % per_group
    return ((within // BLOCK) * groups + group_id) * BLOCK + within % BLOCK


def reference(a_mat):
    blocks = N // BLOCK
    natural = a_mat.reshape(ROW_GROUPS, blocks // ROW_GROUPS, BLOCK, M_COLS).transpose(1, 0, 2, 3)
    col_order = natural.reshape(blocks // COL_GROUPS, COL_GROUPS, BLOCK, M_COLS).transpose(1, 0, 2, 3).reshape(N, M_COLS)
    col_trans = col_order.T
    row_index = global_index(N, ROW_GROUPS).reshape(blocks, BLOCK)
    col_index = global_index(N, COL_GROUPS)

    def one_block(block_item):
        row_blk, idx_blk = block_item
        product = jnp.dot(row_blk, col_trans, preferred_element_type=jnp.float32)
        return jnp.where(idx_blk[:, None] >= col_index[None, :], product, 0.0).astype(jnp.bfloat16)

    result = lax.map(one_block, (a_mat.reshape(blocks, BLOCK, M_COLS), row_index))
    return result.reshape(N, N)
```

```python
import functools

import jax
import jax.numpy as jnp
from jax import lax
from jax.experimental import pallas as pl
from jax.experimental.pallas import tpu as pltpu
from jax.sharding import PartitionSpec as P

MESH = pl.DeviceIdType.MESH
NP = 8
NS = 8


def mm(a, b):
    return lax.dot_general(a, b, (((1,), (1,)), ((), ())), preferred_element_type=jnp.float32)


def kernel(a_ref, o_ref, X, Y, W, Pa, Qa, R, PR, ld, s_z, r_y, s_d, r_d, r_w, s_p, r_p, s_q, r_r):
    rows, m = a_ref.shape
    pw = m // (2 * NP)
    ul, dl = pw - pw // 4, pw + pw // 4
    ku = (NP - 1) * pw + ul
    kd = m - ku
    st = rows // NS
    z = lax.axis_index("row")
    c = lax.axis_index("col")
    y = c // 2
    k = c % 2
    sib = 2 * y + 1 - k

    def rcopy(src, dst, ss, rs, row, col):
        return pltpu.make_async_remote_copy(
            src_ref=src, dst_ref=dst, send_sem=ss, recv_sem=rs, device_id={"row": row, "col": col}, device_id_type=MESH)

    def wait_recv(ref, sem):
        pltpu.make_async_copy(ref, ref, sem).wait()

    def up(p, w):
        return pl.ds(pl.multiple_of(p * pw, 128), w)

    def dn(p, w):
        return pl.ds(pl.multiple_of(ku + p * pw, 128), w)

    def off(p, w):
        return pl.ds(pl.multiple_of(p * pw, 128), w)

    def strip(s):
        return pl.ds(pl.multiple_of(s * st, st), st)

    DALL = pl.ds(ku, kd)

    def each(n, fn):
        lax.fori_loop(0, n, lambda i, u: (fn(i), u)[1], 0)

    load = pltpu.make_async_copy(a_ref, X.at[k], ld.at[0])
    load.start()
    bar = pltpu.get_barrier_semaphore()
    for dz in range(4):
        for dc in range(4):
            if dz or dc:
                pl.semaphore_signal(bar, inc=1, device_id={"row": (z + dz) % 4, "col": (c + dc) % 4}, device_id_type=MESH)
    pl.semaphore_wait(bar, 15)

    def z0_send(kind, p):
        if kind == "d":
            cs = dn(p, dl if p == NP - 1 else pw)
            n = p
        else:
            cs = up(p, ul if p == NP - 1 else pw)
            n = NP + p
        return rcopy(a_ref.at[:, cs], Y.at[k, :, cs], s_z.at[n], r_y.at[n], 1, c)

    def z3_send(kind, p):
        if kind == "u":
            cs = up(p, ul if p == NP - 1 else pw)
            return rcopy(a_ref.at[:, cs], Y.at[k, :, cs], s_z.at[p], r_y.at[p], 2, c)
        return rcopy(a_ref.at[strip(p), DALL], Y.at[k, strip(p), DALL], s_z.at[NP + p], r_y.at[NP + p], 2, c)

    def z1_send(p):
        w = ul if p == NP - 1 else pw
        return rcopy(a_ref.at[:, up(p, w)], W.at[k, :, up(p, w)], s_z.at[p], r_w.at[k, p], 2, 2 * y + 1)

    def z2_send(p):
        w = dl if p == NP - 1 else pw
        return rcopy(a_ref.at[:, dn(p, w)], W.at[k, :, off(p, w)], s_z.at[p], r_w.at[k, p], 1, 2 * y)

    @pl.when(z == 0)
    def _():
        for p in range(NP - 2):
            z0_send("d", p).start()
        z0_send("u", 0).start()
        for p in range(NP - 2, NP):
            z0_send("d", p).start()
        for p in range(1, NP):
            z0_send("u", p).start()

    @pl.when(z == 3)
    def _():
        for p in range(NP - 2):
            z3_send("u", p).start()
        z3_send("d", 0).start()
        for p in range(NP - 2, NP):
            z3_send("u", p).start()
        for p in range(1, NS):
            z3_send("d", p).start()

    x_d = rcopy(a_ref.at[:, DALL], X.at[k, :, DALL], s_d.at[NP], r_d.at[NP], z, sib)
    x_u = rcopy(a_ref.at[:, pl.ds(0, ku)], X.at[k, :, pl.ds(0, ku)], s_d.at[NP], r_d.at[NP], z, sib)

    @pl.when(z == 1)
    def _():
        for p in range(NP):
            z1_send(p).start()
        x_d.start()

    @pl.when(z == 2)
    def _():
        for p in range(NP):
            z2_send(p).start()
        x_u.start()

    Pa[...] = jnp.zeros_like(Pa)
    Qa[...] = jnp.zeros_like(Qa)
    load.wait()
    dq = jnp.where(z == 1, 1, 0)

    def diag(p):
        cs = off(p, pw)
        Qa[dq] += mm(X[k, :, cs], X[k, :, cs])

    each(2 * NP, diag)

    def slot(owner):
        return (c - owner + 3) % 4

    dsend = rcopy(Qa.at[dq], R.at[slot(z)], s_q.at[NS], r_r.at[slot(z), 0], z, z)

    @pl.when(c != z)
    def _():
        dsend.start()

    def a_fwd(p, w):
        return rcopy(Y.at[k, :, dn(p, w)], Y.at[k, :, dn(p, w)], s_d.at[p], r_d.at[p], z, sib)

    def zA(p, w):
        cs = dn(p, w)
        wait_recv(Y.at[k, :, cs], r_y.at[p])
        a_fwd(p, w).start()
        Qa[0] += mm(X[k, :, cs], Y[k, :, cs])

    def zC(q, w):
        cs, ws = dn(q, w), off(q, w)
        wait_recv(Y.at[1 - k, :, cs], r_d.at[q])
        for h in range(2):
            wait_recv(W.at[h, :, ws], r_w.at[h, q])
        for h in range(2):
            Pa[0] += mm(W[h, :, ws], Y[h, :, cs])
            Pa[1] += mm(W[h, :, ws], X[h, :, cs])

    def b_fwd(p, w):
        return rcopy(Y.at[k, :, up(p, w)], W.at[k, :, up(p, w)], s_z.at[NP + p], r_w.at[k, p], 2, 2 * y)

    def zB(p, w):
        cs = up(p, w)
        wait_recv(Y.at[k, :, cs], r_y.at[NP + p])
        b_fwd(p, w).start()
        Qa[0] += mm(X[k, :, cs], Y[k, :, cs])

    def p_send(j):
        return rcopy(Pa.at[j], PR.at[0], s_p.at[j], r_p.at[NS], 2, 2 * y + j)

    def ps_send(j, s):
        return rcopy(Pa.at[j, strip(s)], PR.at[1, strip(s)], s_p.at[2 * s + j], r_p.at[s], 2, 2 * y + j)

    def zS(s):
        for h in range(2):
            wait_recv(W.at[h, strip(s), pl.ds(0, kd)], r_w.at[h, s])
        for j, B in ((0, Y), (1, X)):
            acc = mm(W[0, strip(s), :kd], B[0, :, DALL])
            acc += mm(W[1, strip(s), :kd], B[1, :, DALL])
            Pa[j, strip(s), :] = acc
        for j in range(2):
            ps_send(j, s).start()

    q0send = rcopy(Qa.at[0], R.at[slot(0)], s_q.at[0], r_r.at[slot(0), 0], 1, 0)

    @pl.when(z == 1)
    def _():
        wait_recv(X.at[1 - k, :, DALL], r_d.at[NP])

        def step_a(p):
            zA(p, pw)

            @pl.when((k == 0) & (p >= 1))
            def _():
                zC(p - 1, pw)

        each(NP - 1, step_a)
        zA(NP - 1, dl)

        @pl.when(k == 0)
        def _():
            zC(NP - 2, pw)

        zB(0, pw)

        @pl.when(k == 0)
        def _():
            zC(NP - 1, dl)
            p_send(0).start()
            p_send(1).start()

        @pl.when(k == 1)
        def _():
            each(NP - 1, lambda p: wait_recv(Y.at[0, :, dn(p, pw)], r_d.at[p]))
            wait_recv(Y.at[0, :, dn(NP - 1, dl)], r_d.at[NP - 1])

        def step_b(i):
            zB(i + 1, pw)

            @pl.when((k == 1) & (i >= 1))
            def _():
                zS(i - 1)

        each(NP - 2, step_b)
        zB(NP - 1, ul)

        @pl.when(c != 0)
        def _():
            q0send.start()

        @pl.when(k == 1)
        def _():
            each(NS - (NP - 3), lambda i: zS(i + NP - 3))

    def u_fwd(p, w):
        return rcopy(Y.at[k, :, up(p, w)], Y.at[k, :, up(p, w)], s_d.at[p], r_d.at[p], z, sib)

    def yA(p, w):
        cs = up(p, w)
        wait_recv(Y.at[k, :, cs], r_y.at[p])
        u_fwd(p, w).start()
        Qa[1] += mm(Y[k, :, cs], X[k, :, cs])

    def yC(q, w):
        cs = up(q, w)
        for h in range(2):
            wait_recv(W.at[h, :, cs], r_w.at[h, q])
        for h in range(2):
            Pa[0] += mm(X[h, :, cs], W[h, :, cs])
            Pa[1] += mm(Y[h, :, cs], W[h, :, cs])

    def d_fwd(s):
        return rcopy(Y.at[k, strip(s), DALL], W.at[k, strip(s), pl.ds(0, kd)], s_z.at[NP + s], r_w.at[k, s], 1, 2 * y + 1)

    def q1send(s):
        return rcopy(Qa.at[1, strip(s)], R.at[c, strip(s)], s_q.at[s], r_r.at[c, s], 3, 2)

    def yB(s):
        wait_recv(Y.at[k, strip(s), DALL], r_y.at[NP + s])
        d_fwd(s).start()
        Qa[1, strip(s), :] += mm(Y[k, strip(s), DALL], X[k, :, DALL])
        q1send(s).start()

    s2send = rcopy(Pa.at[0], R.at[0], s_p.at[NS], r_r.at[0, 0], 2, k)

    def s3send(s):
        return rcopy(Pa.at[1, strip(s)], R.at[y, strip(s)], s_p.at[s], r_r.at[y, s], 3, k)

    def fin(s):
        wait_recv(PR.at[1, strip(s)], r_p.at[s])
        Pa[1, strip(s), :] += PR[1, strip(s), :]
        s3send(s).start()

    @pl.when(z == 2)
    def _():
        wait_recv(X.at[1 - k, :, pl.ds(0, ku)], r_d.at[NP])

        def step_a(p):
            yA(p, pw)

            @pl.when((k == 1) & (p >= 1))
            def _():
                wait_recv(Y.at[0, :, up(p - 1, pw)], r_d.at[p - 1])
                yC(p - 1, pw)

        each(NP - 1, step_a)
        yA(NP - 1, ul)

        @pl.when(k == 1)
        def _():
            wait_recv(Y.at[0, :, up(NP - 2, pw)], r_d.at[NP - 2])
            yC(NP - 2, pw)

        yB(0)

        @pl.when(k == 1)
        def _():
            wait_recv(Y.at[0, :, up(NP - 1, ul)], r_d.at[NP - 1])
            yC(NP - 1, ul)

        @pl.when(k == 0)
        def _():
            each(NP - 1, lambda p: wait_recv(Y.at[1, :, up(p, pw)], r_d.at[p]))
            wait_recv(Y.at[1, :, up(NP - 1, ul)], r_d.at[NP - 1])

        def step_b(i):
            yB(i + 1)

            @pl.when((k == 0) & (i >= 1))
            def _():
                yC(i - 1, pw)

        each(NS - 1, step_b)

        @pl.when(k == 0)
        def _():
            each(NP - 1 - (NS - 2), lambda i: yC(i + NS - 2, pw))
            yC(NP - 1, ul)

        wait_recv(PR.at[0], r_p.at[NS])
        Pa[0] += PR[0]

        @pl.when(y == 1)
        def _():
            s2send.start()

        each(NS, fin)

    diff = lax.broadcasted_iota(jnp.int32, (rows, rows), 0) - lax.broadcasted_iota(jnp.int32, (rows, rows), 1)

    @pl.when(c > z)
    def _():
        o_ref[...] = jnp.zeros_like(o_ref)

    @pl.when(c == z)
    def _():
        for i in range(3):
            wait_recv(R.at[i], r_r.at[i, 0])
        total = Qa[dq] + R[0] + R[1] + R[2]
        o_ref[...] = jnp.where(diff >= 0, total, 0.0).astype(o_ref.dtype)

    @pl.when((z == 1) & (c == 0))
    def _():
        for i in range(3):
            wait_recv(R.at[i], r_r.at[i, 0])
        o_ref[...] = (Qa[0] + R[0] + R[1] + R[2]).astype(o_ref.dtype)

    @pl.when((z == 2) & (y == 0))
    def _():
        wait_recv(R.at[0], r_r.at[0, 0])
        o_ref[...] = (Pa[0] + R[0]).astype(o_ref.dtype)

    @pl.when((z == 3) & (c == 2))
    def _():
        for s in range(NS):
            for i in range(4):
                wait_recv(R.at[i, strip(s)], r_r.at[i, s])
        o_ref[...] = (R[0] + R[1] + R[2] + R[3]).astype(o_ref.dtype)

    @pl.when((z == 3) & (y == 0))
    def _():
        for s in range(NS):
            for i in range(2):
                wait_recv(R.at[i, strip(s)], r_r.at[i, s])
        o_ref[...] = (R[0] + R[1]).astype(o_ref.dtype)

    @pl.when(c != z)
    def _():
        dsend.wait_send()

    @pl.when(z == 0)
    def _():
        for p in range(NP):
            z0_send("d", p).wait_send()
            z0_send("u", p).wait_send()

    @pl.when(z == 3)
    def _():
        for p in range(NP):
            z3_send("u", p).wait_send()
        for p in range(NS):
            z3_send("d", p).wait_send()

    @pl.when(z == 1)
    def _():
        x_d.wait_send()
        for p in range(NP):
            z1_send(p).wait_send()
            a_fwd(p, dl if p == NP - 1 else pw).wait_send()
            b_fwd(p, ul if p == NP - 1 else pw).wait_send()

        @pl.when(k == 0)
        def _():
            for j in range(2):
                p_send(j).wait_send()

        @pl.when(k == 1)
        def _():
            for s in range(NS):
                for j in range(2):
                    ps_send(j, s).wait_send()

        @pl.when(c != 0)
        def _():
            q0send.wait_send()

    @pl.when(z == 2)
    def _():
        x_u.wait_send()
        for p in range(NP):
            z2_send(p).wait_send()
            u_fwd(p, ul if p == NP - 1 else pw).wait_send()
        for s in range(NS):
            d_fwd(s).wait_send()
            q1send(s).wait_send()
            s3send(s).wait_send()

        @pl.when(y == 1)
        def _():
            s2send.wait_send()


def solution(mesh):
    def local_fn(a_local):
        rows, m = a_local.shape
        pw = m // (2 * NP)
        kd = NP * pw + pw // 4
        f32, bf16 = jnp.float32, jnp.bfloat16
        dma = pltpu.SemaphoreType.DMA
        return pl.pallas_call(
            kernel,
            out_shape=jax.ShapeDtypeStruct((rows, rows), bf16),
            in_specs=[pl.BlockSpec(memory_space=pl.ANY)],
            out_specs=pl.BlockSpec(memory_space=pltpu.VMEM),
            scratch_shapes=[
                pltpu.VMEM((2, rows, m), bf16),
                pltpu.VMEM((2, rows, m), bf16),
                pltpu.VMEM((2, rows, kd), bf16),
                pltpu.VMEM((2, rows, rows), f32),
                pltpu.VMEM((2, rows, rows), f32),
                pltpu.VMEM((4, rows, rows), f32),
                pltpu.VMEM((2, rows, rows), f32),
                dma((1,)), dma((2 * NP,)), dma((2 * NP,)), dma((NP + 1,)), dma((NP + 1,)), dma((2, NP,)),
                dma((2 * NS,)), dma((NS + 1,)), dma((NS + 1,)), dma((4, NS)),
            ],
            compiler_params=pltpu.CompilerParams(
                collective_id=0, has_side_effects=True, vmem_limit_bytes=50 * 1024 * 1024),
        )(a_local)

    part_spec = P(("batch", "row"), "col")
    return jax.shard_map(local_fn, mesh=mesh, in_specs=(part_spec,), out_specs=part_spec, check_vma=False)
```

```python
import jax
import jax.numpy as jnp
from jax import lax
from jax.experimental import pallas as pl
from jax.experimental.pallas import tpu as pltpu
from jax.sharding import PartitionSpec as P

MESH = pl.DeviceIdType.MESH
PW = 256
NU = 15
NL = 2
NS = 8
G0 = 5
NG = NS - G0 + 1


def mm(a, b):
    return lax.dot_general(a, b, (((1,), (1,)), ((), ())), preferred_element_type=jnp.float32)


def kernel(a_ref, o_ref, X, Y, W, Pa, Qa, R, PR, far, ld, s_z, r_y, s_d, r_d, r_w, s_p, r_p, s_q, r_r):
    rows, m = a_ref.shape
    ku = NU * PW
    kd = m - ku
    nd = kd // PW
    half = rows // 2
    st = half // NS
    us = rows // NS
    z = lax.axis_index("row")
    c = lax.axis_index("col")
    y = c // 2
    k = c % 2
    sib = 2 * y + 1 - k

    def rcopy(src, dst, ss, rs, row, col):
        return pltpu.make_async_remote_copy(
            src_ref=src, dst_ref=dst, send_sem=ss, recv_sem=rs, device_id={"row": row, "col": col}, device_id_type=MESH)

    def wait_recv(ref, sem):
        pltpu.make_async_copy(ref, ref, sem).wait()

    def up(p):
        return pl.ds(pl.multiple_of(p * PW, 128), PW)

    def dn(p):
        return pl.ds(pl.multiple_of(ku + p * PW, 128), PW)

    def rs_(h, s, n=1):
        return pl.ds(pl.multiple_of(h * half + s * st, st), n * st)

    def ws_(i, s, n=1):
        return pl.ds(pl.multiple_of(i * half + s * st, st), n * st)

    def us_(s):
        return pl.ds(pl.multiple_of(s * us, us), us)

    DALL = pl.ds(ku, kd)
    UALL = pl.ds(0, ku)

    def each(lo, hi, fn):
        lax.fori_loop(lo, hi, lambda i, u: (fn(i), u)[1], 0)

    load = pltpu.make_async_copy(a_ref, X.at[k], ld.at[0])
    load.start()

    def near(sem):
        for dz in (-1, 1):
            @pl.when((z + dz >= 0) & (z + dz <= 3))
            def _():
                for kk in range(2):
                    pl.semaphore_signal(sem, inc=1, device_id={"row": z + dz, "col": 2 * y + kk}, device_id_type=MESH)
        for dc in range(1, 4):
            pl.semaphore_signal(sem, inc=1, device_id={"row": z, "col": (c + dc) % 4}, device_id_type=MESH)

    n_near = jnp.where((z == 0) | (z == 3), 5, 7)
    bar = pltpu.get_barrier_semaphore()
    near(bar)
    pl.semaphore_wait(bar, n_near)

    def z0_u(q):
        return rcopy(a_ref.at[:, up(q)], Y.at[k, :, up(q)], s_z.at[q], r_y.at[q], 1, c)

    def z0_d(p):
        return rcopy(a_ref.at[:, dn(p)], Y.at[k, :, dn(p)], s_z.at[NU + p], r_y.at[NU + p], 1, c)

    def z3_d(t):
        r = rs_(t % 2, t // 2)
        return rcopy(a_ref.at[r, DALL], Y.at[k, r, DALL], s_z.at[t], r_y.at[t], 2, c)

    def z3_u(s):
        r = us_(s)
        return rcopy(a_ref.at[r, UALL], Y.at[k, r, UALL], s_z.at[2 * NS + s], r_y.at[2 * NS + s], 2, c)

    def z1_u(q):
        return rcopy(a_ref.at[:, up(q)], W.at[k, :, up(q)], s_z.at[q], r_w.at[k, q], 2, 2 * y + 1)

    def z2_d(t):
        h, s = t % 2, t // 2
        return rcopy(a_ref.at[rs_(h, s), DALL], W.at[k, ws_(1, s), pl.ds(0, kd)], s_z.at[t], r_w.at[k, NS + s], 1, 2 * y + h)

    @pl.when(z == 0)
    def _():
        each(0, NU - NL, lambda q: z0_u(q).start())
        each(0, nd, lambda p: z0_d(p).start())
        each(NU - NL, NU, lambda q: z0_u(q).start())

    @pl.when(z == 3)
    def _():
        each(0, 2 * NS, lambda t: z3_d(t).start())
        each(0, NS, lambda s: z3_u(s).start())

    x_d = rcopy(a_ref.at[:, DALL], X.at[k, :, DALL], s_d.at[nd], r_d.at[nd], z, sib)
    x_u = rcopy(a_ref.at[:, UALL], X.at[k, :, UALL], s_d.at[nd], r_d.at[nd], z, sib)

    @pl.when(z == 1)
    def _():
        each(0, NU, lambda q: z1_u(q).start())
        x_d.start()

    @pl.when(z == 2)
    def _():
        z2_d(0).start()
        z2_d(1).start()
        x_u.start()

    near(far)

    Pa[...] = jnp.zeros_like(Pa)
    Qa[...] = jnp.zeros_like(Qa)
    load.wait()
    dq = jnp.where(z == 1, 1, 0)

    def diag(p):
        cs = pl.ds(pl.multiple_of(p * 512, 512), 512)
        Qa[dq] += mm(X[k, :, cs], X[k, :, cs])

    each(0, m // 512, diag)

    def slot(owner):
        return (c - owner + 3) % 4

    dsend = rcopy(Qa.at[dq], R.at[slot(z)], s_q.at[NS], r_r.at[slot(z), 0], z, z)

    @pl.when(c != z)
    def _():
        dsend.start()

    def u_fwd(q):
        return rcopy(Y.at[k, :, up(q)], W.at[k, :, up(q)], s_z.at[NU + q], r_w.at[k, q], 2, 2 * y)

    def zU(q):
        wait_recv(Y.at[k, :, up(q)], r_y.at[q])
        u_fwd(q).start()
        Qa[0] += mm(X[k, :, up(q)], Y[k, :, up(q)])

    def d_sib(p):
        return rcopy(Y.at[k, :, dn(p)], Y.at[k, :, dn(p)], s_d.at[p], r_d.at[p], z, sib)

    def zD(p):
        wait_recv(Y.at[k, :, dn(p)], r_y.at[NU + p])
        d_sib(p).start()
        Qa[0] += mm(X[k, :, dn(p)], Y[k, :, dn(p)])

    def p3send(j):
        return rcopy(Pa.at[j, ws_(0, 0, NS)], PR.at[1, rs_(k, 0, NS)], s_p.at[j], r_p.at[k], 2, 2 * y + j)

    def p2send(g, s, n, j):
        return rcopy(Pa.at[j, ws_(1, s, n)], PR.at[0, rs_(k, s, n)], s_p.at[2 + 2 * g + j], r_p.at[2 + 2 * g + k], 2, 2 * y + j)

    def part(i, s, n, j):
        B = X if j == 1 else Y
        r = ws_(i, s, n)
        Pa[j, r, :] = mm(W[0, r, :kd], B[0, :, DALL]) + mm(W[1, r, :kd], B[1, :, DALL])

    def wait_w(i, s):
        for h in range(2):
            wait_recv(W.at[h, ws_(i, s), pl.ds(0, kd)], r_w.at[h, i * NS + s])

    q0send = rcopy(Qa.at[0], R.at[slot(0)], s_q.at[0], r_r.at[slot(0), 0], 1, 0)

    @pl.when(z == 1)
    def _():
        each(0, NU - NL, zU)
        each(0, 8, zD)
        wait_recv(X.at[1 - k, :, DALL], r_d.at[nd])
        each(0, NS, lambda s: wait_w(0, s))
        part(0, 0, NS, 1)
        p3send(1).start()
        each(8, nd - 2, zD)
        each(0, G0, lambda s: wait_w(1, s))
        part(1, 0, G0, 1)
        p2send(0, 0, G0, 1).start()
        each(nd - 2, nd, zD)
        each(0, nd, lambda p: wait_recv(Y.at[1 - k, :, dn(p)], r_d.at[p]))
        part(0, 0, NS, 0)
        p3send(0).start()
        part(1, 0, G0, 0)
        p2send(0, 0, G0, 0).start()

        def last(i):
            @pl.when(i < NL)
            def _():
                zU(NU - NL + i)

            s = G0 + i
            wait_w(1, s)
            for j in range(2):
                part(1, s, 1, j)
                p2send(1 + i, s, 1, j).start()

        each(0, NS - G0, last)

        @pl.when(c != 0)
        def _():
            q0send.start()

    def d_fwd(t):
        h, s = t % 2, t // 2
        return rcopy(Y.at[k, rs_(h, s), DALL], W.at[k, ws_(0, s), pl.ds(0, kd)], s_z.at[2 * NS + t], r_w.at[k, s], 1, 2 * y + h)

    def u_sib(s):
        return rcopy(Y.at[k, us_(s), UALL], Y.at[k, us_(s), UALL], s_d.at[s], r_d.at[s], z, sib)

    def q1send(s):
        return rcopy(Qa.at[1, us_(s)], R.at[c, us_(s)], s_q.at[s], r_r.at[c, s], 3, 2)

    def y2(q):
        for h in range(2):
            wait_recv(W.at[h, :, up(q)], r_w.at[h, q])
        Pa[0] += mm(X[0, :, up(q)], W[0, :, up(q)]) + mm(X[1, :, up(q)], W[1, :, up(q)])

    def y3(q):
        Pa[1] += mm(Y[0, :, up(q)], W[0, :, up(q)]) + mm(Y[1, :, up(q)], W[1, :, up(q)])

    s3send = rcopy(Pa.at[1], R.at[y], s_p.at[0], r_r.at[y, 0], 3, k)

    def grp(g, h):
        return rs_(h, 0, G0) if g == 0 else rs_(h, G0 + g - 1)

    def s2send(g, h):
        r = grp(g, h)
        return rcopy(Pa.at[0, r], R.at[0, r], s_p.at[1 + 2 * g + h], r_r.at[0, 2 * g + h], 2, k)

    @pl.when(z == 2)
    def _():
        def step_d(t):
            wait_recv(Y.at[k, rs_(t % 2, t // 2), DALL], r_y.at[t])
            d_fwd(t).start()

            @pl.when(t == 1)
            def _():
                wait_recv(X.at[1 - k, :, UALL], r_d.at[nd])

            @pl.when((k == 1) & (t >= 1) & (t <= NU))
            def _():
                y2(t - 1)

        each(0, 2 * NS, step_d)
        each(2, 2 * NS, lambda t: z2_d(t).start())
        pl.semaphore_wait(far, n_near)

        def step_u(s):
            wait_recv(Y.at[k, us_(s), UALL], r_y.at[2 * NS + s])
            u_sib(s).start()
            Qa[1, us_(s), :] = mm(Y[k, us_(s), :], X[k])
            q1send(s).start()
            for dq_ in range(2):
                q = 2 * s - 2 + dq_

                @pl.when((k == 0) & (q >= 0) & (q < NU - NL))
                def _():
                    y2(q)

        each(0, NS, step_u)
        each(0, NS, lambda s: wait_recv(Y.at[1 - k, us_(s), UALL], r_d.at[s]))
        each(0, NU - NL, y3)

        def last(q):
            @pl.when(k == 0)
            def _():
                y2(q)

            y3(q)

        each(NU - NL, NU, last)
        for h in range(2):
            wait_recv(PR.at[1, rs_(h, 0, NS)], r_p.at[h])
        Pa[1] += PR[1]
        s3send.start()
        for g in range(NG):
            for h in range(2):
                r = grp(g, h)
                wait_recv(PR.at[0, r], r_p.at[2 + 2 * g + h])
                Pa[0, r, :] += PR[0, r, :]

                @pl.when(y == 1)
                def _():
                    s2send(g, h).start()

    @pl.when(z != 2)
    def _():
        pl.semaphore_wait(far, n_near)

    @pl.when(c > z)
    def _():
        o_ref[...] = jnp.zeros_like(o_ref)

    @pl.when(c == z)
    def _():
        for i in range(3):
            wait_recv(R.at[i], r_r.at[i, 0])
        total = Qa[dq] + R[0] + R[1] + R[2]
        diff = lax.broadcasted_iota(jnp.int32, (rows, rows), 0) - lax.broadcasted_iota(jnp.int32, (rows, rows), 1)
        o_ref[...] = jnp.where(diff >= 0, total, 0.0).astype(o_ref.dtype)

    @pl.when((z == 1) & (c == 0))
    def _():
        for i in range(3):
            wait_recv(R.at[i], r_r.at[i, 0])
        o_ref[...] = (Qa[0] + R[0] + R[1] + R[2]).astype(o_ref.dtype)

    @pl.when((z == 2) & (y == 0))
    def _():
        for g in range(NG):
            for h in range(2):
                wait_recv(R.at[0, grp(g, h)], r_r.at[0, 2 * g + h])
        o_ref[...] = (Pa[0] + R[0]).astype(o_ref.dtype)

    @pl.when((z == 3) & (c == 2))
    def _():
        def take(s):
            for i in range(4):
                wait_recv(R.at[i, us_(s)], r_r.at[i, s])

        each(0, NS, take)
        o_ref[...] = (R[0] + R[1] + R[2] + R[3]).astype(o_ref.dtype)

    @pl.when((z == 3) & (y == 0))
    def _():
        for i in range(2):
            wait_recv(R.at[i], r_r.at[i, 0])
        o_ref[...] = (R[0] + R[1]).astype(o_ref.dtype)

    @pl.when(c != z)
    def _():
        dsend.wait_send()

    @pl.when(z == 0)
    def _():
        each(0, NU, lambda q: z0_u(q).wait_send())
        each(0, nd, lambda p: z0_d(p).wait_send())

    @pl.when(z == 3)
    def _():
        each(0, 2 * NS, lambda t: z3_d(t).wait_send())
        each(0, NS, lambda s: z3_u(s).wait_send())

    @pl.when(z == 1)
    def _():
        x_d.wait_send()
        each(0, NU, lambda q: z1_u(q).wait_send())
        each(0, NU, lambda q: u_fwd(q).wait_send())
        each(0, nd, lambda p: d_sib(p).wait_send())
        for j in range(2):
            p3send(j).wait_send()
            p2send(0, 0, G0, j).wait_send()
            for g in range(1, NG):
                p2send(g, G0 + g - 1, 1, j).wait_send()

        @pl.when(c != 0)
        def _():
            q0send.wait_send()

    @pl.when(z == 2)
    def _():
        x_u.wait_send()
        each(0, 2 * NS, lambda t: z2_d(t).wait_send())
        each(0, 2 * NS, lambda t: d_fwd(t).wait_send())
        each(0, NS, lambda s: u_sib(s).wait_send())
        each(0, NS, lambda s: q1send(s).wait_send())
        s3send.wait_send()

        @pl.when(y == 1)
        def _():
            for g in range(NG):
                for h in range(2):
                    s2send(g, h).wait_send()


def solution(mesh):
    def local_fn(a_local):
        rows, m = a_local.shape
        nd = m // PW - NU
        wide = max(NU, nd) * PW
        f32, bf16 = jnp.float32, jnp.bfloat16
        dma = pltpu.SemaphoreType.DMA
        return pl.pallas_call(
            kernel,
            out_shape=jax.ShapeDtypeStruct((rows, rows), bf16),
            in_specs=[pl.BlockSpec(memory_space=pl.ANY)],
            out_specs=pl.BlockSpec(memory_space=pltpu.VMEM),
            scratch_shapes=[
                pltpu.VMEM((2, rows, m), bf16),
                pltpu.VMEM((2, rows, m), bf16),
                pltpu.VMEM((2, rows, wide), bf16),
                pltpu.VMEM((2, rows, rows), f32),
                pltpu.VMEM((2, rows, rows), f32),
                pltpu.VMEM((4, rows, rows), f32),
                pltpu.VMEM((2, rows, rows), f32),
                pltpu.SemaphoreType.REGULAR,
                dma((1,)), dma((2 * max(NU, 2 * NS) + 2,)), dma((NU + nd,)), dma((nd + 1,)), dma((nd + 1,)),
                dma((2, max(NU, 2 * NS))), dma((2 + 2 * NG,)), dma((2 + 2 * NG,)), dma((NS + 1,)),
                dma((4, max(NS, 2 * NG))),
            ],
            compiler_params=pltpu.CompilerParams(
                collective_id=0, has_side_effects=True, vmem_limit_bytes=50 * 1024 * 1024),
        )(a_local)

    part_spec = P(("batch", "row"), "col")
    return jax.shard_map(local_fn, mesh=mesh, in_specs=(part_spec,), out_specs=part_spec, check_vma=False)
```

```python
import jax
import jax.numpy as jnp
from jax import lax
from jax.experimental import pallas as pl
from jax.experimental.pallas import tpu as pltpu
from jax.sharding import PartitionSpec as P

MESH = pl.DeviceIdType.MESH
PW = 256
NU = 15
NL = 2
NS = 8
G0 = 6
NG = NS - G0 + 1


def mm(a, b):
    return lax.dot_general(a, b, (((1,), (1,)), ((), ())), preferred_element_type=jnp.float32)


def kernel(a_ref, o_ref, X, Y, W, Pa, Qa, R, PR, far, ld, s_z, r_y, s_d, r_d, r_w, s_p, r_p, s_q, r_r):
    rows, m = a_ref.shape
    ku = NU * PW
    kd = m - ku
    nd = kd // PW
    half = rows // 2
    st = half // NS
    us = rows // NS
    z = lax.axis_index("row")
    c = lax.axis_index("col")
    y = c // 2
    k = c % 2
    sib = 2 * y + 1 - k

    def rcopy(src, dst, ss, rs, row, col):
        return pltpu.make_async_remote_copy(
            src_ref=src, dst_ref=dst, send_sem=ss, recv_sem=rs, device_id={"row": row, "col": col}, device_id_type=MESH)

    def wait_recv(ref, sem):
        pltpu.make_async_copy(ref, ref, sem).wait()

    def up(p):
        return pl.ds(pl.multiple_of(p * PW, 128), PW)

    def dn(p):
        return pl.ds(pl.multiple_of(ku + p * PW, 128), PW)

    def rs_(h, s, n=1):
        return pl.ds(pl.multiple_of(h * half + s * st, st), n * st)

    def ws_(i, s, n=1):
        return pl.ds(pl.multiple_of(i * half + s * st, st), n * st)

    def us_(s):
        return pl.ds(pl.multiple_of(s * us, us), us)

    DALL = pl.ds(ku, kd)
    UALL = pl.ds(0, ku)

    def each(lo, hi, fn):
        lax.fori_loop(lo, hi, lambda i, u: (fn(i), u)[1], 0)

    load = pltpu.make_async_copy(a_ref, X.at[k], ld.at[0])
    load.start()

    def near(sem):
        for dz in (-1, 1):
            @pl.when((z + dz >= 0) & (z + dz <= 3))
            def _():
                for kk in range(2):
                    pl.semaphore_signal(sem, inc=1, device_id={"row": z + dz, "col": 2 * y + kk}, device_id_type=MESH)
        for dc in range(1, 4):
            pl.semaphore_signal(sem, inc=1, device_id={"row": z, "col": (c + dc) % 4}, device_id_type=MESH)

    n_near = jnp.where((z == 0) | (z == 3), 5, 7)
    bar = pltpu.get_barrier_semaphore()
    near(bar)
    pl.semaphore_wait(bar, n_near)

    def z0_u(q):
        return rcopy(a_ref.at[:, up(q)], Y.at[k, :, up(q)], s_z.at[q], r_y.at[q], 1, c)

    def z0_d(p):
        return rcopy(a_ref.at[:, dn(p)], Y.at[k, :, dn(p)], s_z.at[NU + p], r_y.at[NU + p], 1, c)

    def z3_d(t):
        r = rs_(t % 2, t // 2)
        return rcopy(a_ref.at[r, DALL], Y.at[k, r, DALL], s_z.at[t], r_y.at[t], 2, c)

    def z3_u(s):
        r = us_(s)
        return rcopy(a_ref.at[r, UALL], Y.at[k, r, UALL], s_z.at[2 * NS + s], r_y.at[2 * NS + s], 2, c)

    def z1_u(q):
        return rcopy(a_ref.at[:, up(q)], W.at[k, :, up(q)], s_z.at[q], r_w.at[k, q], 2, 2 * y + 1)

    def z2_d(t):
        h, s = t % 2, t // 2
        return rcopy(a_ref.at[rs_(h, s), DALL], W.at[k, ws_(1, s), pl.ds(0, kd)], s_z.at[t], r_w.at[k, NS + s], 1, 2 * y + h)

    @pl.when(z == 0)
    def _():
        each(0, NU - NL, lambda q: z0_u(q).start())
        each(0, nd, lambda p: z0_d(p).start())
        each(NU - NL, NU, lambda q: z0_u(q).start())

    @pl.when(z == 3)
    def _():
        each(0, 2 * NS, lambda t: z3_d(t).start())
        each(0, NS, lambda s: z3_u(s).start())

    x_d = rcopy(a_ref.at[:, DALL], X.at[k, :, DALL], s_d.at[nd], r_d.at[nd], z, sib)
    x_u = rcopy(a_ref.at[:, UALL], X.at[k, :, UALL], s_d.at[nd], r_d.at[nd], z, sib)

    @pl.when(z == 1)
    def _():
        each(0, NU, lambda q: z1_u(q).start())
        x_d.start()

    @pl.when(z == 2)
    def _():
        z2_d(0).start()
        z2_d(1).start()
        x_u.start()

    near(far)

    Pa[...] = jnp.zeros_like(Pa)
    Qa[...] = jnp.zeros_like(Qa)
    load.wait()
    dq = jnp.where(z == 1, 1, 0)

    def diag(p):
        cs = pl.ds(pl.multiple_of(p * 512, 512), 512)
        Qa[dq] += mm(X[k, :, cs], X[k, :, cs])

    each(0, m // 512, diag)

    def slot(owner):
        return (c - owner + 3) % 4

    dsend = rcopy(Qa.at[dq], R.at[slot(z)], s_q.at[NS], r_r.at[slot(z), 0], z, z)

    @pl.when(c != z)
    def _():
        dsend.start()

    def u_fwd(q):
        return rcopy(Y.at[k, :, up(q)], W.at[k, :, up(q)], s_z.at[NU + q], r_w.at[k, q], 2, 2 * y)

    def zU(q):
        wait_recv(Y.at[k, :, up(q)], r_y.at[q])
        u_fwd(q).start()
        Qa[0] += mm(X[k, :, up(q)], Y[k, :, up(q)])

    def d_sib(p):
        return rcopy(Y.at[k, :, dn(p)], Y.at[k, :, dn(p)], s_d.at[p], r_d.at[p], z, sib)

    def zD(p):
        wait_recv(Y.at[k, :, dn(p)], r_y.at[NU + p])
        d_sib(p).start()
        Qa[0] += mm(X[k, :, dn(p)], Y[k, :, dn(p)])

    def p3send(j):
        return rcopy(Pa.at[j, ws_(0, 0, NS)], PR.at[1, rs_(k, 0, NS)], s_p.at[j], r_p.at[k], 2, 2 * y + j)

    def p2send(g, s, n, j):
        return rcopy(Pa.at[j, ws_(1, s, n)], PR.at[0, rs_(k, s, n)], s_p.at[2 + 2 * g + j], r_p.at[2 + 2 * g + k], 2, 2 * y + j)

    def part(i, s, n, j, lo, hi, new=True):
        B = X if j == 1 else Y
        r = ws_(i, s, n)
        w, b = pl.ds(lo, hi - lo), pl.ds(ku + lo, hi - lo)
        acc = mm(W[0, r, w], B[0, :, b]) + mm(W[1, r, w], B[1, :, b])
        if new:
            Pa[j, r, :] = acc
        else:
            Pa[j, r, :] += acc

    def thin(s, j):
        B = X if j == 1 else Y
        r = ws_(1, s)
        acc = mm(B[0, :, DALL], W[0, r, :kd]) + mm(B[1, :, DALL], W[1, r, :kd])
        Pa[j, r, :] = acc.T

    def wait_w(i, s):
        for h in range(2):
            wait_recv(W.at[h, ws_(i, s), pl.ds(0, kd)], r_w.at[h, i * NS + s])

    q0send = rcopy(Qa.at[0], R.at[slot(0)], s_q.at[0], r_r.at[slot(0), 0], 1, 0)

    @pl.when(z == 1)
    def _():
        early = nd - 2
        each(0, NU - NL, zU)
        each(0, 8, zD)
        wait_recv(X.at[1 - k, :, DALL], r_d.at[nd])
        each(0, NS, lambda s: wait_w(0, s))
        part(0, 0, NS, 1, 0, kd)
        p3send(1).start()
        each(8, early, zD)
        each(0, G0, lambda s: wait_w(1, s))
        part(1, 0, G0, 1, 0, kd)
        p2send(0, 0, G0, 1).start()
        each(0, early, lambda p: wait_recv(Y.at[1 - k, :, dn(p)], r_d.at[p]))
        part(0, 0, NS + G0, 0, 0, early * PW)
        each(early, nd, zD)
        each(early, nd, lambda p: wait_recv(Y.at[1 - k, :, dn(p)], r_d.at[p]))
        part(0, 0, NS + G0, 0, early * PW, kd, new=False)
        p3send(0).start()
        each(NU - NL, NU, zU)

        @pl.when(c != 0)
        def _():
            q0send.start()

        p2send(0, 0, G0, 0).start()

        def last(s):
            wait_w(1, s)
            for j in (1, 0):
                thin(s, j)
                p2send(1 + s - G0, s, 1, j).start()

        each(G0, NS, last)

    def d_fwd(t):
        h, s = t % 2, t // 2
        return rcopy(Y.at[k, rs_(h, s), DALL], W.at[k, ws_(0, s), pl.ds(0, kd)], s_z.at[2 * NS + t], r_w.at[k, s], 1, 2 * y + h)

    def u_sib(s):
        return rcopy(Y.at[k, us_(s), UALL], Y.at[k, us_(s), UALL], s_d.at[s], r_d.at[s], z, sib)

    def q1send(s):
        return rcopy(Qa.at[1, us_(s)], R.at[c, us_(s)], s_q.at[s], r_r.at[c, s], 3, 2)

    def y2(q):
        for h in range(2):
            wait_recv(W.at[h, :, up(q)], r_w.at[h, q])
        Pa[0] += mm(X[0, :, up(q)], W[0, :, up(q)]) + mm(X[1, :, up(q)], W[1, :, up(q)])

    def y3(q):
        Pa[1] += mm(Y[0, :, up(q)], W[0, :, up(q)]) + mm(Y[1, :, up(q)], W[1, :, up(q)])

    s3send = rcopy(Pa.at[1], R.at[y], s_p.at[0], r_r.at[y, 0], 3, k)

    def grp(g, h):
        return rs_(h, 0, G0) if g == 0 else rs_(h, G0 + g - 1)

    def s2send(g, h):
        r = grp(g, h)
        return rcopy(Pa.at[0, r], R.at[0, r], s_p.at[1 + 2 * g + h], r_r.at[0, 2 * g + h], 2, k)

    @pl.when(z == 2)
    def _():
        def step_d(t):
            wait_recv(Y.at[k, rs_(t % 2, t // 2), DALL], r_y.at[t])
            d_fwd(t).start()

            @pl.when(t == 1)
            def _():
                wait_recv(X.at[1 - k, :, UALL], r_d.at[nd])

            @pl.when((k == 1) & (t >= 1) & (t <= NU))
            def _():
                y2(t - 1)

        each(0, 2 * NS, step_d)
        each(2, 2 * NS, lambda t: z2_d(t).start())
        pl.semaphore_wait(far, n_near)

        def step_u(s):
            wait_recv(Y.at[k, us_(s), UALL], r_y.at[2 * NS + s])
            u_sib(s).start()
            Qa[1, us_(s), :] = mm(Y[k, us_(s), :], X[k])
            q1send(s).start()
            for dq_ in range(2):
                q = 2 * s - 2 + dq_

                @pl.when((k == 0) & (q >= 0) & (q < NU - NL))
                def _():
                    y2(q)

        each(0, NS, step_u)
        each(0, NS, lambda s: wait_recv(Y.at[1 - k, us_(s), UALL], r_d.at[s]))
        each(0, NU - NL, y3)

        def last(q):
            @pl.when(k == 0)
            def _():
                y2(q)

            y3(q)

        for h in range(2):
            wait_recv(PR.at[1, rs_(h, 0, NS)], r_p.at[h])
        Pa[1] += PR[1]
        each(NU - NL, NU, last)
        s3send.start()
        for g in range(NG):
            for h in range(2):
                r = grp(g, h)
                wait_recv(PR.at[0, r], r_p.at[2 + 2 * g + h])
                Pa[0, r, :] += PR[0, r, :]

                @pl.when(y == 1)
                def _():
                    s2send(g, h).start()

    @pl.when(z != 2)
    def _():
        pl.semaphore_wait(far, n_near)

    @pl.when(c > z)
    def _():
        o_ref[...] = jnp.zeros_like(o_ref)

    @pl.when(c == z)
    def _():
        for i in range(3):
            wait_recv(R.at[i], r_r.at[i, 0])
        total = Qa[dq] + R[0] + R[1] + R[2]
        diff = lax.broadcasted_iota(jnp.int32, (rows, rows), 0) - lax.broadcasted_iota(jnp.int32, (rows, rows), 1)
        o_ref[...] = jnp.where(diff >= 0, total, 0.0).astype(o_ref.dtype)

    @pl.when((z == 1) & (c == 0))
    def _():
        for i in range(3):
            wait_recv(R.at[i], r_r.at[i, 0])
        o_ref[...] = (Qa[0] + R[0] + R[1] + R[2]).astype(o_ref.dtype)

    @pl.when((z == 2) & (y == 0))
    def _():
        for g in range(NG):
            for h in range(2):
                wait_recv(R.at[0, grp(g, h)], r_r.at[0, 2 * g + h])
        o_ref[...] = (Pa[0] + R[0]).astype(o_ref.dtype)

    @pl.when((z == 3) & (c == 2))
    def _():
        def take(s):
            for i in range(4):
                wait_recv(R.at[i, us_(s)], r_r.at[i, s])

        each(0, NS, take)
        o_ref[...] = (R[0] + R[1] + R[2] + R[3]).astype(o_ref.dtype)

    @pl.when((z == 3) & (y == 0))
    def _():
        for i in range(2):
            wait_recv(R.at[i], r_r.at[i, 0])
        o_ref[...] = (R[0] + R[1]).astype(o_ref.dtype)

    @pl.when(c != z)
    def _():
        dsend.wait_send()

    @pl.when(z == 0)
    def _():
        each(0, NU, lambda q: z0_u(q).wait_send())
        each(0, nd, lambda p: z0_d(p).wait_send())

    @pl.when(z == 3)
    def _():
        each(0, 2 * NS, lambda t: z3_d(t).wait_send())
        each(0, NS, lambda s: z3_u(s).wait_send())

    @pl.when(z == 1)
    def _():
        x_d.wait_send()
        each(0, NU, lambda q: z1_u(q).wait_send())
        each(0, NU, lambda q: u_fwd(q).wait_send())
        each(0, nd, lambda p: d_sib(p).wait_send())
        for j in range(2):
            p3send(j).wait_send()
            p2send(0, 0, G0, j).wait_send()
            for g in range(1, NG):
                p2send(g, G0 + g - 1, 1, j).wait_send()

        @pl.when(c != 0)
        def _():
            q0send.wait_send()

    @pl.when(z == 2)
    def _():
        x_u.wait_send()
        each(0, 2 * NS, lambda t: z2_d(t).wait_send())
        each(0, 2 * NS, lambda t: d_fwd(t).wait_send())
        each(0, NS, lambda s: u_sib(s).wait_send())
        each(0, NS, lambda s: q1send(s).wait_send())
        s3send.wait_send()

        @pl.when(y == 1)
        def _():
            for g in range(NG):
                for h in range(2):
                    s2send(g, h).wait_send()


def solution(mesh):
    def local_fn(a_local):
        rows, m = a_local.shape
        nd = m // PW - NU
        wide = max(NU, nd) * PW
        f32, bf16 = jnp.float32, jnp.bfloat16
        dma = pltpu.SemaphoreType.DMA
        return pl.pallas_call(
            kernel,
            out_shape=jax.ShapeDtypeStruct((rows, rows), bf16),
            in_specs=[pl.BlockSpec(memory_space=pl.ANY)],
            out_specs=pl.BlockSpec(memory_space=pltpu.VMEM),
            scratch_shapes=[
                pltpu.VMEM((2, rows, m), bf16),
                pltpu.VMEM((2, rows, m), bf16),
                pltpu.VMEM((2, rows, wide), bf16),
                pltpu.VMEM((2, rows, rows), f32),
                pltpu.VMEM((2, rows, rows), f32),
                pltpu.VMEM((4, rows, rows), f32),
                pltpu.VMEM((2, rows, rows), f32),
                pltpu.SemaphoreType.REGULAR,
                dma((1,)), dma((2 * max(NU, 2 * NS) + 2,)), dma((NU + nd,)), dma((nd + 1,)), dma((nd + 1,)),
                dma((2, max(NU, 2 * NS))), dma((2 + 2 * NG,)), dma((2 + 2 * NG,)), dma((NS + 1,)),
                dma((4, max(NS, 2 * NG))),
            ],
            compiler_params=pltpu.CompilerParams(
                collective_id=0, has_side_effects=True, vmem_limit_bytes=50 * 1024 * 1024),
        )(a_local)

    part_spec = P(("batch", "row"), "col")
    return jax.shard_map(local_fn, mesh=mesh, in_specs=(part_spec,), out_specs=part_spec, check_vma=False)
```

```python
import jax
import jax.numpy as jnp
from jax import lax
from jax.experimental import pallas as pl
from jax.experimental.pallas import tpu as pltpu
from jax.sharding import PartitionSpec as P

MESH = pl.DeviceIdType.MESH
PW = 256
NU = 15
XU = 128
NS = 8
GROUPS = ((0, 5), (5, 2), (7, 1))


def mm(a, b):
    return lax.dot_general(a, b, (((1,), (1,)), ((), ())), preferred_element_type=jnp.float32)


def mn(a, b):
    return lax.dot_general(a, b, (((1,), (0,)), ((), ())), preferred_element_type=jnp.float32)


def kernel(a_ref, o_ref, X, Y, W, T, Pa, Qa, R, PR, far, ld, s_z, r_y, s_d, r_d, r_w, s_p, r_p, s_q, r_r):
    rows, m = a_ref.shape
    ku = NU * PW + XU
    kd = m - ku
    nd, xd = kd // PW, kd % PW
    half = rows // 2
    st = half // NS
    us = rows // NS
    z = lax.axis_index("row")
    c = lax.axis_index("col")
    y = c // 2
    k = c % 2
    sib = 2 * y + 1 - k

    def rcopy(src, dst, ss, rs, row, col):
        return pltpu.make_async_remote_copy(
            src_ref=src, dst_ref=dst, send_sem=ss, recv_sem=rs, device_id={"row": row, "col": col}, device_id_type=MESH)

    def wait_recv(ref, sem):
        pltpu.make_async_copy(ref, ref, sem).wait()

    def up(p, w=PW):
        return pl.ds(pl.multiple_of(p * PW, 128), w)

    def dn(p, w=PW):
        return pl.ds(pl.multiple_of(ku + p * PW, 128), w)

    def rs_(h, s, n=1):
        return pl.ds(pl.multiple_of(h * half + s * st, st), n * st)

    def us_(s):
        return pl.ds(pl.multiple_of(s * us, us), us)

    DALL = pl.ds(ku, kd)
    UALL = pl.ds(0, ku)
    C0, C1 = pl.ds(0, half), pl.ds(half, half)
    COLS = (C0, C1)

    def each(lo, hi, fn):
        lax.fori_loop(lo, hi, lambda i, u: (fn(i), u)[1], 0)

    load = pltpu.make_async_copy(a_ref, X.at[k], ld.at[0])
    load.start()

    def near(sem):
        for dz in (-1, 1):
            @pl.when((z + dz >= 0) & (z + dz <= 3))
            def _():
                for kk in range(2):
                    pl.semaphore_signal(sem, inc=1, device_id={"row": z + dz, "col": 2 * y + kk}, device_id_type=MESH)
        for dc in range(1, 4):
            pl.semaphore_signal(sem, inc=1, device_id={"row": z, "col": (c + dc) % 4}, device_id_type=MESH)

    n_near = jnp.where((z == 0) | (z == 3), 5, 7)
    bar = pltpu.get_barrier_semaphore()
    near(bar)
    pl.semaphore_wait(bar, n_near)

    def z0_u(q, w=PW):
        return rcopy(a_ref.at[:, up(q, w)], Y.at[k, :, up(q, w)], s_z.at[q], r_y.at[q], 1, c)

    def z0_d(t):
        r = rs_(0, t)
        return rcopy(a_ref.at[r, DALL], Y.at[k, r, DALL], s_z.at[2 * NS + t], r_y.at[2 * NS + t], 1, c)

    def z3_d(t):
        r = rs_(t % 2, t // 2)
        return rcopy(a_ref.at[r, DALL], Y.at[k, r, DALL], s_z.at[t], r_y.at[t], 2, c)

    def z3_u(s):
        r = us_(s)
        return rcopy(a_ref.at[r, UALL], Y.at[k, r, UALL], s_z.at[2 * NS + s], r_y.at[2 * NS + s], 2, c)

    def z1_u(q, w=PW):
        return rcopy(a_ref.at[:, up(q, w)], W.at[k, :, up(q, w)], s_z.at[q], r_w.at[k, q], 2, 2 * y + 1)

    def z2_d(t):
        h, s = t % 2, t // 2
        return rcopy(a_ref.at[rs_(h, s), DALL], W.at[k, rs_(1, s), pl.ds(0, kd)], s_z.at[t], r_w.at[k, NS + s], 1, 2 * y + h)

    @pl.when(z == 0)
    def _():
        each(0, NU, lambda q: z0_u(q).start())
        z0_u(NU, XU).start()
        each(0, 2 * NS, lambda t: z0_d(t).start())

    @pl.when(z == 3)
    def _():
        each(0, 2 * NS, lambda t: z3_d(t).start())
        each(0, NS, lambda s: z3_u(s).start())

    x_d = rcopy(a_ref.at[:, DALL], X.at[k, :, DALL], s_d.at[2 * NS], r_d.at[2 * NS], z, sib)
    x_u = rcopy(a_ref.at[:, UALL], X.at[k, :, UALL], s_d.at[2 * NS], r_d.at[2 * NS], z, sib)

    @pl.when(z == 1)
    def _():
        each(0, NU, lambda q: z1_u(q).start())
        z1_u(NU, XU).start()
        x_d.start()

    @pl.when(z == 2)
    def _():
        z2_d(0).start()
        z2_d(1).start()
        x_u.start()

    near(far)

    Pa[...] = jnp.zeros_like(Pa)
    Qa[...] = jnp.zeros_like(Qa)
    load.wait()
    dq = jnp.where(z == 1, 1, 0)

    def diag(p):
        cs = pl.ds(pl.multiple_of(p * 512, 512), 512)
        Qa[dq] += mm(X[k, :, cs], X[k, :, cs])

    each(0, m // 512, diag)

    def slot(owner):
        return (c - owner + 3) % 4

    dsend = rcopy(Qa.at[dq], R.at[slot(z)], s_q.at[NS], r_r.at[slot(z), 0], z, z)

    @pl.when(c != z)
    def _():
        dsend.start()

    def u_fwd(q, w=PW):
        return rcopy(Y.at[k, :, up(q, w)], W.at[k, :, up(q, w)], s_z.at[2 * NS + q], r_w.at[k, q], 2, 2 * y)

    def zU(q, w=PW):
        wait_recv(Y.at[k, :, up(q, w)], r_y.at[q])
        Qa[0] += mm(X[k, :, up(q, w)], Y[k, :, up(q, w)])

    def turn(p, w=PW):
        for h in range(2):
            T[h, up(p, w), 2 * half:] = X[h, :, dn(p, w)].T

    def d_sib(t):
        return rcopy(Y.at[k, rs_(0, t), DALL], Y.at[k, rs_(0, t), DALL], s_d.at[t], r_d.at[t], z, sib)

    def zD(t):
        wait_recv(Y.at[k, rs_(0, t), DALL], r_y.at[2 * NS + t])
        d_sib(t).start()

    def wait_sib(lo, hi):
        each(lo, hi, lambda t: wait_recv(Y.at[1 - k, rs_(0, t), DALL], r_d.at[t]))

    def turn_half(b):
        for h in range(2):
            T[h, :, b * half:(b + 1) * half] = Y[h, b * half:(b + 1) * half, DALL].T

    def q_half(b):
        Qa[0, :, COLS[b]] += mm(X[k, :, DALL], Y[k, b * half:(b + 1) * half, DALL])

    def wait_w(i, lo, n):
        def one(s):
            for h in range(2):
                wait_recv(W.at[h, rs_(i, s), pl.ds(0, kd)], r_w.at[h, i * NS + s])

        each(lo, lo + n, one)

    def send1(i, s, n, j, cols, ss, rs):
        src = Pa.at[j, rs_(1 - i, s, n), cols]
        return rcopy(src, PR.at[i, rs_(k, s, n), cols], s_p.at[ss], r_p.at[k, rs], 2, 2 * y + j)

    CA = pl.ds(0, rows)
    m31 = send1(1, 0, NS, 1, CA, 0, 0)
    m30a = send1(1, 0, NS, 0, C0, 1, 0)
    m30b = [send1(1, 2 * u, 2, 0, C1, 2 + u, 4 + u) for u in range(4)]
    m21 = [send1(0, s, n, 1, CA, 6 + g, 1 + g) for g, (s, n) in enumerate(GROUPS)]
    m20a = [send1(0, s, n, 0, C0, 9 + g, 1 + g) for g, (s, n) in enumerate(GROUPS[:2])]
    m20b = send1(0, 0, NS - 1, 0, C1, 11, 8)
    m20c = send1(0, NS - 1, 1, 0, CA, 12, 3)
    out1 = [m31, m30a, *m30b, *m21, *m20a, m20b, m20c]

    def part(r, j, cols, tcols):
        Pa[j, r, cols] = mn(W[0, r, :kd], T[0, :, tcols]) + mn(W[1, r, :kd], T[1, :, tcols])

    TJ1 = slice(2 * half, 4 * half)

    def q0send(b):
        return rcopy(Qa.at[0, :, COLS[b]], R.at[slot(0), :, COLS[b]], s_q.at[b], r_r.at[slot(0), b], 1, 0)

    @pl.when(z == 1)
    def _():
        wait_recv(X.at[1 - k, :, DALL], r_d.at[2 * NS])

        def step_u(q):
            zU(q)

            @pl.when(q < 5)
            def _():
                u_fwd(q).start()

            turn(q)

        each(0, NU, step_u)
        zU(NU, XU)
        each(NU, nd, turn)
        if xd:
            turn(nd, xd)
        each(0, 4, zD)
        wait_w(0, 0, NS)
        part(rs_(0, 0, NS), 1, CA, TJ1)
        m31.start()
        each(5, 10, lambda q: u_fwd(q).start())
        each(4, 8, zD)
        wait_sib(0, 8)
        turn_half(0)
        part(rs_(0, 0, NS), 0, C0, slice(0, half))
        m30a.start()
        each(10, NU, lambda q: u_fwd(q).start())
        u_fwd(NU, XU).start()
        q_half(0)

        @pl.when(c != 0)
        def _():
            q0send(0).start()

        for g, stop in ((0, 11), (1, 15)):
            each(8 if g == 0 else 11, stop, zD)
            s, n = GROUPS[g]
            wait_w(1, s, n)
            part(rs_(1, s, n), 1, CA, TJ1)
            m21[g].start()
            part(rs_(1, s, n), 0, C0, slice(0, half))
            m20a[g].start()
        zD(15)
        wait_sib(8, 16)
        r = pl.ds(0, rows - st)
        Pa[0, r, C1] = mm(W[0, r, :kd], Y[0, half:, DALL]) + mm(W[1, r, :kd], Y[1, half:, DALL])
        for x in m30b:
            x.start()
        m20b.start()
        q_half(1)

        @pl.when(c != 0)
        def _():
            q0send(1).start()

        turn_half(1)
        s, n = GROUPS[2]
        wait_w(1, s, n)
        part(rs_(1, s, n), 1, CA, TJ1)
        m21[2].start()
        part(rs_(1, s, n), 0, CA, slice(0, rows))
        m20c.start()

    def d_fwd(t):
        h, s = t % 2, t // 2
        return rcopy(Y.at[k, rs_(h, s), DALL], W.at[k, rs_(0, s), pl.ds(0, kd)], s_z.at[2 * NS + t], r_w.at[k, s], 1, 2 * y + h)

    def u_sib(s):
        return rcopy(Y.at[k, us_(s), UALL], Y.at[k, us_(s), UALL], s_d.at[s], r_d.at[s], z, sib)

    def q1send(s):
        return rcopy(Qa.at[1, us_(s)], R.at[c, us_(s)], s_q.at[s], r_r.at[c, s], 3, 2)

    def y2(q, w=PW):
        for h in range(2):
            wait_recv(W.at[h, :, up(q, w)], r_w.at[h, q])
        Pa[0] += mm(X[0, :, up(q, w)], W[0, :, up(q, w)]) + mm(X[1, :, up(q, w)], W[1, :, up(q, w)])

    def y3(b, q, w=PW):
        r = pl.ds(b * half, half)
        Pa[1, r, :] += mm(Y[0, r, up(q, w)], W[0, :, up(q, w)]) + mm(Y[1, r, up(q, w)], W[1, :, up(q, w)])

    def wait_ysib(s):
        wait_recv(Y.at[1 - k, us_(s), UALL], r_d.at[s])

    def s3(r, cols, n):
        return rcopy(Pa.at[1, r, cols], R.at[y, r, cols], s_p.at[n], r_r.at[y, n], 3, k)

    s3_a = [s3(pl.ds(b * half, half), C0, b) for b in range(2)]
    s3_b = [[s3(rs_(h, 2 * u, 2), C1, 2 + 4 * h + u) for u in range(4)] for h in range(2)]

    def s3_k1(s):
        return s3(us_(s), CA, s)

    def s2(h, s, n, cols, i):
        r = rs_(h, s, n)
        return rcopy(Pa.at[0, r, cols], R.at[0, r, cols], s_p.at[10 + 3 * h + i], r_r.at[0, 3 * h + i], 2, k)

    s2_k1 = [[s2(h, s, n, CA, i) for i, (s, n) in enumerate(GROUPS)] for h in range(2)]
    s2_k0 = [[s2(h, 0, NS - 1, C0, 0), s2(h, 0, NS - 1, C1, 1), s2(h, NS - 1, 1, CA, 2)] for h in range(2)]

    def add(i, r, cols, sem):
        wait_recv(PR.at[i, r, cols], sem)
        Pa[i, r, cols] += PR[i, r, cols]

    def y1_start(x):
        @pl.when(y == 1)
        def _():
            x.start()

    def strip31(s):
        wait_ysib(s)
        r = us_(s)
        Pa[1, r, :] = PR[1, r, :] + mm(Y[0, r, UALL], W[0, :, :ku]) + mm(Y[1, r, UALL], W[1, :, :ku])
        s3_k1(s).start()

    @pl.when(z == 2)
    def _():
        def step_d(t):
            wait_recv(Y.at[k, rs_(t % 2, t // 2), DALL], r_y.at[t])
            d_fwd(t).start()

            @pl.when(t == 1)
            def _():
                wait_recv(X.at[1 - k, :, UALL], r_d.at[2 * NS])

            @pl.when((k == 1) & (t >= 1))
            def _():
                y2(t - 1)

        each(0, 2 * NS, step_d)
        each(2, 2 * NS, lambda t: z2_d(t).start())

        @pl.when(k == 1)
        def _():
            y2(NU, XU)

        pl.semaphore_wait(far, n_near)

        def step_u(s):
            wait_recv(Y.at[k, us_(s), UALL], r_y.at[2 * NS + s])
            u_sib(s).start()
            Qa[1, us_(s), :] = mm(Y[k, us_(s), :], X[k])
            q1send(s).start()

            @pl.when((k == 0) & (s >= 1))
            def _():
                y2(2 * s - 2)
                y2(2 * s - 1)

            @pl.when((k == 0) & (s == 4))
            def _():
                each(0, 4, wait_ysib)
                each(0, 6, lambda q: y3(0, q))

            @pl.when((k == 0) & (s >= 4))
            def _():
                y3(0, 2 * s - 2)
                y3(0, 2 * s - 1)

            @pl.when((k == 1) & (s == 2))
            def _():
                for h in range(2):
                    wait_recv(PR.at[1, rs_(h, 0, NS)], r_p.at[h, 0])

            @pl.when((k == 1) & (s >= 2))
            def _():
                strip31(s - 2)

        each(0, NS, step_u)

        @pl.when(k == 1)
        def _():
            strip31(NS - 2)
            strip31(NS - 1)
            for i, (s, n) in enumerate(GROUPS):
                for h in range(2):
                    add(0, rs_(h, s, n), CA, r_p.at[h, 1 + i])
                    y1_start(s2_k1[h][i])

        @pl.when(k == 0)
        def _():
            y2(NU - 1)
            y2(NU, XU)
            y3(0, NU - 1)
            y3(0, NU, XU)
            add(1, pl.ds(0, half), C0, r_p.at[0, 0])
            s3_a[0].start()
            each(4, NS, wait_ysib)
            each(0, NU, lambda q: y3(1, q))
            y3(1, NU, XU)
            add(1, pl.ds(half, half), C0, r_p.at[1, 0])
            s3_a[1].start()
            for h in range(2):
                for g, (s, n) in enumerate(GROUPS[:2]):
                    add(0, rs_(h, s, n), C0, r_p.at[h, 1 + g])
                y1_start(s2_k0[h][0])
            for u in range(4):
                for h in range(2):
                    add(1, rs_(h, 2 * u, 2), C1, r_p.at[h, 4 + u])
                    s3_b[h][u].start()
            for h in range(2):
                add(0, rs_(h, 0, NS - 1), C1, r_p.at[h, 8])
                y1_start(s2_k0[h][1])
            for h in range(2):
                add(0, rs_(h, NS - 1), CA, r_p.at[h, 3])
                y1_start(s2_k0[h][2])

    @pl.when(z != 2)
    def _():
        pl.semaphore_wait(far, n_near)

    @pl.when(c > z)
    def _():
        o_ref[...] = jnp.zeros_like(o_ref)

    @pl.when(c == z)
    def _():
        for i in range(3):
            wait_recv(R.at[i], r_r.at[i, 0])
        total = Qa[dq] + R[0] + R[1] + R[2]
        diff = lax.broadcasted_iota(jnp.int32, (rows, rows), 0) - lax.broadcasted_iota(jnp.int32, (rows, rows), 1)
        o_ref[...] = jnp.where(diff >= 0, total, 0.0).astype(o_ref.dtype)

    @pl.when((z == 1) & (c == 0))
    def _():
        for i in range(3):
            for b in range(2):
                wait_recv(R.at[i, :, COLS[b]], r_r.at[i, b])
        o_ref[...] = (Qa[0] + R[0] + R[1] + R[2]).astype(o_ref.dtype)

    @pl.when((z == 2) & (y == 0))
    def _():
        @pl.when(k == 0)
        def _():
            for h in range(2):
                wait_recv(R.at[0, rs_(h, 0, NS - 1), C0], r_r.at[0, 3 * h])
                wait_recv(R.at[0, rs_(h, 0, NS - 1), C1], r_r.at[0, 3 * h + 1])
                wait_recv(R.at[0, rs_(h, NS - 1)], r_r.at[0, 3 * h + 2])

        @pl.when(k == 1)
        def _():
            for h in range(2):
                for i, (s, n) in enumerate(GROUPS):
                    wait_recv(R.at[0, rs_(h, s, n)], r_r.at[0, 3 * h + i])

        o_ref[...] = (Pa[0] + R[0]).astype(o_ref.dtype)

    @pl.when((z == 3) & (c == 2))
    def _():
        def take(s):
            for i in range(4):
                wait_recv(R.at[i, us_(s)], r_r.at[i, s])

        each(0, NS, take)
        o_ref[...] = (R[0] + R[1] + R[2] + R[3]).astype(o_ref.dtype)

    @pl.when((z == 3) & (y == 0))
    def _():
        for i in range(2):
            @pl.when(k == 0)
            def _():
                for b in range(2):
                    wait_recv(R.at[i, pl.ds(b * half, half), C0], r_r.at[i, b])
                for h in range(2):
                    for u in range(4):
                        wait_recv(R.at[i, rs_(h, 2 * u, 2), C1], r_r.at[i, 2 + 4 * h + u])

            @pl.when(k == 1)
            def _():
                each(0, NS, lambda s: wait_recv(R.at[i, us_(s)], r_r.at[i, s]))

        o_ref[...] = (R[0] + R[1]).astype(o_ref.dtype)

    @pl.when(c != z)
    def _():
        dsend.wait_send()

    @pl.when(z == 0)
    def _():
        each(0, NU, lambda q: z0_u(q).wait_send())
        z0_u(NU, XU).wait_send()
        each(0, 2 * NS, lambda t: z0_d(t).wait_send())

    @pl.when(z == 3)
    def _():
        each(0, 2 * NS, lambda t: z3_d(t).wait_send())
        each(0, NS, lambda s: z3_u(s).wait_send())

    @pl.when(z == 1)
    def _():
        x_d.wait_send()
        each(0, NU, lambda q: z1_u(q).wait_send())
        z1_u(NU, XU).wait_send()
        each(0, NU, lambda q: u_fwd(q).wait_send())
        u_fwd(NU, XU).wait_send()
        each(0, 2 * NS, lambda t: d_sib(t).wait_send())
        for x in out1:
            x.wait_send()

        @pl.when(c != 0)
        def _():
            for b in range(2):
                q0send(b).wait_send()

    @pl.when(z == 2)
    def _():
        x_u.wait_send()
        each(0, 2 * NS, lambda t: z2_d(t).wait_send())
        each(0, 2 * NS, lambda t: d_fwd(t).wait_send())
        each(0, NS, lambda s: u_sib(s).wait_send())
        each(0, NS, lambda s: q1send(s).wait_send())

        @pl.when(k == 0)
        def _():
            for x in [*s3_a, *s3_b[0], *s3_b[1]]:
                x.wait_send()

            @pl.when(y == 1)
            def _():
                for x in [*s2_k0[0], *s2_k0[1]]:
                    x.wait_send()

        @pl.when(k == 1)
        def _():
            each(0, NS, lambda s: s3_k1(s).wait_send())

            @pl.when(y == 1)
            def _():
                for x in [*s2_k1[0], *s2_k1[1]]:
                    x.wait_send()


def solution(mesh):
    def local_fn(a_local):
        rows, m = a_local.shape
        kd = m - NU * PW - XU
        f32, bf16 = jnp.float32, jnp.bfloat16
        dma = pltpu.SemaphoreType.DMA
        return pl.pallas_call(
            kernel,
            out_shape=jax.ShapeDtypeStruct((rows, rows), bf16),
            in_specs=[pl.BlockSpec(memory_space=pl.ANY)],
            out_specs=pl.BlockSpec(memory_space=pltpu.VMEM),
            scratch_shapes=[
                pltpu.VMEM((2, rows, m), bf16),
                pltpu.VMEM((2, rows, m), bf16),
                pltpu.VMEM((2, rows, kd), bf16),
                pltpu.VMEM((2, kd, 2 * rows), bf16),
                pltpu.VMEM((2, rows, rows), f32),
                pltpu.VMEM((2, rows, rows), f32),
                pltpu.VMEM((4, rows, rows), f32),
                pltpu.VMEM((2, rows, rows), f32),
                pltpu.SemaphoreType.REGULAR,
                dma((1,)), dma((4 * NS,)), dma((4 * NS,)), dma((2 * NS + 1,)), dma((2 * NS + 1,)),
                dma((2, 2 * NS)), dma((16,)), dma((2, 9)), dma((NS + 1,)), dma((4, 10)),
            ],
            compiler_params=pltpu.CompilerParams(
                collective_id=0, has_side_effects=True, vmem_limit_bytes=56 * 1024 * 1024),
        )(a_local)

    part_spec = P(("batch", "row"), "col")
    return jax.shard_map(local_fn, mesh=mesh, in_specs=(part_spec,), out_specs=part_spec, check_vma=False)
```

```python
import jax
import jax.numpy as jnp
from jax import lax
from jax.experimental import pallas as pl
from jax.experimental.pallas import tpu as pltpu
from jax.sharding import PartitionSpec as P

MESH = pl.DeviceIdType.MESH
PW = 256
NU = 15
XU = 128
NS = 8


def mm(a, b):
    return lax.dot_general(a, b, (((1,), (1,)), ((), ())), preferred_element_type=jnp.float32)


def mn(a, b):
    return lax.dot_general(a, b, (((1,), (0,)), ((), ())), preferred_element_type=jnp.float32)


def kernel(a_ref, o_ref, X, Y, W, T0, T1, Pa, Pb, Qa, Qb, R, PR, far, ld, s_z, r_y, s_d, r_d, r_w, s_p, r_p, s_q, r_r):
    rows, m = a_ref.shape
    ku = NU * PW + XU
    kd = m - ku
    nd, xd = kd // PW, kd % PW
    half = rows // 2
    st = half // NS
    us = rows // NS
    z = lax.axis_index("row")
    c = lax.axis_index("col")
    y = c // 2
    k = c % 2
    sib = 2 * y + 1 - k

    def rcopy(src, dst, ss, rs, row, col):
        return pltpu.make_async_remote_copy(
            src_ref=src, dst_ref=dst, send_sem=ss, recv_sem=rs, device_id={"row": row, "col": col}, device_id_type=MESH)

    def wait_recv(ref, sem):
        pltpu.make_async_copy(ref, ref, sem).wait()

    def up(p, w=PW):
        return pl.ds(pl.multiple_of(p * PW, 128), w)

    def dn(p, w=PW):
        return pl.ds(pl.multiple_of(ku + p * PW, 128), w)

    def rs_(h, s, n=1):
        return pl.ds(pl.multiple_of(h * half + s * st, st), n * st)

    def us_(s):
        return pl.ds(pl.multiple_of(s * us, us), us)

    DALL = pl.ds(ku, kd)
    UALL = pl.ds(0, ku)
    C0, C1 = pl.ds(0, half), pl.ds(half, half)
    COLS = (C0, C1)

    def each(lo, hi, fn):
        lax.fori_loop(lo, hi, lambda i, u: (fn(i), u)[1], 0)

    load = pltpu.make_async_copy(a_ref, X.at[k], ld.at[0])
    load.start()

    def near(sem):
        for dz in (-1, 1):
            @pl.when((z + dz >= 0) & (z + dz <= 3))
            def _():
                for kk in range(2):
                    pl.semaphore_signal(sem, inc=1, device_id={"row": z + dz, "col": 2 * y + kk}, device_id_type=MESH)
        for dc in range(1, 4):
            pl.semaphore_signal(sem, inc=1, device_id={"row": z, "col": (c + dc) % 4}, device_id_type=MESH)

    n_near = jnp.where((z == 0) | (z == 3), 5, 7)
    bar = pltpu.get_barrier_semaphore()
    near(bar)
    pl.semaphore_wait(bar, n_near)

    def z0_u(q, w=PW):
        return rcopy(a_ref.at[:, up(q, w)], Y.at[k, :, up(q, w)], s_z.at[q], r_y.at[q], 1, c)

    def z0_d(t):
        r = rs_(0, t)
        return rcopy(a_ref.at[r, DALL], Y.at[k, r, DALL], s_z.at[2 * NS + t], r_y.at[2 * NS + t], 1, c)

    def z3_d(t):
        r = rs_(t % 2, t // 2)
        return rcopy(a_ref.at[r, DALL], Y.at[k, r, DALL], s_z.at[t], r_y.at[t], 2, c)

    def z3_u(s):
        r = us_(s)
        return rcopy(a_ref.at[r, UALL], Y.at[k, r, UALL], s_z.at[2 * NS + s], r_y.at[2 * NS + s], 2, c)

    def z1_u(q, w=PW):
        return rcopy(a_ref.at[:, up(q, w)], W.at[k, :, up(q, w)], s_z.at[q], r_w.at[k, q], 2, 2 * y + 1)

    def z2_d(t):
        h, s = t % 2, t // 2
        return rcopy(a_ref.at[rs_(h, s), DALL], W.at[k, rs_(1, s), pl.ds(0, kd)], s_z.at[t], r_w.at[k, NS + s], 1, 2 * y + h)

    @pl.when(z == 0)
    def _():
        each(0, NU, lambda q: z0_u(q).start())
        z0_u(NU, XU).start()
        each(0, 2 * NS, lambda t: z0_d(t).start())

    @pl.when(z == 3)
    def _():
        each(0, 2 * NS, lambda t: z3_d(t).start())
        each(0, NS, lambda s: z3_u(s).start())

    x_d = rcopy(a_ref.at[:, DALL], X.at[k, :, DALL], s_d.at[2 * NS], r_d.at[2 * NS], z, sib)
    x_u = rcopy(a_ref.at[:, UALL], X.at[k, :, UALL], s_d.at[2 * NS], r_d.at[2 * NS], z, sib)

    @pl.when(z == 1)
    def _():
        each(0, NU, lambda q: z1_u(q).start())
        z1_u(NU, XU).start()
        x_d.start()

    @pl.when(z == 2)
    def _():
        z2_d(0).start()
        z2_d(1).start()
        x_u.start()

    near(far)

    Pa[...] = jnp.zeros_like(Pa)
    Qa[...] = jnp.zeros_like(Qa)
    Qb[...] = jnp.zeros_like(Qb)
    load.wait()
    dq = jnp.where(z == 1, 1, 0)

    def diag(p):
        cs = pl.ds(pl.multiple_of(p * 512, 512), 512)
        Qa[dq] += mm(X[k, :, cs], X[k, :, cs])

    each(0, m // 512, diag)

    def slot(owner):
        return (c - owner + 3) % 4

    dsend = rcopy(Qa.at[dq], R.at[slot(z)], s_q.at[NS], r_r.at[slot(z), 0], z, z)

    @pl.when(c != z)
    def _():
        dsend.start()

    def u_fwd(q, w=PW):
        return rcopy(Y.at[k, :, up(q, w)], W.at[k, :, up(q, w)], s_z.at[2 * NS + q], r_w.at[k, q], 2, 2 * y)

    def zU(q, w=PW):
        wait_recv(Y.at[k, :, up(q, w)], r_y.at[q])
        v = mm(X[k, :, up(q, w)], Y[k, :, up(q, w)])
        Qb[0] += v[:, :half]
        Qb[1] += v[:, half:]

    def turn(p, w=PW):
        for h in range(2):
            T1[h, up(p, w), :] = X[h, :, dn(p, w)].T

    def d_sib(t):
        return rcopy(Y.at[k, rs_(0, t), DALL], Y.at[k, rs_(0, t), DALL], s_d.at[t], r_d.at[t], z, sib)

    def zD(t):
        wait_recv(Y.at[k, rs_(0, t), DALL], r_y.at[2 * NS + t])
        d_sib(t).start()

    def brows(b):
        return pl.ds(pl.multiple_of(b * half, half), half)

    def wait_w(i, lo, n):
        def one(s):
            for h in range(2):
                wait_recv(W.at[h, rs_(i, s), pl.ds(0, kd)], r_w.at[h, i * NS + s])

        each(lo, lo + n, one)

    CA = pl.ds(0, rows)

    def send1(src, i, s, n, j, cols, ss, rs):
        return rcopy(src, PR.at[i, rs_(k, s, n), cols], s_p.at[ss], r_p.at[k, rs], 2, 2 * y + j)

    m31 = send1(Pa.at[1, rs_(0, 0, NS)], 1, 0, NS, 1, CA, 0, 0)

    def m30(b, u):
        return send1(Pb.at[b, rs_(0, 2 * u, 2)], 1, 2 * u, 2, 0, COLS[b], 1 + 4 * b + u, 4 * b + u)

    def m21(g):
        return send1(Pa.at[1, rs_(1, 2 * g, 2)], 0, 2 * g, 2, 1, CA, 9 + g, 1 + g)

    def m20(b, g):
        return send1(Pb.at[b, rs_(1, 2 * g, 2)], 0, 2 * g, 2, 0, COLS[b], 13 + 4 * b + g, 8 + 4 * b + g)

    def part1(r):
        Pa[1, r, :] = mn(W[0, r, :kd], T1[0]) + mn(W[1, r, :kd], T1[1])

    def part0(r, b):
        Pb[b, r, :] = mn(W[0, r, :kd], T0[0, b]) + mn(W[1, r, :kd], T0[1, b])

    def q0send(b):
        return rcopy(Qb.at[b], R.at[slot(0), :, COLS[b]], s_q.at[b], r_r.at[slot(0), b], 1, 0)

    @pl.when(z == 1)
    def _():
        wait_recv(X.at[1 - k, :, DALL], r_d.at[2 * NS])

        def step_u(q):
            zU(q)

            @pl.when(q < 5)
            def _():
                u_fwd(q).start()

            turn(q)

        each(0, NU, step_u)
        zU(NU, XU)
        each(NU, nd, turn)
        if xd:
            turn(nd, xd)

        def step(i):
            @pl.when(i < 2 * NS)
            def _():
                zD(i)

            @pl.when(i == 3)
            def _():
                wait_w(0, 0, NS)
                part1(rs_(0, 0, NS))
                m31.start()
                each(5, 10, lambda q: u_fwd(q).start())

            @pl.when((i == 7) | (i == 16))
            def _():
                b = jnp.where(i == 7, 0, 1)
                each(NS * b, NS * b + NS, lambda t: wait_recv(Y.at[1 - k, rs_(0, t), DALL], r_d.at[t]))
                for h in range(2):
                    T0[h, b] = Y[h, brows(b), DALL].T
                part0(rs_(0, 0, NS), b)
                for bb in range(2):
                    @pl.when(b == bb)
                    def _():
                        for u in range(4):
                            m30(bb, u).start()

            @pl.when((i == 7) | (i == 19))
            def _():
                b = jnp.where(i == 7, 0, 1)
                Qb[b] += mm(X[k, :, DALL], Y[k, brows(b), DALL])
                for bb in range(2):
                    @pl.when((b == bb) & (c != 0))
                    def _():
                        q0send(bb).start()

            @pl.when(i == 7)
            def _():
                each(10, 13, lambda q: u_fwd(q).start())

            @pl.when((i == 8) | (i == 9) | (i == 13) | (i == 20))
            def _():
                g = jnp.where(i == 20, 3, jnp.where(i == 13, 2, i - 8))
                wait_w(1, 2 * g, 2)
                part1(rs_(1, 2 * g, 2))
                m21(g).start()
                part0(rs_(1, 2 * g, 2), 0)
                m20(0, g).start()

            @pl.when(i == 9)
            def _():
                each(13, NU, lambda q: u_fwd(q).start())
                u_fwd(NU, XU).start()

            @pl.when(i >= 17)
            def _():
                g = i - 17
                part0(rs_(1, 2 * g, 2), 1)
                m20(1, g).start()

        each(0, 21, step)

    def d_fwd(t):
        h, s = t % 2, t // 2
        return rcopy(Y.at[k, rs_(h, s), DALL], W.at[k, rs_(0, s), pl.ds(0, kd)], s_z.at[2 * NS + t], r_w.at[k, s], 1, 2 * y + h)

    def u_sib(s):
        return rcopy(Y.at[k, us_(s), UALL], Y.at[k, us_(s), UALL], s_d.at[s], r_d.at[s], z, sib)

    def q1send(s):
        return rcopy(Qa.at[1, us_(s)], R.at[c, us_(s)], s_q.at[s], r_r.at[c, s], 3, 2)

    def y2(q, w=PW):
        for h in range(2):
            wait_recv(W.at[h, :, up(q, w)], r_w.at[h, q])
        Pa[0] += mm(X[0, :, up(q, w)], W[0, :, up(q, w)]) + mm(X[1, :, up(q, w)], W[1, :, up(q, w)])

    def y3(b, q, w=PW):
        r = pl.ds(b * half, half)
        Pa[1, r, :] += mm(Y[0, r, up(q, w)], W[0, :, up(q, w)]) + mm(Y[1, r, up(q, w)], W[1, :, up(q, w)])

    def wait_ysib(s):
        wait_recv(Y.at[1 - k, us_(s), UALL], r_d.at[s])

    def s3(r, cols, n):
        return rcopy(Pa.at[1, r, cols], R.at[y, r, cols], s_p.at[n], r_r.at[y, n], 3, k)

    s3_a = [s3(pl.ds(b * half, half), C0, b) for b in range(2)]
    s3_b = [[s3(rs_(h, 2 * u, 2), C1, 2 + 4 * h + u) for u in range(4)] for h in range(2)]

    def s3_k1(s):
        return s3(us_(s), CA, s)

    def s2(h, s, n, cols, i):
        r = rs_(h, s, n)
        return rcopy(Pa.at[0, r, cols], R.at[0, r, cols], s_p.at[10 + 3 * h + i], r_r.at[0, 3 * h + i], 2, k)

    PART1 = ((0, 4), (4, 2), (6, 2))
    PART0 = ((0, 6, C0), (0, 6, C1), (6, 2, CA))
    s2_k1 = [[s2(h, s, n, CA, i) for i, (s, n) in enumerate(PART1)] for h in range(2)]
    s2_k0 = [[s2(h, s, n, cols, i) for i, (s, n, cols) in enumerate(PART0)] for h in range(2)]

    def add(i, r, cols, sem):
        wait_recv(PR.at[i, r, cols], sem)
        Pa[i, r, cols] += PR[i, r, cols]

    def y1_start(x):
        @pl.when(y == 1)
        def _():
            x.start()

    def strip31(s):
        wait_ysib(s)
        r = us_(s)
        Pa[1, r, :] = PR[1, r, :] + mm(Y[0, r, UALL], W[0, :, :ku]) + mm(Y[1, r, UALL], W[1, :, :ku])
        s3_k1(s).start()

    @pl.when(z == 2)
    def _():
        def step_d(t):
            wait_recv(Y.at[k, rs_(t % 2, t // 2), DALL], r_y.at[t])
            d_fwd(t).start()

            @pl.when(t == 1)
            def _():
                wait_recv(X.at[1 - k, :, UALL], r_d.at[2 * NS])

            @pl.when((k == 1) & (t >= 1))
            def _():
                y2(t - 1)

        each(0, 2 * NS, step_d)
        each(2, 2 * NS, lambda t: z2_d(t).start())

        @pl.when(k == 1)
        def _():
            y2(NU, XU)

        pl.semaphore_wait(far, n_near)

        def step_u(s):
            wait_recv(Y.at[k, us_(s), UALL], r_y.at[2 * NS + s])
            u_sib(s).start()
            Qa[1, us_(s), :] = mm(Y[k, us_(s), :], X[k])
            q1send(s).start()

            @pl.when((k == 0) & (s >= 1))
            def _():
                y2(2 * s - 2)
                y2(2 * s - 1)

            @pl.when((k == 0) & (s == 4))
            def _():
                each(0, 4, wait_ysib)
                each(0, 6, lambda q: y3(0, q))

            @pl.when((k == 0) & (s >= 4))
            def _():
                y3(0, 2 * s - 2)
                y3(0, 2 * s - 1)

            @pl.when((k == 1) & (s == 2))
            def _():
                for h in range(2):
                    wait_recv(PR.at[1, rs_(h, 0, NS)], r_p.at[h, 0])

            @pl.when((k == 1) & (s >= 2))
            def _():
                strip31(s - 2)

        each(0, NS, step_u)

        def add21(gs, i):
            for h in range(2):
                for g in gs:
                    add(0, rs_(h, 2 * g, 2), CA, r_p.at[h, 1 + g])
                y1_start(s2_k1[h][i])

        @pl.when(k == 1)
        def _():
            add21((0, 1), 0)
            each(NS - 2, NS, strip31)
            add21((2,), 1)
            add21((3,), 2)

        @pl.when(k == 0)
        def _():
            y2(NU - 1)
            y2(NU, XU)
            y3(0, NU - 1)
            y3(0, NU, XU)
            for u in range(4):
                add(1, rs_(0, 2 * u, 2), C0, r_p.at[0, u])
            s3_a[0].start()
            for h in range(2):
                for g in range(3):
                    add(0, rs_(h, 2 * g, 2), C0, r_p.at[h, 8 + g])
                y1_start(s2_k0[h][0])
            each(4, NS, wait_ysib)

            def low(b):
                r = pl.ds(pl.multiple_of(b * half, half), half)
                Pa[1, r, :] = mm(Y[0, r, UALL], W[0, :, :ku]) + mm(Y[1, r, UALL], W[1, :, :ku])

            each(1 + k, 2, low)
            for u in range(4):
                add(1, rs_(1, 2 * u, 2), C0, r_p.at[1, u])
            s3_a[1].start()
            for u in range(4):
                for h in range(2):
                    add(1, rs_(h, 2 * u, 2), C1, r_p.at[h, 4 + u])
                    s3_b[h][u].start()
            for h in range(2):
                for g in range(3):
                    add(0, rs_(h, 2 * g, 2), C1, r_p.at[h, 12 + g])
                y1_start(s2_k0[h][1])
            for h in range(2):
                add(0, rs_(h, 6, 2), C0, r_p.at[h, 11])
                add(0, rs_(h, 6, 2), C1, r_p.at[h, 15])
                y1_start(s2_k0[h][2])

    @pl.when(z != 2)
    def _():
        pl.semaphore_wait(far, n_near)

    @pl.when(c > z)
    def _():
        o_ref[...] = jnp.zeros_like(o_ref)

    @pl.when(c == z)
    def _():
        for i in range(3):
            wait_recv(R.at[i], r_r.at[i, 0])
        total = Qa[dq] + R[0] + R[1] + R[2]
        diff = lax.broadcasted_iota(jnp.int32, (rows, rows), 0) - lax.broadcasted_iota(jnp.int32, (rows, rows), 1)
        o_ref[...] = jnp.where(diff >= 0, total, 0.0).astype(o_ref.dtype)

    @pl.when((z == 1) & (c == 0))
    def _():
        for b in range(2):
            for i in range(3):
                wait_recv(R.at[i, :, COLS[b]], r_r.at[i, b])
            o_ref[:, COLS[b]] = (Qb[b] + R[0, :, COLS[b]] + R[1, :, COLS[b]] + R[2, :, COLS[b]]).astype(o_ref.dtype)

    @pl.when((z == 2) & (y == 0))
    def _():
        for h in range(2):
            @pl.when(k == 0)
            def _():
                for i, (s, n, cols) in enumerate(PART0):
                    wait_recv(R.at[0, rs_(h, s, n), cols], r_r.at[0, 3 * h + i])

            @pl.when(k == 1)
            def _():
                for i, (s, n) in enumerate(PART1):
                    wait_recv(R.at[0, rs_(h, s, n)], r_r.at[0, 3 * h + i])

        o_ref[...] = (Pa[0] + R[0]).astype(o_ref.dtype)

    @pl.when((z == 3) & (c == 2))
    def _():
        def take(s):
            for i in range(4):
                wait_recv(R.at[i, us_(s)], r_r.at[i, s])

        each(0, NS, take)
        o_ref[...] = (R[0] + R[1] + R[2] + R[3]).astype(o_ref.dtype)

    @pl.when((z == 3) & (y == 0))
    def _():
        for i in range(2):
            @pl.when(k == 0)
            def _():
                for b in range(2):
                    wait_recv(R.at[i, pl.ds(b * half, half), C0], r_r.at[i, b])
                for h in range(2):
                    for u in range(4):
                        wait_recv(R.at[i, rs_(h, 2 * u, 2), C1], r_r.at[i, 2 + 4 * h + u])

            @pl.when(k == 1)
            def _():
                each(0, NS, lambda s: wait_recv(R.at[i, us_(s)], r_r.at[i, s]))

        o_ref[...] = (R[0] + R[1]).astype(o_ref.dtype)

    @pl.when(c != z)
    def _():
        dsend.wait_send()

    @pl.when(z == 0)
    def _():
        each(0, NU, lambda q: z0_u(q).wait_send())
        z0_u(NU, XU).wait_send()
        each(0, 2 * NS, lambda t: z0_d(t).wait_send())

    @pl.when(z == 3)
    def _():
        each(0, 2 * NS, lambda t: z3_d(t).wait_send())
        each(0, NS, lambda s: z3_u(s).wait_send())

    @pl.when(z == 1)
    def _():
        x_d.wait_send()
        each(0, NU, lambda q: z1_u(q).wait_send())
        z1_u(NU, XU).wait_send()
        each(0, NU, lambda q: u_fwd(q).wait_send())
        u_fwd(NU, XU).wait_send()
        each(0, 2 * NS, lambda t: d_sib(t).wait_send())
        m31.wait_send()
        for b in range(2):
            for u in range(4):
                m30(b, u).wait_send()
                m20(b, u).wait_send()
        for g in range(4):
            m21(g).wait_send()

        @pl.when(c != 0)
        def _():
            for b in range(2):
                q0send(b).wait_send()

    @pl.when(z == 2)
    def _():
        x_u.wait_send()
        each(0, 2 * NS, lambda t: z2_d(t).wait_send())
        each(0, 2 * NS, lambda t: d_fwd(t).wait_send())
        each(0, NS, lambda s: u_sib(s).wait_send())
        each(0, NS, lambda s: q1send(s).wait_send())

        @pl.when(k == 0)
        def _():
            for x in [*s3_a, *s3_b[0], *s3_b[1]]:
                x.wait_send()

            @pl.when(y == 1)
            def _():
                for x in [*s2_k0[0], *s2_k0[1]]:
                    x.wait_send()

        @pl.when(k == 1)
        def _():
            each(0, NS, lambda s: s3_k1(s).wait_send())

            @pl.when(y == 1)
            def _():
                for x in [*s2_k1[0], *s2_k1[1]]:
                    x.wait_send()


def solution(mesh):
    def local_fn(a_local):
        rows, m = a_local.shape
        kd = m - NU * PW - XU
        f32, bf16 = jnp.float32, jnp.bfloat16
        dma = pltpu.SemaphoreType.DMA
        return pl.pallas_call(
            kernel,
            out_shape=pltpu.VMEM((rows, rows), bf16),
            in_specs=[pl.BlockSpec(memory_space=pl.ANY)],
            out_specs=pl.BlockSpec(memory_space=pltpu.VMEM),
            scratch_shapes=[
                pltpu.VMEM((2, rows, m), bf16),
                pltpu.VMEM((2, rows, m), bf16),
                pltpu.VMEM((2, rows, kd), bf16),
                pltpu.VMEM((2, 2, kd, rows // 2), bf16),
                pltpu.VMEM((2, kd, rows), bf16),
                pltpu.VMEM((2, rows, rows), f32),
                pltpu.VMEM((2, rows, rows // 2), f32),
                pltpu.VMEM((2, rows, rows), f32),
                pltpu.VMEM((2, rows, rows // 2), f32),
                pltpu.VMEM((4, rows, rows), f32),
                pltpu.VMEM((2, rows, rows), f32),
                pltpu.SemaphoreType.REGULAR,
                dma((1,)), dma((4 * NS,)), dma((4 * NS,)), dma((2 * NS + 1,)), dma((2 * NS + 1,)),
                dma((2, 2 * NS)), dma((21,)), dma((2, 16)), dma((NS + 1,)), dma((4, 10)),
            ],
            compiler_params=pltpu.CompilerParams(
                collective_id=0, has_side_effects=True, vmem_limit_bytes=56 * 1024 * 1024),
        )(a_local)

    part_spec = P(("batch", "row"), "col")
    return jax.shard_map(local_fn, mesh=mesh, in_specs=(part_spec,), out_specs=part_spec, check_vma=False)
```

```python
import jax
import jax.numpy as jnp
from jax import lax
from jax.experimental import pallas as pl
from jax.experimental.pallas import tpu as pltpu
from jax.sharding import PartitionSpec as P

MESH = pl.DeviceIdType.MESH
PW = 256
NU = 15
XU = 128
NS = 8


def mm(a, b):
    return lax.dot_general(a, b, (((1,), (1,)), ((), ())), preferred_element_type=jnp.float32)


def mn(a, b):
    return lax.dot_general(a, b, (((1,), (0,)), ((), ())), preferred_element_type=jnp.float32)


def kernel(a_ref, o_ref, X, Y, W, T0, T1, Pa, Pb, Qa, Qb, R, PR, far, ld, s_z, r_y, r_d, r_w, r_p, r_r):
    rows, m = a_ref.shape
    ku = NU * PW + XU
    kd = m - ku
    nd, xd = kd // PW, kd % PW
    half = rows // 2
    st = half // NS
    us = rows // NS
    z = lax.axis_index("row")
    c = lax.axis_index("col")
    y = c // 2
    k = c % 2
    sib = 2 * y + 1 - k

    def rcopy(src, dst, ss, rs, row, col):
        return pltpu.make_async_remote_copy(
            src_ref=src, dst_ref=dst, send_sem=ss, recv_sem=rs, device_id={"row": row, "col": col}, device_id_type=MESH)

    def wait_recv(ref, sem):
        pltpu.make_async_copy(ref, ref, sem).wait()

    def up(p, w=PW):
        return pl.ds(pl.multiple_of(p * PW, 128), w)

    def dn(p, w=PW):
        return pl.ds(pl.multiple_of(ku + p * PW, 128), w)

    def rs_(h, s, n=1):
        return pl.ds(pl.multiple_of(h * half + s * st, st), n * st)

    def us_(s):
        return pl.ds(pl.multiple_of(s * us, us), us)

    DALL = pl.ds(ku, kd)
    UALL = pl.ds(0, ku)
    C0, C1 = pl.ds(0, half), pl.ds(half, half)
    COLS = (C0, C1)

    def each(lo, hi, fn):
        lax.fori_loop(lo, hi, lambda i, u: (fn(i), u)[1], 0)

    load = pltpu.make_async_copy(a_ref, X.at[k], ld.at[0])
    load.start()

    def near(sem):
        for dz in (-1, 1):
            @pl.when((z + dz >= 0) & (z + dz <= 3))
            def _():
                for kk in range(2):
                    pl.semaphore_signal(sem, inc=1, device_id={"row": z + dz, "col": 2 * y + kk}, device_id_type=MESH)
        for dc in range(1, 4):
            pl.semaphore_signal(sem, inc=1, device_id={"row": z, "col": (c + dc) % 4}, device_id_type=MESH)

    n_near = jnp.where((z == 0) | (z == 3), 5, 7)
    bar = pltpu.get_barrier_semaphore()
    near(bar)
    pl.semaphore_wait(bar, n_near)

    def z0_u(q, w=PW):
        return rcopy(a_ref.at[:, up(q, w)], Y.at[k, :, up(q, w)], s_z.at[0], r_y.at[q], 1, c)

    def z0_d(t):
        r = rs_(0, t)
        return rcopy(a_ref.at[r, DALL], Y.at[k, r, DALL], s_z.at[0], r_y.at[2 * NS + t], 1, c)

    def z3_d(t):
        r = rs_(t % 2, t // 2)
        return rcopy(a_ref.at[r, DALL], Y.at[k, r, DALL], s_z.at[0], r_y.at[t], 2, c)

    def z3_u(s):
        r = us_(s)
        return rcopy(a_ref.at[r, UALL], Y.at[k, r, UALL], s_z.at[0], r_y.at[2 * NS + s], 2, c)

    def z1_u(q, w=PW):
        return rcopy(a_ref.at[:, up(q, w)], W.at[k, :, up(q, w)], s_z.at[0], r_w.at[q], 2, 2 * y + 1)

    def z2_d(t):
        h, s = t % 2, t // 2
        return rcopy(a_ref.at[rs_(h, s), DALL], W.at[k, rs_(1, s), pl.ds(0, kd)], s_z.at[0], r_w.at[1 + s // 2], 1, 2 * y + h)

    @pl.when(z == 0)
    def _():
        each(0, NU, lambda q: z0_u(q).start())
        z0_u(NU, XU).start()
        each(0, 2 * NS, lambda t: z0_d(t).start())

    @pl.when(z == 3)
    def _():
        each(0, 2 * NS, lambda t: z3_d(t).start())
        each(0, NS, lambda s: z3_u(s).start())

    x_d = rcopy(a_ref.at[:, DALL], X.at[k, :, DALL], s_z.at[1], r_d.at[NS], z, sib)
    x_u = rcopy(a_ref.at[:, UALL], X.at[k, :, UALL], s_z.at[1], r_d.at[NS], z, sib)

    @pl.when(z == 1)
    def _():
        each(0, NU, lambda q: z1_u(q).start())
        z1_u(NU, XU).start()
        x_d.start()

    @pl.when(z == 2)
    def _():
        z2_d(0).start()
        z2_d(1).start()
        x_u.start()

    near(far)

    Pa[...] = jnp.zeros_like(Pa)
    Qa[...] = jnp.zeros_like(Qa)
    Qb[...] = jnp.zeros_like(Qb)
    load.wait()
    dq = jnp.where(z == 1, 1, 0)

    def diag(p):
        cs = pl.ds(pl.multiple_of(p * 512, 512), 512)
        Qa[dq] += mm(X[k, :, cs], X[k, :, cs])

    each(0, m // 512, diag)

    def slot(owner):
        return (c - owner + 3) % 4

    dsend = rcopy(Qa.at[dq], R.at[slot(z)], s_z.at[3], r_r.at[0], z, z)

    @pl.when(c != z)
    def _():
        dsend.start()

    def u_fwd(q, w=PW):
        return rcopy(Y.at[k, :, up(q, w)], W.at[k, :, up(q, w)], s_z.at[0], r_w.at[q], 2, 2 * y)

    def zU(q, w=PW):
        wait_recv(Y.at[k, :, up(q, w)], r_y.at[q])
        v = mm(X[k, :, up(q, w)], Y[k, :, up(q, w)])
        Qb[0] += v[:, :half]
        Qb[1] += v[:, half:]

    def turn(p, w=PW):
        for h in range(2):
            T1[h, up(p, w), :] = X[h, :, dn(p, w)].T

    def d_sib(t):
        return rcopy(Y.at[k, rs_(0, t), DALL], Y.at[k, rs_(0, t), DALL], s_z.at[1], r_d.at[t // NS], z, sib)

    def zD(t):
        wait_recv(Y.at[k, rs_(0, t), DALL], r_y.at[2 * NS + t])
        d_sib(t).start()

    def brows(b):
        return pl.ds(pl.multiple_of(b * half, half), half)

    def wait_w(r, n):
        wait_recv(W.at[:, r, pl.ds(0, kd)], r_w.at[n])

    CA = pl.ds(0, rows)

    def send1(src, i, s, n, j, cols, rs):
        return rcopy(src, PR.at[i, rs_(k, s, n), cols], s_z.at[2], r_p.at[rs], 2, 2 * y + j)

    m31 = send1(Pa.at[1, rs_(0, 0, NS)], 1, 0, NS, 1, CA, 0)

    def m30(b, u):
        return send1(Pb.at[b, rs_(0, 2 * u, 2)], 1, 2 * u, 2, 0, COLS[b], b + b * u)

    def m21(g):
        return send1(Pa.at[1, rs_(1, 2 * g, 2)], 0, 2 * g, 2, 1, CA, 1 + g // 2 + g // 3)

    def m20(b, g):
        return send1(Pb.at[b, rs_(1, 2 * g, 2)], 0, 2 * g, 2, 0, COLS[b], jnp.where(g == 3, 7, 5 + b))

    def part1(r):
        Pa[1, r, :] = mn(W[0, r, :kd], T1[0]) + mn(W[1, r, :kd], T1[1])

    def part0(r, b):
        Pb[b, r, :] = mn(W[0, r, :kd], T0[0, b]) + mn(W[1, r, :kd], T0[1, b])

    def q0send(b):
        return rcopy(Qb.at[b], R.at[slot(0), :, COLS[b]], s_z.at[4], r_r.at[b], 1, 0)

    @pl.when(z == 1)
    def _():
        wait_recv(X.at[1 - k, :, DALL], r_d.at[NS])

        def step_u(q):
            zU(q)

            @pl.when(q < 5)
            def _():
                u_fwd(q).start()

            turn(q)

        each(0, NU, step_u)
        zU(NU, XU)
        each(NU, nd, turn)
        if xd:
            turn(nd, xd)

        def step(i):
            @pl.when(i < 2 * NS)
            def _():
                zD(i)

            @pl.when(i == 3)
            def _():
                wait_w(rs_(0, 0, NS), 0)
                part1(rs_(0, 0, NS))
                m31.start()
                each(5, 10, lambda q: u_fwd(q).start())

            @pl.when((i == 7) | (i == 16))
            def _():
                b = jnp.where(i == 7, 0, 1)
                wait_recv(Y.at[1 - k, brows(b), DALL], r_d.at[b])
                for h in range(2):
                    T0[h, b] = Y[h, brows(b), DALL].T
                part0(rs_(0, 0, NS), b)
                for bb in range(2):
                    @pl.when(b == bb)
                    def _():
                        for u in range(4):
                            m30(bb, u).start()

            @pl.when((i == 7) | (i == 19))
            def _():
                b = jnp.where(i == 7, 0, 1)
                Qb[b] += mm(X[k, :, DALL], Y[k, brows(b), DALL])
                for bb in range(2):
                    @pl.when((b == bb) & (c != 0))
                    def _():
                        q0send(bb).start()

            @pl.when(i == 7)
            def _():
                each(10, 13, lambda q: u_fwd(q).start())

            @pl.when((i == 8) | (i == 9) | (i == 13) | (i == 20))
            def _():
                g = jnp.where(i == 20, 3, jnp.where(i == 13, 2, i - 8))
                wait_w(rs_(1, 2 * g, 2), 1 + g)
                part1(rs_(1, 2 * g, 2))
                m21(g).start()
                part0(rs_(1, 2 * g, 2), 0)
                m20(0, g).start()

            @pl.when(i == 9)
            def _():
                each(13, NU, lambda q: u_fwd(q).start())
                u_fwd(NU, XU).start()

            @pl.when(i >= 17)
            def _():
                g = i - 17
                part0(rs_(1, 2 * g, 2), 1)
                m20(1, g).start()

        each(0, 21, step)

    def d_fwd(t):
        h, s = t % 2, t // 2
        return rcopy(Y.at[k, rs_(h, s), DALL], W.at[k, rs_(0, s), pl.ds(0, kd)], s_z.at[0], r_w.at[0], 1, 2 * y + h)

    def u_sib(s):
        return rcopy(Y.at[k, us_(s), UALL], Y.at[k, us_(s), UALL], s_z.at[1], r_d.at[s], z, sib)

    def q1send(s):
        return rcopy(Qa.at[1, us_(s)], R.at[c, us_(s)], s_z.at[4], r_r.at[0], 3, 2)

    def y2(q, w=PW):
        wait_recv(W.at[:, :, up(q, w)], r_w.at[q])
        Pa[0] += mm(X[0, :, up(q, w)], W[0, :, up(q, w)]) + mm(X[1, :, up(q, w)], W[1, :, up(q, w)])

    def y3(b, q, w=PW):
        r = pl.ds(b * half, half)
        Pa[1, r, :] += mm(Y[0, r, up(q, w)], W[0, :, up(q, w)]) + mm(Y[1, r, up(q, w)], W[1, :, up(q, w)])

    def wait_ysib(s):
        wait_recv(Y.at[1 - k, us_(s), UALL], r_d.at[s])

    def s3(r, cols, n):
        return rcopy(Pa.at[1, r, cols], R.at[y, r, cols], s_z.at[2], r_r.at[0], 3, k)

    s3_a = [s3(pl.ds(b * half, half), C0, b) for b in range(2)]
    s3_b = [[s3(rs_(h, 2 * u, 2), C1, 2 + 4 * h + u) for u in range(4)] for h in range(2)]

    def s3_k1(s):
        return s3(us_(s), CA, s)

    def s2(h, s, n, cols, i):
        r = rs_(h, s, n)
        return rcopy(Pa.at[0, r, cols], R.at[0, r, cols], s_z.at[2], r_r.at[0], 2, k)

    PART1 = ((0, 4), (4, 2), (6, 2))
    PART0 = ((0, 6, C0), (0, 6, C1), (6, 2, CA))
    s2_k1 = [[s2(h, s, n, CA, i) for i, (s, n) in enumerate(PART1)] for h in range(2)]
    s2_k0 = [[s2(h, s, n, cols, i) for i, (s, n, cols) in enumerate(PART0)] for h in range(2)]

    def wait_pr(n, cols, sem):
        wait_recv(PR.at[0, pl.ds(0, n), cols], r_p.at[sem])

    def add(i, r, cols):
        Pa[i, r, cols] += PR[i, r, cols]

    def y1_start(x):
        @pl.when(y == 1)
        def _():
            x.start()

    def strip31(s):
        wait_ysib(s)
        r = us_(s)
        Pa[1, r, :] = PR[1, r, :] + mm(Y[0, r, UALL], W[0, :, :ku]) + mm(Y[1, r, UALL], W[1, :, :ku])
        s3_k1(s).start()

    @pl.when(z == 2)
    def _():
        def step_d(t):
            wait_recv(Y.at[k, rs_(t % 2, t // 2), DALL], r_y.at[t])
            d_fwd(t).start()

            @pl.when(t == 1)
            def _():
                wait_recv(X.at[1 - k, :, UALL], r_d.at[NS])

            @pl.when((k == 1) & (t >= 1))
            def _():
                y2(t - 1)

        each(0, 2 * NS, step_d)
        each(2, 2 * NS, lambda t: z2_d(t).start())

        @pl.when(k == 1)
        def _():
            y2(NU, XU)

        pl.semaphore_wait(far, n_near)

        def step_u(s):
            wait_recv(Y.at[k, us_(s), UALL], r_y.at[2 * NS + s])
            u_sib(s).start()
            Qa[1, us_(s), :] = mm(Y[k, us_(s), :], X[k])
            q1send(s).start()

            @pl.when((k == 0) & (s >= 1))
            def _():
                y2(2 * s - 2)
                y2(2 * s - 1)

            @pl.when((k == 0) & (s == 4))
            def _():
                each(0, 4, wait_ysib)
                each(0, 6, lambda q: y3(0, q))

            @pl.when((k == 0) & (s >= 4))
            def _():
                y3(0, 2 * s - 2)
                y3(0, 2 * s - 1)

            @pl.when((k == 1) & (s == 2))
            def _():
                wait_recv(PR.at[1], r_p.at[0])

            @pl.when((k == 1) & (s >= 2))
            def _():
                strip31(s - 2)

        each(0, NS, step_u)

        def add21(gs, i):
            wait_pr(64 * len(gs), CA, 1 + i)
            for h in range(2):
                add(0, rs_(h, 2 * gs[0], 2 * len(gs)), CA)
                y1_start(s2_k1[h][i])

        @pl.when(k == 1)
        def _():
            add21((0, 1), 0)
            each(NS - 2, NS, strip31)
            add21((2,), 1)
            add21((3,), 2)

        @pl.when(k == 0)
        def _():
            y2(NU - 1)
            y2(NU, XU)
            y3(0, NU - 1)
            y3(0, NU, XU)
            wait_pr(rows, C0, 0)
            add(1, pl.ds(0, half), C0)
            s3_a[0].start()
            wait_pr(192, C0, 5)
            for h in range(2):
                add(0, rs_(h, 0, 6), C0)
                y1_start(s2_k0[h][0])
            each(4, NS, wait_ysib)

            def low(b):
                r = pl.ds(pl.multiple_of(b * half, half), half)
                Pa[1, r, :] = mm(Y[0, r, UALL], W[0, :, :ku]) + mm(Y[1, r, UALL], W[1, :, :ku])

            each(1 + k, 2, low)
            add(1, pl.ds(half, half), C0)
            s3_a[1].start()
            for u in range(4):
                wait_pr(64, C1, 1 + u)
                for h in range(2):
                    add(1, rs_(h, 2 * u, 2), C1)
                    s3_b[h][u].start()
            wait_pr(192, C1, 6)
            for h in range(2):
                add(0, rs_(h, 0, 6), C1)
                y1_start(s2_k0[h][1])
            wait_pr(64, CA, 7)
            for h in range(2):
                add(0, rs_(h, 6, 2), CA)
                y1_start(s2_k0[h][2])

    @pl.when(z != 2)
    def _():
        pl.semaphore_wait(far, n_near)

    @pl.when(c > z)
    def _():
        o_ref[...] = jnp.zeros_like(o_ref)

    @pl.when(c == z)
    def _():
        wait_recv(R.at[pl.ds(0, 3)], r_r.at[0])
        total = Qa[dq] + R[0] + R[1] + R[2]
        diff = lax.broadcasted_iota(jnp.int32, (rows, rows), 0) - lax.broadcasted_iota(jnp.int32, (rows, rows), 1)
        o_ref[...] = jnp.where(diff >= 0, total, 0.0).astype(o_ref.dtype)

    @pl.when((z == 1) & (c == 0))
    def _():
        for b in range(2):
            wait_recv(R.at[pl.ds(0, 3), :, COLS[b]], r_r.at[b])
            o_ref[:, COLS[b]] = (Qb[b] + R[0, :, COLS[b]] + R[1, :, COLS[b]] + R[2, :, COLS[b]]).astype(o_ref.dtype)

    @pl.when((z == 2) & (y == 0))
    def _():
        wait_recv(R.at[0], r_r.at[0])
        o_ref[...] = (Pa[0] + R[0]).astype(o_ref.dtype)

    @pl.when((z == 3) & (c == 2))
    def _():
        wait_recv(R, r_r.at[0])
        o_ref[...] = (R[0] + R[1] + R[2] + R[3]).astype(o_ref.dtype)

    @pl.when((z == 3) & (y == 0))
    def _():
        wait_recv(R.at[pl.ds(0, 2)], r_r.at[0])
        o_ref[...] = (R[0] + R[1]).astype(o_ref.dtype)

    @pl.when(c != z)
    def _():
        wait_recv(Qa.at[0], s_z.at[3])

    @pl.when((z == 0) | (z == 3))
    def _():
        wait_recv(X.at[k], s_z.at[0])

    @pl.when(z == 1)
    def _():
        wait_recv(W.at[:, :, pl.ds(0, ku)], s_z.at[0])
        wait_recv(W.at[:, :, pl.ds(0, kd)], s_z.at[1])
        wait_recv(Pa, s_z.at[2])

        @pl.when(c != 0)
        def _():
            wait_recv(Qb, s_z.at[4])

    @pl.when(z == 2)
    def _():
        wait_recv(W.at[:, :, pl.ds(0, kd)], s_z.at[0])
        wait_recv(W.at[:, :, pl.ds(0, ku)], s_z.at[1])
        wait_recv(Qa.at[1], s_z.at[4])

        @pl.when(y == 0)
        def _():
            wait_recv(Pa.at[0], s_z.at[2])

        @pl.when(y == 1)
        def _():
            wait_recv(Pa, s_z.at[2])


def solution(mesh):
    def local_fn(a_local):
        rows, m = a_local.shape
        kd = m - NU * PW - XU
        f32, bf16 = jnp.float32, jnp.bfloat16
        dma = pltpu.SemaphoreType.DMA
        return pl.pallas_call(
            kernel,
            out_shape=pltpu.VMEM((rows, rows), bf16),
            in_specs=[pl.BlockSpec(memory_space=pl.ANY)],
            out_specs=pl.BlockSpec(memory_space=pltpu.VMEM),
            scratch_shapes=[
                pltpu.VMEM((2, rows, m), bf16),
                pltpu.VMEM((2, rows, m), bf16),
                pltpu.VMEM((2, rows, kd), bf16),
                pltpu.VMEM((2, 2, kd, rows // 2), bf16),
                pltpu.VMEM((2, kd, rows), bf16),
                pltpu.VMEM((2, rows, rows), f32),
                pltpu.VMEM((2, rows, rows // 2), f32),
                pltpu.VMEM((2, rows, rows), f32),
                pltpu.VMEM((2, rows, rows // 2), f32),
                pltpu.VMEM((4, rows, rows), f32),
                pltpu.VMEM((2, rows, rows), f32),
                pltpu.SemaphoreType.REGULAR,
                dma((1,)), dma((5,)), dma((4 * NS,)), dma((NS + 1,)), dma((NU + 1,)), dma((8,)), dma((2,)),
            ],
            compiler_params=pltpu.CompilerParams(
                collective_id=0, has_side_effects=True, vmem_limit_bytes=56 * 1024 * 1024),
        )(a_local)

    part_spec = P(("batch", "row"), "col")
    return jax.shard_map(local_fn, mesh=mesh, in_specs=(part_spec,), out_specs=part_spec, check_vma=False)
```

```python
import jax
import jax.numpy as jnp
from jax import lax
from jax.experimental import pallas as pl
from jax.experimental.pallas import tpu as pltpu
from jax.sharding import PartitionSpec as P

MESH = pl.DeviceIdType.MESH
PW = 256
NU = 15
XU = 128
NS = 8


def mm(a, b):
    return lax.dot_general(a, b, (((1,), (1,)), ((), ())), preferred_element_type=jnp.float32)


def mn(a, b):
    return lax.dot_general(a, b, (((1,), (0,)), ((), ())), preferred_element_type=jnp.float32)


def kernel(a_ref, o_ref, X, Y, W, T0, T1, Pa, Pb, Qa, Qb, R, PR, XA, XB, far, ld, s_z, r_y, r_d, r_w, r_p, r_r, r_x):
    rows, m = a_ref.shape
    ku = NU * PW + XU
    kd = m - ku
    nd, xd = kd // PW, kd % PW
    half = rows // 2
    st = half // NS
    us = rows // NS
    z = lax.axis_index("row")
    c = lax.axis_index("col")
    y = c // 2
    k = c % 2
    sib = 2 * y + 1 - k

    def rcopy(src, dst, ss, rs, row, col):
        return pltpu.make_async_remote_copy(
            src_ref=src, dst_ref=dst, send_sem=ss, recv_sem=rs, device_id={"row": row, "col": col}, device_id_type=MESH)

    def wait_recv(ref, sem):
        pltpu.make_async_copy(ref, ref, sem).wait()

    def up(p, w=PW):
        return pl.ds(pl.multiple_of(p * PW, 128), w)

    def dn(p, w=PW):
        return pl.ds(pl.multiple_of(ku + p * PW, 128), w)

    def rs_(h, s, n=1):
        return pl.ds(pl.multiple_of(h * half + s * st, st), n * st)

    def us_(s):
        return pl.ds(pl.multiple_of(s * us, us), us)

    DALL = pl.ds(ku, kd)
    UALL = pl.ds(0, ku)
    C0, C1 = pl.ds(0, half), pl.ds(half, half)
    COLS = (C0, C1)

    def each(lo, hi, fn):
        lax.fori_loop(lo, hi, lambda i, u: (fn(i), u)[1], 0)

    load = pltpu.make_async_copy(a_ref, X.at[k], ld.at[0])
    load.start()

    def near(sem):
        for dz in (-1, 1):
            @pl.when((z + dz >= 0) & (z + dz <= 3))
            def _():
                for kk in range(2):
                    pl.semaphore_signal(sem, inc=1, device_id={"row": z + dz, "col": 2 * y + kk}, device_id_type=MESH)
        for dc in range(1, 4):
            pl.semaphore_signal(sem, inc=1, device_id={"row": z, "col": (c + dc) % 4}, device_id_type=MESH)

    n_near = jnp.where((z == 0) | (z == 3), 5, 7)
    bar = pltpu.get_barrier_semaphore()
    near(bar)
    pl.semaphore_wait(bar, n_near)

    def z0_u(q, w=PW):
        return rcopy(a_ref.at[:, up(q, w)], Y.at[k, :, up(q, w)], s_z.at[0], r_y.at[q], 1, c)

    def z0_d(t):
        r = rs_(0, t)
        return rcopy(a_ref.at[r, DALL], Y.at[k, r, DALL], s_z.at[0], r_y.at[2 * NS + t], 1, c)

    def z3_d(t):
        r = rs_(t % 2, t // 2)
        return rcopy(a_ref.at[r, DALL], Y.at[k, r, DALL], s_z.at[0], r_y.at[t], 2, c)

    def z3_u(s):
        r = us_(s)
        return rcopy(a_ref.at[r, UALL], Y.at[k, r, UALL], s_z.at[0], r_y.at[2 * NS + s], 2, c)

    def z1_u(q, w=PW):
        return rcopy(a_ref.at[:, up(q, w)], W.at[k, :, up(q, w)], s_z.at[0], r_w.at[q], 2, 2 * y + 1)

    def z2_d(t):
        h, s = t % 2, t // 2
        return rcopy(a_ref.at[rs_(h, s), DALL], W.at[k, rs_(1, s), pl.ds(0, kd)], s_z.at[0], r_w.at[1 + s // 2], 1, 2 * y + h)

    @pl.when(z == 0)
    def _():
        each(0, NU, lambda q: z0_u(q).start())
        z0_u(NU, XU).start()
        each(0, 2 * NS, lambda t: z0_d(t).start())

    @pl.when(z == 3)
    def _():
        each(0, 2 * NS, lambda t: z3_d(t).start())
        each(0, NS, lambda s: z3_u(s).start())

    x_d = rcopy(a_ref.at[:, DALL], X.at[k, :, DALL], s_z.at[1], r_d.at[NS], z, sib)
    x_u = rcopy(a_ref.at[:, UALL], X.at[k, :, UALL], s_z.at[1], r_d.at[NS], z, sib)

    @pl.when(z == 1)
    def _():
        each(0, NU, lambda q: z1_u(q).start())
        z1_u(NU, XU).start()
        x_d.start()

    @pl.when(z == 2)
    def _():
        z2_d(0).start()
        z2_d(1).start()
        x_u.start()

    near(far)

    Pa[...] = jnp.zeros_like(Pa)
    Qa[...] = jnp.zeros_like(Qa)
    Qb[...] = jnp.zeros_like(Qb)
    load.wait()
    dq = jnp.where(z == 1, 1, 0)

    def diag(p):
        cs = pl.ds(pl.multiple_of(p * 512, 512), 512)
        Qa[dq] += mm(X[k, :, cs], X[k, :, cs])

    each(0, m // 512, diag)

    def slot(owner):
        return (c - owner + 3) % 4

    dsend = rcopy(Qa.at[dq], R.at[slot(z)], s_z.at[3], r_r.at[0], z, z)

    @pl.when(c != z)
    def _():
        dsend.start()

    def u_fwd(q, w=PW):
        return rcopy(Y.at[k, :, up(q, w)], W.at[k, :, up(q, w)], s_z.at[0], r_w.at[q], 2, 2 * y)

    def zU(q, w=PW):
        wait_recv(Y.at[k, :, up(q, w)], r_y.at[q])
        v = mm(X[k, :, up(q, w)], Y[k, :, up(q, w)])
        Qb[0] += v[:, :half]
        Qb[1] += v[:, half:]

    def turn(p, w=PW):
        for h in range(2):
            T1[h, up(p, w), :] = X[h, :, dn(p, w)].T

    def d_sib(t):
        return rcopy(Y.at[k, rs_(0, t), DALL], Y.at[k, rs_(0, t), DALL], s_z.at[1], r_d.at[t // NS], z, sib)

    def zD(t):
        wait_recv(Y.at[k, rs_(0, t), DALL], r_y.at[2 * NS + t])
        d_sib(t).start()

    def brows(b):
        return pl.ds(pl.multiple_of(b * half, half), half)

    def wait_w(r, n):
        wait_recv(W.at[:, r, pl.ds(0, kd)], r_w.at[n])

    CA = pl.ds(0, rows)
    peer = (c + 2) % 4

    def r3(u):
        return rs_(0, 4 * u, 4)

    def r2(g):
        return rs_(1, 2 * g, 2)

    def xsend(src, dst, n):
        return rcopy(src, dst, s_z.at[2], r_x.at[n], 1, peer)

    x31 = xsend(Pa.at[1, rs_(0, 0, NS)], XA.at[rs_(0, 0, NS)], 0)

    def x30(b, u):
        return xsend(Pb.at[b, r3(u)], XB.at[b, r3(u)], 1 + 2 * b + u)

    def x21(g):
        return xsend(Pa.at[1, r2(g)], XA.at[r2(g)], 5 + g)

    def x20(b, g):
        return xsend(Pb.at[b, r2(g)], XB.at[b, r2(g)], jnp.where(b == 0, 5 + g, 8))

    def msend(src, i, s, n, j, cols, rs):
        return rcopy(src, PR.at[i, rs_(k, s, n), cols], s_z.at[2], r_p.at[rs], 2, j)

    m31 = msend(Pa.at[1, rs_(0, 0, NS)], 1, 0, NS, 1, CA, 0)

    def m30(b, u):
        src = Pb.at[b, r3(u)]
        if b == 0:
            return msend(src, 1, 4 * u, 4, 0, C0, 0)
        return rcopy(src, R.at[2, rs_(k, 4 * u, 4), C1], s_z.at[2], r_r.at[1], 3, 0)

    def m21(g):
        return msend(Pa.at[1, r2(g)], 0, 2 * g, 2, 1, CA, jnp.where(g == 3, 2, 1))

    def m20(b, g):
        return msend(Pb.at[b, r2(g)], 0, 2 * g, 2, 0, COLS[b], jnp.where(g == 3, 3, 1 + b))

    def d2(src, j, cols):
        return rcopy(src, R.at[1, rs_(k, 6, 2), cols], s_z.at[2], r_r.at[1], 2, j)

    d21 = d2(Pa.at[1, r2(3)], 1, CA)
    d20 = [d2(Pb.at[b, r2(3)], 0, COLS[b]) for b in range(2)]

    def part1(r):
        Pa[1, r, :] = mn(W[0, r, :kd], T1[0]) + mn(W[1, r, :kd], T1[1])

    def part0(r, b):
        Pb[b, r, :] = mn(W[0, r, :kd], T0[0, b]) + mn(W[1, r, :kd], T0[1, b])

    def q0send(b):
        return rcopy(Qb.at[b], R.at[slot(0), :, COLS[b]], s_z.at[4], r_r.at[b], 1, 0)

    @pl.when(z == 1)
    def _():
        wait_recv(X.at[1 - k, :, DALL], r_d.at[NS])

        def step_u(q):
            zU(q)

            @pl.when(q < 5)
            def _():
                u_fwd(q).start()

            turn(q)

        each(0, NU, step_u)
        zU(NU, XU)
        each(NU, nd, turn)
        if xd:
            turn(nd, xd)

        pl.semaphore_wait(far, n_near)

        def merge30(b):
            for u in range(2):
                wait_recv(XB.at[b, r3(u)], r_x.at[1 + 2 * b + u])
                Pb[b, r3(u), :] += XB[b, r3(u), :]
                m30(b, u).start()

        def step(i):
            @pl.when(i < 2 * NS)
            def _():
                zD(i)

            @pl.when(i == 3)
            def _():
                wait_w(rs_(0, 0, NS), 0)
                part1(rs_(0, 0, NS))

                @pl.when(y == 1)
                def _():
                    x31.start()

                each(5, 10, lambda q: u_fwd(q).start())

            @pl.when((i == 5) & (y == 0))
            def _():
                wait_recv(XA.at[rs_(0, 0, NS)], r_x.at[0])
                Pa[1, rs_(0, 0, NS), :] += XA[rs_(0, 0, NS), :]
                m31.start()

            @pl.when((i == 7) | (i == 16))
            def _():
                b = jnp.where(i == 7, 0, 1)
                wait_recv(Y.at[1 - k, brows(b), DALL], r_d.at[b])
                for h in range(2):
                    T0[h, b] = Y[h, brows(b), DALL].T
                part0(rs_(0, 0, NS), b)
                for bb in range(2):
                    @pl.when((b == bb) & (y == 1))
                    def _():
                        for u in range(2):
                            x30(bb, u).start()

            @pl.when((i == 7) | (i == 19))
            def _():
                b = jnp.where(i == 7, 0, 1)
                Qb[b] += mm(X[k, :, DALL], Y[k, brows(b), DALL])
                for bb in range(2):
                    @pl.when((b == bb) & (c != 0))
                    def _():
                        q0send(bb).start()

            @pl.when(i == 7)
            def _():
                each(10, NU, lambda q: u_fwd(q).start())
                u_fwd(NU, XU).start()

            @pl.when((i == 9) & (y == 0))
            def _():
                merge30(0)

            @pl.when((i == 20) & (y == 0))
            def _():
                merge30(1)

            @pl.when((i == 8) | (i == 9) | (i == 13) | (i == 20))
            def _():
                g = jnp.where(i == 20, 3, jnp.where(i == 13, 2, i - 8))
                wait_w(r2(g), 1 + g)
                part1(r2(g))
                part0(r2(g), 0)

                @pl.when((y == 1) & (i < 20))
                def _():
                    x21(g).start()
                    x20(0, g).start()

            @pl.when(((i == 10) | (i == 11) | (i == 15)) & (y == 0))
            def _():
                g = jnp.where(i == 15, 2, i - 10)
                wait_recv(XA.at[pl.ds(0, 48)], r_x.at[5 + g])
                Pa[1, r2(g), :] += XA[r2(g), :]
                Pb[0, r2(g), :] += XB[0, r2(g), :]
                m21(g).start()
                m20(0, g).start()

            @pl.when(i >= 17)
            def _():
                g = i - 17
                part0(r2(g), 1)

                @pl.when((y == 1) & (i < 20))
                def _():
                    x20(1, g).start()

        each(0, 21, step)

        @pl.when(y == 1)
        def _():
            d21.start()
            for x in d20:
                x.start()

        @pl.when(y == 0)
        def _():
            m21(3).start()
            m20(0, 3).start()
            m20(1, 3).start()
            wait_recv(XB.at[0, pl.ds(0, 96)], r_x.at[8])
            r = rs_(1, 0, 6)
            Pb[1, r, :] += XB[1, r, :]
            for g in range(3):
                m20(1, g).start()

    def d_fwd(t):
        h, s = t % 2, t // 2
        return rcopy(Y.at[k, rs_(h, s), DALL], W.at[k, rs_(0, s), pl.ds(0, kd)], s_z.at[0], r_w.at[0], 1, 2 * y + h)

    def u_sib(s):
        return rcopy(Y.at[k, us_(s), UALL], Y.at[k, us_(s), UALL], s_z.at[1], r_d.at[s], z, sib)

    def q1send(s):
        return rcopy(Qa.at[1, us_(s)], R.at[c, us_(s)], s_z.at[4], r_r.at[0], 3, 2)

    def y2(q, w=PW):
        wait_recv(W.at[:, :, up(q, w)], r_w.at[q])
        Pa[0] += mm(X[0, :, up(q, w)], W[0, :, up(q, w)]) + mm(X[1, :, up(q, w)], W[1, :, up(q, w)])

    def y3(b, q, w=PW):
        r = pl.ds(b * half, half)
        Pa[1, r, :] += mm(Y[0, r, up(q, w)], W[0, :, up(q, w)]) + mm(Y[1, r, up(q, w)], W[1, :, up(q, w)])

    def wait_ysib(s):
        wait_recv(Y.at[1 - k, us_(s), UALL], r_d.at[s])

    def s3(r):
        return rcopy(Pa.at[1, r], R.at[y, r], s_z.at[2], r_r.at[0], 3, k)

    s2 = rcopy(Pa.at[0], R.at[0], s_z.at[2], r_r.at[0], 2, k)

    def add(i, r, cols):
        Pa[i, r, cols] += PR[i, r, cols]

    def wait_pr(n, cols, sem):
        wait_recv(PR.at[0, pl.ds(0, n), cols], r_p.at[sem])

    def strip31(s):
        wait_ysib(s)
        r = us_(s)
        Pa[1, r, :] = mm(Y[0, r, UALL], W[0, :, :ku]) + mm(Y[1, r, UALL], W[1, :, :ku])

        @pl.when(y == 0)
        def _():
            add(1, r, CA)

        s3(r).start()

    @pl.when(z == 2)
    def _():
        def step_d(t):
            wait_recv(Y.at[k, rs_(t % 2, t // 2), DALL], r_y.at[t])
            d_fwd(t).start()

            @pl.when(t == 1)
            def _():
                wait_recv(X.at[1 - k, :, UALL], r_d.at[NS])

            @pl.when((k == 1) & (t >= 1))
            def _():
                y2(t - 1)

        each(0, 2 * NS, step_d)
        each(2, 2 * NS, lambda t: z2_d(t).start())

        pl.semaphore_wait(far, n_near)

        @pl.when(k == 1)
        def _():
            y2(NU, XU)

            @pl.when(y == 1)
            def _():
                s2.start()


        def q1(s):
            Qa[1, us_(s), :] = mm(Y[k, us_(s), :], X[k])
            q1send(s).start()

        def step_u(s):
            wait_recv(Y.at[k, us_(s), UALL], r_y.at[2 * NS + s])
            u_sib(s).start()

            @pl.when((k == 0) & (s >= 1))
            def _():
                y2(2 * s - 1)

            @pl.when(k == 0)
            def _():
                y2(2 * s)

            @pl.when((k == 0) & (s == 4))
            def _():
                each(0, 4, wait_ysib)
                each(0, 7, lambda q: y3(0, q))

            @pl.when((k == 0) & (s >= 4))
            def _():
                y3(0, 2 * s - 1)
                y3(0, 2 * s)

            @pl.when((k == 1) & (y == 0) & (s == 4))
            def _():
                wait_recv(PR.at[1], r_p.at[0])

            @pl.when((k == 1) & (s >= 4) & (s <= 6))
            def _():
                strip31(2 * s - 8)
                strip31(2 * s - 7)

            @pl.when(s < NS - 1)
            def _():
                q1(s)

        each(0, NS, step_u)

        @pl.when(k == 1)
        def _():
            each(NS - 2, NS, strip31)
            q1(NS - 1)

            @pl.when(y == 0)
            def _():
                wait_pr(192, CA, 1)
                for h in range(2):
                    add(0, rs_(h, 0, 6), CA)
                wait_pr(64, CA, 2)
                for h in range(2):
                    add(0, rs_(h, 6, 2), CA)

        @pl.when(k == 0)
        def _():
            y2(NU, XU)

            @pl.when(y == 1)
            def _():
                s2.start()

            y3(0, NU, XU)

            @pl.when(y == 0)
            def _():
                wait_pr(rows, C0, 0)
                add(1, pl.ds(0, half), C0)

            s3(pl.ds(0, half)).start()
            each(4, NS, wait_ysib)

            def low(b):
                r = pl.ds(pl.multiple_of(b * half, half), half)
                Pa[1, r, :] = mm(Y[0, r, UALL], W[0, :, :ku]) + mm(Y[1, r, UALL], W[1, :, :ku])

            each(1 + k, 2, low)

            @pl.when(y == 0)
            def _():
                add(1, pl.ds(half, half), C0)

            s3(pl.ds(half, half)).start()
            q1(NS - 1)

            @pl.when(y == 0)
            def _():
                wait_pr(192, C0, 1)
                for h in range(2):
                    add(0, rs_(h, 0, 6), C0)
                wait_pr(64, CA, 3)
                for h in range(2):
                    add(0, rs_(h, 6, 2), CA)
                wait_pr(192, C1, 2)
                for h in range(2):
                    add(0, rs_(h, 0, 6), C1)

    @pl.when((z == 0) | (z == 3))
    def _():
        pl.semaphore_wait(far, n_near)

    @pl.when(c > z)
    def _():
        o_ref[...] = jnp.zeros_like(o_ref)

    @pl.when(c == z)
    def _():
        wait_recv(R.at[pl.ds(0, 3)], r_r.at[0])
        total = Qa[dq] + R[0] + R[1] + R[2]
        diff = lax.broadcasted_iota(jnp.int32, (rows, rows), 0) - lax.broadcasted_iota(jnp.int32, (rows, rows), 1)
        o_ref[...] = jnp.where(diff >= 0, total, 0.0).astype(o_ref.dtype)

    @pl.when((z == 1) & (c == 0))
    def _():
        for b in range(2):
            wait_recv(R.at[pl.ds(0, 3), :, COLS[b]], r_r.at[b])
            o_ref[:, COLS[b]] = (Qb[b] + R[0, :, COLS[b]] + R[1, :, COLS[b]] + R[2, :, COLS[b]]).astype(o_ref.dtype)

    @pl.when((z == 2) & (y == 0))
    def _():
        wait_recv(R.at[0], r_r.at[0])
        wait_recv(R.at[1, pl.ds(0, 64)], r_r.at[1])
        for h in range(2):
            Pa[0, rs_(h, 6, 2), :] += R[1, rs_(h, 6, 2), :]
        o_ref[...] = (Pa[0] + R[0]).astype(o_ref.dtype)

    @pl.when((z == 3) & (c == 2))
    def _():
        wait_recv(R, r_r.at[0])
        o_ref[...] = (R[0] + R[1] + R[2] + R[3]).astype(o_ref.dtype)

    @pl.when((z == 3) & (y == 0))
    def _():
        wait_recv(R.at[pl.ds(0, 2)], r_r.at[0])

        @pl.when(k == 0)
        def _():
            wait_recv(R.at[2, :, C1], r_r.at[1])
            R[0, :, C1] += R[2, :, C1]

        o_ref[...] = (R[0] + R[1]).astype(o_ref.dtype)

    @pl.when(c != z)
    def _():
        wait_recv(Qa.at[0], s_z.at[3])

    @pl.when((z == 0) | (z == 3))
    def _():
        wait_recv(X.at[k], s_z.at[0])

    @pl.when(z == 1)
    def _():
        wait_recv(W.at[:, :, pl.ds(0, ku)], s_z.at[0])
        wait_recv(W.at[:, :, pl.ds(0, kd)], s_z.at[1])
        wait_recv(Pa, s_z.at[2])

        @pl.when(c != 0)
        def _():
            wait_recv(Qb, s_z.at[4])

    @pl.when(z == 2)
    def _():
        wait_recv(W.at[:, :, pl.ds(0, kd)], s_z.at[0])
        wait_recv(W.at[:, :, pl.ds(0, ku)], s_z.at[1])
        wait_recv(Qa.at[1], s_z.at[4])

        @pl.when(y == 0)
        def _():
            wait_recv(Pa.at[0], s_z.at[2])

        @pl.when(y == 1)
        def _():
            wait_recv(Pa, s_z.at[2])


def solution(mesh):
    def local_fn(a_local):
        rows, m = a_local.shape
        kd = m - NU * PW - XU
        f32, bf16 = jnp.float32, jnp.bfloat16
        dma = pltpu.SemaphoreType.DMA
        return pl.pallas_call(
            kernel,
            out_shape=pltpu.VMEM((rows, rows), bf16),
            in_specs=[pl.BlockSpec(memory_space=pl.ANY)],
            out_specs=pl.BlockSpec(memory_space=pltpu.VMEM),
            scratch_shapes=[
                pltpu.VMEM((2, rows, m), bf16),
                pltpu.VMEM((2, rows, m), bf16),
                pltpu.VMEM((2, rows, kd), bf16),
                pltpu.VMEM((2, 2, kd, rows // 2), bf16),
                pltpu.VMEM((2, kd, rows), bf16),
                pltpu.VMEM((2, rows, rows), f32),
                pltpu.VMEM((2, rows, rows // 2), f32),
                pltpu.VMEM((2, rows, rows), f32),
                pltpu.VMEM((2, rows, rows // 2), f32),
                pltpu.VMEM((4, rows, rows), f32),
                pltpu.VMEM((2, rows, rows), f32),
                pltpu.VMEM((rows, rows), f32),
                pltpu.VMEM((2, rows, rows // 2), f32),
                pltpu.SemaphoreType.REGULAR,
                dma((1,)), dma((5,)), dma((4 * NS,)), dma((NS + 1,)), dma((NU + 1,)), dma((4,)), dma((2,)), dma((9,)),
            ],
            compiler_params=pltpu.CompilerParams(
                collective_id=0, has_side_effects=True, vmem_limit_bytes=56 * 1024 * 1024),
        )(a_local)

    part_spec = P(("batch", "row"), "col")
    return jax.shard_map(local_fn, mesh=mesh, in_specs=(part_spec,), out_specs=part_spec, check_vma=False)
```

```python
import jax
import jax.numpy as jnp
from jax import lax
from jax.experimental import pallas as pl
from jax.experimental.pallas import tpu as pltpu
from jax.sharding import PartitionSpec as P

MESH = pl.DeviceIdType.MESH
PW = 256
NU = 15
XU = 128
NS = 8


def mm(a, b):
    return lax.dot_general(a, b, (((1,), (1,)), ((), ())), preferred_element_type=jnp.float32)


def mn(a, b):
    return lax.dot_general(a, b, (((1,), (0,)), ((), ())), preferred_element_type=jnp.float32)


def kernel(a_ref, o_ref, X, Y, W, T0, T1, Pa, Pb, Qa, QD, R, PR, XA, XB, far, ld, s_z, r_y, r_d, r_w, r_p, r_r, r_x):
    rows, m = a_ref.shape
    ku = NU * PW + XU
    kd = m - ku
    nd, xd = kd // PW, kd % PW
    half = rows // 2
    st = half // NS
    us = rows // NS
    z = lax.axis_index("row")
    c = lax.axis_index("col")
    y = c // 2
    k = c % 2
    sib = 2 * y + 1 - k

    def rcopy(src, dst, ss, rs, row, col):
        return pltpu.make_async_remote_copy(
            src_ref=src, dst_ref=dst, send_sem=ss, recv_sem=rs, device_id={"row": row, "col": col}, device_id_type=MESH)

    def wait_recv(ref, sem):
        pltpu.make_async_copy(ref, ref, sem).wait()

    def up(p, w=PW):
        return pl.ds(pl.multiple_of(p * PW, 128), w)

    def dn(p, w=PW):
        return pl.ds(pl.multiple_of(ku + p * PW, 128), w)

    def rs_(h, s, n=1):
        return pl.ds(pl.multiple_of(h * half + s * st, st), n * st)

    def us_(s):
        return pl.ds(pl.multiple_of(s * us, us), us)

    DALL = pl.ds(ku, kd)
    UALL = pl.ds(0, ku)
    C0, C1 = pl.ds(0, half), pl.ds(half, half)
    COLS = (C0, C1)

    def each(lo, hi, fn):
        lax.fori_loop(lo, hi, lambda i, u: (fn(i), u)[1], 0)

    load = pltpu.make_async_copy(a_ref, X.at[k], ld.at[0])
    load.start()

    def near(sem):
        for dz in (-1, 1):
            @pl.when((z + dz >= 0) & (z + dz <= 3))
            def _():
                for kk in range(2):
                    pl.semaphore_signal(sem, inc=1, device_id={"row": z + dz, "col": 2 * y + kk}, device_id_type=MESH)
        for dc in range(1, 4):
            pl.semaphore_signal(sem, inc=1, device_id={"row": z, "col": (c + dc) % 4}, device_id_type=MESH)

    n_near = jnp.where((z == 0) | (z == 3), 5, 7)
    bar = pltpu.get_barrier_semaphore()
    near(bar)
    pl.semaphore_wait(bar, n_near)

    def z0_u(q, w=PW):
        return rcopy(a_ref.at[:, up(q, w)], Y.at[k, :, up(q, w)], s_z.at[0], r_y.at[q], 1, c)

    def z0_d(t):
        r = rs_(0, t)
        return rcopy(a_ref.at[r, DALL], Y.at[k, r, DALL], s_z.at[0], r_y.at[2 * NS + t], 1, c)

    def z3_d(t):
        r = rs_(t % 2, t // 2)
        return rcopy(a_ref.at[r, DALL], Y.at[k, r, DALL], s_z.at[0], r_y.at[t], 2, c)

    def z3_u(s):
        r = us_(s)
        return rcopy(a_ref.at[r, UALL], Y.at[k, r, UALL], s_z.at[0], r_y.at[2 * NS + s], 2, c)

    def z1_u(q, w=PW):
        return rcopy(a_ref.at[:, up(q, w)], W.at[k, :, up(q, w)], s_z.at[0], r_w.at[q], 2, 2 * y + 1)

    def z2_d(t):
        h, s = t % 2, t // 2
        return rcopy(a_ref.at[rs_(h, s), DALL], W.at[k, rs_(1, s), pl.ds(0, kd)], s_z.at[0], r_w.at[jnp.where(s < 6, 1 + s // 2, s - 2)], 1, 2 * y + h)

    @pl.when(z == 0)
    def _():
        each(0, NU, lambda q: z0_u(q).start())
        z0_u(NU, XU).start()
        each(0, 2 * NS, lambda t: z0_d(t).start())

    @pl.when(z == 3)
    def _():
        each(0, 2 * NS, lambda t: z3_d(t).start())
        each(0, NS, lambda s: z3_u(s).start())

    x_d = rcopy(a_ref.at[:, DALL], X.at[k, :, DALL], s_z.at[1], r_d.at[NS], z, sib)
    x_u = rcopy(a_ref.at[:, UALL], X.at[k, :, UALL], s_z.at[1], r_d.at[NS], z, sib)

    @pl.when(z == 1)
    def _():
        each(0, NU, lambda q: z1_u(q).start())
        z1_u(NU, XU).start()
        x_d.start()

    @pl.when(z == 2)
    def _():
        z2_d(0).start()
        z2_d(1).start()
        x_u.start()

    near(far)

    Pa[...] = jnp.zeros_like(Pa)
    Qa[...] = jnp.zeros_like(Qa)
    load.wait()
    dq = jnp.where(z == 1, 1, 0)

    def diag(p):
        cs = pl.ds(pl.multiple_of(p * 512, 512), 512)
        Qa[dq] += mm(X[k, :, cs], X[k, :, cs])

    each(0, m // 512, diag)

    def slot(owner):
        return (c - owner + 3) % 4

    dsend = rcopy(Qa.at[dq], R.at[slot(z)], s_z.at[3], r_r.at[0], z, z)

    @pl.when(c != z)
    def _():
        dsend.start()

    def u_fwd(q, w=PW):
        return rcopy(Y.at[k, :, up(q, w)], W.at[k, :, up(q, w)], s_z.at[0], r_w.at[q], 2, 2 * y)

    def zU(q, w=PW):
        wait_recv(Y.at[k, :, up(q, w)], r_y.at[q])
        Qa[0] += mm(X[k, :, up(q, w)], Y[k, :, up(q, w)])

    def turn(p, w=PW):
        for h in range(2):
            T1[h, up(p, w), :] = X[h, :, dn(p, w)].T

    def d_sib(t):
        return rcopy(Y.at[k, rs_(0, t), DALL], Y.at[k, rs_(0, t), DALL], s_z.at[1], r_d.at[t // NS], z, sib)

    def zD(t):
        wait_recv(Y.at[k, rs_(0, t), DALL], r_y.at[2 * NS + t])
        d_sib(t).start()

    def brows(b):
        return pl.ds(pl.multiple_of(b * half, half), half)

    def wait_w(r, n):
        wait_recv(W.at[:, r, pl.ds(0, kd)], r_w.at[n])

    CA = pl.ds(0, rows)
    peer = (c + 2) % 4

    def r3(u):
        return rs_(0, 4 * u, 4)

    def r2(s, n=2):
        return rs_(1, s, n)

    def xsend(src, dst, n):
        return rcopy(src, dst, s_z.at[2], r_x.at[n], 1, peer)

    x31 = xsend(Pa.at[1, rs_(0, 0, NS)], XA.at[rs_(0, 0, NS)], 0)

    def x30(b, u):
        return xsend(Pb.at[b, r3(u)], XB.at[b, r3(u)], 1 + 2 * b + u)

    def x21(s, n, rs):
        return xsend(Pa.at[1, r2(s, n)], XA.at[r2(s, n)], rs)

    def x20(b, s, n, rs):
        return xsend(Pb.at[b, r2(s, n)], XB.at[b, r2(s, n)], rs)

    def msend(src, i, s, n, j, cols, rs):
        return rcopy(src, PR.at[i, rs_(k, s, n), cols], s_z.at[2], r_p.at[rs], 2, j)

    m31 = msend(Pa.at[1, rs_(0, 0, NS)], 1, 0, NS, 1, CA, 0)

    def m30(b, u):
        src = Pb.at[b, r3(u)]
        if b == 0:
            return msend(src, 1, 4 * u, 4, 0, C0, 0)
        return rcopy(src, R.at[2 + y, rs_(k, 4 * u, 4), C1], s_z.at[2], r_r.at[1], 3, 0)

    def m21(s, n, rs):
        return msend(Pa.at[1, r2(s, n)], 0, s, n, 1, CA, rs)

    def m20(b, s, n, rs):
        return msend(Pb.at[b, r2(s, n)], 0, s, n, 0, COLS[b], rs)

    def d2(src, j, cols):
        return rcopy(src, R.at[1, rs_(k, 7), cols], s_z.at[2], r_r.at[1], 2, j)

    d21 = d2(Pa.at[1, r2(7, 1)], 1, CA)
    d20 = [d2(Pb.at[b, r2(7, 1)], 0, COLS[b]) for b in range(2)]

    def part1(r):
        Pa[1, r, :] = mn(W[0, r, :kd], T1[0]) + mn(W[1, r, :kd], T1[1])

    def part0(r, b):
        Pb[b, r, :] = mn(W[0, r, :kd], T0[0, b]) + mn(W[1, r, :kd], T0[1, b])

    q_u = rcopy(Qa.at[0], R.at[slot(0)], s_z.at[4], r_r.at[0], 1, 0)

    def q_d(b):
        return rcopy(QD.at[b], PR.at[y, rs_(k, 0, NS), COLS[b]], s_z.at[4], r_r.at[1], 1, 0)

    @pl.when(z == 1)
    def _():
        wait_recv(X.at[1 - k, :, DALL], r_d.at[NS])

        def step_u(q):
            zU(q)

            @pl.when(q < 5)
            def _():
                u_fwd(q).start()

            turn(q)

        each(0, NU, step_u)
        zU(NU, XU)
        each(NU, nd, turn)
        if xd:
            turn(nd, xd)

        @pl.when(c != 0)
        def _():
            q_u.start()

        pl.semaphore_wait(far, n_near)

        def step(i):
            @pl.when(i < 2 * NS)
            def _():
                zD(i)

            @pl.when(i == 3)
            def _():
                wait_w(rs_(0, 0, NS), 0)
                part1(rs_(0, 0, NS))

                @pl.when(y == 1)
                def _():
                    x31.start()

                each(5, 10, lambda q: u_fwd(q).start())

            @pl.when((i == 5) & (y == 0))
            def _():
                wait_recv(XA.at[rs_(0, 0, NS)], r_x.at[0])
                Pa[1, rs_(0, 0, NS), :] += XA[rs_(0, 0, NS), :]
                m31.start()

            @pl.when((i == 7) | (i == 16))
            def _():
                b = jnp.where(i == 7, 0, 1)
                wait_recv(Y.at[1 - k, brows(b), DALL], r_d.at[b])
                for h in range(2):
                    T0[h, b] = Y[h, brows(b), DALL].T
                part0(rs_(0, 0, NS), b)
                @pl.when((b == 0) & (y == 1))
                def _():
                    for u in range(2):
                        x30(0, u).start()

                @pl.when(b == 1)
                def _():
                    for u in range(2):
                        m30(1, u).start()

            @pl.when((i == 7) | (i == 20))
            def _():
                b = jnp.where(i == 7, 0, 1)
                r = rs_(k, 0, NS)
                QD[b] = mn(X[0, r, DALL], T0[0, b]) + mn(X[1, r, DALL], T0[1, b])
                for bb in range(2):
                    @pl.when((b == bb) & (c != 0))
                    def _():
                        q_d(bb).start()

            @pl.when(i == 7)
            def _():
                each(10, NU, lambda q: u_fwd(q).start())
                u_fwd(NU, XU).start()

            @pl.when((i == 9) & (y == 0))
            def _():
                for u in range(2):
                    wait_recv(XB.at[0, r3(u)], r_x.at[1 + u])
                    Pb[0, r3(u), :] += XB[0, r3(u), :]
                    m30(0, u).start()

            @pl.when((i == 8) | (i == 9) | (i == 13))
            def _():
                g = jnp.where(i == 13, 2, i - 8)
                wait_w(r2(2 * g), 1 + g)
                part1(r2(2 * g))
                part0(r2(2 * g), 0)

                @pl.when(y == 1)
                def _():
                    x21(2 * g, 2, 5 + g).start()
                    x20(0, 2 * g, 2, 5 + g).start()

            @pl.when(((i == 10) | (i == 11) | (i == 15)) & (y == 0))
            def _():
                g = jnp.where(i == 15, 2, i - 10)
                wait_recv(XA.at[pl.ds(0, 48)], r_x.at[5 + g])
                Pa[1, r2(2 * g), :] += XA[r2(2 * g), :]
                Pb[0, r2(2 * g), :] += XB[0, r2(2 * g), :]
                m21(2 * g, 2, 1).start()
                m20(0, 2 * g, 2, 1).start()

            @pl.when((i >= 17) & (i < 20))
            def _():
                g = i - 17
                part0(r2(2 * g), 1)

                @pl.when(y == 1)
                def _():
                    x20(1, 2 * g, 2, 8).start()

            @pl.when((i == 14) | (i == 21))
            def _():
                t = jnp.where(i == 14, 6, 7)
                wait_w(r2(t, 1), t - 2)
                part1(r2(t, 1))
                part0(r2(t, 1), 0)

                @pl.when((y == 1) & (i == 14))
                def _():
                    x21(6, 1, 8).start()
                    x20(0, 6, 1, 8).start()

            @pl.when(i >= 20)
            def _():
                part0(r2(i - 14, 1), 1)

                @pl.when((y == 1) & (i == 20))
                def _():
                    x20(1, 6, 1, 8).start()

        each(0, 22, step)

        @pl.when(y == 1)
        def _():
            d21.start()
            for x in d20:
                x.start()

        @pl.when(y == 0)
        def _():
            m21(7, 1, 2).start()
            m20(0, 7, 1, 3).start()
            m20(1, 7, 1, 3).start()
            wait_recv(XA.at[pl.ds(0, 80)], r_x.at[8])
            Pb[1, r2(0, 7), :] += XB[1, r2(0, 7), :]
            m20(1, 0, 7, 2).start()
            Pa[1, r2(6, 1), :] += XA[r2(6, 1), :]
            m21(6, 1, 2).start()
            Pb[0, r2(6, 1), :] += XB[0, r2(6, 1), :]
            m20(0, 6, 1, 3).start()

    def d_fwd(t):
        h, s = t % 2, t // 2
        return rcopy(Y.at[k, rs_(h, s), DALL], W.at[k, rs_(0, s), pl.ds(0, kd)], s_z.at[0], r_w.at[0], 1, 2 * y + h)

    def u_sib(s):
        return rcopy(Y.at[k, us_(s), UALL], Y.at[k, us_(s), UALL], s_z.at[1], r_d.at[s], z, sib)

    def q1send(s):
        return rcopy(Qa.at[1, us_(s)], R.at[c, us_(s)], s_z.at[4], r_r.at[0], 3, 2)

    def y2(q, w=PW):
        wait_recv(W.at[:, :, up(q, w)], r_w.at[q])
        Pa[0] += mm(X[0, :, up(q, w)], W[0, :, up(q, w)]) + mm(X[1, :, up(q, w)], W[1, :, up(q, w)])

    def y3(b, q, w=PW):
        r = pl.ds(b * half, half)
        Pa[1, r, :] += mm(Y[0, r, up(q, w)], W[0, :, up(q, w)]) + mm(Y[1, r, up(q, w)], W[1, :, up(q, w)])

    def wait_ysib(s):
        wait_recv(Y.at[1 - k, us_(s), UALL], r_d.at[s])

    def s3(r):
        return rcopy(Pa.at[1, r], R.at[y, r], s_z.at[2], r_r.at[0], 3, k)

    s2 = rcopy(Pa.at[0], R.at[0], s_z.at[2], r_r.at[0], 2, k)

    def add(i, r, cols):
        Pa[i, r, cols] += PR[i, r, cols]

    def wait_pr(n, cols, sem):
        wait_recv(PR.at[0, pl.ds(0, n), cols], r_p.at[sem])

    def strip31(s):
        wait_ysib(s)
        r = us_(s)
        Pa[1, r, :] = mm(Y[0, r, UALL], W[0, :, :ku]) + mm(Y[1, r, UALL], W[1, :, :ku])

        @pl.when(y == 0)
        def _():
            add(1, r, CA)

        s3(r).start()

    @pl.when(z == 2)
    def _():
        def step_d(t):
            wait_recv(Y.at[k, rs_(t % 2, t // 2), DALL], r_y.at[t])
            d_fwd(t).start()

            @pl.when(t == 1)
            def _():
                wait_recv(X.at[1 - k, :, UALL], r_d.at[NS])

            @pl.when((k == 1) & (t >= 1))
            def _():
                y2(t - 1)

        each(0, 2 * NS, step_d)
        each(2, 2 * NS, lambda t: z2_d(t).start())

        pl.semaphore_wait(far, n_near)

        @pl.when(k == 1)
        def _():
            y2(NU, XU)

            @pl.when(y == 1)
            def _():
                s2.start()


        def q1(s):
            Qa[1, us_(s), :] = mm(Y[k, us_(s), :], X[k])
            q1send(s).start()

        def step_u(s):
            wait_recv(Y.at[k, us_(s), UALL], r_y.at[2 * NS + s])
            u_sib(s).start()

            @pl.when((k == 0) & (s >= 1))
            def _():
                y2(2 * s - 1)

            @pl.when(k == 0)
            def _():
                y2(2 * s)

            @pl.when((k == 0) & (s == 4))
            def _():
                each(0, 4, wait_ysib)
                each(0, 7, lambda q: y3(0, q))

            @pl.when((k == 0) & (s >= 4))
            def _():
                y3(0, 2 * s - 1)
                y3(0, 2 * s)

            @pl.when((k == 1) & (y == 0) & (s == 4))
            def _():
                wait_recv(PR.at[1], r_p.at[0])

            @pl.when((k == 1) & (s >= 4) & (s <= 6))
            def _():
                each(2 * s - 8, 2 * s - 6, strip31)

            @pl.when((k == 1) | (s < NS - 1))
            def _():
                q1(s)

        each(0, NS, step_u)

        @pl.when(k == 1)
        def _():
            each(NS - 2, NS, strip31)

            @pl.when(y == 0)
            def _():
                wait_pr(192, CA, 1)
                for h in range(2):
                    add(0, rs_(h, 0, 6), CA)
                wait_pr(64, CA, 2)
                for h in range(2):
                    add(0, rs_(h, 6, 2), CA)

        @pl.when(k == 0)
        def _():
            y2(NU, XU)

            @pl.when(y == 1)
            def _():
                s2.start()

            y3(0, NU, XU)

            @pl.when(y == 0)
            def _():
                wait_pr(rows, C0, 0)
                add(1, pl.ds(0, half), C0)

            s3(pl.ds(0, half)).start()
            each(NS - 1, NS + k, q1)
            each(4, NS, wait_ysib)

            def low(b):
                r = pl.ds(pl.multiple_of(b * half, half), half)
                Pa[1, r, :] = mm(Y[0, r, UALL], W[0, :, :ku]) + mm(Y[1, r, UALL], W[1, :, :ku])

            each(1 + k, 2, low)

            @pl.when(y == 0)
            def _():
                add(1, pl.ds(half, half), C0)

            s3(pl.ds(half, half)).start()

            @pl.when(y == 0)
            def _():
                wait_pr(192, C0, 1)
                for h in range(2):
                    add(0, rs_(h, 0, 6), C0)
                wait_pr(224, C1, 2)
                for h in range(2):
                    add(0, rs_(h, 0, 7), C1)
                wait_pr(96, C0, 3)
                for h in range(2):
                    add(0, rs_(h, 6, 2), C0)
                    add(0, rs_(h, 7), C1)

    @pl.when((z == 0) | (z == 3))
    def _():
        pl.semaphore_wait(far, n_near)

    @pl.when(c > z)
    def _():
        o_ref[...] = jnp.zeros_like(o_ref)

    @pl.when(c == z)
    def _():
        wait_recv(R.at[pl.ds(0, 3)], r_r.at[0])
        total = Qa[dq] + R[0] + R[1] + R[2]
        diff = lax.broadcasted_iota(jnp.int32, (rows, rows), 0) - lax.broadcasted_iota(jnp.int32, (rows, rows), 1)
        o_ref[...] = jnp.where(diff >= 0, total, 0.0).astype(o_ref.dtype)

    @pl.when((z == 1) & (c == 0))
    def _():
        wait_recv(R.at[pl.ds(0, 3)], r_r.at[0])
        Qa[0] += R[0] + R[1] + R[2]
        wait_recv(R.at[pl.ds(0, 3), pl.ds(0, half)], r_r.at[1])
        for b in range(2):
            PR[0, pl.ds(0, half), COLS[b]] = QD[b]
        o_ref[...] = (Qa[0] + PR[0] + PR[1]).astype(o_ref.dtype)

    @pl.when((z == 2) & (y == 0))
    def _():
        wait_recv(R.at[0], r_r.at[0])
        wait_recv(R.at[1, pl.ds(0, 32)], r_r.at[1])
        for h in range(2):
            Pa[0, rs_(h, 7), :] += R[1, rs_(h, 7), :]
        o_ref[...] = (Pa[0] + R[0]).astype(o_ref.dtype)

    @pl.when((z == 3) & (c == 2))
    def _():
        wait_recv(R, r_r.at[0])
        o_ref[...] = (R[0] + R[1] + R[2] + R[3]).astype(o_ref.dtype)

    @pl.when((z == 3) & (y == 0))
    def _():
        wait_recv(R.at[pl.ds(0, 2)], r_r.at[0])

        @pl.when(k == 0)
        def _():
            wait_recv(R.at[2], r_r.at[1])
            R[0, :, C1] += R[2, :, C1] + R[3, :, C1]

        o_ref[...] = (R[0] + R[1]).astype(o_ref.dtype)

    @pl.when(c != z)
    def _():
        wait_recv(Qa.at[0], s_z.at[3])

    @pl.when((z == 0) | (z == 3))
    def _():
        wait_recv(X.at[k], s_z.at[0])

    @pl.when(z == 1)
    def _():
        wait_recv(W.at[:, :, pl.ds(0, ku)], s_z.at[0])
        wait_recv(W.at[:, :, pl.ds(0, kd)], s_z.at[1])
        wait_recv(Pa, s_z.at[2])

        @pl.when(c != 0)
        def _():
            wait_recv(R.at[pl.ds(0, 3), pl.ds(0, half)], s_z.at[4])

    @pl.when(z == 2)
    def _():
        wait_recv(W.at[:, :, pl.ds(0, kd)], s_z.at[0])
        wait_recv(W.at[:, :, pl.ds(0, ku)], s_z.at[1])
        wait_recv(Qa.at[1], s_z.at[4])

        @pl.when(y == 0)
        def _():
            wait_recv(Pa.at[0], s_z.at[2])

        @pl.when(y == 1)
        def _():
            wait_recv(Pa, s_z.at[2])


def solution(mesh):
    def local_fn(a_local):
        rows, m = a_local.shape
        kd = m - NU * PW - XU
        f32, bf16 = jnp.float32, jnp.bfloat16
        dma = pltpu.SemaphoreType.DMA
        return pl.pallas_call(
            kernel,
            out_shape=pltpu.VMEM((rows, rows), bf16),
            in_specs=[pl.BlockSpec(memory_space=pl.ANY)],
            out_specs=pl.BlockSpec(memory_space=pltpu.VMEM),
            scratch_shapes=[
                pltpu.VMEM((2, rows, m), bf16),
                pltpu.VMEM((2, rows, m), bf16),
                pltpu.VMEM((2, rows, kd), bf16),
                pltpu.VMEM((2, 2, kd, rows // 2), bf16),
                pltpu.VMEM((2, kd, rows), bf16),
                pltpu.VMEM((2, rows, rows), f32),
                pltpu.VMEM((2, rows, rows // 2), f32),
                pltpu.VMEM((2, rows, rows), f32),
                pltpu.VMEM((2, rows // 2, rows // 2), f32),
                pltpu.VMEM((4, rows, rows), f32),
                pltpu.VMEM((2, rows, rows), f32),
                pltpu.VMEM((rows, rows), f32),
                pltpu.VMEM((2, rows, rows // 2), f32),
                pltpu.SemaphoreType.REGULAR,
                dma((1,)), dma((5,)), dma((4 * NS,)), dma((NS + 1,)), dma((NU + 1,)), dma((4,)), dma((2,)), dma((9,)),
            ],
            compiler_params=pltpu.CompilerParams(
                collective_id=0, has_side_effects=True, vmem_limit_bytes=56 * 1024 * 1024),
        )(a_local)

    part_spec = P(("batch", "row"), "col")
    return jax.shard_map(local_fn, mesh=mesh, in_specs=(part_spec,), out_specs=part_spec, check_vma=False)
```

```python
import jax
import jax.numpy as jnp
from jax import lax
from jax.experimental import pallas as pl
from jax.experimental.pallas import tpu as pltpu
from jax.sharding import PartitionSpec as P

MESH = pl.DeviceIdType.MESH
PW = 256
NU = 15
XU = 128
NS = 8


def mm(a, b):
    return lax.dot_general(a, b, (((1,), (1,)), ((), ())), preferred_element_type=jnp.float32)


def mn(a, b):
    return lax.dot_general(a, b, (((1,), (0,)), ((), ())), preferred_element_type=jnp.float32)


def kernel(a_ref, o_ref, X, Y, W, T0, T1, Pa, Pb, Qa, QD, R, PR, XA, XB, far, ld, s_z, r_y, r_d, r_w, r_p, r_r, r_x):
    rows, m = a_ref.shape
    ku = NU * PW + XU
    kd = m - ku
    nd, xd = kd // PW, kd % PW
    half = rows // 2
    st = half // NS
    us = rows // NS
    z = lax.axis_index("row")
    c = lax.axis_index("col")
    y = c // 2
    k = c % 2
    sib = 2 * y + 1 - k

    def rcopy(src, dst, ss, rs, row, col):
        return pltpu.make_async_remote_copy(
            src_ref=src, dst_ref=dst, send_sem=ss, recv_sem=rs, device_id={"row": row, "col": col}, device_id_type=MESH)

    def wait_recv(ref, sem):
        pltpu.make_async_copy(ref, ref, sem).wait()

    def up(p, w=PW):
        return pl.ds(pl.multiple_of(p * PW, 128), w)

    def dn(p, w=PW):
        return pl.ds(pl.multiple_of(ku + p * PW, 128), w)

    def rs_(h, s, n=1):
        return pl.ds(pl.multiple_of(h * half + s * st, st), n * st)

    def us_(s):
        return pl.ds(pl.multiple_of(s * us, us), us)

    DALL = pl.ds(ku, kd)
    UALL = pl.ds(0, ku)
    C0, C1 = pl.ds(0, half), pl.ds(half, half)
    COLS = (C0, C1)

    def each(lo, hi, fn):
        lax.fori_loop(lo, hi, lambda i, u: (fn(i), u)[1], 0)

    load = pltpu.make_async_copy(a_ref, X.at[k], ld.at[0])
    load.start()

    def near(sem):
        for dz in (-1, 1):
            @pl.when((z + dz >= 0) & (z + dz <= 3))
            def _():
                for kk in range(2):
                    pl.semaphore_signal(sem, inc=1, device_id={"row": z + dz, "col": 2 * y + kk}, device_id_type=MESH)
        for dc in range(1, 4):
            pl.semaphore_signal(sem, inc=1, device_id={"row": z, "col": (c + dc) % 4}, device_id_type=MESH)

    n_near = jnp.where((z == 0) | (z == 3), 5, 7)
    bar = pltpu.get_barrier_semaphore()
    near(bar)
    pl.semaphore_wait(bar, n_near)

    def z0_u(q, w=PW):
        return rcopy(a_ref.at[:, up(q, w)], Y.at[k, :, up(q, w)], s_z.at[0], r_y.at[q], 1, c)

    def z0_d(t):
        r = rs_(0, t)
        return rcopy(a_ref.at[r, DALL], Y.at[k, r, DALL], s_z.at[0], r_y.at[2 * NS + t], 1, c)

    def z3_d(t):
        r = rs_(t % 2, t // 2)
        return rcopy(a_ref.at[r, DALL], Y.at[k, r, DALL], s_z.at[0], r_y.at[t], 2, c)

    def z3_u(s):
        r = us_(s)
        return rcopy(a_ref.at[r, UALL], Y.at[k, r, UALL], s_z.at[0], r_y.at[2 * NS + s], 2, c)

    def z1_u(q, w=PW):
        return rcopy(a_ref.at[:, up(q, w)], W.at[k, :, up(q, w)], s_z.at[0], r_w.at[q], 2, 2 * y + 1)

    def z2_d(t):
        h, s = t % 2, t // 2
        return rcopy(a_ref.at[rs_(h, s), DALL], W.at[k, rs_(1, s), pl.ds(0, kd)], s_z.at[0], r_w.at[jnp.where(s < 6, 1 + s // 2, s - 2)], 1, 2 * y + h)

    @pl.when(z == 0)
    def _():
        each(0, NU, lambda q: z0_u(q).start())
        z0_u(NU, XU).start()
        each(0, 2 * NS, lambda t: z0_d(t).start())

    @pl.when(z == 3)
    def _():
        each(0, 2 * NS, lambda t: z3_d(t).start())
        each(0, NS, lambda s: z3_u(s).start())

    x_d = rcopy(a_ref.at[:, DALL], X.at[k, :, DALL], s_z.at[1], r_d.at[NS], z, sib)
    x_u = rcopy(a_ref.at[:, UALL], X.at[k, :, UALL], s_z.at[1], r_d.at[NS], z, sib)

    @pl.when(z == 1)
    def _():
        each(0, NU, lambda q: z1_u(q).start())
        z1_u(NU, XU).start()
        x_d.start()

    @pl.when(z == 2)
    def _():
        z2_d(0).start()
        z2_d(1).start()
        x_u.start()

    near(far)

    Pa[...] = jnp.zeros_like(Pa)
    Qa[...] = jnp.zeros_like(Qa)
    Pb[...] = jnp.zeros_like(Pb)
    load.wait()
    dq = jnp.where(z == 1, 1, 0)

    def diag(p):
        cs = pl.ds(pl.multiple_of(p * 512, 512), 512)
        Qa[dq] += mm(X[k, :, cs], X[k, :, cs])

    each(0, m // 512, diag)

    def slot(owner):
        return (c - owner + 3) % 4

    dsend = rcopy(Qa.at[dq], R.at[slot(z)], s_z.at[3], r_r.at[0], z, z)

    @pl.when(c != z)
    def _():
        dsend.start()

    def u_fwd(q, w=PW):
        return rcopy(Y.at[k, :, up(q, w)], W.at[k, :, up(q, w)], s_z.at[0], r_w.at[q], 2, 2 * y)

    def zU(q, w=PW):
        wait_recv(Y.at[k, :, up(q, w)], r_y.at[q])
        Qa[0] += mm(X[k, :, up(q, w)], Y[k, :, up(q, w)])

    def turn(p, w=PW):
        for h in range(2):
            T1[h, up(p, w), :] = X[h, :, dn(p, w)].T

    def d_sib(t):
        return rcopy(Y.at[k, rs_(0, t), DALL], Y.at[k, rs_(0, t), DALL], s_z.at[1], r_d.at[t // NS], z, sib)

    def zD(t):
        wait_recv(Y.at[k, rs_(0, t), DALL], r_y.at[2 * NS + t])
        d_sib(t).start()

    def brows(b):
        return pl.ds(pl.multiple_of(b * half, half), half)

    def wait_w(r, n):
        wait_recv(W.at[:, r, pl.ds(0, kd)], r_w.at[n])

    CA = pl.ds(0, rows)
    peer = (c + 2) % 4

    def r3(u):
        return rs_(0, 4 * u, 4)

    def r2(s, n=2):
        return rs_(1, s, n)

    def xsend(src, dst, n):
        return rcopy(src, dst, s_z.at[2], r_x.at[n], 1, peer)

    x31 = xsend(Pa.at[1, rs_(0, 0, NS)], XA.at[rs_(0, 0, NS)], 0)

    def x30(b, u):
        return xsend(Pb.at[b, r3(u)], XB.at[b, r3(u)], 1 + 2 * b + u)

    def x21(s, n, rs):
        return xsend(Pa.at[1, r2(s, n)], XA.at[r2(s, n)], rs)

    def x20(b, s, n, rs):
        return xsend(Pb.at[b, r2(s, n)], XB.at[b, r2(s, n)], rs)

    def msend(src, i, s, n, j, cols, rs):
        return rcopy(src, PR.at[i, rs_(k, s, n), cols], s_z.at[2], r_p.at[rs], 2, j)

    m31 = msend(Pa.at[1, rs_(0, 0, NS)], 1, 0, NS, 1, CA, 0)

    def m30(b, u):
        src = Pb.at[b, r3(u)]
        if b == 0:
            return msend(src, 1, 4 * u, 4, 0, C0, 0)
        return rcopy(src, R.at[2, rs_(k, 4 * u, 4), C1], s_z.at[2], r_r.at[1], 3, 0)

    def m30r(u):
        return rcopy(Pb.at[1, r3(u)], PR.at[1, rs_(k, 4 * u, 4), C1], s_z.at[2], r_p.at[1 + u], 2, 2)

    def m21(s, n, rs):
        return msend(Pa.at[1, r2(s, n)], 0, s, n, 1, CA, rs)

    def m20(b, s, n, rs):
        return msend(Pb.at[b, r2(s, n)], 0, s, n, 0, COLS[b], rs)

    def d2(src, j, cols):
        return rcopy(src, R.at[1, rs_(k, 7), cols], s_z.at[2], r_r.at[1], 2, j)

    d21 = d2(Pa.at[1, r2(7, 1)], 1, CA)
    d20 = [d2(Pb.at[b, r2(7, 1)], 0, COLS[b]) for b in range(2)]

    def part1(r):
        Pa[1, r, :] = mn(W[0, r, :kd], T1[0]) + mn(W[1, r, :kd], T1[1])

    def part0(r, b):
        Pb[b, r, :] = mn(W[0, r, :kd], T0[0, b]) + mn(W[1, r, :kd], T0[1, b])

    q_u = rcopy(Qa.at[0], R.at[slot(0)], s_z.at[4], r_r.at[0], 1, 0)

    def q_d(b):
        return rcopy(QD.at[b], PR.at[y, rs_(k, 0, NS), COLS[b]], s_z.at[4], r_r.at[1], 1, 0)

    @pl.when(z == 1)
    def _():
        wait_recv(X.at[1 - k, :, DALL], r_d.at[NS])

        def step_u(q):
            zU(q)

            @pl.when(q < 5)
            def _():
                u_fwd(q).start()

            turn(q)

        each(0, NU, step_u)
        zU(NU, XU)
        each(NU, nd, turn)
        if xd:
            turn(nd, xd)

        @pl.when(c != 0)
        def _():
            q_u.start()

        pl.semaphore_wait(far, n_near)

        def step(i):
            @pl.when(i < 2 * NS)
            def _():
                zD(i)

            @pl.when(i == 3)
            def _():
                wait_w(rs_(0, 0, NS), 0)
                part1(rs_(0, 0, NS))

                @pl.when(y == 1)
                def _():
                    x31.start()

                each(5, 10, lambda q: u_fwd(q).start())

            @pl.when((i == 5) & (y == 0))
            def _():
                wait_recv(XA.at[rs_(0, 0, NS)], r_x.at[0])
                Pa[1, rs_(0, 0, NS), :] += XA[rs_(0, 0, NS), :]
                m31.start()

            @pl.when(i == 16)
            def _():
                def chunk(n):
                    ch = jnp.where(n == 0, k, 1 - k)

                    @pl.when(n == 1)
                    def _():
                        wait_recv(Y.at[1 - k, brows(1), DALL], r_d.at[1])

                    Pb[1, pl.ds(0, rows - st), :] += mm(W[ch, pl.ds(0, rows - st), :kd], Y[ch, brows(1), DALL])

                each(0, 2, chunk)

                @pl.when(y == 0)
                def _():
                    for u in range(2):
                        m30(1, u).start()

                @pl.when(y == 1)
                def _():
                    for u in range(2):
                        m30r(u).start()
                    x20(1, 0, 7, 8).start()

            @pl.when((i == 7) | (i == 17))
            def _():
                b = jnp.where(i == 7, 0, 1)

                @pl.when(b == 0)
                def _():
                    wait_recv(Y.at[1 - k, brows(0), DALL], r_d.at[0])

                for h in range(2):
                    T0[h, b] = Y[h, brows(b), DALL].T

                @pl.when(b == 0)
                def _():
                    part0(rs_(0, 0, NS), 0)

                    @pl.when(y == 1)
                    def _():
                        for u in range(2):
                            x30(0, u).start()

            @pl.when((i == 7) | (i == 17))
            def _():
                b = jnp.where(i == 7, 0, 1)
                r = rs_(k, 0, NS)
                QD[b] = mn(X[0, r, DALL], T0[0, b]) + mn(X[1, r, DALL], T0[1, b])
                for bb in range(2):
                    @pl.when((b == bb) & (c != 0))
                    def _():
                        q_d(bb).start()

            @pl.when(i == 7)
            def _():
                each(10, NU, lambda q: u_fwd(q).start())
                u_fwd(NU, XU).start()

            @pl.when((i == 9) & (y == 0))
            def _():
                for u in range(2):
                    wait_recv(XB.at[0, r3(u)], r_x.at[1 + u])
                    Pb[0, r3(u), :] += XB[0, r3(u), :]
                    m30(0, u).start()

            @pl.when((i == 8) | (i == 9) | (i == 13))
            def _():
                g = jnp.where(i == 13, 2, i - 8)
                wait_w(r2(2 * g), 1 + g)
                part1(r2(2 * g))
                part0(r2(2 * g), 0)

                @pl.when(y == 1)
                def _():
                    x21(2 * g, 2, 5 + g).start()
                    x20(0, 2 * g, 2, 5 + g).start()

            @pl.when(((i == 10) | (i == 11) | (i == 15)) & (y == 0))
            def _():
                g = jnp.where(i == 15, 2, i - 10)
                wait_recv(XA.at[pl.ds(0, 48)], r_x.at[5 + g])
                Pa[1, r2(2 * g), :] += XA[r2(2 * g), :]
                Pb[0, r2(2 * g), :] += XB[0, r2(2 * g), :]
                m21(2 * g, 2, 1).start()
                m20(0, 2 * g, 2, 1).start()

            @pl.when((i == 17) & (y == 0))
            def _():
                wait_recv(XA.at[pl.ds(0, 24)], r_x.at[3])
                Pa[1, r2(6, 1), :] += XA[r2(6, 1), :]
                m21(6, 1, 2).start()
                Pb[0, r2(6, 1), :] += XB[0, r2(6, 1), :]
                m20(0, 6, 1, 3).start()

            @pl.when((i == 14) | (i == 18))
            def _():
                t = jnp.where(i == 14, 6, 7)
                wait_w(r2(t, 1), t - 2)
                part1(r2(t, 1))
                part0(r2(t, 1), 0)

                @pl.when((y == 1) & (i == 14))
                def _():
                    x21(6, 1, 3).start()
                    x20(0, 6, 1, 3).start()

                @pl.when(i == 18)
                def _():
                    part0(r2(7, 1), 1)

        each(0, 19, step)

        @pl.when(y == 1)
        def _():
            d21.start()
            for x in d20:
                x.start()

        @pl.when(y == 0)
        def _():
            m21(7, 1, 2).start()
            m20(0, 7, 1, 3).start()
            m20(1, 7, 1, 3).start()
            wait_recv(XB.at[1, r2(0, 7)], r_x.at[8])
            Pb[1, r2(0, 7), :] += XB[1, r2(0, 7), :]
            m20(1, 0, 7, 2).start()

    def d_fwd(t):
        h, s = t % 2, t // 2
        return rcopy(Y.at[k, rs_(h, s), DALL], W.at[k, rs_(0, s), pl.ds(0, kd)], s_z.at[0], r_w.at[0], 1, 2 * y + h)

    def u_sib(s):
        return rcopy(Y.at[k, us_(s), UALL], Y.at[k, us_(s), UALL], s_z.at[1], r_d.at[s], z, sib)

    def q1send(s):
        return rcopy(Qa.at[1, us_(s)], R.at[c, us_(s)], s_z.at[4], r_r.at[0], 3, 2)

    def y2(q, w=PW):
        wait_recv(W.at[:, :, up(q, w)], r_w.at[q])
        Pa[0] += mm(X[0, :, up(q, w)], W[0, :, up(q, w)]) + mm(X[1, :, up(q, w)], W[1, :, up(q, w)])

    def y3(b, q, w=PW):
        r = pl.ds(b * half, half)
        Pa[1, r, :] += mm(Y[0, r, up(q, w)], W[0, :, up(q, w)]) + mm(Y[1, r, up(q, w)], W[1, :, up(q, w)])

    def wait_ysib(s):
        wait_recv(Y.at[1 - k, us_(s), UALL], r_d.at[s])

    def s3(r):
        return rcopy(Pa.at[1, r], R.at[y, r], s_z.at[2], r_r.at[0], 3, k)

    s2 = rcopy(Pa.at[0], R.at[0], s_z.at[2], r_r.at[0], 2, k)

    def relay(h, u):
        r = rs_(h, 4 * u, 4)
        return rcopy(PR.at[1, r, C1], R.at[3, r, C1], s_z.at[3], r_r.at[1], 3, 0)

    def add(i, r, cols):
        Pa[i, r, cols] += PR[i, r, cols]

    def wait_pr(n, cols, sem):
        wait_recv(PR.at[0, pl.ds(0, n), cols], r_p.at[sem])

    def strip31(s):
        wait_ysib(s)
        r = us_(s)
        Pa[1, r, :] = mm(Y[0, r, UALL], W[0, :, :ku]) + mm(Y[1, r, UALL], W[1, :, :ku])

        @pl.when(y == 0)
        def _():
            add(1, r, CA)

        s3(r).start()

    @pl.when(z == 2)
    def _():
        def step_d(t):
            wait_recv(Y.at[k, rs_(t % 2, t // 2), DALL], r_y.at[t])
            d_fwd(t).start()

            @pl.when(t == 1)
            def _():
                wait_recv(X.at[1 - k, :, UALL], r_d.at[NS])

            @pl.when((k == 1) & (t >= 1))
            def _():
                y2(t - 1)

        each(0, 2 * NS, step_d)
        each(2, 2 * NS, lambda t: z2_d(t).start())

        pl.semaphore_wait(far, n_near)

        @pl.when(k == 1)
        def _():
            y2(NU, XU)

            @pl.when(y == 1)
            def _():
                s2.start()


        def q1(s):
            Qa[1, us_(s), :] = mm(Y[k, us_(s), :], X[k])
            q1send(s).start()

        def step_u(s):
            wait_recv(Y.at[k, us_(s), UALL], r_y.at[2 * NS + s])
            u_sib(s).start()

            @pl.when((k == 0) & (s >= 1))
            def _():
                y2(2 * s - 1)

            @pl.when(k == 0)
            def _():
                y2(2 * s)

            @pl.when((k == 0) & (s == 4))
            def _():
                each(0, 4, wait_ysib)
                each(0, 7, lambda q: y3(0, q))

            @pl.when((k == 0) & (s >= 4))
            def _():
                y3(0, 2 * s - 1)
                y3(0, 2 * s)

            @pl.when((k == 1) & (y == 0) & (s == 4))
            def _():
                wait_recv(PR.at[1], r_p.at[0])

            @pl.when((k == 1) & (s >= 4) & (s <= 6))
            def _():
                each(2 * s - 8, 2 * s - 6, strip31)

            @pl.when((k == 1) | (s < NS - 1))
            def _():
                q1(s)

        each(0, NS, step_u)

        @pl.when(k == 1)
        def _():
            each(NS - 2, NS, strip31)

            @pl.when(y == 0)
            def _():
                wait_pr(192, CA, 1)
                for h in range(2):
                    add(0, rs_(h, 0, 6), CA)
                wait_pr(64, CA, 2)
                for h in range(2):
                    add(0, rs_(h, 6, 2), CA)

        @pl.when(k == 0)
        def _():
            y2(NU, XU)

            @pl.when(y == 1)
            def _():
                s2.start()

            y3(0, NU, XU)

            @pl.when(y == 0)
            def _():
                wait_pr(rows, C0, 0)
                add(1, pl.ds(0, half), C0)

            s3(pl.ds(0, half)).start()
            each(NS - 1, NS + k, q1)
            each(4, NS, wait_ysib)

            def low(b):
                r = pl.ds(pl.multiple_of(b * half, half), half)
                Pa[1, r, :] = mm(Y[0, r, UALL], W[0, :, :ku]) + mm(Y[1, r, UALL], W[1, :, :ku])

            each(1 + k, 2, low)

            @pl.when(y == 0)
            def _():
                add(1, pl.ds(half, half), C0)

            s3(pl.ds(half, half)).start()

            @pl.when(y == 1)
            def _():
                for u in range(2):
                    wait_pr(128, C1, 1 + u)
                    for h in range(2):
                        relay(h, u).start()

            @pl.when(y == 0)
            def _():
                wait_pr(192, C0, 1)
                for h in range(2):
                    add(0, rs_(h, 0, 6), C0)
                wait_pr(224, C1, 2)
                for h in range(2):
                    add(0, rs_(h, 0, 7), C1)
                wait_pr(96, C0, 3)
                for h in range(2):
                    add(0, rs_(h, 6, 2), C0)
                    add(0, rs_(h, 7), C1)

    @pl.when((z == 0) | (z == 3))
    def _():
        pl.semaphore_wait(far, n_near)

    @pl.when(c > z)
    def _():
        o_ref[...] = jnp.zeros_like(o_ref)

    @pl.when(c == z)
    def _():
        wait_recv(R.at[pl.ds(0, 3)], r_r.at[0])
        total = Qa[dq] + R[0] + R[1] + R[2]
        diff = lax.broadcasted_iota(jnp.int32, (rows, rows), 0) - lax.broadcasted_iota(jnp.int32, (rows, rows), 1)
        o_ref[...] = jnp.where(diff >= 0, total, 0.0).astype(o_ref.dtype)

    @pl.when((z == 1) & (c == 0))
    def _():
        wait_recv(R.at[pl.ds(0, 3)], r_r.at[0])
        Qa[0] += R[0] + R[1] + R[2]
        wait_recv(R.at[pl.ds(0, 3), pl.ds(0, half)], r_r.at[1])
        for b in range(2):
            PR[0, pl.ds(0, half), COLS[b]] = QD[b]
        o_ref[...] = (Qa[0] + PR[0] + PR[1]).astype(o_ref.dtype)

    @pl.when((z == 2) & (y == 0))
    def _():
        wait_recv(R.at[0], r_r.at[0])
        wait_recv(R.at[1, pl.ds(0, 32)], r_r.at[1])
        for h in range(2):
            Pa[0, rs_(h, 7), :] += R[1, rs_(h, 7), :]
        o_ref[...] = (Pa[0] + R[0]).astype(o_ref.dtype)

    @pl.when((z == 3) & (c == 2))
    def _():
        wait_recv(R, r_r.at[0])
        o_ref[...] = (R[0] + R[1] + R[2] + R[3]).astype(o_ref.dtype)

    @pl.when((z == 3) & (y == 0))
    def _():
        wait_recv(R.at[pl.ds(0, 2)], r_r.at[0])

        @pl.when(k == 0)
        def _():
            wait_recv(R.at[2], r_r.at[1])
            R[0, :, C1] += R[2, :, C1] + R[3, :, C1]

        o_ref[...] = (R[0] + R[1]).astype(o_ref.dtype)

    @pl.when(c != z)
    def _():
        wait_recv(Qa.at[0], s_z.at[3])

    @pl.when((z == 0) | (z == 3))
    def _():
        wait_recv(X.at[k], s_z.at[0])

    @pl.when(z == 1)
    def _():
        wait_recv(W.at[:, :, pl.ds(0, ku)], s_z.at[0])
        wait_recv(W.at[:, :, pl.ds(0, kd)], s_z.at[1])
        wait_recv(Pa, s_z.at[2])

        @pl.when(c != 0)
        def _():
            wait_recv(R.at[pl.ds(0, 3), pl.ds(0, half)], s_z.at[4])

    @pl.when(z == 2)
    def _():
        wait_recv(W.at[:, :, pl.ds(0, kd)], s_z.at[0])
        wait_recv(W.at[:, :, pl.ds(0, ku)], s_z.at[1])
        wait_recv(Qa.at[1], s_z.at[4])

        @pl.when(y == 0)
        def _():
            wait_recv(Pa.at[0], s_z.at[2])

        @pl.when(y == 1)
        def _():
            wait_recv(Pa, s_z.at[2])

            @pl.when(k == 0)
            def _():
                wait_recv(PR.at[1, :, C1], s_z.at[3])


def solution(mesh):
    def local_fn(a_local):
        rows, m = a_local.shape
        kd = m - NU * PW - XU
        f32, bf16 = jnp.float32, jnp.bfloat16
        dma = pltpu.SemaphoreType.DMA
        return pl.pallas_call(
            kernel,
            out_shape=pltpu.VMEM((rows, rows), bf16),
            in_specs=[pl.BlockSpec(memory_space=pl.ANY)],
            out_specs=pl.BlockSpec(memory_space=pltpu.VMEM),
            scratch_shapes=[
                pltpu.VMEM((2, rows, m), bf16),
                pltpu.VMEM((2, rows, m), bf16),
                pltpu.VMEM((2, rows, kd), bf16),
                pltpu.VMEM((2, 2, kd, rows // 2), bf16),
                pltpu.VMEM((2, kd, rows), bf16),
                pltpu.VMEM((2, rows, rows), f32),
                pltpu.VMEM((2, rows, rows // 2), f32),
                pltpu.VMEM((2, rows, rows), f32),
                pltpu.VMEM((2, rows // 2, rows // 2), f32),
                pltpu.VMEM((4, rows, rows), f32),
                pltpu.VMEM((2, rows, rows), f32),
                pltpu.VMEM((rows, rows), f32),
                pltpu.VMEM((2, rows, rows // 2), f32),
                pltpu.SemaphoreType.REGULAR,
                dma((1,)), dma((5,)), dma((4 * NS,)), dma((NS + 1,)), dma((NU + 1,)), dma((4,)), dma((2,)), dma((9,)),
            ],
            compiler_params=pltpu.CompilerParams(
                collective_id=0, has_side_effects=True, vmem_limit_bytes=56 * 1024 * 1024),
        )(a_local)

    part_spec = P(("batch", "row"), "col")
    return jax.shard_map(local_fn, mesh=mesh, in_specs=(part_spec,), out_specs=part_spec, check_vma=False)
```

```python
import jax
import jax.numpy as jnp
from jax import lax
from jax.experimental import pallas as pl
from jax.experimental.pallas import tpu as pltpu
from jax.sharding import PartitionSpec as P

MESH = pl.DeviceIdType.MESH
PW = 256
NU = 15
XU = 128
NS = 8


def mm(a, b):
    return lax.dot_general(a, b, (((1,), (1,)), ((), ())), preferred_element_type=jnp.float32)


def mn(a, b):
    return lax.dot_general(a, b, (((1,), (0,)), ((), ())), preferred_element_type=jnp.float32)


def kernel(a_ref, o_ref, X, Y, W, T0, T1, Pa, Pb, Qa, QD, R, PR, XA, XB, far, ld, s_z, r_y, r_d, r_w, r_p, r_r, r_x):
    rows, m = a_ref.shape
    ku = NU * PW + XU
    kd = m - ku
    nd, xd = kd // PW, kd % PW
    half = rows // 2
    st = half // NS
    us = rows // NS
    z = lax.axis_index("row")
    c = lax.axis_index("col")
    y = c // 2
    k = c % 2
    sib = 2 * y + 1 - k

    def rcopy(src, dst, ss, rs, row, col):
        return pltpu.make_async_remote_copy(
            src_ref=src, dst_ref=dst, send_sem=ss, recv_sem=rs, device_id={"row": row, "col": col}, device_id_type=MESH)

    def wait_recv(ref, sem):
        pltpu.make_async_copy(ref, ref, sem).wait()

    def up(p, w=PW):
        return pl.ds(pl.multiple_of(p * PW, 128), w)

    def dn(p, w=PW):
        return pl.ds(pl.multiple_of(ku + p * PW, 128), w)

    def rs_(h, s, n=1):
        return pl.ds(pl.multiple_of(h * half + s * st, st), n * st)

    def us_(s):
        return pl.ds(pl.multiple_of(s * us, us), us)

    DALL = pl.ds(ku, kd)
    UALL = pl.ds(0, ku)
    C0, C1 = pl.ds(0, half), pl.ds(half, half)
    COLS = (C0, C1)

    def each(lo, hi, fn):
        lax.fori_loop(lo, hi, lambda i, u: (fn(i), u)[1], 0)

    load = pltpu.make_async_copy(a_ref, X.at[k], ld.at[0])
    load.start()

    def near(sem):
        for dz in (-1, 1):
            @pl.when((z + dz >= 0) & (z + dz <= 3))
            def _():
                for kk in range(2):
                    pl.semaphore_signal(sem, inc=1, device_id={"row": z + dz, "col": 2 * y + kk}, device_id_type=MESH)
        for dc in range(1, 4):
            pl.semaphore_signal(sem, inc=1, device_id={"row": z, "col": (c + dc) % 4}, device_id_type=MESH)

    n_near = jnp.where((z == 0) | (z == 3), 5, 7)
    bar = pltpu.get_barrier_semaphore()
    near(bar)
    pl.semaphore_wait(bar, n_near)

    def z0_u(q, w=PW):
        return rcopy(a_ref.at[:, up(q, w)], Y.at[k, :, up(q, w)], s_z.at[0], r_y.at[q], 1, c)

    def z0_d(t):
        r = rs_(0, t)
        return rcopy(a_ref.at[r, DALL], Y.at[k, r, DALL], s_z.at[0], r_y.at[2 * NS + t], 1, c)

    def z3_d(t):
        r = rs_(t % 2, t // 2)
        return rcopy(a_ref.at[r, DALL], Y.at[k, r, DALL], s_z.at[0], r_y.at[t], 2, c)

    def z3_u(s):
        r = us_(s)
        return rcopy(a_ref.at[r, UALL], Y.at[k, r, UALL], s_z.at[0], r_y.at[2 * NS + s], 2, c)

    def z1_u(q, w=PW):
        return rcopy(a_ref.at[:, up(q, w)], W.at[k, :, up(q, w)], s_z.at[0], r_w.at[q], 2, 2 * y + 1)

    def z2_d(t):
        h, s = t % 2, t // 2
        return rcopy(a_ref.at[rs_(h, s), DALL], W.at[k, rs_(1, s), pl.ds(0, kd)], s_z.at[0], r_w.at[jnp.where(s < 6, 1 + s // 2, s - 2)], 1, 2 * y + h)

    @pl.when(z == 0)
    def _():
        each(0, NU, lambda q: z0_u(q).start())
        z0_u(NU, XU).start()
        each(0, 2 * NS, lambda t: z0_d(t).start())

    @pl.when(z == 3)
    def _():
        each(0, 2 * NS, lambda t: z3_d(t).start())
        each(0, NS, lambda s: z3_u(s).start())

    x_d = rcopy(a_ref.at[:, DALL], X.at[k, :, DALL], s_z.at[1], r_d.at[NS], z, sib)
    x_u = rcopy(a_ref.at[:, UALL], X.at[k, :, UALL], s_z.at[1], r_d.at[NS], z, sib)

    @pl.when(z == 1)
    def _():
        each(0, NU, lambda q: z1_u(q).start())
        z1_u(NU, XU).start()
        x_d.start()

    @pl.when(z == 2)
    def _():
        z2_d(0).start()
        z2_d(1).start()
        x_u.start()

    near(far)

    Pa[...] = jnp.zeros_like(Pa)
    Qa[...] = jnp.zeros_like(Qa)
    Pb[...] = jnp.zeros_like(Pb)
    load.wait()
    dq = jnp.where(z == 1, 1, 0)

    def diag(p):
        cs = pl.ds(pl.multiple_of(p * 512, 512), 512)
        Qa[dq] += mm(X[k, :, cs], X[k, :, cs])

    each(0, m // 512, diag)

    def slot(owner):
        return (c - owner + 3) % 4

    dsend = rcopy(Qa.at[dq], R.at[slot(z)], s_z.at[3], r_r.at[0], z, z)

    @pl.when(c != z)
    def _():
        dsend.start()

    def u_fwd(q, w=PW):
        return rcopy(Y.at[k, :, up(q, w)], W.at[k, :, up(q, w)], s_z.at[0], r_w.at[q], 2, 2 * y)

    def zU(q, w=PW):
        wait_recv(Y.at[k, :, up(q, w)], r_y.at[q])
        Qa[0] += mm(X[k, :, up(q, w)], Y[k, :, up(q, w)])

    def turn(p, w=PW):
        for h in range(2):
            T1[h, up(p, w), :] = X[h, :, dn(p, w)].T

    def d_sib(t):
        return rcopy(Y.at[k, rs_(0, t), DALL], Y.at[k, rs_(0, t), DALL], s_z.at[1], r_d.at[t // NS], z, sib)

    def zD(t):
        wait_recv(Y.at[k, rs_(0, t), DALL], r_y.at[2 * NS + t])
        d_sib(t).start()

    def brows(b):
        return pl.ds(pl.multiple_of(b * half, half), half)

    def wait_w(r, n):
        wait_recv(W.at[:, r, pl.ds(0, kd)], r_w.at[n])

    CA = pl.ds(0, rows)
    peer = (c + 2) % 4

    def r3(u):
        return rs_(0, 4 * u, 4)

    def r2(s, n=2):
        return rs_(1, s, n)

    def xsend(src, dst, n):
        return rcopy(src, dst, s_z.at[2], r_x.at[n], 1, peer)

    x31 = xsend(Pa.at[1, rs_(0, 0, NS)], XA.at[rs_(0, 0, NS)], 0)

    def x30(b, u):
        return xsend(Pb.at[b, r3(u)], XB.at[b, r3(u)], 1 + 2 * b + u)

    def x21(s, n, rs):
        return xsend(Pa.at[1, r2(s, n)], XA.at[r2(s, n)], rs)

    def x20(b, s, n, rs):
        return xsend(Pb.at[b, r2(s, n)], XB.at[b, r2(s, n)], rs)

    def msend(src, i, s, n, j, cols, rs):
        return rcopy(src, PR.at[i, rs_(k, s, n), cols], s_z.at[2], r_p.at[rs], 2, j)

    m31 = msend(Pa.at[1, rs_(0, 0, NS)], 1, 0, NS, 1, CA, 0)

    def m30(b, u):
        src = Pb.at[b, r3(u)]
        if b == 0:
            return msend(src, 1, 4 * u, 4, 0, C0, 0)
        return rcopy(src, R.at[2, rs_(k, 4 * u, 4), C1], s_z.at[2], r_r.at[1], 3, 0)

    def m30r(u):
        return rcopy(Pb.at[1, r3(u)], PR.at[1, rs_(k, 4 * u, 4), C1], s_z.at[2], r_p.at[1 + u], 2, 2)

    def m21(s, n, rs):
        return msend(Pa.at[1, r2(s, n)], 0, s, n, 1, CA, rs)

    def m20(b, s, n, rs):
        return msend(Pb.at[b, r2(s, n)], 0, s, n, 0, COLS[b], rs)

    def d2(src, j, cols):
        return rcopy(src, R.at[1, rs_(k, 7), cols], s_z.at[2], r_r.at[1], 2, j)

    d21 = d2(Pa.at[1, r2(7, 1)], 1, CA)
    d20 = [d2(Pb.at[b, r2(7, 1)], 0, COLS[b]) for b in range(2)]

    def part1(r):
        Pa[1, r, :] = mn(W[0, r, :kd], T1[0]) + mn(W[1, r, :kd], T1[1])

    def part0(r, b):
        Pb[b, r, :] = mn(W[0, r, :kd], T0[0, b]) + mn(W[1, r, :kd], T0[1, b])

    q_u = rcopy(Qa.at[0], R.at[slot(0)], s_z.at[4], r_r.at[0], 1, 0)

    def q_d(b):
        return rcopy(QD.at[b], PR.at[y, rs_(k, 0, NS), COLS[b]], s_z.at[4], r_r.at[1], 1, 0)

    @pl.when(z == 1)
    def _():
        wait_recv(X.at[1 - k, :, DALL], r_d.at[NS])

        def step_u(q):
            zU(q)

            @pl.when(q < 5)
            def _():
                u_fwd(q).start()

            turn(q)

        each(0, NU, step_u)
        zU(NU, XU)
        each(NU, nd, turn)
        if xd:
            turn(nd, xd)

        @pl.when(c != 0)
        def _():
            q_u.start()

        pl.semaphore_wait(far, n_near)

        def step(i):
            @pl.when(i < 2 * NS)
            def _():
                zD(i)

            @pl.when(i == 3)
            def _():
                wait_w(rs_(0, 0, NS), 0)
                part1(rs_(0, 0, NS))

                @pl.when(y == 1)
                def _():
                    x31.start()

                each(5, 10, lambda q: u_fwd(q).start())

            @pl.when((i == 5) & (y == 0))
            def _():
                wait_recv(XA.at[rs_(0, 0, NS)], r_x.at[0])
                Pa[1, rs_(0, 0, NS), :] += XA[rs_(0, 0, NS), :]
                m31.start()

            @pl.when(i == 16)
            def _():
                def chunk(n):
                    ch = jnp.where(n == 0, k, 1 - k)

                    @pl.when(n == 1)
                    def _():
                        wait_recv(Y.at[1 - k, brows(1), DALL], r_d.at[1])

                    Pb[1, pl.ds(0, rows - st), :] += mm(W[ch, pl.ds(0, rows - st), :kd], Y[ch, brows(1), DALL])

                each(0, 2, chunk)

                @pl.when(y == 0)
                def _():
                    for u in range(2):
                        m30(1, u).start()

                @pl.when(y == 1)
                def _():
                    for u in range(2):
                        m30r(u).start()
                    x20(1, 0, 7, 8).start()

            @pl.when((i == 7) | (i == 17))
            def _():
                b = jnp.where(i == 7, 0, 1)

                @pl.when(b == 0)
                def _():
                    wait_recv(Y.at[1 - k, brows(0), DALL], r_d.at[0])

                for h in range(2):
                    T0[h, b] = Y[h, brows(b), DALL].T

                @pl.when(b == 0)
                def _():
                    part0(rs_(0, 0, NS), 0)

                    @pl.when(y == 1)
                    def _():
                        for u in range(2):
                            x30(0, u).start()

            @pl.when((i == 7) | (i == 17))
            def _():
                b = jnp.where(i == 7, 0, 1)
                r = rs_(k, 0, NS)
                QD[b] = mn(X[0, r, DALL], T0[0, b]) + mn(X[1, r, DALL], T0[1, b])
                for bb in range(2):
                    @pl.when((b == bb) & (c != 0))
                    def _():
                        q_d(bb).start()

            @pl.when(i == 7)
            def _():
                each(10, NU, lambda q: u_fwd(q).start())
                u_fwd(NU, XU).start()

            @pl.when((i == 9) & (y == 0))
            def _():
                for u in range(2):
                    wait_recv(XB.at[0, r3(u)], r_x.at[1 + u])
                    Pb[0, r3(u), :] += XB[0, r3(u), :]
                    m30(0, u).start()

            @pl.when((i == 8) | (i == 9) | (i == 13))
            def _():
                g = jnp.where(i == 13, 2, i - 8)
                wait_w(r2(2 * g), 1 + g)
                part1(r2(2 * g))
                part0(r2(2 * g), 0)

                @pl.when(y == 1)
                def _():
                    x21(2 * g, 2, 5 + g).start()
                    x20(0, 2 * g, 2, 5 + g).start()

            @pl.when(((i == 10) | (i == 11) | (i == 15)) & (y == 0))
            def _():
                g = jnp.where(i == 15, 2, i - 10)
                wait_recv(XA.at[pl.ds(0, 48)], r_x.at[5 + g])
                Pa[1, r2(2 * g), :] += XA[r2(2 * g), :]
                Pb[0, r2(2 * g), :] += XB[0, r2(2 * g), :]
                m21(2 * g, 2, 1).start()
                m20(0, 2 * g, 2, 1).start()

            @pl.when((i == 17) & (y == 0))
            def _():
                wait_recv(XA.at[pl.ds(0, 24)], r_x.at[3])
                Pa[1, r2(6, 1), :] += XA[r2(6, 1), :]
                m21(6, 1, 2).start()
                Pb[0, r2(6, 1), :] += XB[0, r2(6, 1), :]
                m20(0, 6, 1, 3).start()

            @pl.when((i == 14) | (i == 18))
            def _():
                t = jnp.where(i == 14, 6, 7)
                wait_w(r2(t, 1), t - 2)
                part1(r2(t, 1))

                @pl.when((y == 1) & (i == 18))
                def _():
                    d21.start()

                @pl.when((y == 0) & (i == 18))
                def _():
                    m21(7, 1, 2).start()

                part0(r2(t, 1), 0)

                @pl.when((y == 1) & (i == 14))
                def _():
                    x21(6, 1, 3).start()
                    x20(0, 6, 1, 3).start()

                @pl.when((y == 1) & (i == 18))
                def _():
                    d20[0].start()

                @pl.when((y == 0) & (i == 18))
                def _():
                    m20(0, 7, 1, 3).start()
                    wait_recv(XB.at[1, r2(0, 7)], r_x.at[8])
                    Pb[1, r2(0, 7), :] += XB[1, r2(0, 7), :]
                    m20(1, 0, 7, 2).start()

                @pl.when(i == 18)
                def _():
                    part0(r2(7, 1), 1)

                    @pl.when(y == 1)
                    def _():
                        d20[1].start()

                    @pl.when(y == 0)
                    def _():
                        m20(1, 7, 1, 3).start()

        each(0, 19, step)

    def d_fwd(t):
        h, s = t % 2, t // 2
        return rcopy(Y.at[k, rs_(h, s), DALL], W.at[k, rs_(0, s), pl.ds(0, kd)], s_z.at[0], r_w.at[0], 1, 2 * y + h)

    def u_sib(s):
        return rcopy(Y.at[k, us_(s), UALL], Y.at[k, us_(s), UALL], s_z.at[1], r_d.at[s], z, sib)

    def q1send(s):
        return rcopy(Qa.at[1, us_(s)], R.at[c, us_(s)], s_z.at[4], r_r.at[0], 3, 2)

    def y2(q, w=PW):
        wait_recv(W.at[:, :, up(q, w)], r_w.at[q])
        Pa[0] += mm(X[0, :, up(q, w)], W[0, :, up(q, w)]) + mm(X[1, :, up(q, w)], W[1, :, up(q, w)])

    def y3(b, q, w=PW):
        r = pl.ds(b * half, half)
        Pa[1, r, :] += mm(Y[0, r, up(q, w)], W[0, :, up(q, w)]) + mm(Y[1, r, up(q, w)], W[1, :, up(q, w)])

    def wait_ysib(s):
        wait_recv(Y.at[1 - k, us_(s), UALL], r_d.at[s])

    def s3(r):
        return rcopy(Pa.at[1, r], R.at[y, r], s_z.at[2], r_r.at[0], 3, k)

    s2 = rcopy(Pa.at[0], R.at[0], s_z.at[2], r_r.at[0], 2, k)

    TOP = pl.ds(0, half)
    hop1 = rcopy(Pa.at[1, TOP], PR.at[0, TOP], s_z.at[2], r_p.at[0], 3, 2)
    hop2 = rcopy(PR.at[0, TOP], R.at[1, TOP], s_z.at[1], r_r.at[0], 3, 0)

    def relay(h, u):
        r = rs_(h, 4 * u, 4)
        return rcopy(PR.at[1, r, C1], R.at[3, r, C1], s_z.at[3], r_r.at[1], 3, 0)

    def add(i, r, cols):
        Pa[i, r, cols] += PR[i, r, cols]

    def wait_pr(n, cols, sem):
        wait_recv(PR.at[0, pl.ds(0, n), cols], r_p.at[sem])

    def strip31(s):
        wait_ysib(s)
        r = us_(s)
        Pa[1, r, :] = mm(Y[0, r, UALL], W[0, :, :ku]) + mm(Y[1, r, UALL], W[1, :, :ku])

        @pl.when(y == 0)
        def _():
            add(1, r, CA)

        s3(r).start()

    @pl.when(z == 2)
    def _():
        def step_d(t):
            wait_recv(Y.at[k, rs_(t % 2, t // 2), DALL], r_y.at[t])
            d_fwd(t).start()

            @pl.when(t == 1)
            def _():
                wait_recv(X.at[1 - k, :, UALL], r_d.at[NS])

            @pl.when((k == 1) & (t >= 1))
            def _():
                y2(t - 1)

        each(0, 2 * NS, step_d)
        each(2, 2 * NS, lambda t: z2_d(t).start())

        pl.semaphore_wait(far, n_near)

        @pl.when(k == 1)
        def _():
            y2(NU, XU)

            @pl.when(y == 1)
            def _():
                s2.start()


        def q1(s):
            Qa[1, us_(s), :] = mm(Y[k, us_(s), :], X[k])
            q1send(s).start()

        def step_u(s):
            wait_recv(Y.at[k, us_(s), UALL], r_y.at[2 * NS + s])
            u_sib(s).start()

            @pl.when((k == 0) & (s >= 1))
            def _():
                y2(2 * s - 1)

            @pl.when(k == 0)
            def _():
                y2(2 * s)

            @pl.when((k == 0) & (s == 4))
            def _():
                each(0, 4, wait_ysib)
                each(0, 7, lambda q: y3(0, q))

            @pl.when((k == 0) & (s >= 4))
            def _():
                y3(0, 2 * s - 1)
                y3(0, 2 * s)

            @pl.when((k == 1) & (y == 0) & (s == 4))
            def _():
                wait_recv(PR.at[1], r_p.at[0])

            @pl.when((k == 1) & (s >= 4) & (s <= 6))
            def _():
                each(2 * s - 8, 2 * s - 6, strip31)

            @pl.when((k == 1) | (s < NS - 1))
            def _():
                q1(s)

        each(0, NS, step_u)

        @pl.when(k == 1)
        def _():
            each(NS - 2, NS, strip31)

            @pl.when(y == 0)
            def _():
                wait_pr(192, CA, 1)
                for h in range(2):
                    add(0, rs_(h, 0, 6), CA)
                wait_pr(64, CA, 2)
                for h in range(2):
                    add(0, rs_(h, 6, 2), CA)

        @pl.when(k == 0)
        def _():
            y2(NU, XU)

            @pl.when(y == 1)
            def _():
                s2.start()

            y3(0, NU, XU)

            @pl.when(y == 0)
            def _():
                wait_pr(rows, C0, 0)
                add(1, pl.ds(0, half), C0)


            @pl.when(y == 0)
            def _():
                s3(pl.ds(0, half)).start()

            @pl.when(y == 1)
            def _():
                hop1.start()

            each(4, NS, wait_ysib)

            def low(b):
                r = pl.ds(pl.multiple_of(b * half, half), half)
                Pa[1, r, :] = mm(Y[0, r, UALL], W[0, :, :ku]) + mm(Y[1, r, UALL], W[1, :, :ku])

            each(1 + k, 2, low)

            @pl.when(y == 0)
            def _():
                add(1, pl.ds(half, half), C0)

            s3(pl.ds(half, half)).start()
            each(NS - 1, NS + k, q1)

            @pl.when(y == 1)
            def _():
                for u in range(2):
                    wait_pr(128, C1, 1 + u)
                    for h in range(2):
                        relay(h, u).start()

            @pl.when(y == 0)
            def _():
                wait_pr(192, C0, 1)
                for h in range(2):
                    add(0, rs_(h, 0, 6), C0)
                wait_pr(224, C1, 2)
                for h in range(2):
                    add(0, rs_(h, 0, 7), C1)
                wait_pr(96, C0, 3)
                for h in range(2):
                    add(0, rs_(h, 6, 2), C0)
                    add(0, rs_(h, 7), C1)

    @pl.when((z == 0) | (z == 3))
    def _():
        pl.semaphore_wait(far, n_near)

    @pl.when(c > z)
    def _():
        o_ref[...] = jnp.zeros_like(o_ref)

    @pl.when(c == z)
    def _():
        wait_recv(R.at[pl.ds(0, 3)], r_r.at[0])
        total = Qa[dq] + R[0] + R[1] + R[2]
        diff = lax.broadcasted_iota(jnp.int32, (rows, rows), 0) - lax.broadcasted_iota(jnp.int32, (rows, rows), 1)
        o_ref[...] = jnp.where(diff >= 0, total, 0.0).astype(o_ref.dtype)

    @pl.when((z == 1) & (c == 0))
    def _():
        wait_recv(R.at[pl.ds(0, 3)], r_r.at[0])
        Qa[0] += R[0] + R[1] + R[2]
        wait_recv(R.at[pl.ds(0, 3), pl.ds(0, half)], r_r.at[1])
        for b in range(2):
            PR[0, pl.ds(0, half), COLS[b]] = QD[b]
        o_ref[...] = (Qa[0] + PR[0] + PR[1]).astype(o_ref.dtype)

    @pl.when((z == 2) & (y == 0))
    def _():
        wait_recv(R.at[0], r_r.at[0])
        wait_recv(R.at[1, pl.ds(0, 32)], r_r.at[1])
        for h in range(2):
            Pa[0, rs_(h, 7), :] += R[1, rs_(h, 7), :]
        o_ref[...] = (Pa[0] + R[0]).astype(o_ref.dtype)

    @pl.when((z == 3) & (c == 2))
    def _():
        wait_recv(PR.at[0, TOP], r_p.at[0])
        hop2.start()
        wait_recv(R, r_r.at[0])
        o_ref[...] = (R[0] + R[1] + R[2] + R[3]).astype(o_ref.dtype)

    @pl.when((z == 3) & (y == 0))
    def _():
        wait_recv(R.at[pl.ds(0, 2)], r_r.at[0])

        @pl.when(k == 0)
        def _():
            wait_recv(R.at[2], r_r.at[1])
            R[0, :, C1] += R[2, :, C1] + R[3, :, C1]

        o_ref[...] = (R[0] + R[1]).astype(o_ref.dtype)

    @pl.when(c != z)
    def _():
        wait_recv(Qa.at[0], s_z.at[3])

    @pl.when((z == 0) | (z == 3))
    def _():
        wait_recv(X.at[k], s_z.at[0])

    @pl.when((z == 3) & (c == 2))
    def _():
        wait_recv(PR.at[0, TOP], s_z.at[1])

    @pl.when(z == 1)
    def _():
        wait_recv(W.at[:, :, pl.ds(0, ku)], s_z.at[0])
        wait_recv(W.at[:, :, pl.ds(0, kd)], s_z.at[1])
        wait_recv(Pa, s_z.at[2])

        @pl.when(c != 0)
        def _():
            wait_recv(R.at[pl.ds(0, 3), pl.ds(0, half)], s_z.at[4])

    @pl.when(z == 2)
    def _():
        wait_recv(W.at[:, :, pl.ds(0, kd)], s_z.at[0])
        wait_recv(W.at[:, :, pl.ds(0, ku)], s_z.at[1])
        wait_recv(Qa.at[1], s_z.at[4])

        @pl.when(y == 0)
        def _():
            wait_recv(Pa.at[0], s_z.at[2])

        @pl.when(y == 1)
        def _():
            wait_recv(Pa, s_z.at[2])

            @pl.when(k == 0)
            def _():
                wait_recv(PR.at[1, :, C1], s_z.at[3])


def solution(mesh):
    def local_fn(a_local):
        rows, m = a_local.shape
        kd = m - NU * PW - XU
        f32, bf16 = jnp.float32, jnp.bfloat16
        dma = pltpu.SemaphoreType.DMA
        return pl.pallas_call(
            kernel,
            out_shape=pltpu.VMEM((rows, rows), bf16),
            in_specs=[pl.BlockSpec(memory_space=pl.ANY)],
            out_specs=pl.BlockSpec(memory_space=pltpu.VMEM),
            scratch_shapes=[
                pltpu.VMEM((2, rows, m), bf16),
                pltpu.VMEM((2, rows, m), bf16),
                pltpu.VMEM((2, rows, kd), bf16),
                pltpu.VMEM((2, 2, kd, rows // 2), bf16),
                pltpu.VMEM((2, kd, rows), bf16),
                pltpu.VMEM((2, rows, rows), f32),
                pltpu.VMEM((2, rows, rows // 2), f32),
                pltpu.VMEM((2, rows, rows), f32),
                pltpu.VMEM((2, rows // 2, rows // 2), f32),
                pltpu.VMEM((4, rows, rows), f32),
                pltpu.VMEM((2, rows, rows), f32),
                pltpu.VMEM((rows, rows), f32),
                pltpu.VMEM((2, rows, rows // 2), f32),
                pltpu.SemaphoreType.REGULAR,
                dma((1,)), dma((5,)), dma((4 * NS,)), dma((NS + 1,)), dma((NU + 1,)), dma((4,)), dma((2,)), dma((9,)),
            ],
            compiler_params=pltpu.CompilerParams(
                collective_id=0, has_side_effects=True, vmem_limit_bytes=56 * 1024 * 1024),
        )(a_local)

    part_spec = P(("batch", "row"), "col")
    return jax.shard_map(local_fn, mesh=mesh, in_specs=(part_spec,), out_specs=part_spec, check_vma=False)
```

```python
import jax
import jax.numpy as jnp
from jax import lax
from jax.experimental import pallas as pl
from jax.experimental.pallas import tpu as pltpu
from jax.sharding import PartitionSpec as P

MESH = pl.DeviceIdType.MESH
PW = 256
NU = 15
XU = 128
NS = 8


def mm(a, b):
    return lax.dot_general(a, b, (((1,), (1,)), ((), ())), preferred_element_type=jnp.float32)


def mn(a, b):
    return lax.dot_general(a, b, (((1,), (0,)), ((), ())), preferred_element_type=jnp.float32)


def kernel(a_ref, o_ref, X, Y, W, T0, T1, Pa, Pb, Qa, QD, R, PR, XA, XB, far, ld, s_z, r_y, r_d, r_w, r_p, r_r, r_x):
    rows, m = a_ref.shape
    ku = NU * PW + XU
    kd = m - ku
    nd, xd = kd // PW, kd % PW
    half = rows // 2
    st = half // NS
    us = rows // NS
    z = lax.axis_index("row")
    c = lax.axis_index("col")
    y = c // 2
    k = c % 2
    sib = 2 * y + 1 - k

    def rcopy(src, dst, ss, rs, row, col):
        return pltpu.make_async_remote_copy(
            src_ref=src, dst_ref=dst, send_sem=ss, recv_sem=rs, device_id={"row": row, "col": col}, device_id_type=MESH)

    def wait_recv(ref, sem):
        pltpu.make_async_copy(ref, ref, sem).wait()

    def up(p, w=PW):
        return pl.ds(pl.multiple_of(p * PW, 128), w)

    def dn(p, w=PW):
        return pl.ds(pl.multiple_of(ku + p * PW, 128), w)

    def rs_(h, s, n=1):
        return pl.ds(pl.multiple_of(h * half + s * st, st), n * st)

    def us_(s):
        return pl.ds(pl.multiple_of(s * us, us), us)

    DALL = pl.ds(ku, kd)
    UALL = pl.ds(0, ku)
    C0, C1 = pl.ds(0, half), pl.ds(half, half)
    COLS = (C0, C1)

    def each(lo, hi, fn):
        lax.fori_loop(lo, hi, lambda i, u: (fn(i), u)[1], 0)

    load = pltpu.make_async_copy(a_ref, X.at[k], ld.at[0])
    load.start()

    def near(sem):
        for dz in (-1, 1):
            @pl.when((z + dz >= 0) & (z + dz <= 3))
            def _():
                for kk in range(2):
                    pl.semaphore_signal(sem, inc=1, device_id={"row": z + dz, "col": 2 * y + kk}, device_id_type=MESH)
        for dc in range(1, 4):
            pl.semaphore_signal(sem, inc=1, device_id={"row": z, "col": (c + dc) % 4}, device_id_type=MESH)

    n_near = jnp.where((z == 0) | (z == 3), 5, 7)
    bar = pltpu.get_barrier_semaphore()
    near(bar)
    pl.semaphore_wait(bar, n_near)

    def z0_u(q, w=PW):
        return rcopy(a_ref.at[:, up(q, w)], Y.at[k, :, up(q, w)], s_z.at[0], r_y.at[q], 1, c)

    def z0_d(t):
        r = rs_(0, t)
        return rcopy(a_ref.at[r, DALL], Y.at[k, r, DALL], s_z.at[0], r_y.at[2 * NS + t], 1, c)

    def z3_d(t):
        r = rs_(t % 2, t // 2)
        return rcopy(a_ref.at[r, DALL], Y.at[k, r, DALL], s_z.at[0], r_y.at[t], 2, c)

    def z3_u(s):
        r = us_(s)
        return rcopy(a_ref.at[r, UALL], Y.at[k, r, UALL], s_z.at[0], r_y.at[2 * NS + s], 2, c)

    def z1_u(q, w=PW):
        return rcopy(a_ref.at[:, up(q, w)], W.at[k, :, up(q, w)], s_z.at[0], r_w.at[q], 2, 2 * y + 1)

    def z2_d(t):
        h, s = t % 2, t // 2
        return rcopy(a_ref.at[rs_(h, s), DALL], W.at[k, rs_(1, s), pl.ds(0, kd)], s_z.at[0], r_w.at[jnp.where(s < 6, 1 + s // 2, s - 2)], 1, 2 * y + h)

    @pl.when(z == 0)
    def _():
        each(0, NU, lambda q: z0_u(q).start())
        z0_u(NU, XU).start()
        each(0, 2 * NS, lambda t: z0_d(t).start())

    @pl.when(z == 3)
    def _():
        each(0, 2 * NS, lambda t: z3_d(t).start())
        each(0, NS, lambda s: z3_u(s).start())

    x_d = rcopy(a_ref.at[:, DALL], X.at[k, :, DALL], s_z.at[1], r_d.at[NS], z, sib)
    x_u = rcopy(a_ref.at[:, UALL], X.at[k, :, UALL], s_z.at[1], r_d.at[NS], z, sib)

    @pl.when(z == 1)
    def _():
        each(0, NU, lambda q: z1_u(q).start())
        z1_u(NU, XU).start()
        x_d.start()

    @pl.when(z == 2)
    def _():
        z2_d(0).start()
        z2_d(1).start()
        x_u.start()

    near(far)

    Pa[...] = jnp.zeros_like(Pa)
    Qa[...] = jnp.zeros_like(Qa)
    Pb[...] = jnp.zeros_like(Pb)
    load.wait()
    dq = jnp.where(z == 1, 1, 0)

    def diag(p):
        cs = pl.ds(pl.multiple_of(p * 512, 512), 512)
        Qa[dq] += mm(X[k, :, cs], X[k, :, cs])

    each(0, m // 512, diag)

    def slot(owner):
        return (c - owner + 3) % 4

    dsend = rcopy(Qa.at[dq], R.at[slot(z)], s_z.at[3], r_r.at[0], z, z)

    @pl.when(c != z)
    def _():
        dsend.start()

    def u_fwd(q, w=PW):
        return rcopy(Y.at[k, :, up(q, w)], W.at[k, :, up(q, w)], s_z.at[0], r_w.at[q], 2, 2 * y)

    def zU(q, w=PW):
        wait_recv(Y.at[k, :, up(q, w)], r_y.at[q])
        Qa[0] += mm(X[k, :, up(q, w)], Y[k, :, up(q, w)])

    def turn(p, w=PW):
        for h in range(2):
            T1[h, up(p, w), :] = X[h, :, dn(p, w)].T

    def d_sib(t):
        return rcopy(Y.at[k, rs_(0, t), DALL], Y.at[k, rs_(0, t), DALL], s_z.at[1], r_d.at[t // NS], z, sib)

    def zD(t):
        wait_recv(Y.at[k, rs_(0, t), DALL], r_y.at[2 * NS + t])
        d_sib(t).start()

    def brows(b):
        return pl.ds(pl.multiple_of(b * half, half), half)

    def wait_w(r, n):
        wait_recv(W.at[:, r, pl.ds(0, kd)], r_w.at[n])

    CA = pl.ds(0, rows)
    peer = (c + 2) % 4

    def r3(u):
        return rs_(0, 4 * u, 4)

    def r2(s, n=2):
        return rs_(1, s, n)

    def xsend(src, dst, n):
        return rcopy(src, dst, s_z.at[2], r_x.at[n], 1, peer)

    x31 = xsend(Pa.at[1, rs_(0, 0, NS)], XA.at[rs_(0, 0, NS)], 0)

    def x30(b, u):
        return xsend(Pb.at[b, r3(u)], XB.at[b, r3(u)], 1 + 2 * b + u)

    def x21(s, n, rs):
        return xsend(Pa.at[1, r2(s, n)], XA.at[r2(s, n)], rs)

    def x20(b, s, n, rs):
        return xsend(Pb.at[b, r2(s, n)], XB.at[b, r2(s, n)], rs)

    def msend(src, i, s, n, j, cols, rs):
        return rcopy(src, PR.at[i, rs_(k, s, n), cols], s_z.at[2], r_p.at[rs], 2, j)

    m31 = msend(Pa.at[1, rs_(0, 0, NS)], 1, 0, NS, 1, CA, 0)

    def m30(b, u):
        src = Pb.at[b, r3(u)]
        if b == 0:
            return msend(src, 1, 4 * u, 4, 0, C0, 0)
        return rcopy(src, R.at[2, rs_(k, 4 * u, 4), C1], s_z.at[2], r_r.at[1], 3, 0)

    def m30r(u):
        return rcopy(Pb.at[1, r3(u)], PR.at[1, rs_(k, 4 * u, 4), C1], s_z.at[2], r_p.at[1], 2, 2)

    def m21(s, n, rs):
        return msend(Pa.at[1, r2(s, n)], 0, s, n, 1, CA, rs)

    def m20(b, s, n, rs):
        return msend(Pb.at[b, r2(s, n)], 0, s, n, 0, COLS[b], rs)

    def d2(src, j, cols):
        return rcopy(src, R.at[1, rs_(k, 7), cols], s_z.at[2], r_r.at[1], 2, j)

    d21 = d2(Pa.at[1, r2(7, 1)], 1, CA)
    d20 = [d2(Pb.at[b, r2(7, 1)], 0, COLS[b]) for b in range(2)]

    def part1(r):
        Pa[1, r, :] = mn(W[0, r, :kd], T1[0]) + mn(W[1, r, :kd], T1[1])

    def part0(r, b):
        Pb[b, r, :] = mn(W[0, r, :kd], T0[0, b]) + mn(W[1, r, :kd], T0[1, b])

    q_u = rcopy(Qa.at[0], R.at[slot(0)], s_z.at[4], r_r.at[0], 1, 0)

    def q_d(b):
        return rcopy(QD.at[b], PR.at[y, rs_(k, 0, NS), COLS[b]], s_z.at[4], r_r.at[1], 1, 0)

    @pl.when(z == 1)
    def _():
        wait_recv(X.at[1 - k, :, DALL], r_d.at[NS])

        def step_u(q):
            zU(q)

            @pl.when(q < 5)
            def _():
                u_fwd(q).start()

            turn(q)

        each(0, NU, step_u)
        zU(NU, XU)
        each(NU, nd, turn)
        if xd:
            turn(nd, xd)

        @pl.when(c != 0)
        def _():
            q_u.start()

        pl.semaphore_wait(far, n_near)

        def step(i):
            @pl.when(i < 2 * NS)
            def _():
                zD(i)

            @pl.when(i == 3)
            def _():
                wait_w(rs_(0, 0, NS), 0)
                part1(rs_(0, 0, NS))

                @pl.when(y == 1)
                def _():
                    x31.start()

                each(5, 10, lambda q: u_fwd(q).start())

            @pl.when((i == 5) & (y == 0))
            def _():
                wait_recv(XA.at[rs_(0, 0, NS)], r_x.at[0])
                Pa[1, rs_(0, 0, NS), :] += XA[rs_(0, 0, NS), :]
                m31.start()

            @pl.when(i == 16)
            def _():
                def chunk(n):
                    ch = jnp.where(n == 0, k, 1 - k)

                    @pl.when(n == 1)
                    def _():
                        wait_recv(Y.at[1 - k, brows(1), DALL], r_d.at[1])

                    Pb[1, pl.ds(0, rows - st), :] += mm(W[ch, pl.ds(0, rows - st), :kd], Y[ch, brows(1), DALL])

                each(0, 2, chunk)

                @pl.when(y == 0)
                def _():
                    for u in range(2):
                        m30(1, u).start()

                @pl.when(y == 1)
                def _():
                    for u in range(2):
                        m30r(u).start()
                    x20(1, 0, 7, 8).start()

            @pl.when((i == 7) | (i == 17))
            def _():
                b = jnp.where(i == 7, 0, 1)

                @pl.when(b == 0)
                def _():
                    wait_recv(Y.at[1 - k, brows(0), DALL], r_d.at[0])

                for h in range(2):
                    T0[h, b] = Y[h, brows(b), DALL].T

                @pl.when(b == 0)
                def _():
                    part0(rs_(0, 0, NS), 0)

                    @pl.when(y == 1)
                    def _():
                        for u in range(2):
                            x30(0, u).start()

            @pl.when((i == 7) | (i == 17))
            def _():
                b = jnp.where(i == 7, 0, 1)
                r = rs_(k, 0, NS)
                QD[b] = mn(X[0, r, DALL], T0[0, b]) + mn(X[1, r, DALL], T0[1, b])
                for bb in range(2):
                    @pl.when((b == bb) & (c != 0))
                    def _():
                        q_d(bb).start()

            @pl.when(i == 7)
            def _():
                each(10, NU, lambda q: u_fwd(q).start())
                u_fwd(NU, XU).start()

            @pl.when((i == 9) & (y == 0))
            def _():
                for u in range(2):
                    wait_recv(XB.at[0, r3(u)], r_x.at[1 + u])
                    Pb[0, r3(u), :] += XB[0, r3(u), :]
                    m30(0, u).start()

            @pl.when((i == 8) | (i == 9) | (i == 13))
            def _():
                g = jnp.where(i == 13, 2, i - 8)
                wait_w(r2(2 * g), 1 + g)
                part1(r2(2 * g))
                part0(r2(2 * g), 0)

                @pl.when(y == 1)
                def _():
                    x21(2 * g, 2, 5 + g).start()
                    x20(0, 2 * g, 2, 5 + g).start()

            @pl.when(((i == 10) | (i == 11) | (i == 15)) & (y == 0))
            def _():
                g = jnp.where(i == 15, 2, i - 10)
                wait_recv(XA.at[pl.ds(0, 48)], r_x.at[5 + g])
                Pa[1, r2(2 * g), :] += XA[r2(2 * g), :]
                Pb[0, r2(2 * g), :] += XB[0, r2(2 * g), :]
                m21(2 * g, 2, 1).start()
                m20(0, 2 * g, 2, 1).start()

            @pl.when((i == 17) & (y == 0))
            def _():
                wait_recv(XA.at[pl.ds(0, 24)], r_x.at[3])
                Pa[1, r2(6, 1), :] += XA[r2(6, 1), :]
                m21(6, 1, 2).start()
                Pb[0, r2(6, 1), :] += XB[0, r2(6, 1), :]
                m20(0, 6, 1, 3).start()

            @pl.when((i == 14) | (i == 18))
            def _():
                t = jnp.where(i == 14, 6, 7)
                wait_w(r2(t, 1), t - 2)
                part1(r2(t, 1))

                @pl.when((y == 1) & (i == 18))
                def _():
                    d21.start()

                @pl.when((y == 0) & (i == 18))
                def _():
                    m21(7, 1, 2).start()

                part0(r2(t, 1), 0)

                @pl.when((y == 1) & (i == 14))
                def _():
                    x21(6, 1, 3).start()
                    x20(0, 6, 1, 3).start()

                @pl.when((y == 1) & (i == 18))
                def _():
                    d20[0].start()

                @pl.when((y == 0) & (i == 18))
                def _():
                    m20(0, 7, 1, 3).start()
                    wait_recv(XB.at[1, r2(0, 7)], r_x.at[8])
                    Pb[1, r2(0, 7), :] += XB[1, r2(0, 7), :]
                    m20(1, 0, 7, 2).start()

                @pl.when(i == 18)
                def _():
                    part0(r2(7, 1), 1)

                    @pl.when(y == 1)
                    def _():
                        d20[1].start()

                    @pl.when(y == 0)
                    def _():
                        m20(1, 7, 1, 3).start()

        each(0, 19, step)

    def d_fwd(t):
        h, s = t % 2, t // 2
        return rcopy(Y.at[k, rs_(h, s), DALL], W.at[k, rs_(0, s), pl.ds(0, kd)], s_z.at[0], r_w.at[0], 1, 2 * y + h)

    def u_sib(s):
        return rcopy(Y.at[k, us_(s), UALL], Y.at[k, us_(s), UALL], s_z.at[1], r_d.at[s], z, sib)

    def q1send(s):
        return rcopy(Qa.at[1, us_(s)], R.at[c, us_(s)], s_z.at[4], r_r.at[0], 3, 2)

    def y2(q, w=PW):
        wait_recv(W.at[:, :, up(q, w)], r_w.at[q])
        Pa[0] += mm(X[0, :, up(q, w)], W[0, :, up(q, w)]) + mm(X[1, :, up(q, w)], W[1, :, up(q, w)])

    def y3(b, q, w=PW):
        r = pl.ds(b * half, half)
        Pa[1, r, :] += mm(Y[0, r, up(q, w)], W[0, :, up(q, w)]) + mm(Y[1, r, up(q, w)], W[1, :, up(q, w)])

    def wait_ysib(s):
        wait_recv(Y.at[1 - k, us_(s), UALL], r_d.at[s])

    def s3(r, cols=CA):
        return rcopy(Pa.at[1, r, cols], R.at[y, r, cols], s_z.at[2], r_r.at[0], 3, k)

    s2 = rcopy(Pa.at[0], R.at[0], s_z.at[2], r_r.at[0], 2, k)

    def add(i, r, cols):
        Pa[i, r, cols] += PR[i, r, cols]

    def wait_pr(n, cols, sem):
        wait_recv(PR.at[0, pl.ds(0, n), cols], r_p.at[sem])

    def strip31(s):
        wait_ysib(s)
        r = us_(s)
        Pa[1, r, :] = mm(Y[0, r, UALL], W[0, :, :ku]) + mm(Y[1, r, UALL], W[1, :, :ku])

        @pl.when(y == 0)
        def _():
            add(1, r, CA)

        s3(r).start()

    @pl.when(z == 2)
    def _():
        def step_d(t):
            wait_recv(Y.at[k, rs_(t % 2, t // 2), DALL], r_y.at[t])
            d_fwd(t).start()

            @pl.when(t == 1)
            def _():
                wait_recv(X.at[1 - k, :, UALL], r_d.at[NS])

            @pl.when((k == 1) & (t >= 1))
            def _():
                y2(t - 1)

        each(0, 2 * NS, step_d)
        each(2, 2 * NS, lambda t: z2_d(t).start())

        pl.semaphore_wait(far, n_near)

        @pl.when(k == 1)
        def _():
            y2(NU, XU)

            @pl.when(y == 1)
            def _():
                s2.start()


        def q1(s):
            Qa[1, us_(s), :] = mm(Y[k, us_(s), :], X[k])
            q1send(s).start()

        def step_u(s):
            @pl.when((k == 0) & (s >= 1))
            def _():
                y2(2 * s - 1)

            @pl.when(k == 0)
            def _():
                y2(2 * s)

            @pl.when((k == 0) & (s == 4))
            def _():
                each(0, 4, wait_ysib)
                each(0, 7, lambda q: y3(0, q))

            @pl.when((k == 0) & (s >= 4))
            def _():
                y3(0, 2 * s - 1)
                y3(0, 2 * s)

            wait_recv(Y.at[k, us_(s), UALL], r_y.at[2 * NS + s])
            u_sib(s).start()

            @pl.when((k == 1) & (y == 0) & (s == 4))
            def _():
                wait_recv(PR.at[1], r_p.at[0])

            @pl.when((k == 1) & (s >= 4) & (s <= 6))
            def _():
                each(2 * s - 8, 2 * s - 6, strip31)

            @pl.when((k == 1) | (s < NS - 1))
            def _():
                q1(s)

        each(0, NS, step_u)

        @pl.when(k == 1)
        def _():
            each(NS - 2, NS, strip31)

            @pl.when(y == 0)
            def _():
                wait_pr(192, CA, 1)
                for h in range(2):
                    add(0, rs_(h, 0, 6), CA)
                wait_pr(64, CA, 2)
                for h in range(2):
                    add(0, rs_(h, 6, 2), CA)

        @pl.when(k == 0)
        def _():
            y2(NU, XU)

            @pl.when(y == 1)
            def _():
                s2.start()

            y3(0, NU, XU)

            @pl.when(y == 0)
            def _():
                wait_pr(rows, C0, 0)
                add(1, pl.ds(0, half), C0)


            @pl.when(y == 0)
            def _():
                s3(pl.ds(0, half)).start()

            @pl.when(y == 1)
            def _():
                s3(pl.ds(0, half), C0).start()

            each(4, NS, wait_ysib)

            def low(b):
                r = pl.ds(pl.multiple_of(b * half, half), half)
                Pa[1, r, :] = mm(Y[0, r, UALL], W[0, :, :ku]) + mm(Y[1, r, UALL], W[1, :, :ku])

            each(1 + k, 2, low)

            @pl.when(y == 0)
            def _():
                add(1, pl.ds(half, half), C0)

            @pl.when(y == 0)
            def _():
                s3(pl.ds(half, half)).start()

            @pl.when(y == 1)
            def _():
                s3(pl.ds(half, half), C0).start()

            each(NS - 1, NS + k, q1)

            @pl.when(y == 1)
            def _():
                wait_pr(rows, C1, 1)
                add(1, CA, C1)
                s3(CA, C1).start()

            @pl.when(y == 0)
            def _():
                wait_pr(192, C0, 1)
                for h in range(2):
                    add(0, rs_(h, 0, 6), C0)
                wait_pr(224, C1, 2)
                for h in range(2):
                    add(0, rs_(h, 0, 7), C1)
                wait_pr(96, C0, 3)
                for h in range(2):
                    add(0, rs_(h, 6, 2), C0)
                    add(0, rs_(h, 7), C1)

    @pl.when((z == 0) | (z == 3))
    def _():
        pl.semaphore_wait(far, n_near)

    @pl.when(c > z)
    def _():
        o_ref[...] = jnp.zeros_like(o_ref)

    @pl.when(c == z)
    def _():
        wait_recv(R.at[pl.ds(0, 3)], r_r.at[0])
        total = Qa[dq] + R[0] + R[1] + R[2]
        diff = lax.broadcasted_iota(jnp.int32, (rows, rows), 0) - lax.broadcasted_iota(jnp.int32, (rows, rows), 1)
        o_ref[...] = jnp.where(diff >= 0, total, 0.0).astype(o_ref.dtype)

    @pl.when((z == 1) & (c == 0))
    def _():
        wait_recv(R.at[pl.ds(0, 3)], r_r.at[0])
        Qa[0] += R[0] + R[1] + R[2]
        wait_recv(R.at[pl.ds(0, 3), pl.ds(0, half)], r_r.at[1])
        for b in range(2):
            PR[0, pl.ds(0, half), COLS[b]] = QD[b]
        o_ref[...] = (Qa[0] + PR[0] + PR[1]).astype(o_ref.dtype)

    @pl.when((z == 2) & (y == 0))
    def _():
        wait_recv(R.at[0], r_r.at[0])
        wait_recv(R.at[1, pl.ds(0, 32)], r_r.at[1])
        for h in range(2):
            Pa[0, rs_(h, 7), :] += R[1, rs_(h, 7), :]
        o_ref[...] = (Pa[0] + R[0]).astype(o_ref.dtype)

    @pl.when((z == 3) & (c == 2))
    def _():
        wait_recv(R, r_r.at[0])
        o_ref[...] = (R[0] + R[1] + R[2] + R[3]).astype(o_ref.dtype)

    @pl.when((z == 3) & (y == 0))
    def _():
        wait_recv(R.at[pl.ds(0, 2)], r_r.at[0])

        @pl.when(k == 0)
        def _():
            wait_recv(R.at[2, :, C1], r_r.at[1])
            R[0, :, C1] += R[2, :, C1]

        o_ref[...] = (R[0] + R[1]).astype(o_ref.dtype)

    @pl.when(c != z)
    def _():
        wait_recv(Qa.at[0], s_z.at[3])

    @pl.when((z == 0) | (z == 3))
    def _():
        wait_recv(X.at[k], s_z.at[0])

    @pl.when(z == 1)
    def _():
        wait_recv(W.at[:, :, pl.ds(0, ku)], s_z.at[0])
        wait_recv(W.at[:, :, pl.ds(0, kd)], s_z.at[1])
        wait_recv(Pa, s_z.at[2])

        @pl.when(c != 0)
        def _():
            wait_recv(R.at[pl.ds(0, 3), pl.ds(0, half)], s_z.at[4])

    @pl.when(z == 2)
    def _():
        wait_recv(W.at[:, :, pl.ds(0, kd)], s_z.at[0])
        wait_recv(W.at[:, :, pl.ds(0, ku)], s_z.at[1])
        wait_recv(Qa.at[1], s_z.at[4])

        @pl.when(y == 0)
        def _():
            wait_recv(Pa.at[0], s_z.at[2])

        @pl.when(y == 1)
        def _():
            wait_recv(Pa, s_z.at[2])


def solution(mesh):
    def local_fn(a_local):
        rows, m = a_local.shape
        kd = m - NU * PW - XU
        f32, bf16 = jnp.float32, jnp.bfloat16
        dma = pltpu.SemaphoreType.DMA
        return pl.pallas_call(
            kernel,
            out_shape=pltpu.VMEM((rows, rows), bf16),
            in_specs=[pl.BlockSpec(memory_space=pl.ANY)],
            out_specs=pl.BlockSpec(memory_space=pltpu.VMEM),
            scratch_shapes=[
                pltpu.VMEM((2, rows, m), bf16),
                pltpu.VMEM((2, rows, m), bf16),
                pltpu.VMEM((2, rows, kd), bf16),
                pltpu.VMEM((2, 2, kd, rows // 2), bf16),
                pltpu.VMEM((2, kd, rows), bf16),
                pltpu.VMEM((2, rows, rows), f32),
                pltpu.VMEM((2, rows, rows // 2), f32),
                pltpu.VMEM((2, rows, rows), f32),
                pltpu.VMEM((2, rows // 2, rows // 2), f32),
                pltpu.VMEM((4, rows, rows), f32),
                pltpu.VMEM((2, rows, rows), f32),
                pltpu.VMEM((rows, rows), f32),
                pltpu.VMEM((2, rows, rows // 2), f32),
                pltpu.SemaphoreType.REGULAR,
                dma((1,)), dma((5,)), dma((4 * NS,)), dma((NS + 1,)), dma((NU + 1,)), dma((4,)), dma((2,)), dma((9,)),
            ],
            compiler_params=pltpu.CompilerParams(
                collective_id=0, has_side_effects=True, vmem_limit_bytes=56 * 1024 * 1024),
        )(a_local)

    part_spec = P(("batch", "row"), "col")
    return jax.shard_map(local_fn, mesh=mesh, in_specs=(part_spec,), out_specs=part_spec, check_vma=False)
```

```python
import jax
import jax.numpy as jnp
from jax import lax
from jax.experimental import pallas as pl
from jax.experimental.pallas import tpu as pltpu
from jax.sharding import PartitionSpec as P

MESH = pl.DeviceIdType.MESH
PW = 256
NU = 15
XU = 128
NS = 8


def mm(a, b):
    return lax.dot_general(a, b, (((1,), (1,)), ((), ())), preferred_element_type=jnp.float32)


def mn(a, b):
    return lax.dot_general(a, b, (((1,), (0,)), ((), ())), preferred_element_type=jnp.float32)


def kernel(a_ref, o_ref, X, Y, W, T0, T1, Pa, Pb, Qa, QD, R, PR, XA, XB, far, ld, s_z, r_y, r_d, r_w, r_p, r_r, r_x):
    rows, m = a_ref.shape
    ku = NU * PW + XU
    kd = m - ku
    nd, xd = kd // PW, kd % PW
    half = rows // 2
    st = half // NS
    us = rows // NS
    z = lax.axis_index("row")
    c = lax.axis_index("col")
    y = c // 2
    k = c % 2
    sib = 2 * y + 1 - k

    def rcopy(src, dst, ss, rs, row, col):
        return pltpu.make_async_remote_copy(
            src_ref=src, dst_ref=dst, send_sem=ss, recv_sem=rs, device_id={"row": row, "col": col}, device_id_type=MESH)

    def wait_recv(ref, sem):
        pltpu.make_async_copy(ref, ref, sem).wait()

    def up(p, w=PW):
        return pl.ds(pl.multiple_of(p * PW, 128), w)

    def dn(p, w=PW):
        return pl.ds(pl.multiple_of(ku + p * PW, 128), w)

    def rs_(h, s, n=1):
        return pl.ds(pl.multiple_of(h * half + s * st, st), n * st)

    def us_(s):
        return pl.ds(pl.multiple_of(s * us, us), us)

    DALL = pl.ds(ku, kd)
    UALL = pl.ds(0, ku)
    C0, C1 = pl.ds(0, half), pl.ds(half, half)
    COLS = (C0, C1)

    def each(lo, hi, fn):
        lax.fori_loop(lo, hi, lambda i, u: (fn(i), u)[1], 0)

    load = pltpu.make_async_copy(a_ref, X.at[k], ld.at[0])

    def near(sem):
        for dz in (-1, 1):
            @pl.when((z + dz >= 0) & (z + dz <= 3))
            def _():
                for kk in range(2):
                    pl.semaphore_signal(sem, inc=1, device_id={"row": z + dz, "col": 2 * y + kk}, device_id_type=MESH)
        for dc in range(1, 4):
            pl.semaphore_signal(sem, inc=1, device_id={"row": z, "col": (c + dc) % 4}, device_id_type=MESH)

    n_near = jnp.where((z == 0) | (z == 3), 5, 7)
    bar = pltpu.get_barrier_semaphore()
    near(bar)
    load.start()
    pl.semaphore_wait(bar, n_near)

    def z0_u(q, w=PW):
        return rcopy(a_ref.at[:, up(q, w)], Y.at[k, :, up(q, w)], s_z.at[0], r_y.at[q], 1, c)

    def z0_d(t):
        r = rs_(0, t)
        return rcopy(a_ref.at[r, DALL], Y.at[k, r, DALL], s_z.at[0], r_y.at[2 * NS + t], 1, c)

    def z3_d(t):
        r = rs_(t % 2, t // 2)
        return rcopy(a_ref.at[r, DALL], Y.at[k, r, DALL], s_z.at[0], r_y.at[t], 2, c)

    def z3_u(s):
        r = us_(s)
        return rcopy(a_ref.at[r, UALL], Y.at[k, r, UALL], s_z.at[0], r_y.at[2 * NS + s], 2, c)

    def z1_u(q, w=PW):
        return rcopy(a_ref.at[:, up(q, w)], W.at[k, :, up(q, w)], s_z.at[0], r_w.at[q], 2, 2 * y + 1)

    def z2_d(t):
        h, s = t % 2, t // 2
        return rcopy(a_ref.at[rs_(h, s), DALL], W.at[k, rs_(1, s), pl.ds(0, kd)], s_z.at[0], r_w.at[jnp.where(s < 6, 1 + s // 2, s - 2)], 1, 2 * y + h)

    @pl.when(z == 0)
    def _():
        each(0, NU, lambda q: z0_u(q).start())
        z0_u(NU, XU).start()
        each(0, 2 * NS, lambda t: z0_d(t).start())

    @pl.when(z == 3)
    def _():
        each(0, 2 * NS, lambda t: z3_d(t).start())
        each(0, NS, lambda s: z3_u(s).start())

    x_d = rcopy(a_ref.at[:, DALL], X.at[k, :, DALL], s_z.at[1], r_d.at[NS], z, sib)
    x_u = rcopy(a_ref.at[:, UALL], X.at[k, :, UALL], s_z.at[1], r_d.at[NS], z, sib)

    @pl.when(z == 1)
    def _():
        each(0, NU, lambda q: z1_u(q).start())
        z1_u(NU, XU).start()
        x_d.start()

    @pl.when(z == 2)
    def _():
        z2_d(0).start()
        z2_d(1).start()
        x_u.start()

    near(far)

    Pa[...] = jnp.zeros_like(Pa)
    Qa[...] = jnp.zeros_like(Qa)
    Pb[...] = jnp.zeros_like(Pb)
    load.wait()
    dq = jnp.where(z == 1, 1, 0)

    def diag(p):
        cs = pl.ds(pl.multiple_of(p * 512, 512), 512)
        Qa[dq] += mm(X[k, :, cs], X[k, :, cs])

    each(0, m // 512, diag)

    def slot(owner):
        return (c - owner + 3) % 4

    dsend = rcopy(Qa.at[dq], R.at[slot(z)], s_z.at[3], r_r.at[0], z, z)

    @pl.when(c != z)
    def _():
        dsend.start()

    def u_fwd(q, w=PW):
        return rcopy(Y.at[k, :, up(q, w)], W.at[k, :, up(q, w)], s_z.at[0], r_w.at[q], 2, 2 * y)

    def zU(q, w=PW):
        wait_recv(Y.at[k, :, up(q, w)], r_y.at[q])
        Qa[0] += mm(X[k, :, up(q, w)], Y[k, :, up(q, w)])

    def turn(p, w=PW):
        for h in range(2):
            T1[h, up(p, w), :] = X[h, :, dn(p, w)].T

    def d_sib(t):
        return rcopy(Y.at[k, rs_(0, t), DALL], Y.at[k, rs_(0, t), DALL], s_z.at[1], r_d.at[t // NS], z, sib)

    def zD(t):
        wait_recv(Y.at[k, rs_(0, t), DALL], r_y.at[2 * NS + t])
        d_sib(t).start()

    def brows(b):
        return pl.ds(pl.multiple_of(b * half, half), half)

    def wait_w(r, n):
        wait_recv(W.at[:, r, pl.ds(0, kd)], r_w.at[n])

    CA = pl.ds(0, rows)
    peer = (c + 2) % 4

    def r3(u):
        return rs_(0, 4 * u, 4)

    def r2(s, n=2):
        return rs_(1, s, n)

    def xsend(src, dst, n):
        return rcopy(src, dst, s_z.at[2], r_x.at[n], 1, peer)

    x31 = xsend(Pa.at[1, rs_(0, 0, NS)], XA.at[rs_(0, 0, NS)], 0)

    def x30(b, u):
        return xsend(Pb.at[b, r3(u)], XB.at[b, r3(u)], 1 + 2 * b + u)

    def x21(s, n, rs):
        return xsend(Pa.at[1, r2(s, n)], XA.at[r2(s, n)], rs)

    def x20(b, s, n, rs):
        return xsend(Pb.at[b, r2(s, n)], XB.at[b, r2(s, n)], rs)

    def msend(src, i, s, n, j, cols, rs):
        return rcopy(src, PR.at[i, rs_(k, s, n), cols], s_z.at[2], r_p.at[rs], 2, j)

    m31 = msend(Pa.at[1, rs_(0, 0, NS)], 1, 0, NS, 1, CA, 0)

    def m30(b, u):
        src = Pb.at[b, r3(u)]
        if b == 0:
            return msend(src, 1, 4 * u, 4, 0, C0, 0)
        return rcopy(src, R.at[2, rs_(k, 4 * u, 4), C1], s_z.at[2], r_r.at[1], 3, 0)

    def m30r(u):
        return rcopy(Pb.at[1, r3(u)], PR.at[1, rs_(k, 4 * u, 4), C1], s_z.at[2], r_p.at[1 + u], 2, 2)

    def m21(s, n, rs):
        return msend(Pa.at[1, r2(s, n)], 0, s, n, 1, CA, rs)

    def m20(b, s, n, rs):
        return msend(Pb.at[b, r2(s, n)], 0, s, n, 0, COLS[b], rs)

    def d2(src, j, cols):
        return rcopy(src, R.at[1, rs_(k, 7), cols], s_z.at[2], r_r.at[1], 2, j)

    d21 = d2(Pa.at[1, r2(7, 1)], 1, CA)
    d20 = [d2(Pb.at[b, r2(7, 1)], 0, COLS[b]) for b in range(2)]

    def part1(r):
        Pa[1, r, :] = mn(W[0, r, :kd], T1[0]) + mn(W[1, r, :kd], T1[1])

    def part0(r, b):
        Pb[b, r, :] = mn(W[0, r, :kd], T0[0, b]) + mn(W[1, r, :kd], T0[1, b])

    q_u = rcopy(Qa.at[0], R.at[slot(0)], s_z.at[4], r_r.at[0], 1, 0)

    def q_d(b):
        return rcopy(QD.at[b], PR.at[y, rs_(k, 0, NS), COLS[b]], s_z.at[4], r_r.at[1], 1, 0)

    @pl.when(z == 1)
    def _():
        wait_recv(X.at[1 - k, :, DALL], r_d.at[NS])

        def step_u(q):
            zU(q)

            @pl.when(q < 5)
            def _():
                u_fwd(q).start()

            turn(q)

        each(0, NU, step_u)
        zU(NU, XU)
        each(NU, nd, turn)
        if xd:
            turn(nd, xd)

        @pl.when(c != 0)
        def _():
            q_u.start()

        pl.semaphore_wait(far, n_near)

        def step(i):
            @pl.when(i < 2 * NS)
            def _():
                zD(i)

            @pl.when(i == 3)
            def _():
                wait_w(rs_(0, 0, NS), 0)
                part1(rs_(0, 0, NS))

                @pl.when(y == 1)
                def _():
                    x31.start()

                each(5, 10, lambda q: u_fwd(q).start())

            @pl.when((i == 5) & (y == 0))
            def _():
                wait_recv(XA.at[rs_(0, 0, NS)], r_x.at[0])
                Pa[1, rs_(0, 0, NS), :] += XA[rs_(0, 0, NS), :]
                m31.start()

            @pl.when(i == 16)
            def _():
                def chunk(n):
                    ch = jnp.where(n == 0, k, 1 - k)

                    @pl.when(n == 1)
                    def _():
                        wait_recv(Y.at[1 - k, brows(1), DALL], r_d.at[1])

                    Pb[1, pl.ds(0, rows - st), :] += mm(W[ch, pl.ds(0, rows - st), :kd], Y[ch, brows(1), DALL])

                each(0, 2, chunk)

                @pl.when(y == 0)
                def _():
                    for u in range(2):
                        m30(1, u).start()

                @pl.when(y == 1)
                def _():
                    for u in range(2):
                        m30r(u).start()
                    x20(1, 0, 7, 8).start()

            @pl.when((i == 7) | (i == 17))
            def _():
                b = jnp.where(i == 7, 0, 1)

                @pl.when(b == 0)
                def _():
                    wait_recv(Y.at[1 - k, brows(0), DALL], r_d.at[0])

                for h in range(2):
                    T0[h, b] = Y[h, brows(b), DALL].T

                @pl.when(b == 0)
                def _():
                    part0(rs_(0, 0, NS), 0)

                    @pl.when(y == 1)
                    def _():
                        for u in range(2):
                            x30(0, u).start()

            @pl.when((i == 7) | (i == 17))
            def _():
                b = jnp.where(i == 7, 0, 1)
                r = rs_(k, 0, NS)
                QD[b] = mn(X[0, r, DALL], T0[0, b]) + mn(X[1, r, DALL], T0[1, b])
                for bb in range(2):
                    @pl.when((b == bb) & (c != 0))
                    def _():
                        q_d(bb).start()

            @pl.when(i == 7)
            def _():
                each(10, NU, lambda q: u_fwd(q).start())
                u_fwd(NU, XU).start()

            @pl.when((i == 9) & (y == 0))
            def _():
                for u in range(2):
                    wait_recv(XB.at[0, r3(u)], r_x.at[1 + u])
                    Pb[0, r3(u), :] += XB[0, r3(u), :]
                    m30(0, u).start()

            @pl.when((i == 8) | (i == 9) | (i == 13))
            def _():
                g = jnp.where(i == 13, 2, i - 8)
                wait_w(r2(2 * g), 1 + g)
                part1(r2(2 * g))
                part0(r2(2 * g), 0)

                @pl.when(y == 1)
                def _():
                    x21(2 * g, 2, 5 + g).start()
                    x20(0, 2 * g, 2, 5 + g).start()

            @pl.when(((i == 10) | (i == 11) | (i == 15)) & (y == 0))
            def _():
                g = jnp.where(i == 15, 2, i - 10)
                wait_recv(XA.at[pl.ds(0, 48)], r_x.at[5 + g])
                Pa[1, r2(2 * g), :] += XA[r2(2 * g), :]
                Pb[0, r2(2 * g), :] += XB[0, r2(2 * g), :]
                m21(2 * g, 2, 1).start()
                m20(0, 2 * g, 2, 1).start()

            @pl.when((i == 17) & (y == 0))
            def _():
                wait_recv(XA.at[pl.ds(0, 24)], r_x.at[3])
                Pa[1, r2(6, 1), :] += XA[r2(6, 1), :]
                m21(6, 1, 2).start()
                Pb[0, r2(6, 1), :] += XB[0, r2(6, 1), :]
                m20(0, 6, 1, 3).start()

            @pl.when((i == 14) | (i == 18))
            def _():
                t = jnp.where(i == 14, 6, 7)
                wait_w(r2(t, 1), t - 2)
                part1(r2(t, 1))

                @pl.when((y == 1) & (i == 18))
                def _():
                    d21.start()

                @pl.when((y == 0) & (i == 18))
                def _():
                    m21(7, 1, 2).start()

                part0(r2(t, 1), 0)

                @pl.when((y == 1) & (i == 14))
                def _():
                    x21(6, 1, 3).start()
                    x20(0, 6, 1, 3).start()

                @pl.when((y == 1) & (i == 18))
                def _():
                    d20[0].start()

                @pl.when((y == 0) & (i == 18))
                def _():
                    m20(0, 7, 1, 3).start()
                    wait_recv(XB.at[1, r2(0, 7)], r_x.at[8])
                    Pb[1, r2(0, 7), :] += XB[1, r2(0, 7), :]
                    m20(1, 0, 7, 2).start()

                @pl.when(i == 18)
                def _():
                    part0(r2(7, 1), 1)

                    @pl.when(y == 1)
                    def _():
                        d20[1].start()

                    @pl.when(y == 0)
                    def _():
                        m20(1, 7, 1, 3).start()

        each(0, 19, step)

    def d_fwd(t):
        h, s = t % 2, t // 2
        return rcopy(Y.at[k, rs_(h, s), DALL], W.at[k, rs_(0, s), pl.ds(0, kd)], s_z.at[0], r_w.at[0], 1, 2 * y + h)

    def u_sib(s):
        return rcopy(Y.at[k, us_(s), UALL], Y.at[k, us_(s), UALL], s_z.at[1], r_d.at[s], z, sib)

    def q1send(s):
        return rcopy(Qa.at[1, us_(s)], R.at[c, us_(s)], s_z.at[4], r_r.at[0], 3, 2)

    def y2(q, w=PW):
        wait_recv(W.at[:, :, up(q, w)], r_w.at[q])
        Pa[0] += mm(X[0, :, up(q, w)], W[0, :, up(q, w)]) + mm(X[1, :, up(q, w)], W[1, :, up(q, w)])

    def y3(b, q, w=PW):
        r = pl.ds(b * half, half)
        Pa[1, r, :] += mm(Y[0, r, up(q, w)], W[0, :, up(q, w)]) + mm(Y[1, r, up(q, w)], W[1, :, up(q, w)])

    def wait_ysib(s):
        wait_recv(Y.at[1 - k, us_(s), UALL], r_d.at[s])

    def s3(r, cols=CA):
        return rcopy(Pa.at[1, r, cols], R.at[y, r, cols], s_z.at[2], r_r.at[0], 3, k)

    s2 = rcopy(Pa.at[0], R.at[0], s_z.at[2], r_r.at[0], 2, k)

    def add(i, r, cols):
        Pa[i, r, cols] += PR[i, r, cols]

    def wait_pr(n, cols, sem):
        wait_recv(PR.at[0, pl.ds(0, n), cols], r_p.at[sem])

    def strip31(s):
        wait_ysib(s)
        r = us_(s)
        Pa[1, r, :] = mm(Y[0, r, UALL], W[0, :, :ku]) + mm(Y[1, r, UALL], W[1, :, :ku])

        @pl.when(y == 0)
        def _():
            add(1, r, CA)

        s3(r).start()

    @pl.when(z == 2)
    def _():
        def step_d(t):
            wait_recv(Y.at[k, rs_(t % 2, t // 2), DALL], r_y.at[t])
            d_fwd(t).start()

            @pl.when(t == 1)
            def _():
                wait_recv(X.at[1 - k, :, UALL], r_d.at[NS])

            @pl.when((k == 1) & (t >= 1))
            def _():
                y2(t - 1)

            r = rs_(t % 2, t // 2)
            Qa[1, r, :] = mm(Y[k, r, DALL], X[k, :, DALL])

        each(0, 2 * NS, step_d)
        each(2, 2 * NS, lambda t: z2_d(t).start())

        pl.semaphore_wait(far, n_near)

        @pl.when(k == 1)
        def _():
            y2(NU, XU)

            @pl.when(y == 1)
            def _():
                s2.start()


        def q1(s):
            Qa[1, us_(s), :] += mm(Y[k, us_(s), UALL], X[k, :, UALL])
            q1send(s).start()

        def step_u(s):
            @pl.when((k == 0) & (s >= 1))
            def _():
                y2(2 * s - 1)

            @pl.when(k == 0)
            def _():
                y2(2 * s)

            @pl.when((k == 0) & (s == 4))
            def _():
                each(0, 4, wait_ysib)
                each(0, 7, lambda q: y3(0, q))

            @pl.when((k == 0) & (s >= 4))
            def _():
                y3(0, 2 * s - 1)
                y3(0, 2 * s)

            wait_recv(Y.at[k, us_(s), UALL], r_y.at[2 * NS + s])
            u_sib(s).start()

            @pl.when((k == 1) & (y == 0) & (s == 4))
            def _():
                wait_recv(PR.at[1], r_p.at[0])

            @pl.when((k == 1) & (s >= 4) & (s <= 6))
            def _():
                each(2 * s - 8, 2 * s - 6, strip31)

            @pl.when((k == 1) | (s < NS - 1))
            def _():
                q1(s)

        each(0, NS, step_u)

        @pl.when(k == 1)
        def _():
            each(NS - 2, NS, strip31)

            @pl.when(y == 0)
            def _():
                wait_pr(192, CA, 1)
                for h in range(2):
                    add(0, rs_(h, 0, 6), CA)
                wait_pr(64, CA, 2)
                for h in range(2):
                    add(0, rs_(h, 6, 2), CA)

        @pl.when(k == 0)
        def _():
            y2(NU, XU)

            @pl.when(y == 1)
            def _():
                s2.start()

            y3(0, NU, XU)

            @pl.when(y == 0)
            def _():
                wait_pr(rows, C0, 0)
                add(1, pl.ds(0, half), C0)


            @pl.when(y == 0)
            def _():
                s3(pl.ds(0, half)).start()

            @pl.when(y == 1)
            def _():
                s3(pl.ds(0, half), C0).start()

            each(4, NS, wait_ysib)

            def low(b):
                r = pl.ds(pl.multiple_of(b * half, half), half)
                Pa[1, r, :] = mm(Y[0, r, UALL], W[0, :, :ku]) + mm(Y[1, r, UALL], W[1, :, :ku])

            each(1 + k, 2, low)

            @pl.when(y == 0)
            def _():
                add(1, pl.ds(half, half), C0)

            @pl.when(y == 0)
            def _():
                s3(pl.ds(half, half)).start()

            @pl.when(y == 1)
            def _():
                s3(pl.ds(half, half), C0).start()

            each(NS - 1, NS + k, q1)

            @pl.when(y == 1)
            def _():
                for u in range(2):
                    wait_pr(half, C1, 1 + u)
                    for h in range(2):
                        add(1, rs_(h, 4 * u, 4), C1)
                        s3(rs_(h, 4 * u, 4), C1).start()

            @pl.when(y == 0)
            def _():
                wait_pr(192, C0, 1)
                for h in range(2):
                    add(0, rs_(h, 0, 6), C0)
                wait_pr(224, C1, 2)
                for h in range(2):
                    add(0, rs_(h, 0, 7), C1)
                wait_pr(96, C0, 3)
                for h in range(2):
                    add(0, rs_(h, 6, 2), C0)
                    add(0, rs_(h, 7), C1)

    @pl.when((z == 0) | (z == 3))
    def _():
        pl.semaphore_wait(far, n_near)

    @pl.when(c > z)
    def _():
        o_ref[...] = jnp.zeros_like(o_ref)

    @pl.when(c == z)
    def _():
        wait_recv(R.at[pl.ds(0, 3)], r_r.at[0])
        total = Qa[dq] + R[0] + R[1] + R[2]
        diff = lax.broadcasted_iota(jnp.int32, (rows, rows), 0) - lax.broadcasted_iota(jnp.int32, (rows, rows), 1)
        o_ref[...] = jnp.where(diff >= 0, total, 0.0).astype(o_ref.dtype)

    @pl.when((z == 1) & (c == 0))
    def _():
        wait_recv(R.at[pl.ds(0, 3)], r_r.at[0])
        Qa[0] += R[0] + R[1] + R[2]
        wait_recv(R.at[pl.ds(0, 3), pl.ds(0, half)], r_r.at[1])
        for b in range(2):
            PR[0, pl.ds(0, half), COLS[b]] = QD[b]
        o_ref[...] = (Qa[0] + PR[0] + PR[1]).astype(o_ref.dtype)

    @pl.when((z == 2) & (y == 0))
    def _():
        wait_recv(R.at[0], r_r.at[0])
        wait_recv(R.at[1, pl.ds(0, 32)], r_r.at[1])
        for h in range(2):
            Pa[0, rs_(h, 7), :] += R[1, rs_(h, 7), :]
        o_ref[...] = (Pa[0] + R[0]).astype(o_ref.dtype)

    @pl.when((z == 3) & (c == 2))
    def _():
        wait_recv(R, r_r.at[0])
        o_ref[...] = (R[0] + R[1] + R[2] + R[3]).astype(o_ref.dtype)

    @pl.when((z == 3) & (y == 0))
    def _():
        wait_recv(R.at[pl.ds(0, 2)], r_r.at[0])

        @pl.when(k == 0)
        def _():
            wait_recv(R.at[2, :, C1], r_r.at[1])
            R[0, :, C1] += R[2, :, C1]

        o_ref[...] = (R[0] + R[1]).astype(o_ref.dtype)

    @pl.when(c != z)
    def _():
        wait_recv(Qa.at[0], s_z.at[3])

    @pl.when((z == 0) | (z == 3))
    def _():
        wait_recv(X.at[k], s_z.at[0])

    @pl.when(z == 1)
    def _():
        wait_recv(W.at[:, :, pl.ds(0, ku)], s_z.at[0])
        wait_recv(W.at[:, :, pl.ds(0, kd)], s_z.at[1])
        wait_recv(Pa, s_z.at[2])

        @pl.when(c != 0)
        def _():
            wait_recv(R.at[pl.ds(0, 3), pl.ds(0, half)], s_z.at[4])

    @pl.when(z == 2)
    def _():
        wait_recv(W.at[:, :, pl.ds(0, kd)], s_z.at[0])
        wait_recv(W.at[:, :, pl.ds(0, ku)], s_z.at[1])
        wait_recv(Qa.at[1], s_z.at[4])

        @pl.when(y == 0)
        def _():
            wait_recv(Pa.at[0], s_z.at[2])

        @pl.when(y == 1)
        def _():
            wait_recv(Pa, s_z.at[2])


def solution(mesh):
    def local_fn(a_local):
        rows, m = a_local.shape
        kd = m - NU * PW - XU
        f32, bf16 = jnp.float32, jnp.bfloat16
        dma = pltpu.SemaphoreType.DMA
        return pl.pallas_call(
            kernel,
            out_shape=pltpu.VMEM((rows, rows), bf16),
            in_specs=[pl.BlockSpec(memory_space=pl.ANY)],
            out_specs=pl.BlockSpec(memory_space=pltpu.VMEM),
            scratch_shapes=[
                pltpu.VMEM((2, rows, m), bf16),
                pltpu.VMEM((2, rows, m), bf16),
                pltpu.VMEM((2, rows, kd), bf16),
                pltpu.VMEM((2, 2, kd, rows // 2), bf16),
                pltpu.VMEM((2, kd, rows), bf16),
                pltpu.VMEM((2, rows, rows), f32),
                pltpu.VMEM((2, rows, rows // 2), f32),
                pltpu.VMEM((2, rows, rows), f32),
                pltpu.VMEM((2, rows // 2, rows // 2), f32),
                pltpu.VMEM((4, rows, rows), f32),
                pltpu.VMEM((2, rows, rows), f32),
                pltpu.VMEM((rows, rows), f32),
                pltpu.VMEM((2, rows, rows // 2), f32),
                pltpu.SemaphoreType.REGULAR,
                dma((1,)), dma((5,)), dma((4 * NS,)), dma((NS + 1,)), dma((NU + 1,)), dma((4,)), dma((2,)), dma((9,)),
            ],
            compiler_params=pltpu.CompilerParams(
                collective_id=0, has_side_effects=True, vmem_limit_bytes=56 * 1024 * 1024),
        )(a_local)

    part_spec = P(("batch", "row"), "col")
    return jax.shard_map(local_fn, mesh=mesh, in_specs=(part_spec,), out_specs=part_spec, check_vma=False)
```

```python
import jax
import jax.numpy as jnp
from jax import lax
from jax.experimental import pallas as pl
from jax.experimental.pallas import tpu as pltpu
from jax.sharding import PartitionSpec as P

MESH = pl.DeviceIdType.MESH
PW = 256
NU = 15
XU = 128
NS = 8


def mm(a, b):
    return lax.dot_general(a, b, (((1,), (1,)), ((), ())), preferred_element_type=jnp.float32)


def mn(a, b):
    return lax.dot_general(a, b, (((1,), (0,)), ((), ())), preferred_element_type=jnp.float32)


def kernel(a_ref, o_ref, X, Y, W, T0, T1, Pa, Pb, Qa, QD, R, PR, XA, XB, far, ld, s_z, r_y, r_d, r_w, r_p, r_r, r_x):
    rows, m = a_ref.shape
    ku = NU * PW + XU
    kd = m - ku
    nd, xd = kd // PW, kd % PW
    half = rows // 2
    st = half // NS
    us = rows // NS
    z = lax.axis_index("row")
    c = lax.axis_index("col")
    y = c // 2
    k = c % 2
    sib = 2 * y + 1 - k

    def rcopy(src, dst, ss, rs, row, col):
        return pltpu.make_async_remote_copy(
            src_ref=src, dst_ref=dst, send_sem=ss, recv_sem=rs, device_id={"row": row, "col": col}, device_id_type=MESH)

    def wait_recv(ref, sem):
        pltpu.make_async_copy(ref, ref, sem).wait()

    def up(p, w=PW):
        return pl.ds(pl.multiple_of(p * PW, 128), w)

    def dn(p, w=PW):
        return pl.ds(pl.multiple_of(ku + p * PW, 128), w)

    def rs_(h, s, n=1):
        return pl.ds(pl.multiple_of(h * half + s * st, st), n * st)

    def us_(s):
        return pl.ds(pl.multiple_of(s * us, us), us)

    DALL = pl.ds(ku, kd)
    UALL = pl.ds(0, ku)
    C0, C1 = pl.ds(0, half), pl.ds(half, half)
    COLS = (C0, C1)

    def each(lo, hi, fn):
        lax.fori_loop(lo, hi, lambda i, u: (fn(i), u)[1], 0)

    load = pltpu.make_async_copy(a_ref, X.at[k], ld.at[0])

    def near(sem):
        for dz in (-1, 1):
            @pl.when((z + dz >= 0) & (z + dz <= 3))
            def _():
                for kk in range(2):
                    pl.semaphore_signal(sem, inc=1, device_id={"row": z + dz, "col": 2 * y + kk}, device_id_type=MESH)
        for dc in range(1, 4):
            pl.semaphore_signal(sem, inc=1, device_id={"row": z, "col": (c + dc) % 4}, device_id_type=MESH)

    n_near = jnp.where((z == 0) | (z == 3), 5, 7)
    bar = pltpu.get_barrier_semaphore()
    near(bar)
    load.start()
    pl.semaphore_wait(bar, n_near)

    def z0_u(q, w=PW):
        return rcopy(a_ref.at[:, up(q, w)], Y.at[k, :, up(q, w)], s_z.at[0], r_y.at[q], 1, c)

    def z0_d(t):
        r = rs_(0, t)
        return rcopy(a_ref.at[r, DALL], Y.at[k, r, DALL], s_z.at[0], r_y.at[2 * NS + t], 1, c)

    def z3_d(t):
        r = rs_(t % 2, t // 2)
        return rcopy(a_ref.at[r, DALL], Y.at[k, r, DALL], s_z.at[0], r_y.at[t], 2, c)

    def z3_u(s):
        r = us_(s)
        return rcopy(a_ref.at[r, UALL], Y.at[k, r, UALL], s_z.at[0], r_y.at[2 * NS + s], 2, c)

    def z1_u(q, w=PW):
        return rcopy(a_ref.at[:, up(q, w)], W.at[k, :, up(q, w)], s_z.at[0], r_w.at[q], 2, 2 * y + 1)

    def z2_d(t):
        h, s = t % 2, t // 2
        return rcopy(a_ref.at[rs_(h, s), DALL], W.at[k, rs_(1, s), pl.ds(0, kd)], s_z.at[0], r_w.at[jnp.where(s < 6, 1 + s // 2, s - 2)], 1, 2 * y + h)

    @pl.when(z == 0)
    def _():
        each(0, NU, lambda q: z0_u(q).start())
        z0_u(NU, XU).start()
        each(0, 2 * NS, lambda t: z0_d(t).start())

    @pl.when(z == 3)
    def _():
        each(0, 2 * NS, lambda t: z3_d(t).start())
        each(0, NS, lambda s: z3_u(s).start())

    x_d = rcopy(a_ref.at[:, DALL], X.at[k, :, DALL], s_z.at[1], r_d.at[NS], z, sib)
    x_u = rcopy(a_ref.at[:, UALL], X.at[k, :, UALL], s_z.at[1], r_d.at[NS], z, sib)

    @pl.when(z == 1)
    def _():
        each(0, NU, lambda q: z1_u(q).start())
        z1_u(NU, XU).start()
        x_d.start()

    @pl.when(z == 2)
    def _():
        z2_d(0).start()
        z2_d(1).start()
        x_u.start()

    near(far)

    Pa[...] = jnp.zeros_like(Pa)
    Qa[...] = jnp.zeros_like(Qa)
    Pb[...] = jnp.zeros_like(Pb)
    load.wait()
    dq = jnp.where(z == 1, 1, 0)

    def diag(p):
        cs = pl.ds(pl.multiple_of(p * 512, 512), 512)
        Qa[dq] += mm(X[k, :, cs], X[k, :, cs])

    each(0, m // 512, diag)

    def slot(owner):
        return (c - owner + 3) % 4

    dsend = rcopy(Qa.at[dq], R.at[slot(z)], s_z.at[3], r_r.at[0], z, z)

    @pl.when(c != z)
    def _():
        dsend.start()

    def u_fwd(q, w=PW):
        return rcopy(Y.at[k, :, up(q, w)], W.at[k, :, up(q, w)], s_z.at[0], r_w.at[q], 2, 2 * y)

    def zU(q, w=PW):
        wait_recv(Y.at[k, :, up(q, w)], r_y.at[q])
        Qa[0] += mm(X[k, :, up(q, w)], Y[k, :, up(q, w)])

    def turn(p, w=PW):
        for h in range(2):
            T1[h, up(p, w), :] = X[h, :, dn(p, w)].T

    def d_sib(t):
        return rcopy(Y.at[k, rs_(0, t), DALL], Y.at[k, rs_(0, t), DALL], s_z.at[1], r_d.at[t // NS], z, sib)

    def zD(t):
        wait_recv(Y.at[k, rs_(0, t), DALL], r_y.at[2 * NS + t])
        d_sib(t).start()

    def brows(b):
        return pl.ds(pl.multiple_of(b * half, half), half)

    def wait_w(r, n):
        wait_recv(W.at[:, r, pl.ds(0, kd)], r_w.at[n])

    CA = pl.ds(0, rows)
    peer = (c + 2) % 4

    def r3(u):
        return rs_(0, 4 * u, 4)

    def r2(s, n=2):
        return rs_(1, s, n)

    def xsend(src, dst, n):
        return rcopy(src, dst, s_z.at[2], r_x.at[n], 1, peer)

    x31 = xsend(Pa.at[1, rs_(0, 0, NS)], XA.at[rs_(0, 0, NS)], 0)

    def x30(b, u):
        return xsend(Pb.at[b, r3(u)], XB.at[b, r3(u)], 1 + 2 * b + u)

    def x21(s, n, rs):
        return xsend(Pa.at[1, r2(s, n)], XA.at[r2(s, n)], rs)

    def x20(b, s, n, rs):
        return xsend(Pb.at[b, r2(s, n)], XB.at[b, r2(s, n)], rs)

    def msend(src, i, s, n, j, cols, rs):
        return rcopy(src, PR.at[i, rs_(k, s, n), cols], s_z.at[2], r_p.at[rs], 2, j)

    m31 = msend(Pa.at[1, rs_(0, 0, NS)], 1, 0, NS, 3, CA, 0)

    def m30(b, u):
        src = Pb.at[b, r3(u)]
        if b == 0:
            return msend(src, 1, 4 * u, 4, 0, C0, 0)
        return rcopy(src, R.at[2, rs_(k, 4 * u, 4), C1], s_z.at[2], r_r.at[1], 3, 0)

    def m30r(u):
        return rcopy(Pb.at[1, r3(u)], PR.at[1, rs_(k, 4 * u, 4), C1], s_z.at[2], r_p.at[1 + u], 2, 2)

    def m21(s, n, rs):
        return msend(Pa.at[1, r2(s, n)], 0, s, n, 1, CA, rs)

    def m20(b, s, n, rs):
        return msend(Pb.at[b, r2(s, n)], 0, s, n, 0, COLS[b], rs)

    def d2(src, j, cols):
        return rcopy(src, R.at[1, rs_(k, 7), cols], s_z.at[2], r_r.at[1], 2, j)

    d21 = d2(Pa.at[1, r2(7, 1)], 1, CA)
    d20 = [d2(Pb.at[b, r2(7, 1)], 0, COLS[b]) for b in range(2)]

    def part1(r):
        Pa[1, r, :] = mn(W[0, r, :kd], T1[0]) + mn(W[1, r, :kd], T1[1])

    def part0(r, b):
        Pb[b, r, :] = mn(W[0, r, :kd], T0[0, b]) + mn(W[1, r, :kd], T0[1, b])

    q_u = rcopy(Qa.at[0], R.at[slot(0)], s_z.at[4], r_r.at[0], 1, 0)

    def q_d(b):
        return rcopy(QD.at[b], PR.at[y, rs_(k, 0, NS), COLS[b]], s_z.at[4], r_r.at[1], 1, 0)

    @pl.when(z == 1)
    def _():
        wait_recv(X.at[1 - k, :, DALL], r_d.at[NS])

        def step_u(q):
            zU(q)

            @pl.when(q < 5)
            def _():
                u_fwd(q).start()

            turn(q)

        each(0, NU, step_u)
        zU(NU, XU)
        each(NU, nd, turn)
        if xd:
            turn(nd, xd)

        @pl.when(c != 0)
        def _():
            q_u.start()

        pl.semaphore_wait(far, n_near)

        def step(i):
            @pl.when(i < 2 * NS)
            def _():
                zD(i)

            @pl.when(i == 3)
            def _():
                wait_w(rs_(0, 0, NS), 0)
                part1(rs_(0, 0, NS))

                @pl.when(y == 0)
                def _():
                    x31.start()

                each(5, 10, lambda q: u_fwd(q).start())

            @pl.when((i == 5) & (y == 1))
            def _():
                wait_recv(XA.at[rs_(0, 0, NS)], r_x.at[0])
                Pa[1, rs_(0, 0, NS), :] += XA[rs_(0, 0, NS), :]
                m31.start()

            @pl.when(i == 16)
            def _():
                def chunk(n):
                    ch = jnp.where(n == 0, k, 1 - k)

                    @pl.when(n == 1)
                    def _():
                        wait_recv(Y.at[1 - k, brows(1), DALL], r_d.at[1])

                    Pb[1, pl.ds(0, rows - st), :] += mm(W[ch, pl.ds(0, rows - st), :kd], Y[ch, brows(1), DALL])

                each(0, 2, chunk)

                @pl.when(y == 0)
                def _():
                    for u in range(2):
                        m30(1, u).start()

                @pl.when(y == 1)
                def _():
                    for u in range(2):
                        m30r(u).start()
                    x20(1, 0, 7, 8).start()

            @pl.when((i == 7) | (i == 17))
            def _():
                b = jnp.where(i == 7, 0, 1)

                @pl.when(b == 0)
                def _():
                    wait_recv(Y.at[1 - k, brows(0), DALL], r_d.at[0])

                for h in range(2):
                    T0[h, b] = Y[h, brows(b), DALL].T

                @pl.when(b == 0)
                def _():
                    part0(rs_(0, 0, NS), 0)

                    @pl.when(y == 1)
                    def _():
                        for u in range(2):
                            x30(0, u).start()

            @pl.when((i == 7) | (i == 17))
            def _():
                b = jnp.where(i == 7, 0, 1)
                r = rs_(k, 0, NS)
                QD[b] = mn(X[0, r, DALL], T0[0, b]) + mn(X[1, r, DALL], T0[1, b])
                for bb in range(2):
                    @pl.when((b == bb) & (c != 0))
                    def _():
                        q_d(bb).start()

            @pl.when(i == 7)
            def _():
                each(10, NU, lambda q: u_fwd(q).start())
                u_fwd(NU, XU).start()

            @pl.when((i == 9) & (y == 0))
            def _():
                for u in range(2):
                    wait_recv(XB.at[0, r3(u)], r_x.at[1 + u])
                    Pb[0, r3(u), :] += XB[0, r3(u), :]
                    m30(0, u).start()

            @pl.when((i == 8) | (i == 9) | (i == 13))
            def _():
                g = jnp.where(i == 13, 2, i - 8)
                wait_w(r2(2 * g), 1 + g)
                part1(r2(2 * g))
                part0(r2(2 * g), 0)

                @pl.when(y == 1)
                def _():
                    x21(2 * g, 2, 5 + g).start()
                    x20(0, 2 * g, 2, 5 + g).start()

            @pl.when(((i == 10) | (i == 11) | (i == 15)) & (y == 0))
            def _():
                g = jnp.where(i == 15, 2, i - 10)
                wait_recv(XA.at[pl.ds(0, 48)], r_x.at[5 + g])
                Pa[1, r2(2 * g), :] += XA[r2(2 * g), :]
                Pb[0, r2(2 * g), :] += XB[0, r2(2 * g), :]
                m21(2 * g, 2, 1).start()
                m20(0, 2 * g, 2, 1).start()

            @pl.when((i == 17) & (y == 0))
            def _():
                wait_recv(XA.at[pl.ds(0, 24)], r_x.at[3])
                Pa[1, r2(6, 1), :] += XA[r2(6, 1), :]
                m21(6, 1, 2).start()
                Pb[0, r2(6, 1), :] += XB[0, r2(6, 1), :]
                m20(0, 6, 1, 3).start()

            @pl.when((i == 14) | (i == 18))
            def _():
                t = jnp.where(i == 14, 6, 7)
                wait_w(r2(t, 1), t - 2)
                part1(r2(t, 1))

                @pl.when((y == 1) & (i == 18))
                def _():
                    d21.start()

                @pl.when((y == 0) & (i == 18))
                def _():
                    m21(7, 1, 2).start()

                part0(r2(t, 1), 0)

                @pl.when((y == 1) & (i == 14))
                def _():
                    x21(6, 1, 3).start()
                    x20(0, 6, 1, 3).start()

                @pl.when((y == 1) & (i == 18))
                def _():
                    d20[0].start()

                @pl.when((y == 0) & (i == 18))
                def _():
                    m20(0, 7, 1, 3).start()
                    wait_recv(XB.at[1, r2(0, 7)], r_x.at[8])
                    Pb[1, r2(0, 7), :] += XB[1, r2(0, 7), :]
                    m20(1, 0, 7, 2).start()

                @pl.when(i == 18)
                def _():
                    part0(r2(7, 1), 1)

                    @pl.when(y == 1)
                    def _():
                        d20[1].start()

                    @pl.when(y == 0)
                    def _():
                        m20(1, 7, 1, 3).start()

        each(0, 19, step)

    def d_fwd(t):
        h, s = t % 2, t // 2
        return rcopy(Y.at[k, rs_(h, s), DALL], W.at[k, rs_(0, s), pl.ds(0, kd)], s_z.at[0], r_w.at[0], 1, 2 * y + h)

    def u_sib(s):
        return rcopy(Y.at[k, us_(s), UALL], Y.at[k, us_(s), UALL], s_z.at[1], r_d.at[s], z, sib)

    def q1send(s):
        return rcopy(Qa.at[1, us_(s)], R.at[c, us_(s)], s_z.at[4], r_r.at[0], 3, 2)

    def y2(q, w=PW):
        wait_recv(W.at[:, :, up(q, w)], r_w.at[q])
        Pa[0] += mm(X[0, :, up(q, w)], W[0, :, up(q, w)]) + mm(X[1, :, up(q, w)], W[1, :, up(q, w)])

    def y3(b, q, w=PW):
        r = pl.ds(b * half, half)
        Pa[1, r, :] += mm(Y[0, r, up(q, w)], W[0, :, up(q, w)]) + mm(Y[1, r, up(q, w)], W[1, :, up(q, w)])

    def wait_ysib(s):
        wait_recv(Y.at[1 - k, us_(s), UALL], r_d.at[s])

    def s3(r, cols=CA):
        return rcopy(Pa.at[1, r, cols], R.at[y, r, cols], s_z.at[2], r_r.at[0], 3, k)

    s2 = rcopy(Pa.at[0], R.at[0], s_z.at[2], r_r.at[0], 2, k)

    def add(i, r, cols):
        Pa[i, r, cols] += PR[i, r, cols]

    def wait_pr(n, cols, sem):
        wait_recv(PR.at[0, pl.ds(0, n), cols], r_p.at[sem])

    def strip31(s):
        wait_ysib(s)
        r = us_(s)
        Pa[1, r, :] = mm(Y[0, r, UALL], W[0, :, :ku]) + mm(Y[1, r, UALL], W[1, :, :ku])

        @pl.when(y == 1)
        def _():
            add(1, r, CA)

        s3(r).start()

    @pl.when(z == 2)
    def _():
        def step_d(t):
            wait_recv(Y.at[k, rs_(t % 2, t // 2), DALL], r_y.at[t])
            d_fwd(t).start()

            @pl.when(t == 1)
            def _():
                wait_recv(X.at[1 - k, :, UALL], r_d.at[NS])

            @pl.when((k == 1) & (t >= 1))
            def _():
                y2(t - 1)

            r = rs_(t % 2, t // 2)
            Qa[1, r, :] = mm(Y[k, r, DALL], X[k, :, DALL])

        each(0, 2 * NS, step_d)
        each(2, 2 * NS, lambda t: z2_d(t).start())

        pl.semaphore_wait(far, n_near)

        @pl.when(k == 1)
        def _():
            y2(NU, XU)

            @pl.when(y == 1)
            def _():
                s2.start()


        def q1(s):
            Qa[1, us_(s), :] += mm(Y[k, us_(s), UALL], X[k, :, UALL])
            q1send(s).start()

        def step_u(s):
            @pl.when((k == 0) & (s >= 1))
            def _():
                y2(2 * s - 1)

            @pl.when(k == 0)
            def _():
                y2(2 * s)

            @pl.when((k == 0) & (s == 4))
            def _():
                each(0, 4, wait_ysib)
                each(0, 7, lambda q: y3(0, q))

            @pl.when((k == 0) & (s >= 4))
            def _():
                y3(0, 2 * s - 1)
                y3(0, 2 * s)

            wait_recv(Y.at[k, us_(s), UALL], r_y.at[2 * NS + s])
            u_sib(s).start()

            @pl.when((k == 1) & (y == 1) & (s == 4))
            def _():
                wait_recv(PR.at[1], r_p.at[0])

            @pl.when((k == 1) & (s >= 4) & (s <= 6))
            def _():
                each(2 * s - 8, 2 * s - 6, strip31)

            @pl.when((k == 1) | (s < NS - 1))
            def _():
                q1(s)

        each(0, NS, step_u)

        @pl.when(k == 1)
        def _():
            each(NS - 2, NS, strip31)

            @pl.when(y == 0)
            def _():
                wait_pr(192, CA, 1)
                for h in range(2):
                    add(0, rs_(h, 0, 6), CA)
                wait_pr(64, CA, 2)
                for h in range(2):
                    add(0, rs_(h, 6, 2), CA)

        @pl.when(k == 0)
        def _():
            y2(NU, XU)

            @pl.when(y == 1)
            def _():
                s2.start()

            y3(0, NU, XU)
            each(NS - 1, NS - y, q1)

            @pl.when(y == 0)
            def _():
                wait_pr(rows, C0, 0)
                add(1, pl.ds(0, half), C0)


            @pl.when(y == 0)
            def _():
                s3(pl.ds(0, half)).start()

            @pl.when(y == 1)
            def _():
                s3(pl.ds(0, half), C0).start()

            each(4, NS, wait_ysib)

            def low(b):
                r = pl.ds(pl.multiple_of(b * half, half), half)
                Pa[1, r, :] = mm(Y[0, r, UALL], W[0, :, :ku]) + mm(Y[1, r, UALL], W[1, :, :ku])

            each(1 + k, 2, low)

            @pl.when(y == 0)
            def _():
                add(1, pl.ds(half, half), C0)

            @pl.when(y == 0)
            def _():
                s3(pl.ds(half, half)).start()

            @pl.when(y == 1)
            def _():
                s3(pl.ds(half, half), C0).start()

            each(NS - 1, NS - 1 + y, q1)

            @pl.when(y == 1)
            def _():
                for u in range(2):
                    wait_pr(half, C1, 1 + u)
                    for h in range(2):
                        add(1, rs_(h, 4 * u, 4), C1)
                        s3(rs_(h, 4 * u, 4), C1).start()

            @pl.when(y == 0)
            def _():
                wait_pr(192, C0, 1)
                for h in range(2):
                    add(0, rs_(h, 0, 6), C0)
                wait_pr(224, C1, 2)
                for h in range(2):
                    add(0, rs_(h, 0, 7), C1)
                wait_pr(96, C0, 3)
                for h in range(2):
                    add(0, rs_(h, 6, 2), C0)
                    add(0, rs_(h, 7), C1)

    @pl.when((z == 0) | (z == 3))
    def _():
        pl.semaphore_wait(far, n_near)

    @pl.when(c > z)
    def _():
        o_ref[...] = jnp.zeros_like(o_ref)

    @pl.when(c == z)
    def _():
        wait_recv(R.at[pl.ds(0, 3)], r_r.at[0])
        total = Qa[dq] + R[0] + R[1] + R[2]
        diff = lax.broadcasted_iota(jnp.int32, (rows, rows), 0) - lax.broadcasted_iota(jnp.int32, (rows, rows), 1)
        o_ref[...] = jnp.where(diff >= 0, total, 0.0).astype(o_ref.dtype)

    @pl.when((z == 1) & (c == 0))
    def _():
        wait_recv(R.at[pl.ds(0, 3)], r_r.at[0])
        Qa[0] += R[0] + R[1] + R[2]
        wait_recv(R.at[pl.ds(0, 3), pl.ds(0, half)], r_r.at[1])
        for b in range(2):
            PR[0, pl.ds(0, half), COLS[b]] = QD[b]
        o_ref[...] = (Qa[0] + PR[0] + PR[1]).astype(o_ref.dtype)

    @pl.when((z == 2) & (y == 0))
    def _():
        wait_recv(R.at[0], r_r.at[0])
        wait_recv(R.at[1, pl.ds(0, 32)], r_r.at[1])
        for h in range(2):
            Pa[0, rs_(h, 7), :] += R[1, rs_(h, 7), :]
        o_ref[...] = (Pa[0] + R[0]).astype(o_ref.dtype)

    @pl.when((z == 3) & (c == 2))
    def _():
        wait_recv(R, r_r.at[0])
        o_ref[...] = (R[0] + R[1] + R[2] + R[3]).astype(o_ref.dtype)

    @pl.when((z == 3) & (y == 0))
    def _():
        wait_recv(R.at[pl.ds(0, 2)], r_r.at[0])

        @pl.when(k == 0)
        def _():
            wait_recv(R.at[2, :, C1], r_r.at[1])
            R[0, :, C1] += R[2, :, C1]

        o_ref[...] = (R[0] + R[1]).astype(o_ref.dtype)

    @pl.when(c != z)
    def _():
        wait_recv(Qa.at[0], s_z.at[3])

    @pl.when((z == 0) | (z == 3))
    def _():
        wait_recv(X.at[k], s_z.at[0])

    @pl.when(z == 1)
    def _():
        wait_recv(W.at[:, :, pl.ds(0, ku)], s_z.at[0])
        wait_recv(W.at[:, :, pl.ds(0, kd)], s_z.at[1])
        wait_recv(Pa, s_z.at[2])

        @pl.when(c != 0)
        def _():
            wait_recv(R.at[pl.ds(0, 3), pl.ds(0, half)], s_z.at[4])

    @pl.when(z == 2)
    def _():
        wait_recv(W.at[:, :, pl.ds(0, kd)], s_z.at[0])
        wait_recv(W.at[:, :, pl.ds(0, ku)], s_z.at[1])
        wait_recv(Qa.at[1], s_z.at[4])

        @pl.when(y == 0)
        def _():
            wait_recv(Pa.at[0], s_z.at[2])

        @pl.when(y == 1)
        def _():
            wait_recv(Pa, s_z.at[2])


def solution(mesh):
    def local_fn(a_local):
        rows, m = a_local.shape
        kd = m - NU * PW - XU
        f32, bf16 = jnp.float32, jnp.bfloat16
        dma = pltpu.SemaphoreType.DMA
        return pl.pallas_call(
            kernel,
            out_shape=pltpu.VMEM((rows, rows), bf16),
            in_specs=[pl.BlockSpec(memory_space=pl.ANY)],
            out_specs=pl.BlockSpec(memory_space=pltpu.VMEM),
            scratch_shapes=[
                pltpu.VMEM((2, rows, m), bf16),
                pltpu.VMEM((2, rows, m), bf16),
                pltpu.VMEM((2, rows, kd), bf16),
                pltpu.VMEM((2, 2, kd, rows // 2), bf16),
                pltpu.VMEM((2, kd, rows), bf16),
                pltpu.VMEM((2, rows, rows), f32),
                pltpu.VMEM((2, rows, rows // 2), f32),
                pltpu.VMEM((2, rows, rows), f32),
                pltpu.VMEM((2, rows // 2, rows // 2), f32),
                pltpu.VMEM((4, rows, rows), f32),
                pltpu.VMEM((2, rows, rows), f32),
                pltpu.VMEM((rows, rows), f32),
                pltpu.VMEM((2, rows, rows // 2), f32),
                pltpu.SemaphoreType.REGULAR,
                dma((1,)), dma((5,)), dma((4 * NS,)), dma((NS + 1,)), dma((NU + 1,)), dma((4,)), dma((2,)), dma((9,)),
            ],
            compiler_params=pltpu.CompilerParams(
                collective_id=0, has_side_effects=True, vmem_limit_bytes=56 * 1024 * 1024),
        )(a_local)

    part_spec = P(("batch", "row"), "col")
    return jax.shard_map(local_fn, mesh=mesh, in_specs=(part_spec,), out_specs=part_spec, check_vma=False)
```

```python
import jax
import jax.numpy as jnp
from jax import lax
from jax.experimental import pallas as pl
from jax.experimental.pallas import tpu as pltpu
from jax.sharding import PartitionSpec as P

MESH = pl.DeviceIdType.MESH
PW = 256
NU = 15
XU = 128
NS = 8


def mm(a, b):
    return lax.dot_general(a, b, (((1,), (1,)), ((), ())), preferred_element_type=jnp.float32)


def mn(a, b):
    return lax.dot_general(a, b, (((1,), (0,)), ((), ())), preferred_element_type=jnp.float32)


def kernel(a_ref, o_ref, X, Y, W, T0, T1, Pa, Pb, Qa, QD, R, PR, XA, XB, far, ld, s_z, r_y, r_d, r_w, r_p, r_r, r_x):
    rows, m = a_ref.shape
    ku = NU * PW + XU
    kd = m - ku
    nd, xd = kd // PW, kd % PW
    half = rows // 2
    st = half // NS
    us = rows // NS
    z = lax.axis_index("row")
    c = lax.axis_index("col")
    y = c // 2
    k = c % 2
    sib = 2 * y + 1 - k

    def rcopy(src, dst, ss, rs, row, col):
        return pltpu.make_async_remote_copy(
            src_ref=src, dst_ref=dst, send_sem=ss, recv_sem=rs, device_id={"row": row, "col": col}, device_id_type=MESH)

    def wait_recv(ref, sem):
        pltpu.make_async_copy(ref, ref, sem).wait()

    def up(p, w=PW):
        return pl.ds(pl.multiple_of(p * PW, 128), w)

    def dn(p, w=PW):
        return pl.ds(pl.multiple_of(ku + p * PW, 128), w)

    def rs_(h, s, n=1):
        return pl.ds(pl.multiple_of(h * half + s * st, st), n * st)

    def us_(s):
        return pl.ds(pl.multiple_of(s * us, us), us)

    DALL = pl.ds(ku, kd)
    UALL = pl.ds(0, ku)
    C0, C1 = pl.ds(0, half), pl.ds(half, half)
    COLS = (C0, C1)

    def each(lo, hi, fn):
        lax.fori_loop(lo, hi, lambda i, u: (fn(i), u)[1], 0)

    load = pltpu.make_async_copy(a_ref, X.at[k], ld.at[0])

    def near(sem):
        for dz in (-1, 1):
            @pl.when((z + dz >= 0) & (z + dz <= 3))
            def _():
                for kk in range(2):
                    pl.semaphore_signal(sem, inc=1, device_id={"row": z + dz, "col": 2 * y + kk}, device_id_type=MESH)
        for dc in range(1, 4):
            pl.semaphore_signal(sem, inc=1, device_id={"row": z, "col": (c + dc) % 4}, device_id_type=MESH)

    n_near = jnp.where((z == 0) | (z == 3), 5, 7)
    bar = pltpu.get_barrier_semaphore()
    near(bar)
    load.start()
    pl.semaphore_wait(bar, n_near)

    def z0_u(q, w=PW):
        return rcopy(a_ref.at[:, up(q, w)], Y.at[k, :, up(q, w)], s_z.at[0], r_y.at[q], 1, c)

    def z0_d(t):
        r = rs_(0, t)
        return rcopy(a_ref.at[r, DALL], Y.at[k, r, DALL], s_z.at[0], r_y.at[2 * NS + t], 1, c)

    def z3_d(t):
        r = rs_(t % 2, t // 2)
        return rcopy(a_ref.at[r, DALL], Y.at[k, r, DALL], s_z.at[0], r_y.at[t], 2, c)

    def z3_u(s):
        r = us_(s)
        return rcopy(a_ref.at[r, UALL], Y.at[k, r, UALL], s_z.at[0], r_y.at[2 * NS + s], 2, c)

    def z1_u(q, w=PW):
        return rcopy(a_ref.at[:, up(q, w)], W.at[k, :, up(q, w)], s_z.at[0], r_w.at[q], 2, 2 * y + 1)

    def z2_d(t):
        h, s = t % 2, t // 2
        return rcopy(a_ref.at[rs_(h, s), DALL], W.at[k, rs_(1, s), pl.ds(0, kd)], s_z.at[0], r_w.at[jnp.where(s < 6, 1 + s // 2, s - 2)], 1, 2 * y + h)

    @pl.when(z == 0)
    def _():
        each(0, NU, lambda q: z0_u(q).start())
        z0_u(NU, XU).start()
        each(0, 2 * NS, lambda t: z0_d(t).start())

    @pl.when(z == 3)
    def _():
        each(0, 2 * NS, lambda t: z3_d(t).start())
        each(0, NS, lambda s: z3_u(s).start())

    x_d = rcopy(a_ref.at[:, DALL], X.at[k, :, DALL], s_z.at[1], r_d.at[NS], z, sib)
    x_u = rcopy(a_ref.at[:, UALL], X.at[k, :, UALL], s_z.at[1], r_d.at[NS], z, sib)

    @pl.when(z == 1)
    def _():
        each(0, NU, lambda q: z1_u(q).start())
        z1_u(NU, XU).start()
        x_d.start()

    @pl.when(z == 2)
    def _():
        z2_d(0).start()
        z2_d(1).start()
        x_u.start()

    near(far)

    Pa[...] = jnp.zeros_like(Pa)
    Qa[...] = jnp.zeros_like(Qa)
    Pb[...] = jnp.zeros_like(Pb)
    load.wait()
    dq = jnp.where(z == 1, 1, 0)

    def diag(p):
        cs = pl.ds(pl.multiple_of(p * 512, 512), 512)
        Qa[dq] += mm(X[k, :, cs], X[k, :, cs])

    each(0, m // 512, diag)

    def slot(owner):
        return (c - owner + 3) % 4

    dsend = rcopy(Qa.at[dq], R.at[slot(z)], s_z.at[3], r_r.at[0], z, z)

    @pl.when(c != z)
    def _():
        dsend.start()

    def u_fwd(q, w=PW):
        return rcopy(Y.at[k, :, up(q, w)], W.at[k, :, up(q, w)], s_z.at[0], r_w.at[q], 2, 2 * y)

    def zU(q, w=PW):
        wait_recv(Y.at[k, :, up(q, w)], r_y.at[q])
        Qa[0] += mm(X[k, :, up(q, w)], Y[k, :, up(q, w)])

    def turn(p, w=PW):
        for h in range(2):
            T1[h, up(p, w), :] = X[h, :, dn(p, w)].T

    def d_sib(t):
        return rcopy(Y.at[k, rs_(0, t), DALL], Y.at[k, rs_(0, t), DALL], s_z.at[1], r_d.at[t // NS], z, sib)

    def zD(t):
        wait_recv(Y.at[k, rs_(0, t), DALL], r_y.at[2 * NS + t])
        d_sib(t).start()

    def brows(b):
        return pl.ds(pl.multiple_of(b * half, half), half)

    def wait_w(r, n):
        wait_recv(W.at[:, r, pl.ds(0, kd)], r_w.at[n])

    CA = pl.ds(0, rows)
    peer = (c + 2) % 4

    def r3(u):
        return rs_(0, 4 * u, 4)

    def r2(s, n=2):
        return rs_(1, s, n)

    def xsend(src, dst, n):
        return rcopy(src, dst, s_z.at[2], r_x.at[n], 1, peer)

    x31 = xsend(Pa.at[1, rs_(0, 0, NS)], XA.at[rs_(0, 0, NS)], 0)

    def x30(b, u):
        return xsend(Pb.at[b, r3(u)], XB.at[b, r3(u)], 1 + 2 * b + u)

    def x21(s, n, rs):
        return xsend(Pa.at[1, r2(s, n)], XA.at[r2(s, n)], rs)

    def x20(b, s, n, rs):
        return xsend(Pb.at[b, r2(s, n)], XB.at[b, r2(s, n)], rs)

    def msend(src, i, s, n, j, cols, rs):
        return rcopy(src, PR.at[i, rs_(k, s, n), cols], s_z.at[2], r_p.at[rs], 2, j)

    m31 = msend(Pa.at[1, rs_(0, 0, NS)], 1, 0, NS, 3, CA, 0)

    def m30(b, u):
        src = Pb.at[b, r3(u)]
        if b == 0:
            return msend(src, 1, 4 * u, 4, 0, C0, 0)
        return rcopy(src, R.at[2 + y, rs_(k, 4 * u, 4), C1], s_z.at[2], r_r.at[1], 3, 0)

    def m21(s, n, rs):
        return msend(Pa.at[1, r2(s, n)], 0, s, n, 1, CA, rs)

    def m20(b, s, n, rs):
        return msend(Pb.at[b, r2(s, n)], 0, s, n, 0, COLS[b], rs)

    def d2(src, j, cols):
        return rcopy(src, R.at[1, rs_(k, 7), cols], s_z.at[2], r_r.at[1], 2, j)

    d21 = d2(Pa.at[1, r2(7, 1)], 1, CA)
    d20 = [d2(Pb.at[b, r2(7, 1)], 0, COLS[b]) for b in range(2)]

    def part1(r):
        Pa[1, r, :] = mn(W[0, r, :kd], T1[0]) + mn(W[1, r, :kd], T1[1])

    def part0(r, b):
        Pb[b, r, :] = mn(W[0, r, :kd], T0[0, b]) + mn(W[1, r, :kd], T0[1, b])

    q_u = rcopy(Qa.at[0], R.at[slot(0)], s_z.at[4], r_r.at[0], 1, 0)

    def q_d(b):
        return rcopy(QD.at[b], PR.at[y, rs_(k, 0, NS), COLS[b]], s_z.at[4], r_r.at[1], 1, 0)

    @pl.when(z == 1)
    def _():
        wait_recv(X.at[1 - k, :, DALL], r_d.at[NS])

        def step_u(q):
            zU(q)

            @pl.when(q < 5)
            def _():
                u_fwd(q).start()

            turn(q)

        each(0, NU, step_u)
        zU(NU, XU)
        each(NU, nd, turn)
        if xd:
            turn(nd, xd)

        @pl.when(c != 0)
        def _():
            q_u.start()

        pl.semaphore_wait(far, n_near)

        def step(i):
            @pl.when(i < 2 * NS)
            def _():
                zD(i)

            @pl.when(i == 3)
            def _():
                wait_w(rs_(0, 0, NS), 0)
                part1(rs_(0, 0, NS))

                @pl.when(y == 0)
                def _():
                    x31.start()

                each(5, 10, lambda q: u_fwd(q).start())

            @pl.when((i == 5) & (y == 1))
            def _():
                wait_recv(XA.at[rs_(0, 0, NS)], r_x.at[0])
                Pa[1, rs_(0, 0, NS), :] += XA[rs_(0, 0, NS), :]
                m31.start()

            @pl.when(i == 16)
            def _():
                def chunk(n):
                    ch = jnp.where(n == 0, k, 1 - k)

                    @pl.when(n == 1)
                    def _():
                        wait_recv(Y.at[1 - k, brows(1), DALL], r_d.at[1])

                    Pb[1, pl.ds(0, rows - st), :] += mm(W[ch, pl.ds(0, rows - st), :kd], Y[ch, brows(1), DALL])

                each(0, 2, chunk)

                @pl.when(y == 0)
                def _():
                    for u in range(2):
                        m30(1, u).start()

                @pl.when(y == 1)
                def _():
                    x20(1, 0, 4, 8).start()
                    x20(1, 4, 3, 4).start()
                    for u in range(2):
                        m30(1, u).start()

            @pl.when((i == 7) | (i == 17))
            def _():
                b = jnp.where(i == 7, 0, 1)

                @pl.when(b == 0)
                def _():
                    wait_recv(Y.at[1 - k, brows(0), DALL], r_d.at[0])

                for h in range(2):
                    T0[h, b] = Y[h, brows(b), DALL].T

                @pl.when(b == 0)
                def _():
                    part0(rs_(0, 0, NS), 0)

                    @pl.when(y == 1)
                    def _():
                        for u in range(2):
                            x30(0, u).start()

            @pl.when((i == 7) | (i == 17))
            def _():
                b = jnp.where(i == 7, 0, 1)
                r = rs_(k, 0, NS)
                QD[b] = mn(X[0, r, DALL], T0[0, b]) + mn(X[1, r, DALL], T0[1, b])
                for bb in range(2):
                    @pl.when((b == bb) & (c != 0))
                    def _():
                        q_d(bb).start()

            @pl.when(i == 7)
            def _():
                each(10, NU, lambda q: u_fwd(q).start())
                u_fwd(NU, XU).start()

            @pl.when((i == 9) & (y == 0))
            def _():
                for u in range(2):
                    wait_recv(XB.at[0, r3(u)], r_x.at[1 + u])
                    Pb[0, r3(u), :] += XB[0, r3(u), :]
                    m30(0, u).start()

            @pl.when((i == 8) | (i == 9) | (i == 13))
            def _():
                g = jnp.where(i == 13, 2, i - 8)
                wait_w(r2(2 * g), 1 + g)
                part1(r2(2 * g))
                part0(r2(2 * g), 0)

                @pl.when(y == 1)
                def _():
                    x21(2 * g, 2, 5 + g).start()
                    x20(0, 2 * g, 2, 5 + g).start()

            @pl.when(((i == 10) | (i == 11) | (i == 15)) & (y == 0))
            def _():
                g = jnp.where(i == 15, 2, i - 10)
                wait_recv(XA.at[pl.ds(0, 48)], r_x.at[5 + g])
                Pa[1, r2(2 * g), :] += XA[r2(2 * g), :]
                Pb[0, r2(2 * g), :] += XB[0, r2(2 * g), :]
                m21(2 * g, 2, 1).start()
                m20(0, 2 * g, 2, 1).start()

            @pl.when((i == 17) & (y == 0))
            def _():
                wait_recv(XA.at[pl.ds(0, 24)], r_x.at[3])
                Pa[1, r2(6, 1), :] += XA[r2(6, 1), :]
                m21(6, 1, 2).start()
                Pb[0, r2(6, 1), :] += XB[0, r2(6, 1), :]
                m20(0, 6, 1, 3).start()

            @pl.when((i == 14) | (i == 18))
            def _():
                t = jnp.where(i == 14, 6, 7)
                wait_w(r2(t, 1), t - 2)
                part1(r2(t, 1))

                @pl.when((y == 1) & (i == 18))
                def _():
                    d21.start()

                @pl.when((y == 0) & (i == 18))
                def _():
                    m21(7, 1, 2).start()

                part0(r2(t, 1), 0)

                @pl.when((y == 1) & (i == 14))
                def _():
                    x21(6, 1, 3).start()
                    x20(0, 6, 1, 3).start()

                @pl.when((y == 1) & (i == 18))
                def _():
                    d20[0].start()

                @pl.when((y == 0) & (i == 18))
                def _():
                    m20(0, 7, 1, 3).start()
                    for f, n, x in ((0, 4, 8), (4, 3, 4)):
                        wait_recv(XB.at[1, r2(f, n)], r_x.at[x])
                        Pb[1, r2(f, n), :] += XB[1, r2(f, n), :]
                        m20(1, f, n, 2).start()

                @pl.when(i == 18)
                def _():
                    part0(r2(7, 1), 1)

                    @pl.when(y == 1)
                    def _():
                        d20[1].start()

                    @pl.when(y == 0)
                    def _():
                        m20(1, 7, 1, 3).start()

        each(0, 19, step)

    def d_fwd(t):
        h, s = t % 2, t // 2
        return rcopy(Y.at[k, rs_(h, s), DALL], W.at[k, rs_(0, s), pl.ds(0, kd)], s_z.at[0], r_w.at[0], 1, 2 * y + h)

    def u_sib(s):
        return rcopy(Y.at[k, us_(s), UALL], Y.at[k, us_(s), UALL], s_z.at[1], r_d.at[s], z, sib)

    def q1send(s):
        return rcopy(Qa.at[1, us_(s)], R.at[c, us_(s)], s_z.at[4], r_r.at[0], 3, 2)

    def y2(q, w=PW):
        wait_recv(W.at[:, :, up(q, w)], r_w.at[q])
        Pa[0] += mm(X[0, :, up(q, w)], W[0, :, up(q, w)]) + mm(X[1, :, up(q, w)], W[1, :, up(q, w)])

    def y3(b, q, w=PW):
        r = pl.ds(b * half, half)
        Pa[1, r, :] += mm(Y[0, r, up(q, w)], W[0, :, up(q, w)]) + mm(Y[1, r, up(q, w)], W[1, :, up(q, w)])

    def wait_ysib(s):
        wait_recv(Y.at[1 - k, us_(s), UALL], r_d.at[s])

    def s3(r, cols=CA):
        return rcopy(Pa.at[1, r, cols], R.at[y, r, cols], s_z.at[2], r_r.at[0], 3, k)

    s2 = rcopy(Pa.at[0], R.at[0], s_z.at[2], r_r.at[0], 2, k)

    def add(i, r, cols):
        Pa[i, r, cols] += PR[i, r, cols]

    def wait_pr(n, cols, sem):
        wait_recv(PR.at[0, pl.ds(0, n), cols], r_p.at[sem])

    def strip31(s):
        wait_ysib(s)
        r = us_(s)
        Pa[1, r, :] = mm(Y[0, r, UALL], W[0, :, :ku]) + mm(Y[1, r, UALL], W[1, :, :ku])

        @pl.when(y == 1)
        def _():
            add(1, r, CA)

        s3(r).start()

    @pl.when(z == 2)
    def _():
        def step_d(t):
            wait_recv(Y.at[k, rs_(t % 2, t // 2), DALL], r_y.at[t])
            d_fwd(t).start()

            @pl.when(t == 1)
            def _():
                wait_recv(X.at[1 - k, :, UALL], r_d.at[NS])

            @pl.when((k == 1) & (t >= 1))
            def _():
                y2(t - 1)

            r = rs_(t % 2, t // 2)
            Qa[1, r, :] = mm(Y[k, r, DALL], X[k, :, DALL])

        each(0, 2 * NS, step_d)
        each(2, 2 * NS, lambda t: z2_d(t).start())

        pl.semaphore_wait(far, n_near)

        @pl.when(k == 1)
        def _():
            y2(NU, XU)

            @pl.when(y == 1)
            def _():
                s2.start()


        def q1(s):
            Qa[1, us_(s), :] += mm(Y[k, us_(s), UALL], X[k, :, UALL])
            q1send(s).start()

        def step_u(s):
            @pl.when((k == 0) & (s >= 1))
            def _():
                y2(2 * s - 1)

            @pl.when(k == 0)
            def _():
                y2(2 * s)

            @pl.when((k == 0) & (s == 4))
            def _():
                each(0, 4, wait_ysib)
                each(0, 7, lambda q: y3(0, q))

            @pl.when((k == 0) & (s >= 4))
            def _():
                y3(0, 2 * s - 1)
                y3(0, 2 * s)

            wait_recv(Y.at[k, us_(s), UALL], r_y.at[2 * NS + s])
            u_sib(s).start()

            @pl.when((k == 1) & (y == 1) & (s == 4))
            def _():
                wait_recv(PR.at[1], r_p.at[0])

            @pl.when((k == 1) & (s >= 4) & (s <= 6))
            def _():
                each(2 * s - 8, 2 * s - 6, strip31)

            @pl.when((k == 1) | (s < NS - 1))
            def _():
                q1(s)

        each(0, NS, step_u)

        @pl.when(k == 1)
        def _():
            each(NS - 2, NS, strip31)

            @pl.when(y == 0)
            def _():
                wait_pr(192, CA, 1)
                for h in range(2):
                    add(0, rs_(h, 0, 6), CA)
                wait_pr(64, CA, 2)
                for h in range(2):
                    add(0, rs_(h, 6, 2), CA)

        @pl.when(k == 0)
        def _():
            y2(NU, XU)

            @pl.when(y == 1)
            def _():
                s2.start()

            y3(0, NU, XU)
            each(NS - 1, NS - y, q1)

            @pl.when(y == 0)
            def _():
                wait_pr(rows, C0, 0)
                add(1, pl.ds(0, half), C0)


            s3(pl.ds(0, half)).start()
            each(4, NS, wait_ysib)

            def low(b):
                r = pl.ds(pl.multiple_of(b * half, half), half)
                Pa[1, r, :] = mm(Y[0, r, UALL], W[0, :, :ku]) + mm(Y[1, r, UALL], W[1, :, :ku])

            each(1 + k, 2, low)

            @pl.when(y == 0)
            def _():
                add(1, pl.ds(half, half), C0)

            s3(pl.ds(half, half)).start()
            each(NS - 1, NS - 1 + y, q1)

            @pl.when(y == 0)
            def _():
                wait_pr(192, C0, 1)
                for h in range(2):
                    add(0, rs_(h, 0, 6), C0)
                wait_pr(224, C1, 2)
                for h in range(2):
                    add(0, rs_(h, 0, 7), C1)
                wait_pr(96, C0, 3)
                for h in range(2):
                    add(0, rs_(h, 6, 2), C0)
                    add(0, rs_(h, 7), C1)

    @pl.when((z == 0) | (z == 3))
    def _():
        pl.semaphore_wait(far, n_near)

    @pl.when(c > z)
    def _():
        o_ref[...] = jnp.zeros_like(o_ref)

    @pl.when(c == z)
    def _():
        wait_recv(R.at[pl.ds(0, 3)], r_r.at[0])
        total = Qa[dq] + R[0] + R[1] + R[2]
        diff = lax.broadcasted_iota(jnp.int32, (rows, rows), 0) - lax.broadcasted_iota(jnp.int32, (rows, rows), 1)
        o_ref[...] = jnp.where(diff >= 0, total, 0.0).astype(o_ref.dtype)

    @pl.when((z == 1) & (c == 0))
    def _():
        wait_recv(R.at[pl.ds(0, 3)], r_r.at[0])
        Qa[0] += R[0] + R[1] + R[2]
        wait_recv(R.at[pl.ds(0, 3), pl.ds(0, half)], r_r.at[1])
        for b in range(2):
            PR[0, pl.ds(0, half), COLS[b]] = QD[b]
        o_ref[...] = (Qa[0] + PR[0] + PR[1]).astype(o_ref.dtype)

    @pl.when((z == 2) & (y == 0))
    def _():
        wait_recv(R.at[0], r_r.at[0])
        wait_recv(R.at[1, pl.ds(0, 32)], r_r.at[1])
        for h in range(2):
            Pa[0, rs_(h, 7), :] += R[1, rs_(h, 7), :]
        o_ref[...] = (Pa[0] + R[0]).astype(o_ref.dtype)

    @pl.when((z == 3) & (c == 2))
    def _():
        wait_recv(R, r_r.at[0])
        o_ref[...] = (R[0] + R[1] + R[2] + R[3]).astype(o_ref.dtype)

    @pl.when((z == 3) & (y == 0))
    def _():
        wait_recv(R.at[pl.ds(0, 2)], r_r.at[0])

        @pl.when(k == 0)
        def _():
            wait_recv(R.at[2], r_r.at[1])
            R[0, :, C1] += R[2, :, C1] + R[3, :, C1]

        o_ref[...] = (R[0] + R[1]).astype(o_ref.dtype)

    @pl.when(c != z)
    def _():
        wait_recv(Qa.at[0], s_z.at[3])

    @pl.when((z == 0) | (z == 3))
    def _():
        wait_recv(X.at[k], s_z.at[0])

    @pl.when(z == 1)
    def _():
        wait_recv(W.at[:, :, pl.ds(0, ku)], s_z.at[0])
        wait_recv(W.at[:, :, pl.ds(0, kd)], s_z.at[1])
        wait_recv(Pa, s_z.at[2])

        @pl.when(c != 0)
        def _():
            wait_recv(R.at[pl.ds(0, 3), pl.ds(0, half)], s_z.at[4])

    @pl.when(z == 2)
    def _():
        wait_recv(W.at[:, :, pl.ds(0, kd)], s_z.at[0])
        wait_recv(W.at[:, :, pl.ds(0, ku)], s_z.at[1])
        wait_recv(Qa.at[1], s_z.at[4])

        @pl.when(y == 0)
        def _():
            wait_recv(Pa.at[0], s_z.at[2])

        @pl.when(y == 1)
        def _():
            wait_recv(Pa, s_z.at[2])


def solution(mesh):
    def local_fn(a_local):
        rows, m = a_local.shape
        kd = m - NU * PW - XU
        f32, bf16 = jnp.float32, jnp.bfloat16
        dma = pltpu.SemaphoreType.DMA
        return pl.pallas_call(
            kernel,
            out_shape=pltpu.VMEM((rows, rows), bf16),
            in_specs=[pl.BlockSpec(memory_space=pl.ANY)],
            out_specs=pl.BlockSpec(memory_space=pltpu.VMEM),
            scratch_shapes=[
                pltpu.VMEM((2, rows, m), bf16),
                pltpu.VMEM((2, rows, m), bf16),
                pltpu.VMEM((2, rows, kd), bf16),
                pltpu.VMEM((2, 2, kd, rows // 2), bf16),
                pltpu.VMEM((2, kd, rows), bf16),
                pltpu.VMEM((2, rows, rows), f32),
                pltpu.VMEM((2, rows, rows // 2), f32),
                pltpu.VMEM((2, rows, rows), f32),
                pltpu.VMEM((2, rows // 2, rows // 2), f32),
                pltpu.VMEM((4, rows, rows), f32),
                pltpu.VMEM((2, rows, rows), f32),
                pltpu.VMEM((rows, rows), f32),
                pltpu.VMEM((2, rows, rows // 2), f32),
                pltpu.SemaphoreType.REGULAR,
                dma((1,)), dma((5,)), dma((4 * NS,)), dma((NS + 1,)), dma((NU + 1,)), dma((4,)), dma((2,)), dma((9,)),
            ],
            compiler_params=pltpu.CompilerParams(
                collective_id=0, has_side_effects=True, vmem_limit_bytes=56 * 1024 * 1024),
        )(a_local)

    part_spec = P(("batch", "row"), "col")
    return jax.shard_map(local_fn, mesh=mesh, in_specs=(part_spec,), out_specs=part_spec, check_vma=False)
```

```python
import jax
import jax.numpy as jnp
from jax import lax
from jax.experimental import pallas as pl
from jax.experimental.pallas import tpu as pltpu
from jax.sharding import PartitionSpec as P

MESH = pl.DeviceIdType.MESH
PW = 256
NU = 15
XU = 128
NS = 8


def mm(a, b):
    return lax.dot_general(a, b, (((1,), (1,)), ((), ())), preferred_element_type=jnp.float32)


def mn(a, b):
    return lax.dot_general(a, b, (((1,), (0,)), ((), ())), preferred_element_type=jnp.float32)


def kernel(a_ref, o_ref, X, Y, W, T0, T1, Pa, Pb, Qa, QD, R, PR, XA, XB, far, ld, s_z, r_y, r_d, r_w, r_p, r_r, r_x):
    rows, m = a_ref.shape
    ku = NU * PW + XU
    kd = m - ku
    nd, xd = kd // PW, kd % PW
    half = rows // 2
    st = half // NS
    us = rows // NS
    z = lax.axis_index("row")
    c = lax.axis_index("col")
    y = c // 2
    k = c % 2
    sib = 2 * y + 1 - k

    def rcopy(src, dst, ss, rs, row, col):
        return pltpu.make_async_remote_copy(
            src_ref=src, dst_ref=dst, send_sem=ss, recv_sem=rs, device_id={"row": row, "col": col}, device_id_type=MESH)

    def wait_recv(ref, sem):
        pltpu.make_async_copy(ref, ref, sem).wait()

    def up(p, w=PW):
        return pl.ds(pl.multiple_of(p * PW, 128), w)

    def dn(p, w=PW):
        return pl.ds(pl.multiple_of(ku + p * PW, 128), w)

    def rs_(h, s, n=1):
        return pl.ds(pl.multiple_of(h * half + s * st, st), n * st)

    def us_(s):
        return pl.ds(pl.multiple_of(s * us, us), us)

    DALL = pl.ds(ku, kd)
    UALL = pl.ds(0, ku)
    C0, C1 = pl.ds(0, half), pl.ds(half, half)
    COLS = (C0, C1)

    def each(lo, hi, fn):
        lax.fori_loop(lo, hi, lambda i, u: (fn(i), u)[1], 0)

    load = pltpu.make_async_copy(a_ref, X.at[k], ld.at[0])

    def near(sem):
        for dz in (-1, 1):
            @pl.when((z + dz >= 0) & (z + dz <= 3))
            def _():
                for kk in range(2):
                    pl.semaphore_signal(sem, inc=1, device_id={"row": z + dz, "col": 2 * y + kk}, device_id_type=MESH)
        for dc in range(1, 4):
            pl.semaphore_signal(sem, inc=1, device_id={"row": z, "col": (c + dc) % 4}, device_id_type=MESH)

    n_near = jnp.where((z == 0) | (z == 3), 5, 7)
    bar = pltpu.get_barrier_semaphore()
    near(bar)
    load.start()
    pl.semaphore_wait(bar, n_near)

    def z0_u(q, w=PW):
        return rcopy(a_ref.at[:, up(q, w)], Y.at[k, :, up(q, w)], s_z.at[0], r_y.at[q], 1, c)

    def z0_d(t):
        r = rs_(0, t)
        return rcopy(a_ref.at[r, DALL], Y.at[k, r, DALL], s_z.at[0], r_y.at[2 * NS + t], 1, c)

    def z3_d(t):
        r = rs_(t % 2, t // 2)
        return rcopy(a_ref.at[r, DALL], Y.at[k, r, DALL], s_z.at[0], r_y.at[t], 2, c)

    def z3_u(s):
        r = us_(s)
        return rcopy(a_ref.at[r, UALL], Y.at[k, r, UALL], s_z.at[0], r_y.at[2 * NS + s], 2, c)

    def z1_u(q, w=PW):
        return rcopy(a_ref.at[:, up(q, w)], W.at[k, :, up(q, w)], s_z.at[0], r_w.at[q], 2, 2 * y + 1)

    def z2_d(t):
        h, s = t % 2, t // 2
        return rcopy(a_ref.at[rs_(h, s), DALL], W.at[k, rs_(1, s), pl.ds(0, kd)], s_z.at[0], r_w.at[jnp.where(s < 6, 1 + s // 2, s - 2)], 1, 2 * y + h)

    @pl.when(z == 0)
    def _():
        each(0, NU, lambda q: z0_u(q).start())
        z0_u(NU, XU).start()
        each(0, 2 * NS, lambda t: z0_d(t).start())

    @pl.when(z == 3)
    def _():
        each(0, 2 * NS, lambda t: z3_d(t).start())
        each(0, NS, lambda s: z3_u(s).start())

    x_d = rcopy(a_ref.at[:, DALL], X.at[k, :, DALL], s_z.at[1], r_d.at[NS], z, sib)
    x_u = rcopy(a_ref.at[:, UALL], X.at[k, :, UALL], s_z.at[1], r_d.at[NS], z, sib)

    @pl.when(z == 1)
    def _():
        each(0, NU, lambda q: z1_u(q).start())
        z1_u(NU, XU).start()
        x_d.start()

    @pl.when(z == 2)
    def _():
        z2_d(0).start()
        z2_d(1).start()
        x_u.start()

    near(far)

    Pa[...] = jnp.zeros_like(Pa)
    Qa[...] = jnp.zeros_like(Qa)
    Pb[...] = jnp.zeros_like(Pb)
    load.wait()
    dq = jnp.where(z == 1, 1, 0)

    def diag(p):
        cs = pl.ds(pl.multiple_of(p * 512, 512), 512)
        Qa[dq] += mm(X[k, :, cs], X[k, :, cs])

    each(0, m // 512, diag)

    def slot(owner):
        return (c - owner + 3) % 4

    dsend = rcopy(Qa.at[dq], R.at[slot(z)], s_z.at[3], r_r.at[0], z, z)

    @pl.when(c != z)
    def _():
        dsend.start()

    def u_fwd(q, w=PW):
        return rcopy(Y.at[k, :, up(q, w)], W.at[k, :, up(q, w)], s_z.at[0], r_w.at[q], 2, 2 * y)

    def zU(q, w=PW):
        wait_recv(Y.at[k, :, up(q, w)], r_y.at[q])
        Qa[0] += mm(X[k, :, up(q, w)], Y[k, :, up(q, w)])

    def turn(p, w=PW):
        for h in range(2):
            T1[h, up(p, w), :] = X[h, :, dn(p, w)].T

    def d_sib(t):
        return rcopy(Y.at[k, rs_(0, t), DALL], Y.at[k, rs_(0, t), DALL], s_z.at[1], r_d.at[t // NS], z, sib)

    def zD(t):
        wait_recv(Y.at[k, rs_(0, t), DALL], r_y.at[2 * NS + t])
        d_sib(t).start()

    def brows(b):
        return pl.ds(pl.multiple_of(b * half, half), half)

    def wait_w(r, n):
        wait_recv(W.at[:, r, pl.ds(0, kd)], r_w.at[n])

    CA = pl.ds(0, rows)
    peer = (c + 2) % 4

    def r3(u):
        return rs_(0, 4 * u, 4)

    def r2(s, n=2):
        return rs_(1, s, n)

    def xsend(src, dst, n):
        return rcopy(src, dst, s_z.at[2], r_x.at[n], 1, peer)

    x31 = xsend(Pa.at[1, rs_(0, 0, NS)], XA.at[rs_(0, 0, NS)], 0)

    def x30(b, u):
        return xsend(Pb.at[b, r3(u)], XB.at[b, r3(u)], 1 + 2 * b + u)

    def x21(s, n, rs):
        return xsend(Pa.at[1, r2(s, n)], XA.at[r2(s, n)], rs)

    def x20(b, s, n, rs):
        return xsend(Pb.at[b, r2(s, n)], XB.at[b, r2(s, n)], rs)

    def msend(src, i, s, n, j, cols, rs):
        return rcopy(src, PR.at[i, rs_(k, s, n), cols], s_z.at[2], r_p.at[rs], 2, j)

    m31 = msend(Pa.at[1, rs_(0, 0, NS)], 1, 0, NS, 3, CA, 0)

    def m30(b, u):
        src = Pb.at[b, r3(u)]
        if b == 0:
            return msend(src, 1, 4 * u, 4, 0, C0, 0)
        return rcopy(src, R.at[2, rs_(k, 4 * u, 4), C1], s_z.at[2], r_r.at[1], 3, 0)

    def m30r(u):
        return rcopy(Pb.at[1, r3(u)], PR.at[1, rs_(k, 4 * u, 4), C1], s_z.at[2], r_p.at[1 + u], 2, 2)

    def m21(s, n, rs):
        return msend(Pa.at[1, r2(s, n)], 0, s, n, 1, CA, rs)

    def m20(b, s, n, rs):
        return msend(Pb.at[b, r2(s, n)], 0, s, n, 0, COLS[b], rs)

    def d2(src, j, cols):
        return rcopy(src, R.at[1, rs_(k, 7), cols], s_z.at[2], r_r.at[1], 2, j)

    d21 = d2(Pa.at[1, r2(7, 1)], 1, CA)
    d20 = [d2(Pb.at[b, r2(7, 1)], 0, COLS[b]) for b in range(2)]

    def part1(r):
        Pa[1, r, :] = mn(W[0, r, :kd], T1[0]) + mn(W[1, r, :kd], T1[1])

    def part0(r, b):
        Pb[b, r, :] = mn(W[0, r, :kd], T0[0, b]) + mn(W[1, r, :kd], T0[1, b])

    q_u = rcopy(Qa.at[0], R.at[slot(0)], s_z.at[4], r_r.at[0], 1, 0)

    def q_d(b):
        return rcopy(QD.at[b], PR.at[y, rs_(k, 0, NS), COLS[b]], s_z.at[4], r_r.at[1], 1, 0)

    @pl.when(z == 1)
    def _():
        wait_recv(X.at[1 - k, :, DALL], r_d.at[NS])

        def step_u(q):
            zU(q)

            @pl.when(q < 5)
            def _():
                u_fwd(q).start()

            turn(q)

        each(0, NU, step_u)
        zU(NU, XU)
        each(NU, nd, turn)
        if xd:
            turn(nd, xd)

        @pl.when(c != 0)
        def _():
            q_u.start()

        pl.semaphore_wait(far, n_near)

        def step(i):
            @pl.when(i < 2 * NS)
            def _():
                zD(i)

            @pl.when(i == 3)
            def _():
                wait_w(rs_(0, 0, NS), 0)
                part1(rs_(0, 0, NS))

                @pl.when(y == 0)
                def _():
                    x31.start()

                each(5, 10, lambda q: u_fwd(q).start())

            @pl.when((i == 5) & (y == 1))
            def _():
                wait_recv(XA.at[rs_(0, 0, NS)], r_x.at[0])
                Pa[1, rs_(0, 0, NS), :] += XA[rs_(0, 0, NS), :]
                m31.start()

            @pl.when(i == 16)
            def _():
                def chunk(n):
                    ch = jnp.where(n == 0, k, 1 - k)

                    @pl.when(n == 1)
                    def _():
                        T0[k, 1] = Y[k, brows(1), DALL].T
                        wait_recv(Y.at[1 - k, brows(1), DALL], r_d.at[1])

                    Pb[1, pl.ds(0, rows - st), :] += mm(W[ch, pl.ds(0, rows - st), :kd], Y[ch, brows(1), DALL])

                each(0, 2, chunk)

                @pl.when(y == 0)
                def _():
                    for u in range(2):
                        m30(1, u).start()

                @pl.when(y == 1)
                def _():
                    for u in range(2):
                        m30r(u).start()
                    x20(1, 0, 4, 8).start()
                    x20(1, 4, 3, 4).start()

            @pl.when((i == 7) | (i == 17))
            def _():
                b = jnp.where(i == 7, 0, 1)

                @pl.when(b == 0)
                def _():
                    wait_recv(Y.at[1 - k, brows(0), DALL], r_d.at[0])

                T0[1 - k, b] = Y[1 - k, brows(b), DALL].T

                @pl.when(b == 0)
                def _():
                    T0[k, 0] = Y[k, brows(0), DALL].T
                    part0(rs_(0, 0, NS), 0)

                    @pl.when(y == 1)
                    def _():
                        for u in range(2):
                            x30(0, u).start()

            @pl.when((i == 7) | (i == 17))
            def _():
                b = jnp.where(i == 7, 0, 1)
                r = rs_(k, 0, NS)
                QD[b] = mn(X[0, r, DALL], T0[0, b]) + mn(X[1, r, DALL], T0[1, b])
                for bb in range(2):
                    @pl.when((b == bb) & (c != 0))
                    def _():
                        q_d(bb).start()

            @pl.when(i == 7)
            def _():
                each(10, NU, lambda q: u_fwd(q).start())
                u_fwd(NU, XU).start()

            @pl.when((i == 9) & (y == 0))
            def _():
                for u in range(2):
                    wait_recv(XB.at[0, r3(u)], r_x.at[1 + u])
                    Pb[0, r3(u), :] += XB[0, r3(u), :]
                    m30(0, u).start()

            @pl.when((i == 8) | (i == 9) | (i == 13))
            def _():
                g = jnp.where(i == 13, 2, i - 8)
                wait_w(r2(2 * g), 1 + g)
                part1(r2(2 * g))
                part0(r2(2 * g), 0)

                @pl.when(y == 1)
                def _():
                    x21(2 * g, 2, 5 + g).start()
                    x20(0, 2 * g, 2, 5 + g).start()

            @pl.when(((i == 10) | (i == 11) | (i == 15)) & (y == 0))
            def _():
                g = jnp.where(i == 15, 2, i - 10)
                wait_recv(XA.at[pl.ds(0, 48)], r_x.at[5 + g])
                Pa[1, r2(2 * g), :] += XA[r2(2 * g), :]
                Pb[0, r2(2 * g), :] += XB[0, r2(2 * g), :]
                m21(2 * g, 2, 1).start()
                m20(0, 2 * g, 2, 1).start()

            @pl.when((i == 17) & (y == 0))
            def _():
                wait_recv(XA.at[pl.ds(0, 24)], r_x.at[3])
                Pa[1, r2(6, 1), :] += XA[r2(6, 1), :]
                m21(6, 1, 2).start()
                Pb[0, r2(6, 1), :] += XB[0, r2(6, 1), :]
                m20(0, 6, 1, 3).start()

            @pl.when((i == 14) | (i == 18))
            def _():
                t = jnp.where(i == 14, 6, 7)
                wait_w(r2(t, 1), t - 2)
                part1(r2(t, 1))

                @pl.when((y == 1) & (i == 18))
                def _():
                    d21.start()

                @pl.when((y == 0) & (i == 18))
                def _():
                    m21(7, 1, 2).start()

                part0(r2(t, 1), 0)

                @pl.when((y == 1) & (i == 14))
                def _():
                    x21(6, 1, 3).start()
                    x20(0, 6, 1, 3).start()

                @pl.when((y == 1) & (i == 18))
                def _():
                    d20[0].start()

                @pl.when((y == 0) & (i == 18))
                def _():
                    m20(0, 7, 1, 3).start()
                    for f, n, x in ((0, 4, 8), (4, 3, 4)):
                        wait_recv(XB.at[1, r2(f, n)], r_x.at[x])
                        Pb[1, r2(f, n), :] += XB[1, r2(f, n), :]
                        m20(1, f, n, 2).start()

                @pl.when(i == 18)
                def _():
                    part0(r2(7, 1), 1)

                    @pl.when(y == 1)
                    def _():
                        d20[1].start()

                    @pl.when(y == 0)
                    def _():
                        m20(1, 7, 1, 3).start()

        each(0, 19, step)

    def d_fwd(t):
        h, s = t % 2, t // 2
        return rcopy(Y.at[k, rs_(h, s), DALL], W.at[k, rs_(0, s), pl.ds(0, kd)], s_z.at[0], r_w.at[0], 1, 2 * y + h)

    def u_sib(s):
        return rcopy(Y.at[k, us_(s), UALL], Y.at[k, us_(s), UALL], s_z.at[1], r_d.at[s], z, sib)

    def q1send(s):
        return rcopy(Qa.at[1, us_(s)], R.at[c, us_(s)], s_z.at[4], r_r.at[0], 3, 2)

    def y2(q, w=PW):
        wait_recv(W.at[:, :, up(q, w)], r_w.at[q])
        Pa[0] += mm(X[0, :, up(q, w)], W[0, :, up(q, w)]) + mm(X[1, :, up(q, w)], W[1, :, up(q, w)])

    def y3(b, q, w=PW):
        r = pl.ds(b * half, half)
        Pa[1, r, :] += mm(Y[0, r, up(q, w)], W[0, :, up(q, w)]) + mm(Y[1, r, up(q, w)], W[1, :, up(q, w)])

    def wait_ysib(s):
        wait_recv(Y.at[1 - k, us_(s), UALL], r_d.at[s])

    def s3(r, cols=CA):
        return rcopy(Pa.at[1, r, cols], R.at[y, r, cols], s_z.at[2], r_r.at[0], 3, k)

    s2 = rcopy(Pa.at[0], R.at[0], s_z.at[2], r_r.at[0], 2, k)

    def add(i, r, cols):
        Pa[i, r, cols] += PR[i, r, cols]

    def wait_pr(n, cols, sem):
        wait_recv(PR.at[0, pl.ds(0, n), cols], r_p.at[sem])

    def strip31(s):
        wait_ysib(s)
        r = us_(s)
        Pa[1, r, :] = mm(Y[0, r, UALL], W[0, :, :ku]) + mm(Y[1, r, UALL], W[1, :, :ku])

        @pl.when(y == 1)
        def _():
            add(1, r, CA)

        s3(r).start()

    @pl.when(z == 2)
    def _():
        def step_d(t):
            wait_recv(Y.at[k, rs_(t % 2, t // 2), DALL], r_y.at[t])
            d_fwd(t).start()

            @pl.when(t == 1)
            def _():
                wait_recv(X.at[1 - k, :, UALL], r_d.at[NS])

            @pl.when((k == 1) & (t >= 1))
            def _():
                y2(t - 1)

            r = rs_(t % 2, t // 2)
            Qa[1, r, :] = mm(Y[k, r, DALL], X[k, :, DALL])

        each(0, 2 * NS, step_d)
        each(2, 2 * NS, lambda t: z2_d(t).start())

        pl.semaphore_wait(far, n_near)

        @pl.when(k == 1)
        def _():
            y2(NU, XU)

            @pl.when(y == 1)
            def _():
                s2.start()


        def q1(s):
            Qa[1, us_(s), :] += mm(Y[k, us_(s), UALL], X[k, :, UALL])
            q1send(s).start()

        def step_u(s):
            @pl.when((k == 0) & (s >= 1))
            def _():
                y2(2 * s - 1)

            @pl.when(k == 0)
            def _():
                y2(2 * s)

            @pl.when((k == 0) & (s == 4))
            def _():
                each(0, 4, wait_ysib)
                each(0, 7, lambda q: y3(0, q))

            @pl.when((k == 0) & (s >= 4))
            def _():
                y3(0, 2 * s - 1)
                y3(0, 2 * s)

            wait_recv(Y.at[k, us_(s), UALL], r_y.at[2 * NS + s])
            u_sib(s).start()

            @pl.when((k == 1) & (y == 1) & (s == 4))
            def _():
                wait_recv(PR.at[1], r_p.at[0])

            @pl.when((k == 1) & (s >= 4) & (s <= 6))
            def _():
                each(2 * s - 8, 2 * s - 6, strip31)

            @pl.when((k == 1) | (s < NS - 1))
            def _():
                q1(s)

        each(0, NS, step_u)

        @pl.when(k == 1)
        def _():
            each(NS - 2, NS, strip31)

            @pl.when(y == 0)
            def _():
                wait_pr(192, CA, 1)
                for h in range(2):
                    add(0, rs_(h, 0, 6), CA)
                wait_pr(64, CA, 2)
                for h in range(2):
                    add(0, rs_(h, 6, 2), CA)

        @pl.when(k == 0)
        def _():
            y2(NU, XU)

            @pl.when(y == 1)
            def _():
                s2.start()

            y3(0, NU, XU)
            each(NS - 1, NS - y, q1)

            @pl.when(y == 0)
            def _():
                wait_pr(rows, C0, 0)
                add(1, pl.ds(0, half), C0)


            @pl.when(y == 0)
            def _():
                s3(pl.ds(0, half)).start()

            @pl.when(y == 1)
            def _():
                s3(pl.ds(0, half), C0).start()

            each(4, NS, wait_ysib)

            def low(b):
                r = pl.ds(pl.multiple_of(b * half, half), half)
                Pa[1, r, :] = mm(Y[0, r, UALL], W[0, :, :ku]) + mm(Y[1, r, UALL], W[1, :, :ku])

            each(1 + k, 2, low)

            @pl.when(y == 0)
            def _():
                add(1, pl.ds(half, half), C0)

            @pl.when(y == 0)
            def _():
                s3(pl.ds(half, half)).start()

            @pl.when(y == 1)
            def _():
                s3(pl.ds(half, half), C0).start()

            each(NS - 1, NS - 1 + y, q1)

            @pl.when(y == 1)
            def _():
                for u in range(2):
                    wait_pr(half, C1, 1 + u)
                    for h in range(2):
                        add(1, rs_(h, 4 * u, 4), C1)
                        s3(rs_(h, 4 * u, 4), C1).start()

            @pl.when(y == 0)
            def _():
                wait_pr(192, C0, 1)
                for h in range(2):
                    add(0, rs_(h, 0, 6), C0)
                wait_pr(224, C1, 2)
                for h in range(2):
                    add(0, rs_(h, 0, 7), C1)
                wait_pr(96, C0, 3)
                for h in range(2):
                    add(0, rs_(h, 6, 2), C0)
                    add(0, rs_(h, 7), C1)

    @pl.when((z == 0) | (z == 3))
    def _():
        pl.semaphore_wait(far, n_near)

    @pl.when(c > z)
    def _():
        o_ref[...] = jnp.zeros_like(o_ref)

    @pl.when(c == z)
    def _():
        wait_recv(R.at[pl.ds(0, 3)], r_r.at[0])
        total = Qa[dq] + R[0] + R[1] + R[2]
        diff = lax.broadcasted_iota(jnp.int32, (rows, rows), 0) - lax.broadcasted_iota(jnp.int32, (rows, rows), 1)
        o_ref[...] = jnp.where(diff >= 0, total, 0.0).astype(o_ref.dtype)

    @pl.when((z == 1) & (c == 0))
    def _():
        wait_recv(R.at[pl.ds(0, 3)], r_r.at[0])
        Qa[0] += R[0] + R[1] + R[2]
        wait_recv(R.at[pl.ds(0, 3), pl.ds(0, half)], r_r.at[1])
        for b in range(2):
            PR[0, pl.ds(0, half), COLS[b]] = QD[b]
        o_ref[...] = (Qa[0] + PR[0] + PR[1]).astype(o_ref.dtype)

    @pl.when((z == 2) & (y == 0))
    def _():
        wait_recv(R.at[0], r_r.at[0])
        wait_recv(R.at[1, pl.ds(0, 32)], r_r.at[1])
        for h in range(2):
            Pa[0, rs_(h, 7), :] += R[1, rs_(h, 7), :]
        o_ref[...] = (Pa[0] + R[0]).astype(o_ref.dtype)

    @pl.when((z == 3) & (c == 2))
    def _():
        wait_recv(R, r_r.at[0])
        o_ref[...] = (R[0] + R[1] + R[2] + R[3]).astype(o_ref.dtype)

    @pl.when((z == 3) & (y == 0))
    def _():
        wait_recv(R.at[pl.ds(0, 2)], r_r.at[0])

        @pl.when(k == 0)
        def _():
            wait_recv(R.at[2, :, C1], r_r.at[1])
            R[0, :, C1] += R[2, :, C1]

        o_ref[...] = (R[0] + R[1]).astype(o_ref.dtype)

    @pl.when(c != z)
    def _():
        wait_recv(Qa.at[0], s_z.at[3])

    @pl.when((z == 0) | (z == 3))
    def _():
        wait_recv(X.at[k], s_z.at[0])

    @pl.when(z == 1)
    def _():
        wait_recv(W.at[:, :, pl.ds(0, ku)], s_z.at[0])
        wait_recv(W.at[:, :, pl.ds(0, kd)], s_z.at[1])
        wait_recv(Pa, s_z.at[2])

        @pl.when(c != 0)
        def _():
            wait_recv(R.at[pl.ds(0, 3), pl.ds(0, half)], s_z.at[4])

    @pl.when(z == 2)
    def _():
        wait_recv(W.at[:, :, pl.ds(0, kd)], s_z.at[0])
        wait_recv(W.at[:, :, pl.ds(0, ku)], s_z.at[1])
        wait_recv(Qa.at[1], s_z.at[4])

        @pl.when(y == 0)
        def _():
            wait_recv(Pa.at[0], s_z.at[2])

        @pl.when(y == 1)
        def _():
            wait_recv(Pa, s_z.at[2])


def solution(mesh):
    def local_fn(a_local):
        rows, m = a_local.shape
        kd = m - NU * PW - XU
        f32, bf16 = jnp.float32, jnp.bfloat16
        dma = pltpu.SemaphoreType.DMA
        return pl.pallas_call(
            kernel,
            out_shape=pltpu.VMEM((rows, rows), bf16),
            in_specs=[pl.BlockSpec(memory_space=pl.ANY)],
            out_specs=pl.BlockSpec(memory_space=pltpu.VMEM),
            scratch_shapes=[
                pltpu.VMEM((2, rows, m), bf16),
                pltpu.VMEM((2, rows, m), bf16),
                pltpu.VMEM((2, rows, kd), bf16),
                pltpu.VMEM((2, 2, kd, rows // 2), bf16),
                pltpu.VMEM((2, kd, rows), bf16),
                pltpu.VMEM((2, rows, rows), f32),
                pltpu.VMEM((2, rows, rows // 2), f32),
                pltpu.VMEM((2, rows, rows), f32),
                pltpu.VMEM((2, rows // 2, rows // 2), f32),
                pltpu.VMEM((4, rows, rows), f32),
                pltpu.VMEM((2, rows, rows), f32),
                pltpu.VMEM((rows, rows), f32),
                pltpu.VMEM((2, rows, rows // 2), f32),
                pltpu.SemaphoreType.REGULAR,
                dma((1,)), dma((5,)), dma((4 * NS,)), dma((NS + 1,)), dma((NU + 1,)), dma((4,)), dma((2,)), dma((9,)),
            ],
            compiler_params=pltpu.CompilerParams(
                collective_id=0, has_side_effects=True, vmem_limit_bytes=56 * 1024 * 1024),
        )(a_local)

    part_spec = P(("batch", "row"), "col")
    return jax.shard_map(local_fn, mesh=mesh, in_specs=(part_spec,), out_specs=part_spec, check_vma=False)
```

```python
import jax
import jax.numpy as jnp
from jax import lax
from jax.experimental import pallas as pl
from jax.experimental.pallas import tpu as pltpu
from jax.sharding import PartitionSpec as P

MESH = pl.DeviceIdType.MESH
PW = 256
NU = 15
XU = 128
NS = 8


def mm(a, b):
    return lax.dot_general(a, b, (((1,), (1,)), ((), ())), preferred_element_type=jnp.float32)


def mn(a, b):
    return lax.dot_general(a, b, (((1,), (0,)), ((), ())), preferred_element_type=jnp.float32)


def kernel(a_ref, o_ref, X, Y, W, T0, T1, Pa, Pb, Qa, QD, R, PR, XA, XB, far, ld, s_z, r_y, r_d, r_w, r_p, r_r, r_x):
    rows, m = a_ref.shape
    ku = NU * PW + XU
    kd = m - ku
    nd, xd = kd // PW, kd % PW
    half = rows // 2
    st = half // NS
    us = rows // NS
    z = lax.axis_index("row")
    c = lax.axis_index("col")
    y = c // 2
    k = c % 2
    sib = 2 * y + 1 - k

    def rcopy(src, dst, ss, rs, row, col):
        return pltpu.make_async_remote_copy(
            src_ref=src, dst_ref=dst, send_sem=ss, recv_sem=rs, device_id={"row": row, "col": col}, device_id_type=MESH)

    def wait_recv(ref, sem):
        pltpu.make_async_copy(ref, ref, sem).wait()

    def up(p, w=PW):
        return pl.ds(pl.multiple_of(p * PW, 128), w)

    def dn(p, w=PW):
        return pl.ds(pl.multiple_of(ku + p * PW, 128), w)

    def rs_(h, s, n=1):
        return pl.ds(pl.multiple_of(h * half + s * st, st), n * st)

    def us_(s):
        return pl.ds(pl.multiple_of(s * us, us), us)

    DALL = pl.ds(ku, kd)
    UALL = pl.ds(0, ku)
    C0, C1 = pl.ds(0, half), pl.ds(half, half)
    COLS = (C0, C1)

    def each(lo, hi, fn):
        lax.fori_loop(lo, hi, lambda i, u: (fn(i), u)[1], 0)

    load = pltpu.make_async_copy(a_ref, X.at[k], ld.at[0])

    def near(sem):
        for dz in (-1, 1):
            @pl.when((z + dz >= 0) & (z + dz <= 3))
            def _():
                for kk in range(2):
                    pl.semaphore_signal(sem, inc=1, device_id={"row": z + dz, "col": 2 * y + kk}, device_id_type=MESH)
        for dc in range(1, 4):
            pl.semaphore_signal(sem, inc=1, device_id={"row": z, "col": (c + dc) % 4}, device_id_type=MESH)

    n_near = jnp.where((z == 0) | (z == 3), 5, 7)
    bar = pltpu.get_barrier_semaphore()
    near(bar)
    load.start()
    pl.semaphore_wait(bar, n_near)

    def z0_u(q, w=PW):
        return rcopy(a_ref.at[:, up(q, w)], Y.at[k, :, up(q, w)], s_z.at[0], r_y.at[q], 1, c)

    def z0_d(t):
        r = rs_(0, t)
        return rcopy(a_ref.at[r, DALL], Y.at[k, r, DALL], s_z.at[0], r_y.at[2 * NS + t], 1, c)

    def z3_d(t):
        r = rs_(t % 2, t // 2)
        return rcopy(a_ref.at[r, DALL], Y.at[k, r, DALL], s_z.at[0], r_y.at[t], 2, c)

    def z3_u(s):
        r = us_(s)
        return rcopy(a_ref.at[r, UALL], Y.at[k, r, UALL], s_z.at[0], r_y.at[2 * NS + s], 2, c)

    def z1_u(q, w=PW):
        return rcopy(a_ref.at[:, up(q, w)], W.at[k, :, up(q, w)], s_z.at[0], r_w.at[q], 2, 2 * y + 1)

    def z2_d(t):
        h, s = t % 2, t // 2
        return rcopy(a_ref.at[rs_(h, s), DALL], W.at[k, rs_(1, s), pl.ds(0, kd)], s_z.at[0], r_w.at[jnp.where(s < 6, 1 + s // 2, s - 2)], 1, 2 * y + h)

    @pl.when(z == 0)
    def _():
        each(0, NU, lambda q: z0_u(q).start())
        z0_u(NU, XU).start()
        each(0, 2 * NS, lambda t: z0_d(t).start())

    @pl.when(z == 3)
    def _():
        each(0, 2 * NS, lambda t: z3_d(t).start())
        each(0, NS, lambda s: z3_u(s).start())

    x_d = rcopy(a_ref.at[:, DALL], X.at[k, :, DALL], s_z.at[1], r_d.at[NS], z, sib)
    x_u = rcopy(a_ref.at[:, UALL], X.at[k, :, UALL], s_z.at[1], r_d.at[NS], z, sib)

    @pl.when(z == 1)
    def _():
        each(0, NU, lambda q: z1_u(q).start())
        z1_u(NU, XU).start()
        x_d.start()

    @pl.when(z == 2)
    def _():
        z2_d(0).start()
        z2_d(1).start()
        x_u.start()

    near(far)

    Pa[...] = jnp.zeros_like(Pa)
    Qa[...] = jnp.zeros_like(Qa)
    Pb[...] = jnp.zeros_like(Pb)
    load.wait()
    dq = jnp.where(z == 1, 1, 0)

    def diag(p):
        cs = pl.ds(pl.multiple_of(p * 512, 512), 512)
        Qa[dq] += mm(X[k, :, cs], X[k, :, cs])

    each(0, m // 512, diag)

    def slot(owner):
        return (c - owner + 3) % 4

    dsend = rcopy(Qa.at[dq], R.at[slot(z)], s_z.at[3], r_r.at[0], z, z)

    @pl.when(c != z)
    def _():
        dsend.start()

    def u_fwd(q, w=PW):
        return rcopy(Y.at[k, :, up(q, w)], W.at[k, :, up(q, w)], s_z.at[0], r_w.at[q], 2, 2 * y)

    def zU(q, w=PW):
        wait_recv(Y.at[k, :, up(q, w)], r_y.at[q])
        Qa[0] += mm(X[k, :, up(q, w)], Y[k, :, up(q, w)])

    def turn(p, w=PW):
        for h in range(2):
            T1[h, up(p, w), :] = X[h, :, dn(p, w)].T

    def d_sib(t):
        return rcopy(Y.at[k, rs_(0, t), DALL], Y.at[k, rs_(0, t), DALL], s_z.at[1], r_d.at[t // NS], z, sib)

    def zD(t):
        wait_recv(Y.at[k, rs_(0, t), DALL], r_y.at[2 * NS + t])
        d_sib(t).start()

    def brows(b):
        return pl.ds(pl.multiple_of(b * half, half), half)

    def wait_w(r, n):
        wait_recv(W.at[:, r, pl.ds(0, kd)], r_w.at[n])

    CA = pl.ds(0, rows)
    peer = (c + 2) % 4

    def r3(u):
        return rs_(0, 4 * u, 4)

    def r2(s, n=2):
        return rs_(1, s, n)

    def xsend(src, dst, n):
        return rcopy(src, dst, s_z.at[2], r_x.at[n], 1, peer)

    x31 = xsend(Pa.at[1, rs_(0, 0, NS)], XA.at[rs_(0, 0, NS)], 0)

    def x30(b, u):
        return xsend(Pb.at[b, r3(u)], XB.at[b, r3(u)], 1 + 2 * b + u)

    def x21(s, n, rs):
        return xsend(Pa.at[1, r2(s, n)], XA.at[r2(s, n)], rs)

    def x20(b, s, n, rs):
        return xsend(Pb.at[b, r2(s, n)], XB.at[b, r2(s, n)], rs)

    def msend(src, i, s, n, j, cols, rs):
        return rcopy(src, PR.at[i, rs_(k, s, n), cols], s_z.at[2], r_p.at[rs], 2, j)

    m31 = msend(Pa.at[1, rs_(0, 0, NS)], 1, 0, NS, 3, CA, 0)

    def m30(b, u):
        src = Pb.at[b, r3(u)]
        if b == 0:
            return msend(src, 1, 4 * u, 4, 0, C0, 0)
        return rcopy(src, R.at[2, rs_(k, 4 * u, 4), C1], s_z.at[2], r_r.at[1], 3, 0)

    def m30r(u):
        return rcopy(Pb.at[1, rs_(0, 2 * u, 2)], PR.at[1, rs_(k, 2 * u, 2), C1], s_z.at[2], r_p.at[1 + u], 2, 2)

    def m21(s, n, rs):
        return msend(Pa.at[1, r2(s, n)], 0, s, n, 1, CA, rs)

    def m20(b, s, n, rs):
        return msend(Pb.at[b, r2(s, n)], 0, s, n, 0, COLS[b], rs)

    def d2(src, j, cols):
        return rcopy(src, R.at[1, rs_(k, 7), cols], s_z.at[2], r_r.at[1], 2, j)

    d21 = d2(Pa.at[1, r2(7, 1)], 1, CA)
    d20 = [d2(Pb.at[b, r2(7, 1)], 0, COLS[b]) for b in range(2)]

    def part1(r):
        Pa[1, r, :] = mn(W[0, r, :kd], T1[0]) + mn(W[1, r, :kd], T1[1])

    def part0(r, b):
        Pb[b, r, :] = mn(W[0, r, :kd], T0[0, b]) + mn(W[1, r, :kd], T0[1, b])

    q_u = rcopy(Qa.at[0], R.at[slot(0)], s_z.at[4], r_r.at[0], 1, 0)

    def q_d(b):
        return rcopy(QD.at[b], PR.at[y, rs_(k, 0, NS), COLS[b]], s_z.at[4], r_r.at[1], 1, 0)

    @pl.when(z == 1)
    def _():
        wait_recv(X.at[1 - k, :, DALL], r_d.at[NS])

        def step_u(q):
            zU(q)

            @pl.when(q < 5)
            def _():
                u_fwd(q).start()

            turn(q)

        each(0, NU, step_u)
        zU(NU, XU)
        each(NU, nd, turn)
        if xd:
            turn(nd, xd)

        @pl.when(c != 0)
        def _():
            q_u.start()

        pl.semaphore_wait(far, n_near)

        def turn0(h, b, lo, hi):
            T0[h, b, lo:hi, :] = Y[h, brows(b), pl.ds(ku + lo, hi - lo)].T

        def step(i):
            @pl.when(i < 2 * NS)
            def _():
                zD(i)

            @pl.when(i == 3)
            def _():
                wait_w(rs_(0, 0, NS), 0)
                part1(rs_(0, 0, NS))

                @pl.when(y == 0)
                def _():
                    x31.start()

                each(5, 10, lambda q: u_fwd(q).start())

            @pl.when((i == 5) & (y == 1))
            def _():
                wait_recv(XA.at[rs_(0, 0, NS)], r_x.at[0])
                Pa[1, rs_(0, 0, NS), :] += XA[rs_(0, 0, NS), :]
                m31.start()

            @pl.when(i == 16)
            def _():
                def chunk(n):
                    ch = jnp.where(n == 0, k, 1 - k)

                    @pl.when(n == 1)
                    def _():
                        turn0(k, 1, 0, 2048)
                        wait_recv(Y.at[1 - k, brows(1), DALL], r_d.at[1])

                    Pb[1, pl.ds(0, rows - st), :] += mm(W[ch, pl.ds(0, rows - st), :kd], Y[ch, brows(1), DALL])

                each(0, 2, chunk)

                @pl.when(y == 0)
                def _():
                    for u in range(2):
                        m30(1, u).start()

                @pl.when(y == 1)
                def _():
                    for u in range(4):
                        m30r(u).start()
                    x20(1, 0, 4, 8).start()
                    x20(1, 4, 3, 4).start()

            @pl.when((i == 7) | (i == 17))
            def _():
                b = jnp.where(i == 7, 0, 1)

                @pl.when(b == 0)
                def _():
                    wait_recv(Y.at[1 - k, brows(0), DALL], r_d.at[0])

                turn0(1 - k, b, 0, kd)
                turn0(k, b, 2048, kd)

                @pl.when(b == 0)
                def _():
                    turn0(k, 0, 0, 2048)
                    part0(rs_(0, 0, NS), 0)

                    @pl.when(y == 1)
                    def _():
                        for u in range(2):
                            x30(0, u).start()

            @pl.when((i == 7) | (i == 17))
            def _():
                b = jnp.where(i == 7, 0, 1)
                r = rs_(k, 0, NS)
                QD[b] = mn(X[0, r, DALL], T0[0, b]) + mn(X[1, r, DALL], T0[1, b])
                for bb in range(2):
                    @pl.when((b == bb) & (c != 0))
                    def _():
                        q_d(bb).start()

            @pl.when(i == 7)
            def _():
                each(10, NU, lambda q: u_fwd(q).start())
                u_fwd(NU, XU).start()

            @pl.when((i == 9) & (y == 0))
            def _():
                for u in range(2):
                    wait_recv(XB.at[0, r3(u)], r_x.at[1 + u])
                    Pb[0, r3(u), :] += XB[0, r3(u), :]
                    m30(0, u).start()

            @pl.when((i == 8) | (i == 9) | (i == 13))
            def _():
                g = jnp.where(i == 13, 2, i - 8)
                wait_w(r2(2 * g), 1 + g)
                part1(r2(2 * g))
                part0(r2(2 * g), 0)

                @pl.when(y == 1)
                def _():
                    x21(2 * g, 2, 5 + g).start()
                    x20(0, 2 * g, 2, 5 + g).start()

            @pl.when(((i == 10) | (i == 11) | (i == 15)) & (y == 0))
            def _():
                g = jnp.where(i == 15, 2, i - 10)
                wait_recv(XA.at[pl.ds(0, 48)], r_x.at[5 + g])
                Pa[1, r2(2 * g), :] += XA[r2(2 * g), :]
                Pb[0, r2(2 * g), :] += XB[0, r2(2 * g), :]
                m21(2 * g, 2, 1).start()
                m20(0, 2 * g, 2, 1).start()

            @pl.when((i == 17) & (y == 0))
            def _():
                wait_recv(XA.at[pl.ds(0, 24)], r_x.at[3])
                Pa[1, r2(6, 1), :] += XA[r2(6, 1), :]
                m21(6, 1, 2).start()
                Pb[0, r2(6, 1), :] += XB[0, r2(6, 1), :]
                m20(0, 6, 1, 3).start()

            @pl.when((i == 14) | (i == 18))
            def _():
                t = jnp.where(i == 14, 6, 7)
                wait_w(r2(t, 1), t - 2)
                part1(r2(t, 1))

                @pl.when((y == 1) & (i == 18))
                def _():
                    d21.start()

                @pl.when((y == 0) & (i == 18))
                def _():
                    m21(7, 1, 2).start()

                part0(r2(t, 1), 0)

                @pl.when((y == 1) & (i == 14))
                def _():
                    x21(6, 1, 3).start()
                    x20(0, 6, 1, 3).start()

                @pl.when((y == 1) & (i == 18))
                def _():
                    d20[0].start()

                @pl.when((y == 0) & (i == 18))
                def _():
                    m20(0, 7, 1, 3).start()
                    for f, n, x in ((0, 4, 8), (4, 3, 4)):
                        wait_recv(XB.at[1, r2(f, n)], r_x.at[x])
                        Pb[1, r2(f, n), :] += XB[1, r2(f, n), :]
                        m20(1, f, n, 2).start()

                @pl.when(i == 18)
                def _():
                    part0(r2(7, 1), 1)

                    @pl.when(y == 1)
                    def _():
                        d20[1].start()

                    @pl.when(y == 0)
                    def _():
                        m20(1, 7, 1, 3).start()

        each(0, 19, step)

    def d_fwd(t):
        h, s = t % 2, t // 2
        return rcopy(Y.at[k, rs_(h, s), DALL], W.at[k, rs_(0, s), pl.ds(0, kd)], s_z.at[0], r_w.at[0], 1, 2 * y + h)

    def u_sib(s):
        return rcopy(Y.at[k, us_(s), UALL], Y.at[k, us_(s), UALL], s_z.at[1], r_d.at[s], z, sib)

    def q1send(s):
        return rcopy(Qa.at[1, us_(s)], R.at[c, us_(s)], s_z.at[4], r_r.at[0], 3, 2)

    def y2(q, w=PW):
        wait_recv(W.at[:, :, up(q, w)], r_w.at[q])
        Pa[0] += mm(X[0, :, up(q, w)], W[0, :, up(q, w)]) + mm(X[1, :, up(q, w)], W[1, :, up(q, w)])

    def y3(b, q, w=PW):
        r = pl.ds(b * half, half)
        Pa[1, r, :] += mm(Y[0, r, up(q, w)], W[0, :, up(q, w)]) + mm(Y[1, r, up(q, w)], W[1, :, up(q, w)])

    def wait_ysib(s):
        wait_recv(Y.at[1 - k, us_(s), UALL], r_d.at[s])

    def s3(r, cols=CA):
        return rcopy(Pa.at[1, r, cols], R.at[y, r, cols], s_z.at[2], r_r.at[0], 3, k)

    s2 = rcopy(Pa.at[0], R.at[0], s_z.at[2], r_r.at[0], 2, k)

    def add(i, r, cols):
        Pa[i, r, cols] += PR[i, r, cols]

    def wait_pr(n, cols, sem):
        wait_recv(PR.at[0, pl.ds(0, n), cols], r_p.at[sem])

    def strip31(s):
        wait_ysib(s)
        r = us_(s)
        Pa[1, r, :] = mm(Y[0, r, UALL], W[0, :, :ku]) + mm(Y[1, r, UALL], W[1, :, :ku])

        @pl.when(y == 1)
        def _():
            add(1, r, CA)

        s3(r).start()

    @pl.when(z == 2)
    def _():
        def step_d(t):
            wait_recv(Y.at[k, rs_(t % 2, t // 2), DALL], r_y.at[t])
            d_fwd(t).start()

            @pl.when(t == 1)
            def _():
                wait_recv(X.at[1 - k, :, UALL], r_d.at[NS])

            @pl.when((k == 1) & (t >= 1))
            def _():
                y2(t - 1)

            r = rs_(t % 2, t // 2)
            Qa[1, r, :] = mm(Y[k, r, DALL], X[k, :, DALL])

        each(0, 2 * NS, step_d)
        each(2, 2 * NS, lambda t: z2_d(t).start())

        pl.semaphore_wait(far, n_near)

        @pl.when(k == 1)
        def _():
            y2(NU, XU)

            @pl.when(y == 1)
            def _():
                s2.start()


        def q1(s):
            Qa[1, us_(s), :] += mm(Y[k, us_(s), UALL], X[k, :, UALL])
            q1send(s).start()

        def step_u(s):
            @pl.when((k == 0) & (s >= 1))
            def _():
                y2(2 * s - 1)

            @pl.when(k == 0)
            def _():
                y2(2 * s)

            @pl.when((k == 0) & (s == 4))
            def _():
                each(0, 4, wait_ysib)
                each(0, 7, lambda q: y3(0, q))

            @pl.when((k == 0) & (s >= 4))
            def _():
                y3(0, 2 * s - 1)
                y3(0, 2 * s)

            wait_recv(Y.at[k, us_(s), UALL], r_y.at[2 * NS + s])
            u_sib(s).start()

            @pl.when((k == 1) & (y == 1) & (s == 4))
            def _():
                wait_recv(PR.at[1], r_p.at[0])

            @pl.when((k == 1) & (s >= 4) & (s <= 6))
            def _():
                each(2 * s - 8, 2 * s - 6, strip31)

            @pl.when((k == 1) | (s < NS - 1))
            def _():
                q1(s)

        each(0, NS, step_u)

        @pl.when(k == 1)
        def _():
            each(NS - 2, NS, strip31)

            @pl.when(y == 0)
            def _():
                wait_pr(192, CA, 1)
                for h in range(2):
                    add(0, rs_(h, 0, 6), CA)
                wait_pr(64, CA, 2)
                for h in range(2):
                    add(0, rs_(h, 6, 2), CA)

        @pl.when(k == 0)
        def _():
            y2(NU, XU)

            @pl.when(y == 1)
            def _():
                s2.start()

            y3(0, NU, XU)
            each(NS - 1, NS - y, q1)

            @pl.when(y == 0)
            def _():
                wait_pr(rows, C0, 0)
                add(1, pl.ds(0, half), C0)


            @pl.when(y == 0)
            def _():
                s3(pl.ds(0, half)).start()

            @pl.when(y == 1)
            def _():
                s3(pl.ds(0, half), C0).start()

            each(4, NS, wait_ysib)

            def low(b):
                r = pl.ds(pl.multiple_of(b * half, half), half)
                Pa[1, r, :] = mm(Y[0, r, UALL], W[0, :, :ku]) + mm(Y[1, r, UALL], W[1, :, :ku])

            each(1 + k, 2, low)

            @pl.when(y == 0)
            def _():
                add(1, pl.ds(half, half), C0)

            @pl.when(y == 0)
            def _():
                s3(pl.ds(half, half)).start()

            @pl.when(y == 1)
            def _():
                s3(pl.ds(half, half), C0).start()

            each(NS - 1, NS - 1 + y, q1)

            @pl.when(y == 1)
            def _():
                for u in range(4):
                    wait_pr(64, C1, 1 + u)
                    for h in range(2):
                        add(1, rs_(h, 2 * u, 2), C1)
                        s3(rs_(h, 2 * u, 2), C1).start()

            @pl.when(y == 0)
            def _():
                wait_pr(192, C0, 1)
                for h in range(2):
                    add(0, rs_(h, 0, 6), C0)
                wait_pr(224, C1, 2)
                for h in range(2):
                    add(0, rs_(h, 0, 7), C1)
                wait_pr(96, C0, 3)
                for h in range(2):
                    add(0, rs_(h, 6, 2), C0)
                    add(0, rs_(h, 7), C1)

    @pl.when((z == 0) | (z == 3))
    def _():
        pl.semaphore_wait(far, n_near)

    @pl.when(c > z)
    def _():
        o_ref[...] = jnp.zeros_like(o_ref)

    @pl.when(c == z)
    def _():
        wait_recv(R.at[pl.ds(0, 3)], r_r.at[0])
        total = Qa[dq] + R[0] + R[1] + R[2]
        diff = lax.broadcasted_iota(jnp.int32, (rows, rows), 0) - lax.broadcasted_iota(jnp.int32, (rows, rows), 1)
        o_ref[...] = jnp.where(diff >= 0, total, 0.0).astype(o_ref.dtype)

    @pl.when((z == 1) & (c == 0))
    def _():
        wait_recv(R.at[pl.ds(0, 3)], r_r.at[0])
        Qa[0] += R[0] + R[1] + R[2]
        wait_recv(R.at[pl.ds(0, 3), pl.ds(0, half)], r_r.at[1])
        for b in range(2):
            PR[0, pl.ds(0, half), COLS[b]] = QD[b]
        o_ref[...] = (Qa[0] + PR[0] + PR[1]).astype(o_ref.dtype)

    @pl.when((z == 2) & (y == 0))
    def _():
        wait_recv(R.at[0], r_r.at[0])
        wait_recv(R.at[1, pl.ds(0, 32)], r_r.at[1])
        for h in range(2):
            Pa[0, rs_(h, 7), :] += R[1, rs_(h, 7), :]
        o_ref[...] = (Pa[0] + R[0]).astype(o_ref.dtype)

    @pl.when((z == 3) & (c == 2))
    def _():
        wait_recv(R, r_r.at[0])
        o_ref[...] = (R[0] + R[1] + R[2] + R[3]).astype(o_ref.dtype)

    @pl.when((z == 3) & (y == 0))
    def _():
        wait_recv(R.at[pl.ds(0, 2)], r_r.at[0])

        @pl.when(k == 0)
        def _():
            wait_recv(R.at[2, :, C1], r_r.at[1])
            R[0, :, C1] += R[2, :, C1]

        o_ref[...] = (R[0] + R[1]).astype(o_ref.dtype)

    @pl.when(c != z)
    def _():
        wait_recv(Qa.at[0], s_z.at[3])

    @pl.when((z == 0) | (z == 3))
    def _():
        wait_recv(X.at[k], s_z.at[0])

    @pl.when(z == 1)
    def _():
        wait_recv(W.at[:, :, pl.ds(0, ku)], s_z.at[0])
        wait_recv(W.at[:, :, pl.ds(0, kd)], s_z.at[1])
        wait_recv(Pa, s_z.at[2])

        @pl.when(c != 0)
        def _():
            wait_recv(R.at[pl.ds(0, 3), pl.ds(0, half)], s_z.at[4])

    @pl.when(z == 2)
    def _():
        wait_recv(W.at[:, :, pl.ds(0, kd)], s_z.at[0])
        wait_recv(W.at[:, :, pl.ds(0, ku)], s_z.at[1])
        wait_recv(Qa.at[1], s_z.at[4])

        @pl.when(y == 0)
        def _():
            wait_recv(Pa.at[0], s_z.at[2])

        @pl.when(y == 1)
        def _():
            wait_recv(Pa, s_z.at[2])


def solution(mesh):
    def local_fn(a_local):
        rows, m = a_local.shape
        kd = m - NU * PW - XU
        f32, bf16 = jnp.float32, jnp.bfloat16
        dma = pltpu.SemaphoreType.DMA
        return pl.pallas_call(
            kernel,
            out_shape=pltpu.VMEM((rows, rows), bf16),
            in_specs=[pl.BlockSpec(memory_space=pl.ANY)],
            out_specs=pl.BlockSpec(memory_space=pltpu.VMEM),
            scratch_shapes=[
                pltpu.VMEM((2, rows, m), bf16),
                pltpu.VMEM((2, rows, m), bf16),
                pltpu.VMEM((2, rows, kd), bf16),
                pltpu.VMEM((2, 2, kd, rows // 2), bf16),
                pltpu.VMEM((2, kd, rows), bf16),
                pltpu.VMEM((2, rows, rows), f32),
                pltpu.VMEM((2, rows, rows // 2), f32),
                pltpu.VMEM((2, rows, rows), f32),
                pltpu.VMEM((2, rows // 2, rows // 2), f32),
                pltpu.VMEM((4, rows, rows), f32),
                pltpu.VMEM((2, rows, rows), f32),
                pltpu.VMEM((rows, rows), f32),
                pltpu.VMEM((2, rows, rows // 2), f32),
                pltpu.SemaphoreType.REGULAR,
                dma((1,)), dma((5,)), dma((4 * NS,)), dma((NS + 1,)), dma((NU + 1,)), dma((5,)), dma((2,)), dma((9,)),
            ],
            compiler_params=pltpu.CompilerParams(
                collective_id=0, has_side_effects=True, vmem_limit_bytes=56 * 1024 * 1024),
        )(a_local)

    part_spec = P(("batch", "row"), "col")
    return jax.shard_map(local_fn, mesh=mesh, in_specs=(part_spec,), out_specs=part_spec, check_vma=False)
```

```python
import jax
import jax.numpy as jnp
from jax import lax
from jax.experimental import pallas as pl
from jax.experimental.pallas import tpu as pltpu
from jax.sharding import PartitionSpec as P

MESH = pl.DeviceIdType.MESH
PW = 256
NU = 15
XU = 128
NS = 8


def mm(a, b):
    return lax.dot_general(a, b, (((1,), (1,)), ((), ())), preferred_element_type=jnp.float32)


def mn(a, b):
    return lax.dot_general(a, b, (((1,), (0,)), ((), ())), preferred_element_type=jnp.float32)


def kernel(a_ref, o_ref, X, Y, W, T0, T1, Pa, Pb, Qa, QD, R, PR, XA, XB, far, ld, s_z, r_y, r_d, r_w, r_p, r_r, r_x):
    rows, m = a_ref.shape
    ku = NU * PW + XU
    kd = m - ku
    nd, xd = kd // PW, kd % PW
    half = rows // 2
    st = half // NS
    us = rows // NS
    z = lax.axis_index("row")
    c = lax.axis_index("col")
    y = c // 2
    k = c % 2
    sib = 2 * y + 1 - k

    def rcopy(src, dst, ss, rs, row, col):
        return pltpu.make_async_remote_copy(
            src_ref=src, dst_ref=dst, send_sem=ss, recv_sem=rs, device_id={"row": row, "col": col}, device_id_type=MESH)

    def wait_recv(ref, sem):
        pltpu.make_async_copy(ref, ref, sem).wait()

    def up(p, w=PW):
        return pl.ds(pl.multiple_of(p * PW, 128), w)

    def dn(p, w=PW):
        return pl.ds(pl.multiple_of(ku + p * PW, 128), w)

    def rs_(h, s, n=1):
        return pl.ds(pl.multiple_of(h * half + s * st, st), n * st)

    def us_(s):
        return pl.ds(pl.multiple_of(s * us, us), us)

    DALL = pl.ds(ku, kd)
    UALL = pl.ds(0, ku)
    C0, C1 = pl.ds(0, half), pl.ds(half, half)
    COLS = (C0, C1)

    def each(lo, hi, fn):
        lax.fori_loop(lo, hi, lambda i, u: (fn(i), u)[1], 0)

    load = pltpu.make_async_copy(a_ref, X.at[k], ld.at[0])

    def near(sem):
        for dz in (-1, 1):
            @pl.when((z + dz >= 0) & (z + dz <= 3))
            def _():
                for kk in range(2):
                    pl.semaphore_signal(sem, inc=1, device_id={"row": z + dz, "col": 2 * y + kk}, device_id_type=MESH)
        for dc in range(1, 4):
            pl.semaphore_signal(sem, inc=1, device_id={"row": z, "col": (c + dc) % 4}, device_id_type=MESH)

    n_near = jnp.where((z == 0) | (z == 3), 5, 7)
    bar = pltpu.get_barrier_semaphore()
    near(bar)
    load.start()
    pl.semaphore_wait(bar, n_near)

    def z0_u(q, w=PW):
        return rcopy(a_ref.at[:, up(q, w)], Y.at[k, :, up(q, w)], s_z.at[0], r_y.at[q], 1, c)

    def z0_d(t):
        r = rs_(0, t)
        return rcopy(a_ref.at[r, DALL], Y.at[k, r, DALL], s_z.at[0], r_y.at[2 * NS + t], 1, c)

    def z3_d(t):
        r = rs_(t % 2, t // 2)
        return rcopy(a_ref.at[r, DALL], Y.at[k, r, DALL], s_z.at[0], r_y.at[t], 2, c)

    def z3_u(s):
        r = us_(s)
        return rcopy(a_ref.at[r, UALL], Y.at[k, r, UALL], s_z.at[0], r_y.at[2 * NS + s], 2, c)

    def z1_u(q, w=PW):
        return rcopy(a_ref.at[:, up(q, w)], W.at[k, :, up(q, w)], s_z.at[0], r_w.at[q], 2, 2 * y + 1)

    def z2_d(t):
        h, s = t % 2, t // 2
        return rcopy(a_ref.at[rs_(h, s), DALL], W.at[k, rs_(1, s), pl.ds(0, kd)], s_z.at[0], r_w.at[jnp.where(s < 6, 1 + s // 2, s - 2)], 1, 2 * y + h)

    @pl.when(z == 0)
    def _():
        each(0, NU, lambda q: z0_u(q).start())
        z0_u(NU, XU).start()
        each(0, 2 * NS, lambda t: z0_d(t).start())

    @pl.when(z == 3)
    def _():
        each(0, 2 * NS, lambda t: z3_d(t).start())
        each(0, NS, lambda s: z3_u(s).start())

    x_d = rcopy(a_ref.at[:, DALL], X.at[k, :, DALL], s_z.at[1], r_d.at[NS], z, sib)
    x_u = rcopy(a_ref.at[:, UALL], X.at[k, :, UALL], s_z.at[1], r_d.at[NS], z, sib)

    @pl.when(z == 1)
    def _():
        each(0, NU, lambda q: z1_u(q).start())
        z1_u(NU, XU).start()
        x_d.start()

    @pl.when(z == 2)
    def _():
        z2_d(0).start()
        z2_d(1).start()
        x_u.start()

    near(far)

    Pa[...] = jnp.zeros_like(Pa)
    Qa[...] = jnp.zeros_like(Qa)
    Pb[...] = jnp.zeros_like(Pb)
    load.wait()
    dq = jnp.where(z == 1, 1, 0)

    def diag(p):
        cs = pl.ds(pl.multiple_of(p * 512, 512), 512)
        Qa[dq] += mm(X[k, :, cs], X[k, :, cs])

    each(0, m // 512, diag)

    def slot(owner):
        return (c - owner + 3) % 4

    dsend = rcopy(Qa.at[dq], R.at[slot(z)], s_z.at[3], r_r.at[0], z, z)

    @pl.when(c != z)
    def _():
        dsend.start()

    def u_fwd(q, w=PW):
        return rcopy(Y.at[k, :, up(q, w)], W.at[k, :, up(q, w)], s_z.at[0], r_w.at[q], 2, 2 * y)

    def zU(q, w=PW):
        wait_recv(Y.at[k, :, up(q, w)], r_y.at[q])
        Qa[0] += mm(X[k, :, up(q, w)], Y[k, :, up(q, w)])

    def turn(p, w=PW):
        for h in range(2):
            T1[h, up(p, w), :] = X[h, :, dn(p, w)].T

    def d_sib(t):
        return rcopy(Y.at[k, rs_(0, t), DALL], Y.at[k, rs_(0, t), DALL], s_z.at[1], r_d.at[t // NS], z, sib)

    def zD(t):
        wait_recv(Y.at[k, rs_(0, t), DALL], r_y.at[2 * NS + t])
        d_sib(t).start()

    def brows(b):
        return pl.ds(pl.multiple_of(b * half, half), half)

    def wait_w(r, n):
        wait_recv(W.at[:, r, pl.ds(0, kd)], r_w.at[n])

    CA = pl.ds(0, rows)
    peer = (c + 2) % 4

    def r3(u):
        return rs_(0, 4 * u, 4)

    def r2(s, n=2):
        return rs_(1, s, n)

    def xsend(src, dst, n):
        return rcopy(src, dst, s_z.at[2], r_x.at[n], 1, peer)

    x31 = xsend(Pa.at[1, rs_(0, 0, NS)], XA.at[rs_(0, 0, NS)], 0)

    def x30(b, u):
        return xsend(Pb.at[b, r3(u)], XB.at[b, r3(u)], 1 + 2 * b + u)

    def x21(s, n, rs):
        return xsend(Pa.at[1, r2(s, n)], XA.at[r2(s, n)], rs)

    def x20(b, s, n, rs):
        return xsend(Pb.at[b, r2(s, n)], XB.at[b, r2(s, n)], rs)

    def msend(src, i, s, n, j, cols, rs):
        return rcopy(src, PR.at[i, rs_(k, s, n), cols], s_z.at[2], r_p.at[rs], 2, j)

    m31 = msend(Pa.at[1, rs_(0, 0, NS)], 1, 0, NS, 3, CA, 0)

    def m30(b, u):
        return msend(Pb.at[b, r3(u)], 1, 4 * u, 4, 0, C0, 0)

    def m30r(u):
        return rcopy(Pb.at[1, rs_(0, 2 * u, 2)], PR.at[1, rs_(k, 2 * u, 2), C1], s_z.at[2], r_p.at[1 + u], 2, 2 * y)

    def m21(s, n, rs):
        return msend(Pa.at[1, r2(s, n)], 0, s, n, 1, CA, rs)

    def m20(b, s, n, rs):
        return msend(Pb.at[b, r2(s, n)], 0, s, n, 0, COLS[b], rs)

    def d2(src, j, cols):
        return rcopy(src, R.at[1, rs_(k, 7), cols], s_z.at[2], r_r.at[1], 2, j)

    d21 = d2(Pa.at[1, r2(7, 1)], 1, CA)
    d20 = [d2(Pb.at[b, r2(7, 1)], 0, COLS[b]) for b in range(2)]

    def part1(r):
        Pa[1, r, :] = mn(W[0, r, :kd], T1[0]) + mn(W[1, r, :kd], T1[1])

    def part0(r, b):
        Pb[b, r, :] = mn(W[0, r, :kd], T0[0, b]) + mn(W[1, r, :kd], T0[1, b])

    q_u = rcopy(Qa.at[0], R.at[slot(0)], s_z.at[4], r_r.at[0], 1, 0)

    def q_d(b):
        return rcopy(QD.at[b], PR.at[y, rs_(k, 0, NS), COLS[b]], s_z.at[4], r_r.at[1], 1, 0)

    @pl.when(z == 1)
    def _():
        wait_recv(X.at[1 - k, :, DALL], r_d.at[NS])

        def step_u(q):
            zU(q)

            @pl.when(q < 5)
            def _():
                u_fwd(q).start()

            turn(q)

        each(0, NU, step_u)
        zU(NU, XU)
        each(NU, nd, turn)
        if xd:
            turn(nd, xd)

        @pl.when(c != 0)
        def _():
            q_u.start()

        pl.semaphore_wait(far, n_near)

        def turn0(h, b, lo, hi):
            T0[h, b, lo:hi, :] = Y[h, brows(b), pl.ds(ku + lo, hi - lo)].T

        def step(i):
            @pl.when(i < 2 * NS)
            def _():
                zD(i)

            @pl.when(i == 3)
            def _():
                wait_w(rs_(0, 0, NS), 0)
                part1(rs_(0, 0, NS))

                @pl.when(y == 0)
                def _():
                    x31.start()

                each(5, 10, lambda q: u_fwd(q).start())

            @pl.when((i == 5) & (y == 1))
            def _():
                wait_recv(XA.at[rs_(0, 0, NS)], r_x.at[0])
                Pa[1, rs_(0, 0, NS), :] += XA[rs_(0, 0, NS), :]
                m31.start()

            @pl.when(i == 16)
            def _():
                def chunk(n):
                    ch = jnp.where(n == 0, k, 1 - k)

                    @pl.when(n == 1)
                    def _():
                        turn0(k, 1, 0, 2048)
                        wait_recv(Y.at[1 - k, brows(1), DALL], r_d.at[1])

                    Pb[1, pl.ds(0, rows - st), :] += mm(W[ch, pl.ds(0, rows - st), :kd], Y[ch, brows(1), DALL])

                each(0, 2, chunk)

                for u in range(4):
                    m30r(u).start()

                @pl.when(y == 1)
                def _():
                    x20(1, 0, 4, 8).start()
                    x20(1, 4, 3, 4).start()

            @pl.when((i == 7) | (i == 17))
            def _():
                b = jnp.where(i == 7, 0, 1)

                @pl.when(b == 0)
                def _():
                    wait_recv(Y.at[1 - k, brows(0), DALL], r_d.at[0])

                turn0(1 - k, b, 0, kd)
                turn0(k, b, 2048, kd)

                @pl.when(b == 0)
                def _():
                    turn0(k, 0, 0, 2048)
                    part0(rs_(0, 0, NS), 0)

                    @pl.when(y == 1)
                    def _():
                        for u in range(2):
                            x30(0, u).start()

            @pl.when((i == 7) | (i == 17))
            def _():
                b = jnp.where(i == 7, 0, 1)
                r = rs_(k, 0, NS)
                QD[b] = mn(X[0, r, DALL], T0[0, b]) + mn(X[1, r, DALL], T0[1, b])
                for bb in range(2):
                    @pl.when((b == bb) & (c != 0))
                    def _():
                        q_d(bb).start()

            @pl.when(i == 7)
            def _():
                each(10, NU, lambda q: u_fwd(q).start())
                u_fwd(NU, XU).start()

            @pl.when((i == 9) & (y == 0))
            def _():
                for u in range(2):
                    wait_recv(XB.at[0, r3(u)], r_x.at[1 + u])
                    Pb[0, r3(u), :] += XB[0, r3(u), :]
                    m30(0, u).start()

            @pl.when((i == 8) | (i == 9) | (i == 13))
            def _():
                g = jnp.where(i == 13, 2, i - 8)
                wait_w(r2(2 * g), 1 + g)
                part1(r2(2 * g))
                part0(r2(2 * g), 0)

                @pl.when(y == 1)
                def _():
                    x21(2 * g, 2, 5 + g).start()
                    x20(0, 2 * g, 2, 5 + g).start()

            @pl.when(((i == 10) | (i == 11) | (i == 15)) & (y == 0))
            def _():
                g = jnp.where(i == 15, 2, i - 10)
                wait_recv(XA.at[pl.ds(0, 48)], r_x.at[5 + g])
                Pa[1, r2(2 * g), :] += XA[r2(2 * g), :]
                Pb[0, r2(2 * g), :] += XB[0, r2(2 * g), :]
                m21(2 * g, 2, 1).start()
                m20(0, 2 * g, 2, 5).start()

            @pl.when((i == 17) & (y == 0))
            def _():
                wait_recv(XA.at[pl.ds(0, 24)], r_x.at[3])
                Pa[1, r2(6, 1), :] += XA[r2(6, 1), :]
                m21(6, 1, 2).start()
                Pb[0, r2(6, 1), :] += XB[0, r2(6, 1), :]
                m20(0, 6, 1, 7).start()

            @pl.when((i == 14) | (i == 18))
            def _():
                t = jnp.where(i == 14, 6, 7)
                wait_w(r2(t, 1), t - 2)
                part1(r2(t, 1))

                @pl.when((y == 1) & (i == 18))
                def _():
                    d21.start()

                @pl.when((y == 0) & (i == 18))
                def _():
                    m21(7, 1, 2).start()

                part0(r2(t, 1), 0)

                @pl.when((y == 1) & (i == 14))
                def _():
                    x21(6, 1, 3).start()
                    x20(0, 6, 1, 3).start()

                @pl.when((y == 1) & (i == 18))
                def _():
                    d20[0].start()

                @pl.when((y == 0) & (i == 18))
                def _():
                    m20(0, 7, 1, 7).start()
                    for f, n, x in ((0, 4, 8), (4, 3, 4)):
                        wait_recv(XB.at[1, r2(f, n)], r_x.at[x])
                        Pb[1, r2(f, n), :] += XB[1, r2(f, n), :]
                        m20(1, f, n, 6).start()

                @pl.when(i == 18)
                def _():
                    part0(r2(7, 1), 1)

                    @pl.when(y == 1)
                    def _():
                        d20[1].start()

                    @pl.when(y == 0)
                    def _():
                        m20(1, 7, 1, 7).start()

        each(0, 19, step)

    def d_fwd(t):
        h, s = t % 2, t // 2
        return rcopy(Y.at[k, rs_(h, s), DALL], W.at[k, rs_(0, s), pl.ds(0, kd)], s_z.at[0], r_w.at[0], 1, 2 * y + h)

    def u_sib(s):
        return rcopy(Y.at[k, us_(s), UALL], Y.at[k, us_(s), UALL], s_z.at[1], r_d.at[s], z, sib)

    def q1send(s):
        return rcopy(Qa.at[1, us_(s)], R.at[c, us_(s)], s_z.at[4], r_r.at[0], 3, 2)

    def y2(q, w=PW):
        wait_recv(W.at[:, :, up(q, w)], r_w.at[q])
        Pa[0] += mm(X[0, :, up(q, w)], W[0, :, up(q, w)]) + mm(X[1, :, up(q, w)], W[1, :, up(q, w)])

    def y3(b, q, w=PW):
        r = pl.ds(b * half, half)
        Pa[1, r, :] += mm(Y[0, r, up(q, w)], W[0, :, up(q, w)]) + mm(Y[1, r, up(q, w)], W[1, :, up(q, w)])

    def wait_ysib(s):
        wait_recv(Y.at[1 - k, us_(s), UALL], r_d.at[s])

    def s3(r, cols=CA):
        return rcopy(Pa.at[1, r, cols], R.at[y, r, cols], s_z.at[2], r_r.at[0], 3, k)

    s2 = rcopy(Pa.at[0], R.at[0], s_z.at[2], r_r.at[0], 2, k)

    def add(i, r, cols):
        Pa[i, r, cols] += PR[i, r, cols]

    def wait_pr(n, cols, sem):
        wait_recv(PR.at[0, pl.ds(0, n), cols], r_p.at[sem])

    def strip31(s):
        wait_ysib(s)
        r = us_(s)
        Pa[1, r, :] = mm(Y[0, r, UALL], W[0, :, :ku]) + mm(Y[1, r, UALL], W[1, :, :ku])

        @pl.when(y == 1)
        def _():
            add(1, r, CA)

        s3(r).start()

    @pl.when(z == 2)
    def _():
        def step_d(t):
            wait_recv(Y.at[k, rs_(t % 2, t // 2), DALL], r_y.at[t])
            d_fwd(t).start()

            @pl.when(t == 1)
            def _():
                wait_recv(X.at[1 - k, :, UALL], r_d.at[NS])

            @pl.when((k == 1) & (t >= 1))
            def _():
                y2(t - 1)

            r = rs_(t % 2, t // 2)
            Qa[1, r, :] = mm(Y[k, r, DALL], X[k, :, DALL])

        each(0, 2 * NS, step_d)
        each(2, 2 * NS, lambda t: z2_d(t).start())

        pl.semaphore_wait(far, n_near)

        @pl.when(k == 1)
        def _():
            y2(NU, XU)

            @pl.when(y == 1)
            def _():
                s2.start()


        def q1(s):
            Qa[1, us_(s), :] += mm(Y[k, us_(s), UALL], X[k, :, UALL])
            q1send(s).start()

        def step_u(s):
            @pl.when((k == 0) & (s >= 1))
            def _():
                y2(2 * s - 1)

            @pl.when(k == 0)
            def _():
                y2(2 * s)

            @pl.when((k == 0) & (s == 4))
            def _():
                each(0, 4, wait_ysib)
                each(0, 7, lambda q: y3(0, q))

            @pl.when((k == 0) & (s >= 4))
            def _():
                y3(0, 2 * s - 1)
                y3(0, 2 * s)

            wait_recv(Y.at[k, us_(s), UALL], r_y.at[2 * NS + s])
            u_sib(s).start()

            @pl.when((k == 1) & (y == 1) & (s == 4))
            def _():
                wait_recv(PR.at[1], r_p.at[0])

            @pl.when((k == 1) & (s >= 4) & (s <= 6))
            def _():
                each(2 * s - 8, 2 * s - 6, strip31)

            @pl.when((k == 1) | (s < NS - 1))
            def _():
                q1(s)

        each(0, NS, step_u)

        @pl.when(k == 1)
        def _():
            each(NS - 2, NS, strip31)

            @pl.when(y == 0)
            def _():
                wait_pr(192, CA, 1)
                for h in range(2):
                    add(0, rs_(h, 0, 6), CA)
                wait_pr(64, CA, 2)
                for h in range(2):
                    add(0, rs_(h, 6, 2), CA)

        @pl.when(k == 0)
        def _():
            y2(NU, XU)

            @pl.when(y == 1)
            def _():
                s2.start()

            y3(0, NU, XU)
            each(NS - 1, NS - y, q1)

            @pl.when(y == 0)
            def _():
                wait_pr(rows, C0, 0)
                add(1, pl.ds(0, half), C0)


            s3(pl.ds(0, half), C0).start()

            each(4, NS, wait_ysib)

            def low(b):
                r = pl.ds(pl.multiple_of(b * half, half), half)
                Pa[1, r, :] = mm(Y[0, r, UALL], W[0, :, :ku]) + mm(Y[1, r, UALL], W[1, :, :ku])

            each(1 + k, 2, low)

            @pl.when(y == 0)
            def _():
                add(1, pl.ds(half, half), C0)

            s3(pl.ds(half, half), C0).start()
            each(NS - 1, NS - 1 + y, q1)

            for u in range(4):
                wait_pr(64, C1, 1 + u)
                for h in range(2):
                    add(1, rs_(h, 2 * u, 2), C1)
                    s3(rs_(h, 2 * u, 2), C1).start()

            @pl.when(y == 0)
            def _():
                wait_pr(192, C0, 5)
                for h in range(2):
                    add(0, rs_(h, 0, 6), C0)
                wait_pr(224, C1, 6)
                for h in range(2):
                    add(0, rs_(h, 0, 7), C1)
                wait_pr(96, C0, 7)
                for h in range(2):
                    add(0, rs_(h, 6, 2), C0)
                    add(0, rs_(h, 7), C1)

    @pl.when((z == 0) | (z == 3))
    def _():
        pl.semaphore_wait(far, n_near)

    @pl.when(c > z)
    def _():
        o_ref[...] = jnp.zeros_like(o_ref)

    @pl.when(c == z)
    def _():
        wait_recv(R.at[pl.ds(0, 3)], r_r.at[0])
        total = Qa[dq] + R[0] + R[1] + R[2]
        diff = lax.broadcasted_iota(jnp.int32, (rows, rows), 0) - lax.broadcasted_iota(jnp.int32, (rows, rows), 1)
        o_ref[...] = jnp.where(diff >= 0, total, 0.0).astype(o_ref.dtype)

    @pl.when((z == 1) & (c == 0))
    def _():
        wait_recv(R.at[pl.ds(0, 3)], r_r.at[0])
        Qa[0] += R[0] + R[1] + R[2]
        wait_recv(R.at[pl.ds(0, 3), pl.ds(0, half)], r_r.at[1])
        for b in range(2):
            PR[0, pl.ds(0, half), COLS[b]] = QD[b]
        o_ref[...] = (Qa[0] + PR[0] + PR[1]).astype(o_ref.dtype)

    @pl.when((z == 2) & (y == 0))
    def _():
        wait_recv(R.at[0], r_r.at[0])
        wait_recv(R.at[1, pl.ds(0, 32)], r_r.at[1])
        for h in range(2):
            Pa[0, rs_(h, 7), :] += R[1, rs_(h, 7), :]
        o_ref[...] = (Pa[0] + R[0]).astype(o_ref.dtype)

    @pl.when((z == 3) & (c == 2))
    def _():
        wait_recv(R, r_r.at[0])
        o_ref[...] = (R[0] + R[1] + R[2] + R[3]).astype(o_ref.dtype)

    @pl.when((z == 3) & (y == 0))
    def _():
        wait_recv(R.at[pl.ds(0, 2)], r_r.at[0])

        o_ref[...] = (R[0] + R[1]).astype(o_ref.dtype)

    @pl.when(c != z)
    def _():
        wait_recv(Qa.at[0], s_z.at[3])

    @pl.when((z == 0) | (z == 3))
    def _():
        wait_recv(X.at[k], s_z.at[0])

    @pl.when(z == 1)
    def _():
        wait_recv(W.at[:, :, pl.ds(0, ku)], s_z.at[0])
        wait_recv(W.at[:, :, pl.ds(0, kd)], s_z.at[1])
        wait_recv(Pa, s_z.at[2])

        @pl.when(c != 0)
        def _():
            wait_recv(R.at[pl.ds(0, 3), pl.ds(0, half)], s_z.at[4])

    @pl.when(z == 2)
    def _():
        wait_recv(W.at[:, :, pl.ds(0, kd)], s_z.at[0])
        wait_recv(W.at[:, :, pl.ds(0, ku)], s_z.at[1])
        wait_recv(Qa.at[1], s_z.at[4])

        @pl.when(y == 0)
        def _():
            wait_recv(Pa.at[0], s_z.at[2])

        @pl.when(y == 1)
        def _():
            wait_recv(Pa, s_z.at[2])


def solution(mesh):
    def local_fn(a_local):
        rows, m = a_local.shape
        kd = m - NU * PW - XU
        f32, bf16 = jnp.float32, jnp.bfloat16
        dma = pltpu.SemaphoreType.DMA
        return pl.pallas_call(
            kernel,
            out_shape=pltpu.VMEM((rows, rows), bf16),
            in_specs=[pl.BlockSpec(memory_space=pl.ANY)],
            out_specs=pl.BlockSpec(memory_space=pltpu.VMEM),
            scratch_shapes=[
                pltpu.VMEM((2, rows, m), bf16),
                pltpu.VMEM((2, rows, m), bf16),
                pltpu.VMEM((2, rows, kd), bf16),
                pltpu.VMEM((2, 2, kd, rows // 2), bf16),
                pltpu.VMEM((2, kd, rows), bf16),
                pltpu.VMEM((2, rows, rows), f32),
                pltpu.VMEM((2, rows, rows // 2), f32),
                pltpu.VMEM((2, rows, rows), f32),
                pltpu.VMEM((2, rows // 2, rows // 2), f32),
                pltpu.VMEM((4, rows, rows), f32),
                pltpu.VMEM((2, rows, rows), f32),
                pltpu.VMEM((rows, rows), f32),
                pltpu.VMEM((2, rows, rows // 2), f32),
                pltpu.SemaphoreType.REGULAR,
                dma((1,)), dma((5,)), dma((4 * NS,)), dma((NS + 1,)), dma((NU + 1,)), dma((8,)), dma((2,)), dma((9,)),
            ],
            compiler_params=pltpu.CompilerParams(
                collective_id=0, has_side_effects=True, vmem_limit_bytes=56 * 1024 * 1024),
        )(a_local)

    part_spec = P(("batch", "row"), "col")
    return jax.shard_map(local_fn, mesh=mesh, in_specs=(part_spec,), out_specs=part_spec, check_vma=False)
```

```python
import jax
import jax.numpy as jnp
from jax import lax
from jax.experimental import pallas as pl
from jax.experimental.pallas import tpu as pltpu
from jax.sharding import PartitionSpec as P

MESH = pl.DeviceIdType.MESH
PW = 256
NU = 15
XU = 256
NS = 8


def mm(a, b):
    return lax.dot_general(a, b, (((1,), (1,)), ((), ())), preferred_element_type=jnp.float32)


def mn(a, b):
    return lax.dot_general(a, b, (((1,), (0,)), ((), ())), preferred_element_type=jnp.float32)


def kernel(a_ref, o_ref, X, Y, W, T0, T1, Pa, Pb, Qa, QD, R, PR, XA, XB, far, ld, s_z, r_y, r_d, r_w, r_p, r_r, r_x):
    rows, m = a_ref.shape
    ku = NU * PW + XU
    kd = m - ku
    nd, xd = kd // PW, kd % PW
    half = rows // 2
    st = half // NS
    us = rows // NS
    z = lax.axis_index("row")
    c = lax.axis_index("col")
    y = c // 2
    k = c % 2
    sib = 2 * y + 1 - k

    def rcopy(src, dst, ss, rs, row, col):
        return pltpu.make_async_remote_copy(
            src_ref=src, dst_ref=dst, send_sem=ss, recv_sem=rs, device_id={"row": row, "col": col}, device_id_type=MESH)

    def wait_recv(ref, sem):
        pltpu.make_async_copy(ref, ref, sem).wait()

    def up(p, w=PW):
        return pl.ds(pl.multiple_of(p * PW, 128), w)

    def dn(p, w=PW):
        return pl.ds(pl.multiple_of(ku + p * PW, 128), w)

    def rs_(h, s, n=1):
        return pl.ds(pl.multiple_of(h * half + s * st, st), n * st)

    def us_(s):
        return pl.ds(pl.multiple_of(s * us, us), us)

    DALL = pl.ds(ku, kd)
    UALL = pl.ds(0, ku)
    C0, C1 = pl.ds(0, half), pl.ds(half, half)
    COLS = (C0, C1)

    def each(lo, hi, fn):
        lax.fori_loop(lo, hi, lambda i, u: (fn(i), u)[1], 0)

    load = pltpu.make_async_copy(a_ref, X.at[k], ld.at[0])

    def near(sem):
        for dz in (-1, 1):
            @pl.when((z + dz >= 0) & (z + dz <= 3))
            def _():
                for kk in range(2):
                    pl.semaphore_signal(sem, inc=1, device_id={"row": z + dz, "col": 2 * y + kk}, device_id_type=MESH)
        for dc in range(1, 4):
            pl.semaphore_signal(sem, inc=1, device_id={"row": z, "col": (c + dc) % 4}, device_id_type=MESH)

    n_near = jnp.where((z == 0) | (z == 3), 5, 7)
    bar = pltpu.get_barrier_semaphore()
    near(bar)
    load.start()
    pl.semaphore_wait(bar, n_near)

    def z0_u(q, w=PW):
        return rcopy(a_ref.at[:, up(q, w)], Y.at[k, :, up(q, w)], s_z.at[0], r_y.at[q], 1, c)

    def z0_d(t):
        r = rs_(0, t)
        return rcopy(a_ref.at[r, DALL], Y.at[k, r, DALL], s_z.at[0], r_y.at[2 * NS + t], 1, c)

    def z3_d(t):
        r = rs_(t % 2, t // 2)
        return rcopy(a_ref.at[r, DALL], Y.at[k, r, DALL], s_z.at[0], r_y.at[t], 2, c)

    def z3_u(s):
        r = us_(s)
        return rcopy(a_ref.at[r, UALL], Y.at[k, r, UALL], s_z.at[0], r_y.at[2 * NS + s], 2, c)

    def z1_u(q, w=PW):
        return rcopy(a_ref.at[:, up(q, w)], W.at[k, :, up(q, w)], s_z.at[0], r_w.at[q], 2, 2 * y + 1)

    def z2_d(t):
        h, s = t % 2, t // 2
        return rcopy(a_ref.at[rs_(h, s), DALL], W.at[k, rs_(1, s), pl.ds(0, kd)], s_z.at[0], r_w.at[jnp.where(s < 6, 1 + s // 2, s - 2)], 1, 2 * y + h)

    @pl.when(z == 0)
    def _():
        each(0, NU, lambda q: z0_u(q).start())
        z0_u(NU, XU).start()
        each(0, 2 * NS, lambda t: z0_d(t).start())

    @pl.when(z == 3)
    def _():
        each(0, 2 * NS, lambda t: z3_d(t).start())
        each(0, NS, lambda s: z3_u(s).start())

    x_d = rcopy(a_ref.at[:, DALL], X.at[k, :, DALL], s_z.at[1], r_d.at[NS], z, sib)
    x_u = rcopy(a_ref.at[:, UALL], X.at[k, :, UALL], s_z.at[1], r_d.at[NS], z, sib)

    @pl.when(z == 1)
    def _():
        each(0, NU, lambda q: z1_u(q).start())
        z1_u(NU, XU).start()
        x_d.start()

    @pl.when(z == 2)
    def _():
        z2_d(0).start()
        z2_d(1).start()
        x_u.start()

    near(far)

    Pa[...] = jnp.zeros_like(Pa)
    Qa[...] = jnp.zeros_like(Qa)
    Pb[...] = jnp.zeros_like(Pb)
    load.wait()
    dq = jnp.where(z == 1, 1, 0)

    def diag(p):
        cs = pl.ds(pl.multiple_of(p * 512, 512), 512)
        Qa[dq] += mm(X[k, :, cs], X[k, :, cs])

    each(0, m // 512, diag)

    def slot(owner):
        return (c - owner + 3) % 4

    dsend = rcopy(Qa.at[dq], R.at[slot(z)], s_z.at[3], r_r.at[0], z, z)

    @pl.when(c != z)
    def _():
        dsend.start()

    def u_fwd(q, w=PW):
        return rcopy(Y.at[k, :, up(q, w)], W.at[k, :, up(q, w)], s_z.at[0], r_w.at[q], 2, 2 * y)

    def zU(q, w=PW):
        wait_recv(Y.at[k, :, up(q, w)], r_y.at[q])
        Qa[0] += mm(X[k, :, up(q, w)], Y[k, :, up(q, w)])

    def turn(p, w=PW):
        for h in range(2):
            T1[h, up(p, w), :] = X[h, :, dn(p, w)].T

    def d_sib(t):
        return rcopy(Y.at[k, rs_(0, t), DALL], Y.at[k, rs_(0, t), DALL], s_z.at[1], r_d.at[t // NS], z, sib)

    def zD(t):
        wait_recv(Y.at[k, rs_(0, t), DALL], r_y.at[2 * NS + t])
        d_sib(t).start()

    def brows(b):
        return pl.ds(pl.multiple_of(b * half, half), half)

    def wait_w(r, n):
        wait_recv(W.at[:, r, pl.ds(0, kd)], r_w.at[n])

    CA = pl.ds(0, rows)
    peer = (c + 2) % 4

    def r3(u):
        return rs_(0, 4 * u, 4)

    def r2(s, n=2):
        return rs_(1, s, n)

    def xsend(src, dst, n):
        return rcopy(src, dst, s_z.at[2], r_x.at[n], 1, peer)

    x31 = xsend(Pa.at[1, rs_(0, 0, NS)], XA.at[rs_(0, 0, NS)], 0)

    def x30(b, u):
        return xsend(Pb.at[b, r3(u)], XB.at[b, r3(u)], 1 + 2 * b + u)

    def x21(s, n, rs):
        return xsend(Pa.at[1, r2(s, n)], XA.at[r2(s, n)], rs)

    def x20(b, s, n, rs):
        return xsend(Pb.at[b, r2(s, n)], XB.at[b, r2(s, n)], rs)

    def msend(src, i, s, n, j, cols, rs):
        return rcopy(src, PR.at[i, rs_(k, s, n), cols], s_z.at[2], r_p.at[rs], 2, j)

    m31 = msend(Pa.at[1, rs_(0, 0, NS)], 1, 0, NS, 3, CA, 0)

    def m30(b, u):
        return msend(Pb.at[b, r3(u)], 1, 4 * u, 4, 0, C0, 0)

    def m30r(u):
        return rcopy(Pb.at[1, rs_(0, 2 * u, 2)], PR.at[1, rs_(k, 2 * u, 2), C1], s_z.at[2], r_p.at[1 + u], 2, 2 * y)

    def m21(s, n, rs):
        return msend(Pa.at[1, r2(s, n)], 0, s, n, 1, CA, rs)

    def m20(b, s, n, rs):
        return msend(Pb.at[b, r2(s, n)], 0, s, n, 0, COLS[b], rs)

    def d2(src, j, cols):
        return rcopy(src, R.at[1, rs_(k, 7), cols], s_z.at[2], r_r.at[1], 2, j)

    d21 = d2(Pa.at[1, r2(7, 1)], 1, CA)
    d20 = [d2(Pb.at[b, r2(7, 1)], 0, COLS[b]) for b in range(2)]

    def part1(r):
        Pa[1, r, :] = mn(W[0, r, :kd], T1[0]) + mn(W[1, r, :kd], T1[1])

    def part0(r, b):
        Pb[b, r, :] = mn(W[0, r, :kd], T0[0, b]) + mn(W[1, r, :kd], T0[1, b])

    q_u = rcopy(Qa.at[0], R.at[slot(0)], s_z.at[4], r_r.at[0], 1, 0)

    def q_d(b):
        return rcopy(QD.at[b], PR.at[y, rs_(k, 0, NS), COLS[b]], s_z.at[4], r_r.at[1], 1, 0)

    @pl.when(z == 1)
    def _():
        wait_recv(X.at[1 - k, :, DALL], r_d.at[NS])

        def step_u(q):
            zU(q)

            @pl.when(q < 5)
            def _():
                u_fwd(q).start()

            turn(q)

        each(0, NU, step_u)
        zU(NU, XU)
        each(NU, nd, turn)
        if xd:
            turn(nd, xd)

        @pl.when(c != 0)
        def _():
            q_u.start()

        pl.semaphore_wait(far, n_near)

        def turn0(h, b, lo, hi):
            T0[h, b, lo:hi, :] = Y[h, brows(b), pl.ds(ku + lo, hi - lo)].T

        def step(i):
            @pl.when(i < 2 * NS)
            def _():
                zD(i)

            @pl.when(i == 3)
            def _():
                wait_w(rs_(0, 0, NS), 0)
                part1(rs_(0, 0, NS))

                @pl.when(y == 0)
                def _():
                    x31.start()

                each(5, 10, lambda q: u_fwd(q).start())

            @pl.when((i == 5) & (y == 1))
            def _():
                wait_recv(XA.at[rs_(0, 0, NS)], r_x.at[0])
                Pa[1, rs_(0, 0, NS), :] += XA[rs_(0, 0, NS), :]
                m31.start()

            @pl.when(i == 16)
            def _():
                def chunk(n):
                    ch = jnp.where(n == 0, k, 1 - k)

                    @pl.when(n == 1)
                    def _():
                        turn0(k, 1, 0, 2048)
                        wait_recv(Y.at[1 - k, brows(1), DALL], r_d.at[1])

                    Pb[1, pl.ds(0, rows - st), :] += mm(W[ch, pl.ds(0, rows - st), :kd], Y[ch, brows(1), DALL])

                each(0, 2, chunk)

                for u in range(4):
                    m30r(u).start()

                @pl.when(y == 1)
                def _():
                    x20(1, 0, 4, 8).start()
                    x20(1, 4, 3, 4).start()

            @pl.when((i == 7) | (i == 17))
            def _():
                b = jnp.where(i == 7, 0, 1)

                @pl.when(b == 0)
                def _():
                    wait_recv(Y.at[1 - k, brows(0), DALL], r_d.at[0])

                turn0(1 - k, b, 0, kd)
                turn0(k, b, 2048, kd)

                @pl.when(b == 0)
                def _():
                    turn0(k, 0, 0, 2048)
                    part0(rs_(0, 0, NS), 0)

                    @pl.when(y == 1)
                    def _():
                        for u in range(2):
                            x30(0, u).start()

            @pl.when((i == 7) | (i == 17))
            def _():
                b = jnp.where(i == 7, 0, 1)
                r = rs_(k, 0, NS)
                QD[b] = mn(X[0, r, DALL], T0[0, b]) + mn(X[1, r, DALL], T0[1, b])
                for bb in range(2):
                    @pl.when((b == bb) & (c != 0))
                    def _():
                        q_d(bb).start()

            @pl.when(i == 7)
            def _():
                each(10, NU, lambda q: u_fwd(q).start())
                u_fwd(NU, XU).start()

            @pl.when((i == 9) & (y == 0))
            def _():
                for u in range(2):
                    wait_recv(XB.at[0, r3(u)], r_x.at[1 + u])
                    Pb[0, r3(u), :] += XB[0, r3(u), :]
                    m30(0, u).start()

            @pl.when((i == 8) | (i == 9) | (i == 13))
            def _():
                g = jnp.where(i == 13, 2, i - 8)
                wait_w(r2(2 * g), 1 + g)
                part1(r2(2 * g))
                part0(r2(2 * g), 0)

                @pl.when(y == 1)
                def _():
                    x21(2 * g, 2, 5 + g).start()
                    x20(0, 2 * g, 2, 5 + g).start()

            @pl.when(((i == 10) | (i == 11) | (i == 15)) & (y == 0))
            def _():
                g = jnp.where(i == 15, 2, i - 10)
                wait_recv(XA.at[pl.ds(0, 48)], r_x.at[5 + g])
                Pa[1, r2(2 * g), :] += XA[r2(2 * g), :]
                Pb[0, r2(2 * g), :] += XB[0, r2(2 * g), :]
                m21(2 * g, 2, 1).start()
                m20(0, 2 * g, 2, 5).start()

            @pl.when((i == 17) & (y == 0))
            def _():
                wait_recv(XA.at[pl.ds(0, 24)], r_x.at[3])
                Pa[1, r2(6, 1), :] += XA[r2(6, 1), :]
                m21(6, 1, 2).start()
                Pb[0, r2(6, 1), :] += XB[0, r2(6, 1), :]
                m20(0, 6, 1, 7).start()

            @pl.when((i == 14) | (i == 18))
            def _():
                t = jnp.where(i == 14, 6, 7)
                wait_w(r2(t, 1), t - 2)
                part1(r2(t, 1))

                @pl.when((y == 1) & (i == 18))
                def _():
                    d21.start()

                @pl.when((y == 0) & (i == 18))
                def _():
                    m21(7, 1, 2).start()

                part0(r2(t, 1), 0)

                @pl.when((y == 1) & (i == 14))
                def _():
                    x21(6, 1, 3).start()
                    x20(0, 6, 1, 3).start()

                @pl.when((y == 1) & (i == 18))
                def _():
                    d20[0].start()

                @pl.when((y == 0) & (i == 18))
                def _():
                    m20(0, 7, 1, 7).start()
                    for f, n, x in ((0, 4, 8), (4, 3, 4)):
                        wait_recv(XB.at[1, r2(f, n)], r_x.at[x])
                        Pb[1, r2(f, n), :] += XB[1, r2(f, n), :]
                        m20(1, f, n, 6).start()

                @pl.when(i == 18)
                def _():
                    part0(r2(7, 1), 1)

                    @pl.when(y == 1)
                    def _():
                        d20[1].start()

                    @pl.when(y == 0)
                    def _():
                        m20(1, 7, 1, 7).start()

        each(0, 19, step)

    def d_fwd(t):
        h, s = t % 2, t // 2
        return rcopy(Y.at[k, rs_(h, s), DALL], W.at[k, rs_(0, s), pl.ds(0, kd)], s_z.at[0], r_w.at[0], 1, 2 * y + h)

    def u_sib(s):
        return rcopy(Y.at[k, us_(s), UALL], Y.at[k, us_(s), UALL], s_z.at[1], r_d.at[s], z, sib)

    def q1send(s):
        return rcopy(Qa.at[1, us_(s)], R.at[c, us_(s)], s_z.at[4], r_r.at[0], 3, 2)

    def y2(q, w=PW):
        wait_recv(W.at[:, :, up(q, w)], r_w.at[q])
        Pa[0] += mm(X[0, :, up(q, w)], W[0, :, up(q, w)]) + mm(X[1, :, up(q, w)], W[1, :, up(q, w)])

    def y3(b, q, w=PW):
        r = pl.ds(b * half, half)
        Pa[1, r, :] += mm(Y[0, r, up(q, w)], W[0, :, up(q, w)]) + mm(Y[1, r, up(q, w)], W[1, :, up(q, w)])

    def wait_ysib(s):
        wait_recv(Y.at[1 - k, us_(s), UALL], r_d.at[s])

    def s3(r, cols=CA):
        return rcopy(Pa.at[1, r, cols], R.at[y, r, cols], s_z.at[2], r_r.at[0], 3, k)

    s2 = rcopy(Pa.at[0], R.at[0], s_z.at[2], r_r.at[0], 2, k)

    def add(i, r, cols):
        Pa[i, r, cols] += PR[i, r, cols]

    def wait_pr(n, cols, sem):
        wait_recv(PR.at[0, pl.ds(0, n), cols], r_p.at[sem])

    def strip31(s):
        wait_ysib(s)
        r = us_(s)
        Pa[1, r, :] = mm(Y[0, r, UALL], W[0, :, :ku]) + mm(Y[1, r, UALL], W[1, :, :ku])

        @pl.when(y == 1)
        def _():
            add(1, r, CA)

        s3(r).start()

    @pl.when(z == 2)
    def _():
        def step_d(t):
            wait_recv(Y.at[k, rs_(t % 2, t // 2), DALL], r_y.at[t])
            d_fwd(t).start()

            @pl.when(t == 1)
            def _():
                wait_recv(X.at[1 - k, :, UALL], r_d.at[NS])

            @pl.when((k == 1) & (t >= 1))
            def _():
                y2(t - 1)

            r = rs_(t % 2, t // 2)
            Qa[1, r, :] = mm(Y[k, r, DALL], X[k, :, DALL])

        each(0, 2 * NS, step_d)
        each(2, 2 * NS, lambda t: z2_d(t).start())

        pl.semaphore_wait(far, n_near)

        @pl.when(k == 1)
        def _():
            y2(NU, XU)

            @pl.when(y == 1)
            def _():
                s2.start()


        def q1(s):
            Qa[1, us_(s), :] += mm(Y[k, us_(s), UALL], X[k, :, UALL])
            q1send(s).start()

        def step_u(s):
            @pl.when((k == 0) & (s >= 1))
            def _():
                y2(2 * s - 1)

            @pl.when(k == 0)
            def _():
                y2(2 * s)

            @pl.when((k == 0) & (s == 4))
            def _():
                each(0, 4, wait_ysib)
                each(0, 7, lambda q: y3(0, q))

            @pl.when((k == 0) & (s >= 4))
            def _():
                y3(0, 2 * s - 1)
                y3(0, 2 * s)

            wait_recv(Y.at[k, us_(s), UALL], r_y.at[2 * NS + s])
            u_sib(s).start()

            @pl.when((k == 1) & (y == 1) & (s == 4))
            def _():
                wait_recv(PR.at[1], r_p.at[0])

            @pl.when((k == 1) & (s >= 4) & (s <= 6))
            def _():
                each(2 * s - 8, 2 * s - 6, strip31)

            @pl.when((k == 1) | (s < NS - 1))
            def _():
                q1(s)

        each(0, NS, step_u)

        @pl.when(k == 1)
        def _():
            each(NS - 2, NS, strip31)

            @pl.when(y == 0)
            def _():
                wait_pr(192, CA, 1)
                for h in range(2):
                    add(0, rs_(h, 0, 6), CA)
                wait_pr(64, CA, 2)
                for h in range(2):
                    add(0, rs_(h, 6, 2), CA)

        @pl.when(k == 0)
        def _():
            y2(NU, XU)

            @pl.when(y == 1)
            def _():
                s2.start()

            y3(0, NU, XU)
            each(NS - 1, NS - y, q1)

            @pl.when(y == 0)
            def _():
                wait_pr(rows, C0, 0)
                add(1, pl.ds(0, half), C0)


            s3(pl.ds(0, half), C0).start()

            each(4, NS, wait_ysib)

            def low(b):
                r = pl.ds(pl.multiple_of(b * half, half), half)
                Pa[1, r, :] = mm(Y[0, r, UALL], W[0, :, :ku]) + mm(Y[1, r, UALL], W[1, :, :ku])

            each(1 + k, 2, low)

            @pl.when(y == 0)
            def _():
                add(1, pl.ds(half, half), C0)

            s3(pl.ds(half, half), C0).start()
            each(NS - 1, NS - 1 + y, q1)

            for u in range(4):
                wait_pr(64, C1, 1 + u)
                for h in range(2):
                    add(1, rs_(h, 2 * u, 2), C1)
                    s3(rs_(h, 2 * u, 2), C1).start()

            @pl.when(y == 0)
            def _():
                wait_pr(192, C0, 5)
                for h in range(2):
                    add(0, rs_(h, 0, 6), C0)
                wait_pr(224, C1, 6)
                for h in range(2):
                    add(0, rs_(h, 0, 7), C1)
                wait_pr(96, C0, 7)
                for h in range(2):
                    add(0, rs_(h, 6, 2), C0)
                    add(0, rs_(h, 7), C1)

    @pl.when((z == 0) | (z == 3))
    def _():
        pl.semaphore_wait(far, n_near)

    @pl.when(c > z)
    def _():
        o_ref[...] = jnp.zeros_like(o_ref)

    @pl.when(c == z)
    def _():
        wait_recv(R.at[pl.ds(0, 3)], r_r.at[0])
        total = Qa[dq] + R[0] + R[1] + R[2]
        diff = lax.broadcasted_iota(jnp.int32, (rows, rows), 0) - lax.broadcasted_iota(jnp.int32, (rows, rows), 1)
        o_ref[...] = jnp.where(diff >= 0, total, 0.0).astype(o_ref.dtype)

    @pl.when((z == 1) & (c == 0))
    def _():
        wait_recv(R.at[pl.ds(0, 3)], r_r.at[0])
        Qa[0] += R[0] + R[1] + R[2]
        wait_recv(R.at[pl.ds(0, 3), pl.ds(0, half)], r_r.at[1])
        for b in range(2):
            PR[0, pl.ds(0, half), COLS[b]] = QD[b]
        o_ref[...] = (Qa[0] + PR[0] + PR[1]).astype(o_ref.dtype)

    @pl.when((z == 2) & (y == 0))
    def _():
        wait_recv(R.at[0], r_r.at[0])
        wait_recv(R.at[1, pl.ds(0, 32)], r_r.at[1])
        for h in range(2):
            Pa[0, rs_(h, 7), :] += R[1, rs_(h, 7), :]
        o_ref[...] = (Pa[0] + R[0]).astype(o_ref.dtype)

    @pl.when((z == 3) & (c == 2))
    def _():
        wait_recv(R, r_r.at[0])
        o_ref[...] = (R[0] + R[1] + R[2] + R[3]).astype(o_ref.dtype)

    @pl.when((z == 3) & (y == 0))
    def _():
        wait_recv(R.at[pl.ds(0, 2)], r_r.at[0])

        o_ref[...] = (R[0] + R[1]).astype(o_ref.dtype)

    @pl.when(c != z)
    def _():
        wait_recv(Qa.at[0], s_z.at[3])

    @pl.when((z == 0) | (z == 3))
    def _():
        wait_recv(X.at[k], s_z.at[0])

    @pl.when(z == 1)
    def _():
        wait_recv(W.at[:, :, pl.ds(0, ku)], s_z.at[0])
        wait_recv(W.at[:, :, pl.ds(0, kd)], s_z.at[1])
        wait_recv(Pa, s_z.at[2])

        @pl.when(c != 0)
        def _():
            wait_recv(R.at[pl.ds(0, 3), pl.ds(0, half)], s_z.at[4])

    @pl.when(z == 2)
    def _():
        wait_recv(W.at[:, :, pl.ds(0, kd)], s_z.at[0])
        wait_recv(W.at[:, :, pl.ds(0, ku)], s_z.at[1])
        wait_recv(Qa.at[1], s_z.at[4])

        @pl.when(y == 0)
        def _():
            wait_recv(Pa.at[0], s_z.at[2])

        @pl.when(y == 1)
        def _():
            wait_recv(Pa, s_z.at[2])


def solution(mesh):
    def local_fn(a_local):
        rows, m = a_local.shape
        kd = m - NU * PW - XU
        f32, bf16 = jnp.float32, jnp.bfloat16
        dma = pltpu.SemaphoreType.DMA
        return pl.pallas_call(
            kernel,
            out_shape=pltpu.VMEM((rows, rows), bf16),
            in_specs=[pl.BlockSpec(memory_space=pl.ANY)],
            out_specs=pl.BlockSpec(memory_space=pltpu.VMEM),
            scratch_shapes=[
                pltpu.VMEM((2, rows, m), bf16),
                pltpu.VMEM((2, rows, m), bf16),
                pltpu.VMEM((2, rows, kd), bf16),
                pltpu.VMEM((2, 2, kd, rows // 2), bf16),
                pltpu.VMEM((2, kd, rows), bf16),
                pltpu.VMEM((2, rows, rows), f32),
                pltpu.VMEM((2, rows, rows // 2), f32),
                pltpu.VMEM((2, rows, rows), f32),
                pltpu.VMEM((2, rows // 2, rows // 2), f32),
                pltpu.VMEM((4, rows, rows), f32),
                pltpu.VMEM((2, rows, rows), f32),
                pltpu.VMEM((rows, rows), f32),
                pltpu.VMEM((2, rows, rows // 2), f32),
                pltpu.SemaphoreType.REGULAR,
                dma((1,)), dma((5,)), dma((4 * NS,)), dma((NS + 1,)), dma((NU + 1,)), dma((8,)), dma((2,)), dma((9,)),
            ],
            compiler_params=pltpu.CompilerParams(
                collective_id=0, has_side_effects=True, vmem_limit_bytes=56 * 1024 * 1024),
        )(a_local)

    part_spec = P(("batch", "row"), "col")
    return jax.shard_map(local_fn, mesh=mesh, in_specs=(part_spec,), out_specs=part_spec, check_vma=False)
```

```python
import jax
import jax.numpy as jnp
from jax import lax
from jax.experimental import pallas as pl
from jax.experimental.pallas import tpu as pltpu
from jax.sharding import PartitionSpec as P

MESH = pl.DeviceIdType.MESH
PW = 256
NU = 15
XU = 128
NS = 8


def mm(a, b):
    return lax.dot_general(a, b, (((1,), (1,)), ((), ())), preferred_element_type=jnp.float32)


def mn(a, b):
    return lax.dot_general(a, b, (((1,), (0,)), ((), ())), preferred_element_type=jnp.float32)


def kernel(a_ref, o_ref, X, Y, W, T0, T1, Pa, Pb, Qa, QD, R, PR, XA, XB, far, ld, s_z, r_y, r_d, r_w, r_p, r_r, r_x):
    rows, m = a_ref.shape
    ku = NU * PW + XU
    kd = m - ku
    nd, xd = kd // PW, kd % PW
    half = rows // 2
    st = half // NS
    us = rows // NS
    z = lax.axis_index("row")
    c = lax.axis_index("col")
    y = c // 2
    k = c % 2
    sib = 2 * y + 1 - k

    def rcopy(src, dst, ss, rs, row, col):
        return pltpu.make_async_remote_copy(
            src_ref=src, dst_ref=dst, send_sem=ss, recv_sem=rs, device_id={"row": row, "col": col}, device_id_type=MESH)

    def wait_recv(ref, sem):
        pltpu.make_async_copy(ref, ref, sem).wait()

    def up(p, w=PW):
        return pl.ds(pl.multiple_of(p * PW, 128), w)

    def dn(p, w=PW):
        return pl.ds(pl.multiple_of(ku + p * PW, 128), w)

    def rs_(h, s, n=1):
        return pl.ds(pl.multiple_of(h * half + s * st, st), n * st)

    def us_(s):
        return pl.ds(pl.multiple_of(s * us, us), us)

    DALL = pl.ds(ku, kd)
    UALL = pl.ds(0, ku)
    C0, C1 = pl.ds(0, half), pl.ds(half, half)
    COLS = (C0, C1)

    def each(lo, hi, fn):
        lax.fori_loop(lo, hi, lambda i, u: (fn(i), u)[1], 0)

    load = pltpu.make_async_copy(a_ref, X.at[k], ld.at[0])

    def near(sem):
        for dz in (-1, 1):
            @pl.when((z + dz >= 0) & (z + dz <= 3))
            def _():
                for kk in range(2):
                    pl.semaphore_signal(sem, inc=1, device_id={"row": z + dz, "col": 2 * y + kk}, device_id_type=MESH)
        for dc in range(1, 4):
            pl.semaphore_signal(sem, inc=1, device_id={"row": z, "col": (c + dc) % 4}, device_id_type=MESH)

    n_near = jnp.where((z == 0) | (z == 3), 5, 7)
    bar = pltpu.get_barrier_semaphore()
    near(bar)
    load.start()
    pl.semaphore_wait(bar, n_near)

    def z0_u(q, w=PW):
        return rcopy(a_ref.at[:, up(q, w)], Y.at[k, :, up(q, w)], s_z.at[0], r_y.at[q // 2], 1, c)

    def z0_d(t):
        r = rs_(0, t)
        return rcopy(a_ref.at[r, DALL], Y.at[k, r, DALL], s_z.at[0], r_y.at[NS + t], 1, c)

    def z3_d(t):
        r = rs_(t % 2, t // 2)
        return rcopy(a_ref.at[r, DALL], Y.at[k, r, DALL], s_z.at[0], r_y.at[t], 2, c)

    def z3_u(s):
        r = us_(s)
        return rcopy(a_ref.at[r, UALL], Y.at[k, r, UALL], s_z.at[0], r_y.at[2 * NS + s], 2, c)

    def z1_u(q, w=PW):
        return rcopy(a_ref.at[:, up(q, w)], W.at[k, :, up(q, w)], s_z.at[0], r_w.at[q], 2, 2 * y + 1)

    def z2_d(t):
        h, s = t % 2, t // 2
        return rcopy(a_ref.at[rs_(h, s), DALL], W.at[k, rs_(1, s), pl.ds(0, kd)], s_z.at[0], r_w.at[jnp.where(s < 6, 1 + s // 2, s - 2)], 1, 2 * y + h)

    @pl.when(z == 0)
    def _():
        each(0, NU, lambda q: z0_u(q).start())
        z0_u(NU, XU).start()
        each(0, 2 * NS, lambda t: z0_d(t).start())

    @pl.when(z == 3)
    def _():
        each(0, 2 * NS, lambda t: z3_d(t).start())
        each(0, NS, lambda s: z3_u(s).start())

    x_d = rcopy(a_ref.at[:, DALL], X.at[k, :, DALL], s_z.at[1], r_d.at[NS], z, sib)
    x_u = rcopy(a_ref.at[:, UALL], X.at[k, :, UALL], s_z.at[1], r_d.at[NS], z, sib)

    @pl.when(z == 1)
    def _():
        each(0, NU, lambda q: z1_u(q).start())
        z1_u(NU, XU).start()
        x_d.start()

    @pl.when(z == 2)
    def _():
        z2_d(0).start()
        z2_d(1).start()
        x_u.start()

    near(far)

    Pa[...] = jnp.zeros_like(Pa)
    Qa[...] = jnp.zeros_like(Qa)
    Pb[...] = jnp.zeros_like(Pb)
    load.wait()
    dq = jnp.where(z == 1, 1, 0)

    def diag(p):
        cs = pl.ds(pl.multiple_of(p * 512, 512), 512)
        Qa[dq] += mm(X[k, :, cs], X[k, :, cs])

    each(0, m // 512, diag)

    def slot(owner):
        return (c - owner + 3) % 4

    dsend = rcopy(Qa.at[dq], R.at[slot(z)], s_z.at[3], r_r.at[0], z, z)

    @pl.when(c != z)
    def _():
        dsend.start()

    def u_fwd(q, w=PW):
        return rcopy(Y.at[k, :, up(q, w)], W.at[k, :, up(q, w)], s_z.at[0], r_w.at[q], 2, 2 * y)

    def zU(q, w=PW):
        wait_recv(Y.at[k, :, up(q, w)], r_y.at[q // 2])
        Qa[0] += mm(X[k, :, up(q, w)], Y[k, :, up(q, w)])

    def turn(p, w=PW):
        for h in range(2):
            T1[h, up(p, w), :] = X[h, :, dn(p, w)].T

    def d_sib(t):
        return rcopy(Y.at[k, rs_(0, t), DALL], Y.at[k, rs_(0, t), DALL], s_z.at[1], r_d.at[t // NS], z, sib)

    def zD(t):
        wait_recv(Y.at[k, rs_(0, t), DALL], r_y.at[NS + t])
        d_sib(t).start()

    def brows(b):
        return pl.ds(pl.multiple_of(b * half, half), half)

    def wait_w(r, n):
        wait_recv(W.at[:, r, pl.ds(0, kd)], r_w.at[n])

    CA = pl.ds(0, rows)
    peer = (c + 2) % 4

    def r3(u):
        return rs_(0, 4 * u, 4)

    def r2(s, n=2):
        return rs_(1, s, n)

    def xsend(src, dst, n):
        return rcopy(src, dst, s_z.at[2], r_x.at[n], 1, peer)

    x31 = xsend(Pa.at[1, rs_(0, 0, NS)], XA.at[rs_(0, 0, NS)], 0)

    def x30(b, u):
        return xsend(Pb.at[b, r3(u)], XB.at[b, r3(u)], 1 + 2 * b + u)

    def x21(s, n, rs):
        return xsend(Pa.at[1, r2(s, n)], XA.at[r2(s, n)], rs)

    def x20(b, s, n, rs):
        return xsend(Pb.at[b, r2(s, n)], XB.at[b, r2(s, n)], rs)

    def msend(src, i, s, n, j, cols, rs):
        return rcopy(src, PR.at[i, rs_(k, s, n), cols], s_z.at[2], r_p.at[rs], 2, j)

    m31 = msend(Pa.at[1, rs_(0, 0, NS)], 1, 0, NS, 3, CA, 0)

    def m30(b, u):
        return msend(Pb.at[b, r3(u)], 1, 4 * u, 4, 0, C0, 0)

    def m30r(u):
        return rcopy(Pb.at[1, rs_(0, 2 * u, 2)], PR.at[1, rs_(k, 2 * u, 2), C1], s_z.at[2], r_p.at[1 + u], 2, 2 * y)

    def m21(s, n, rs):
        return msend(Pa.at[1, r2(s, n)], 0, s, n, 1, CA, rs)

    def m20(b, s, n, rs):
        return msend(Pb.at[b, r2(s, n)], 0, s, n, 0, COLS[b], rs)

    def d2(src, j, cols):
        return rcopy(src, R.at[1, rs_(k, 7), cols], s_z.at[2], r_r.at[1], 2, j)

    d21 = d2(Pa.at[1, r2(7, 1)], 1, CA)
    d20 = [d2(Pb.at[b, r2(7, 1)], 0, COLS[b]) for b in range(2)]

    def part1(r):
        Pa[1, r, :] = mn(W[0, r, :kd], T1[0]) + mn(W[1, r, :kd], T1[1])

    def part0(r, b):
        Pb[b, r, :] = mn(W[0, r, :kd], T0[0, b]) + mn(W[1, r, :kd], T0[1, b])

    q_u = rcopy(Qa.at[0], R.at[slot(0)], s_z.at[4], r_r.at[0], 1, 0)

    def q_d(b):
        return rcopy(QD.at[b], PR.at[y, rs_(k, 0, NS), COLS[b]], s_z.at[4], r_r.at[1], 1, 0)

    @pl.when(z == 1)
    def _():
        wait_recv(X.at[1 - k, :, DALL], r_d.at[NS])

        def step_u(p):
            zU(2 * p, 2 * PW)

            @pl.when(p < 3)
            def _():
                each(2 * p, 2 * p + 2, lambda q: u_fwd(q).start())

            turn(2 * p)
            turn(2 * p + 1)

        each(0, NU // 2, step_u)
        zU(NU - 1, PW + XU)
        turn(NU - 1)
        each(NU, nd, turn)
        if xd:
            turn(nd, xd)

        @pl.when(c != 0)
        def _():
            q_u.start()

        pl.semaphore_wait(far, n_near)

        def turn0(h, b, lo, hi):
            T0[h, b, lo:hi, :] = Y[h, brows(b), pl.ds(ku + lo, hi - lo)].T

        def step(i):
            @pl.when(i < 2 * NS)
            def _():
                zD(i)

            @pl.when(i == 3)
            def _():
                wait_w(rs_(0, 0, NS), 0)
                part1(rs_(0, 0, NS))

                @pl.when(y == 0)
                def _():
                    x31.start()

                each(6, 10, lambda q: u_fwd(q).start())

            @pl.when((i == 5) & (y == 1))
            def _():
                wait_recv(XA.at[rs_(0, 0, NS)], r_x.at[0])
                Pa[1, rs_(0, 0, NS), :] += XA[rs_(0, 0, NS), :]
                m31.start()

            @pl.when(i == 16)
            def _():
                def chunk(n):
                    ch = jnp.where(n == 0, k, 1 - k)

                    @pl.when(n == 1)
                    def _():
                        turn0(k, 1, 0, 2048)
                        wait_recv(Y.at[1 - k, brows(1), DALL], r_d.at[1])

                    Pb[1, pl.ds(0, rows - st), :] += mm(W[ch, pl.ds(0, rows - st), :kd], Y[ch, brows(1), DALL])

                each(0, 2, chunk)

                for u in range(4):
                    m30r(u).start()

                @pl.when(y == 1)
                def _():
                    x20(1, 0, 4, 8).start()
                    x20(1, 4, 3, 4).start()

            @pl.when((i == 7) | (i == 17))
            def _():
                b = jnp.where(i == 7, 0, 1)

                @pl.when(b == 0)
                def _():
                    wait_recv(Y.at[1 - k, brows(0), DALL], r_d.at[0])

                turn0(1 - k, b, 0, kd)
                turn0(k, b, 2048, kd)

                @pl.when(b == 0)
                def _():
                    turn0(k, 0, 0, 2048)
                    part0(rs_(0, 0, NS), 0)

                    @pl.when(y == 1)
                    def _():
                        for u in range(2):
                            x30(0, u).start()

            @pl.when((i == 7) | (i == 17))
            def _():
                b = jnp.where(i == 7, 0, 1)
                r = rs_(k, 0, NS)
                QD[b] = mn(X[0, r, DALL], T0[0, b]) + mn(X[1, r, DALL], T0[1, b])
                for bb in range(2):
                    @pl.when((b == bb) & (c != 0))
                    def _():
                        q_d(bb).start()

            @pl.when(i == 7)
            def _():
                each(10, NU, lambda q: u_fwd(q).start())
                u_fwd(NU, XU).start()

            @pl.when((i == 9) & (y == 0))
            def _():
                for u in range(2):
                    wait_recv(XB.at[0, r3(u)], r_x.at[1 + u])
                    Pb[0, r3(u), :] += XB[0, r3(u), :]
                    m30(0, u).start()

            @pl.when((i == 8) | (i == 9) | (i == 13))
            def _():
                g = jnp.where(i == 13, 2, i - 8)
                wait_w(r2(2 * g), 1 + g)
                part1(r2(2 * g))
                part0(r2(2 * g), 0)

                @pl.when(y == 1)
                def _():
                    x21(2 * g, 2, 5 + g).start()
                    x20(0, 2 * g, 2, 5 + g).start()

            @pl.when(((i == 10) | (i == 11) | (i == 15)) & (y == 0))
            def _():
                g = jnp.where(i == 15, 2, i - 10)
                wait_recv(XA.at[pl.ds(0, 48)], r_x.at[5 + g])
                Pa[1, r2(2 * g), :] += XA[r2(2 * g), :]
                Pb[0, r2(2 * g), :] += XB[0, r2(2 * g), :]
                m21(2 * g, 2, 1).start()
                m20(0, 2 * g, 2, 5).start()

            @pl.when((i == 17) & (y == 0))
            def _():
                wait_recv(XA.at[pl.ds(0, 24)], r_x.at[3])
                Pa[1, r2(6, 1), :] += XA[r2(6, 1), :]
                m21(6, 1, 2).start()
                Pb[0, r2(6, 1), :] += XB[0, r2(6, 1), :]
                m20(0, 6, 1, 7).start()

            @pl.when((i == 14) | (i == 18))
            def _():
                t = jnp.where(i == 14, 6, 7)
                wait_w(r2(t, 1), t - 2)
                part1(r2(t, 1))

                @pl.when((y == 1) & (i == 18))
                def _():
                    d21.start()

                @pl.when((y == 0) & (i == 18))
                def _():
                    m21(7, 1, 2).start()

                part0(r2(t, 1), 0)

                @pl.when((y == 1) & (i == 14))
                def _():
                    x21(6, 1, 3).start()
                    x20(0, 6, 1, 3).start()

                @pl.when((y == 1) & (i == 18))
                def _():
                    d20[0].start()

                @pl.when((y == 0) & (i == 18))
                def _():
                    m20(0, 7, 1, 7).start()
                    for f, n, x in ((0, 4, 8), (4, 3, 4)):
                        wait_recv(XB.at[1, r2(f, n)], r_x.at[x])
                        Pb[1, r2(f, n), :] += XB[1, r2(f, n), :]
                        m20(1, f, n, 6).start()

                @pl.when(i == 18)
                def _():
                    part0(r2(7, 1), 1)

                    @pl.when(y == 1)
                    def _():
                        d20[1].start()

                    @pl.when(y == 0)
                    def _():
                        m20(1, 7, 1, 7).start()

        each(0, 19, step)

    def d_fwd(t):
        h, s = t % 2, t // 2
        return rcopy(Y.at[k, rs_(h, s), DALL], W.at[k, rs_(0, s), pl.ds(0, kd)], s_z.at[0], r_w.at[0], 1, 2 * y + h)

    def u_sib(s):
        return rcopy(Y.at[k, us_(s), UALL], Y.at[k, us_(s), UALL], s_z.at[1], r_d.at[s], z, sib)

    def q1send(s):
        return rcopy(Qa.at[1, us_(s)], R.at[c, us_(s)], s_z.at[4], r_r.at[0], 3, 2)

    def y2(q, w=PW):
        wait_recv(W.at[:, :, up(q, w)], r_w.at[q])
        Pa[0] += mm(X[0, :, up(q, w)], W[0, :, up(q, w)]) + mm(X[1, :, up(q, w)], W[1, :, up(q, w)])

    def y3(b, q, w=PW):
        r = pl.ds(b * half, half)
        Pa[1, r, :] += mm(Y[0, r, up(q, w)], W[0, :, up(q, w)]) + mm(Y[1, r, up(q, w)], W[1, :, up(q, w)])

    def wait_ysib(s):
        wait_recv(Y.at[1 - k, us_(s), UALL], r_d.at[s])

    def s3(r, cols=CA):
        return rcopy(Pa.at[1, r, cols], R.at[y, r, cols], s_z.at[2], r_r.at[0], 3, k)

    s2 = rcopy(Pa.at[0], R.at[0], s_z.at[2], r_r.at[0], 2, k)

    def add(i, r, cols):
        Pa[i, r, cols] += PR[i, r, cols]

    def wait_pr(n, cols, sem):
        wait_recv(PR.at[0, pl.ds(0, n), cols], r_p.at[sem])

    def strip31(s):
        wait_ysib(s)
        r = us_(s)
        Pa[1, r, :] = mm(Y[0, r, UALL], W[0, :, :ku]) + mm(Y[1, r, UALL], W[1, :, :ku])

        @pl.when(y == 1)
        def _():
            add(1, r, CA)

        s3(r).start()

    @pl.when(z == 2)
    def _():
        def step_d(t):
            wait_recv(Y.at[k, rs_(t % 2, t // 2), DALL], r_y.at[t])
            d_fwd(t).start()

            @pl.when(t == 1)
            def _():
                wait_recv(X.at[1 - k, :, UALL], r_d.at[NS])

            @pl.when((k == 1) & (t >= 1))
            def _():
                y2(t - 1)

            r = rs_(t % 2, t // 2)
            Qa[1, r, :] = mm(Y[k, r, DALL], X[k, :, DALL])

        each(0, 2 * NS, step_d)
        each(2, 2 * NS, lambda t: z2_d(t).start())

        pl.semaphore_wait(far, n_near)

        @pl.when(k == 1)
        def _():
            y2(NU, XU)

            @pl.when(y == 1)
            def _():
                s2.start()


        def q1(s):
            Qa[1, us_(s), :] += mm(Y[k, us_(s), UALL], X[k, :, UALL])
            q1send(s).start()

        def step_u(s):
            @pl.when((k == 0) & (s >= 1))
            def _():
                y2(2 * s - 1)

            @pl.when(k == 0)
            def _():
                y2(2 * s)

            @pl.when((k == 0) & (s == 4))
            def _():
                each(0, 4, wait_ysib)
                each(0, 7, lambda q: y3(0, q))

            @pl.when((k == 0) & (s >= 4))
            def _():
                y3(0, 2 * s - 1)
                y3(0, 2 * s)

            wait_recv(Y.at[k, us_(s), UALL], r_y.at[2 * NS + s])
            u_sib(s).start()

            @pl.when((k == 1) & (y == 1) & (s == 4))
            def _():
                wait_recv(PR.at[1], r_p.at[0])

            @pl.when((k == 1) & (s >= 4) & (s <= 6))
            def _():
                each(2 * s - 8, 2 * s - 6, strip31)

            @pl.when((k == 1) | (s < NS - 1))
            def _():
                q1(s)

        each(0, NS, step_u)

        @pl.when(k == 1)
        def _():
            each(NS - 2, NS, strip31)

            @pl.when(y == 0)
            def _():
                wait_pr(192, CA, 1)
                for h in range(2):
                    add(0, rs_(h, 0, 6), CA)
                wait_pr(64, CA, 2)
                for h in range(2):
                    add(0, rs_(h, 6, 2), CA)

        @pl.when(k == 0)
        def _():
            y2(NU, XU)

            @pl.when(y == 1)
            def _():
                s2.start()

            y3(0, NU, XU)
            each(NS - 1, NS - y, q1)

            @pl.when(y == 0)
            def _():
                wait_pr(rows, C0, 0)
                add(1, pl.ds(0, half), C0)


            s3(pl.ds(0, half), C0).start()

            each(4, NS, wait_ysib)

            def low(b):
                r = pl.ds(pl.multiple_of(b * half, half), half)
                Pa[1, r, :] = mm(Y[0, r, UALL], W[0, :, :ku]) + mm(Y[1, r, UALL], W[1, :, :ku])

            each(1 + k, 2, low)

            @pl.when(y == 0)
            def _():
                add(1, pl.ds(half, half), C0)

            s3(pl.ds(half, half), C0).start()
            each(NS - 1, NS - 1 + y, q1)

            for u in range(4):
                wait_pr(64, C1, 1 + u)
                for h in range(2):
                    add(1, rs_(h, 2 * u, 2), C1)
                    s3(rs_(h, 2 * u, 2), C1).start()

            @pl.when(y == 0)
            def _():
                wait_pr(192, C0, 5)
                for h in range(2):
                    add(0, rs_(h, 0, 6), C0)
                wait_pr(224, C1, 6)
                for h in range(2):
                    add(0, rs_(h, 0, 7), C1)
                wait_pr(96, C0, 7)
                for h in range(2):
                    add(0, rs_(h, 6, 2), C0)
                    add(0, rs_(h, 7), C1)

    @pl.when((z == 0) | (z == 3))
    def _():
        pl.semaphore_wait(far, n_near)

    @pl.when(c > z)
    def _():
        o_ref[...] = jnp.zeros_like(o_ref)

    @pl.when(c == z)
    def _():
        wait_recv(R.at[pl.ds(0, 3)], r_r.at[0])
        total = Qa[dq] + R[0] + R[1] + R[2]
        diff = lax.broadcasted_iota(jnp.int32, (rows, rows), 0) - lax.broadcasted_iota(jnp.int32, (rows, rows), 1)
        o_ref[...] = jnp.where(diff >= 0, total, 0.0).astype(o_ref.dtype)

    @pl.when((z == 1) & (c == 0))
    def _():
        wait_recv(R.at[pl.ds(0, 3)], r_r.at[0])
        Qa[0] += R[0] + R[1] + R[2]
        wait_recv(R.at[pl.ds(0, 3), pl.ds(0, half)], r_r.at[1])
        for b in range(2):
            PR[0, pl.ds(0, half), COLS[b]] = QD[b]
        o_ref[...] = (Qa[0] + PR[0] + PR[1]).astype(o_ref.dtype)

    @pl.when((z == 2) & (y == 0))
    def _():
        wait_recv(R.at[0], r_r.at[0])
        wait_recv(R.at[1, pl.ds(0, 32)], r_r.at[1])
        for h in range(2):
            Pa[0, rs_(h, 7), :] += R[1, rs_(h, 7), :]
        o_ref[...] = (Pa[0] + R[0]).astype(o_ref.dtype)

    @pl.when((z == 3) & (c == 2))
    def _():
        wait_recv(R, r_r.at[0])
        o_ref[...] = (R[0] + R[1] + R[2] + R[3]).astype(o_ref.dtype)

    @pl.when((z == 3) & (y == 0))
    def _():
        wait_recv(R.at[pl.ds(0, 2)], r_r.at[0])

        o_ref[...] = (R[0] + R[1]).astype(o_ref.dtype)

    @pl.when(c != z)
    def _():
        wait_recv(Qa.at[0], s_z.at[3])

    @pl.when((z == 0) | (z == 3))
    def _():
        wait_recv(X.at[k], s_z.at[0])

    @pl.when(z == 1)
    def _():
        wait_recv(W.at[:, :, pl.ds(0, ku)], s_z.at[0])
        wait_recv(W.at[:, :, pl.ds(0, kd)], s_z.at[1])
        wait_recv(Pa, s_z.at[2])

        @pl.when(c != 0)
        def _():
            wait_recv(R.at[pl.ds(0, 3), pl.ds(0, half)], s_z.at[4])

    @pl.when(z == 2)
    def _():
        wait_recv(W.at[:, :, pl.ds(0, kd)], s_z.at[0])
        wait_recv(W.at[:, :, pl.ds(0, ku)], s_z.at[1])
        wait_recv(Qa.at[1], s_z.at[4])

        @pl.when(y == 0)
        def _():
            wait_recv(Pa.at[0], s_z.at[2])

        @pl.when(y == 1)
        def _():
            wait_recv(Pa, s_z.at[2])


def solution(mesh):
    def local_fn(a_local):
        rows, m = a_local.shape
        kd = m - NU * PW - XU
        f32, bf16 = jnp.float32, jnp.bfloat16
        dma = pltpu.SemaphoreType.DMA
        return pl.pallas_call(
            kernel,
            out_shape=pltpu.VMEM((rows, rows), bf16),
            in_specs=[pl.BlockSpec(memory_space=pl.ANY)],
            out_specs=pl.BlockSpec(memory_space=pltpu.VMEM),
            scratch_shapes=[
                pltpu.VMEM((2, rows, m), bf16),
                pltpu.VMEM((2, rows, m), bf16),
                pltpu.VMEM((2, rows, kd), bf16),
                pltpu.VMEM((2, 2, kd, rows // 2), bf16),
                pltpu.VMEM((2, kd, rows), bf16),
                pltpu.VMEM((2, rows, rows), f32),
                pltpu.VMEM((2, rows, rows // 2), f32),
                pltpu.VMEM((2, rows, rows), f32),
                pltpu.VMEM((2, rows // 2, rows // 2), f32),
                pltpu.VMEM((4, rows, rows), f32),
                pltpu.VMEM((2, rows, rows), f32),
                pltpu.VMEM((rows, rows), f32),
                pltpu.VMEM((2, rows, rows // 2), f32),
                pltpu.SemaphoreType.REGULAR,
                dma((1,)), dma((5,)), dma((3 * NS,)), dma((NS + 1,)), dma((NU + 1,)), dma((8,)), dma((2,)), dma((9,)),
            ],
            compiler_params=pltpu.CompilerParams(
                collective_id=0, has_side_effects=True, vmem_limit_bytes=56 * 1024 * 1024),
        )(a_local)

    part_spec = P(("batch", "row"), "col")
    return jax.shard_map(local_fn, mesh=mesh, in_specs=(part_spec,), out_specs=part_spec, check_vma=False)
```

```python
import jax
import jax.numpy as jnp
from jax import lax
from jax.experimental import pallas as pl
from jax.experimental.pallas import tpu as pltpu
from jax.sharding import PartitionSpec as P

MESH = pl.DeviceIdType.MESH
PW = 256
NU = 15
XU = 128
NS = 8


def mm(a, b):
    return lax.dot_general(a, b, (((1,), (1,)), ((), ())), preferred_element_type=jnp.float32)


def mn(a, b):
    return lax.dot_general(a, b, (((1,), (0,)), ((), ())), preferred_element_type=jnp.float32)


def kernel(a_ref, o_ref, X, Y, W, T0, T1, Pa, Pb, Qa, QD, R, PR, XA, XB, far, ld, s_z, r_y, r_d, r_w, r_p, r_r, r_x):
    rows, m = a_ref.shape
    ku = NU * PW + XU
    kd = m - ku
    nd, xd = kd // PW, kd % PW
    half = rows // 2
    st = half // NS
    us = rows // NS
    z = lax.axis_index("row")
    c = lax.axis_index("col")
    y = c // 2
    k = c % 2
    sib = 2 * y + 1 - k

    def rcopy(src, dst, ss, rs, row, col):
        return pltpu.make_async_remote_copy(
            src_ref=src, dst_ref=dst, send_sem=ss, recv_sem=rs, device_id={"row": row, "col": col}, device_id_type=MESH)

    def wait_recv(ref, sem):
        pltpu.make_async_copy(ref, ref, sem).wait()

    def up(p, w=PW):
        return pl.ds(pl.multiple_of(p * PW, 128), w)

    def dn(p, w=PW):
        return pl.ds(pl.multiple_of(ku + p * PW, 128), w)

    def rs_(h, s, n=1):
        return pl.ds(pl.multiple_of(h * half + s * st, st), n * st)

    def us_(s):
        return pl.ds(pl.multiple_of(s * us, us), us)

    DALL = pl.ds(ku, kd)
    UALL = pl.ds(0, ku)
    C0, C1 = pl.ds(0, half), pl.ds(half, half)
    COLS = (C0, C1)

    def each(lo, hi, fn):
        lax.fori_loop(lo, hi, lambda i, u: (fn(i), u)[1], 0)

    load = pltpu.make_async_copy(a_ref, X.at[k], ld.at[0])

    def near(sem):
        for dz in (-1, 1):
            @pl.when((z + dz >= 0) & (z + dz <= 3))
            def _():
                for kk in range(2):
                    pl.semaphore_signal(sem, inc=1, device_id={"row": z + dz, "col": 2 * y + kk}, device_id_type=MESH)
        for dc in range(1, 4):
            pl.semaphore_signal(sem, inc=1, device_id={"row": z, "col": (c + dc) % 4}, device_id_type=MESH)

    n_near = jnp.where((z == 0) | (z == 3), 5, 7)
    bar = pltpu.get_barrier_semaphore()
    near(bar)
    load.start()
    pl.semaphore_wait(bar, n_near)

    def z0_u(q, w=PW):
        return rcopy(a_ref.at[:, up(q, w)], Y.at[k, :, up(q, w)], s_z.at[0], r_y.at[q // 2], 1, c)

    def z0_d(t):
        r = rs_(0, t)
        return rcopy(a_ref.at[r, DALL], Y.at[k, r, DALL], s_z.at[0], r_y.at[NS + t], 1, c)

    def z3_d(t):
        r = rs_(t % 2, t // 2)
        return rcopy(a_ref.at[r, DALL], Y.at[k, r, DALL], s_z.at[0], r_y.at[t], 2, c)

    def z3_u(s):
        r = us_(s)
        return rcopy(a_ref.at[r, UALL], Y.at[k, r, UALL], s_z.at[0], r_y.at[2 * NS + s], 2, c)

    def z1_u(q, w=PW):
        return rcopy(a_ref.at[:, up(q, w)], W.at[k, :, up(q, w)], s_z.at[0], r_w.at[(q + 1) // 2], 2, 2 * y + 1)

    def z2_d(t):
        h, s = t % 2, t // 2
        return rcopy(a_ref.at[rs_(h, s), DALL], W.at[k, rs_(1, s), pl.ds(0, kd)], s_z.at[0], r_w.at[jnp.where(s < 6, 1 + s // 2, s - 2)], 1, 2 * y + h)

    @pl.when(z == 0)
    def _():
        each(0, NU, lambda q: z0_u(q).start())
        z0_u(NU, XU).start()
        each(0, 2 * NS, lambda t: z0_d(t).start())

    @pl.when(z == 3)
    def _():
        each(0, 2 * NS, lambda t: z3_d(t).start())
        each(0, NS, lambda s: z3_u(s).start())

    x_d = rcopy(a_ref.at[:, DALL], X.at[k, :, DALL], s_z.at[1], r_d.at[NS], z, sib)
    x_u = rcopy(a_ref.at[:, UALL], X.at[k, :, UALL], s_z.at[1], r_d.at[NS], z, sib)

    @pl.when(z == 1)
    def _():
        each(0, NU, lambda q: z1_u(q).start())
        z1_u(NU, XU).start()
        x_d.start()

    @pl.when(z == 2)
    def _():
        z2_d(0).start()
        z2_d(1).start()
        x_u.start()

    near(far)

    Pa[...] = jnp.zeros_like(Pa)
    Qa[...] = jnp.zeros_like(Qa)
    Pb[...] = jnp.zeros_like(Pb)
    load.wait()
    dq = jnp.where(z == 1, 1, 0)

    def diag(p):
        cs = pl.ds(pl.multiple_of(p * 512, 512), 512)
        Qa[dq] += mm(X[k, :, cs], X[k, :, cs])

    each(0, m // 512, diag)

    def slot(owner):
        return (c - owner + 3) % 4

    dsend = rcopy(Qa.at[dq], R.at[slot(z)], s_z.at[3], r_r.at[0], z, z)

    @pl.when(c != z)
    def _():
        dsend.start()

    def u_fwd(q, w=PW):
        return rcopy(Y.at[k, :, up(q, w)], W.at[k, :, up(q, w)], s_z.at[0], r_w.at[(q + 1) // 2], 2, 2 * y)

    def zU(q, w=PW):
        wait_recv(Y.at[k, :, up(q, w)], r_y.at[q // 2])
        Qa[0] += mm(X[k, :, up(q, w)], Y[k, :, up(q, w)])

    def turn(p, w=PW):
        for h in range(2):
            T1[h, up(p, w), :] = X[h, :, dn(p, w)].T

    def d_sib(t):
        return rcopy(Y.at[k, rs_(0, t), DALL], Y.at[k, rs_(0, t), DALL], s_z.at[1], r_d.at[t // NS], z, sib)

    def zD(t):
        wait_recv(Y.at[k, rs_(0, t), DALL], r_y.at[NS + t])
        d_sib(t).start()

    def brows(b):
        return pl.ds(pl.multiple_of(b * half, half), half)

    def wait_w(r, n):
        wait_recv(W.at[:, r, pl.ds(0, kd)], r_w.at[n])

    CA = pl.ds(0, rows)
    peer = (c + 2) % 4

    def r3(u):
        return rs_(0, 4 * u, 4)

    def r2(s, n=2):
        return rs_(1, s, n)

    def xsend(src, dst, n):
        return rcopy(src, dst, s_z.at[2], r_x.at[n], 1, peer)

    x31 = xsend(Pa.at[1, rs_(0, 0, NS)], XA.at[rs_(0, 0, NS)], 0)

    def x30(b, u):
        return xsend(Pb.at[b, r3(u)], XB.at[b, r3(u)], 1 + 2 * b + u)

    def x21(s, n, rs):
        return xsend(Pa.at[1, r2(s, n)], XA.at[r2(s, n)], rs)

    def x20(b, s, n, rs):
        return xsend(Pb.at[b, r2(s, n)], XB.at[b, r2(s, n)], rs)

    def msend(src, i, s, n, j, cols, rs):
        return rcopy(src, PR.at[i, rs_(k, s, n), cols], s_z.at[2], r_p.at[rs], 2, j)

    m31 = msend(Pa.at[1, rs_(0, 0, NS)], 1, 0, NS, 3, CA, 0)

    def m30(b, u):
        return msend(Pb.at[b, r3(u)], 1, 4 * u, 4, 0, C0, 0)

    def m30r(u):
        return rcopy(Pb.at[1, rs_(0, 2 * u, 2)], PR.at[1, rs_(k, 2 * u, 2), C1], s_z.at[2], r_p.at[1 + u], 2, 2 * y)

    def m21(s, n, rs):
        return msend(Pa.at[1, r2(s, n)], 0, s, n, 1, CA, rs)

    def m20(b, s, n, rs):
        return msend(Pb.at[b, r2(s, n)], 0, s, n, 0, COLS[b], rs)

    def d2(src, j, cols):
        return rcopy(src, R.at[1, rs_(k, 7), cols], s_z.at[2], r_r.at[1], 2, j)

    d21 = d2(Pa.at[1, r2(7, 1)], 1, CA)
    d20 = [d2(Pb.at[b, r2(7, 1)], 0, COLS[b]) for b in range(2)]

    def part1(r):
        Pa[1, r, :] = mn(W[0, r, :kd], T1[0]) + mn(W[1, r, :kd], T1[1])

    def part0(r, b):
        Pb[b, r, :] = mn(W[0, r, :kd], T0[0, b]) + mn(W[1, r, :kd], T0[1, b])

    q_u = rcopy(Qa.at[0], R.at[slot(0)], s_z.at[4], r_r.at[0], 1, 0)

    def q_d(b):
        return rcopy(QD.at[b], PR.at[y, rs_(k, 0, NS), COLS[b]], s_z.at[4], r_r.at[1], 1, 0)

    @pl.when(z == 1)
    def _():
        wait_recv(X.at[1 - k, :, DALL], r_d.at[NS])

        def step_u(p):
            zU(2 * p, 2 * PW)

            @pl.when(p < 3)
            def _():
                each(2 * p, 2 * p + 2, lambda q: u_fwd(q).start())

            turn(2 * p)
            turn(2 * p + 1)

        each(0, NU // 2, step_u)
        zU(NU - 1, PW + XU)
        turn(NU - 1)
        each(NU, nd, turn)
        if xd:
            turn(nd, xd)

        @pl.when(c != 0)
        def _():
            q_u.start()

        pl.semaphore_wait(far, n_near)

        def turn0(h, b, lo, hi):
            T0[h, b, lo:hi, :] = Y[h, brows(b), pl.ds(ku + lo, hi - lo)].T

        def step(i):
            @pl.when(i < 2 * NS)
            def _():
                zD(i)

            @pl.when(i == 3)
            def _():
                wait_w(rs_(0, 0, NS), 0)
                part1(rs_(0, 0, NS))

                @pl.when(y == 0)
                def _():
                    x31.start()

                each(6, 10, lambda q: u_fwd(q).start())

            @pl.when((i == 5) & (y == 1))
            def _():
                wait_recv(XA.at[rs_(0, 0, NS)], r_x.at[0])
                Pa[1, rs_(0, 0, NS), :] += XA[rs_(0, 0, NS), :]
                m31.start()

            @pl.when(i == 16)
            def _():
                def chunk(n):
                    ch = jnp.where(n == 0, k, 1 - k)

                    @pl.when(n == 1)
                    def _():
                        turn0(k, 1, 0, 2048)
                        wait_recv(Y.at[1 - k, brows(1), DALL], r_d.at[1])

                    Pb[1, pl.ds(0, rows - st), :] += mm(W[ch, pl.ds(0, rows - st), :kd], Y[ch, brows(1), DALL])

                each(0, 2, chunk)

                for u in range(4):
                    m30r(u).start()

                @pl.when(y == 1)
                def _():
                    x20(1, 0, 4, 8).start()
                    x20(1, 4, 3, 4).start()

            @pl.when((i == 7) | (i == 17))
            def _():
                b = jnp.where(i == 7, 0, 1)

                @pl.when(b == 0)
                def _():
                    wait_recv(Y.at[1 - k, brows(0), DALL], r_d.at[0])

                turn0(1 - k, b, 0, kd)
                turn0(k, b, 2048, kd)

                @pl.when(b == 0)
                def _():
                    turn0(k, 0, 0, 2048)
                    part0(rs_(0, 0, NS), 0)

                    @pl.when(y == 1)
                    def _():
                        for u in range(2):
                            x30(0, u).start()

            @pl.when((i == 7) | (i == 17))
            def _():
                b = jnp.where(i == 7, 0, 1)
                r = rs_(k, 0, NS)
                QD[b] = mn(X[0, r, DALL], T0[0, b]) + mn(X[1, r, DALL], T0[1, b])
                for bb in range(2):
                    @pl.when((b == bb) & (c != 0))
                    def _():
                        q_d(bb).start()

            @pl.when(i == 7)
            def _():
                each(10, NU, lambda q: u_fwd(q).start())
                u_fwd(NU, XU).start()

            @pl.when((i == 9) & (y == 0))
            def _():
                for u in range(2):
                    wait_recv(XB.at[0, r3(u)], r_x.at[1 + u])
                    Pb[0, r3(u), :] += XB[0, r3(u), :]
                    m30(0, u).start()

            @pl.when((i == 8) | (i == 9) | (i == 13))
            def _():
                g = jnp.where(i == 13, 2, i - 8)
                wait_w(r2(2 * g), 1 + g)
                part1(r2(2 * g))
                part0(r2(2 * g), 0)

                @pl.when(y == 1)
                def _():
                    x21(2 * g, 2, 5 + g).start()
                    x20(0, 2 * g, 2, 5 + g).start()

            @pl.when(((i == 10) | (i == 11) | (i == 15)) & (y == 0))
            def _():
                g = jnp.where(i == 15, 2, i - 10)
                wait_recv(XA.at[pl.ds(0, 48)], r_x.at[5 + g])
                Pa[1, r2(2 * g), :] += XA[r2(2 * g), :]
                Pb[0, r2(2 * g), :] += XB[0, r2(2 * g), :]
                m21(2 * g, 2, 1).start()
                m20(0, 2 * g, 2, 5).start()

            @pl.when((i == 17) & (y == 0))
            def _():
                wait_recv(XA.at[pl.ds(0, 24)], r_x.at[3])
                Pa[1, r2(6, 1), :] += XA[r2(6, 1), :]
                m21(6, 1, 2).start()
                Pb[0, r2(6, 1), :] += XB[0, r2(6, 1), :]
                m20(0, 6, 1, 7).start()

            @pl.when((i == 14) | (i == 18))
            def _():
                t = jnp.where(i == 14, 6, 7)
                wait_w(r2(t, 1), t - 2)
                part1(r2(t, 1))

                @pl.when((y == 1) & (i == 18))
                def _():
                    d21.start()

                @pl.when((y == 0) & (i == 18))
                def _():
                    m21(7, 1, 2).start()

                part0(r2(t, 1), 0)

                @pl.when((y == 1) & (i == 14))
                def _():
                    x21(6, 1, 3).start()
                    x20(0, 6, 1, 3).start()

                @pl.when((y == 1) & (i == 18))
                def _():
                    d20[0].start()

                @pl.when((y == 0) & (i == 18))
                def _():
                    m20(0, 7, 1, 7).start()
                    for f, n, x in ((0, 4, 8), (4, 3, 4)):
                        wait_recv(XB.at[1, r2(f, n)], r_x.at[x])
                        Pb[1, r2(f, n), :] += XB[1, r2(f, n), :]
                        m20(1, f, n, 6).start()

                @pl.when(i == 18)
                def _():
                    part0(r2(7, 1), 1)

                    @pl.when(y == 1)
                    def _():
                        d20[1].start()

                    @pl.when(y == 0)
                    def _():
                        m20(1, 7, 1, 7).start()

        each(0, 19, step)

    def d_fwd(t):
        h, s = t % 2, t // 2
        return rcopy(Y.at[k, rs_(h, s), DALL], W.at[k, rs_(0, s), pl.ds(0, kd)], s_z.at[0], r_w.at[0], 1, 2 * y + h)

    def u_sib(s):
        return rcopy(Y.at[k, us_(s), UALL], Y.at[k, us_(s), UALL], s_z.at[1], r_d.at[s], z, sib)

    def q1send(s):
        return rcopy(Qa.at[1, us_(s)], R.at[c, us_(s)], s_z.at[4], r_r.at[0], 3, 2)

    def y2(q, w=PW):
        @pl.when((q == 0) | (q == NU))
        def _():
            wait_recv(W.at[:, :, up(q, w)], r_w.at[(q + 1) // 2])

        @pl.when((q % 2 == 1) & (q < NU))
        def _():
            wait_recv(W.at[:, :, pl.ds(0, 2 * PW)], r_w.at[(q + 1) // 2])

        Pa[0] += mm(X[0, :, up(q, w)], W[0, :, up(q, w)]) + mm(X[1, :, up(q, w)], W[1, :, up(q, w)])

    def y3(b, q, w=PW):
        r = pl.ds(b * half, half)
        Pa[1, r, :] += mm(Y[0, r, up(q, w)], W[0, :, up(q, w)]) + mm(Y[1, r, up(q, w)], W[1, :, up(q, w)])

    def wait_ysib(s):
        wait_recv(Y.at[1 - k, us_(s), UALL], r_d.at[s])

    def s3(r, cols=CA):
        return rcopy(Pa.at[1, r, cols], R.at[y, r, cols], s_z.at[2], r_r.at[0], 3, k)

    s2 = rcopy(Pa.at[0], R.at[0], s_z.at[2], r_r.at[0], 2, k)

    def add(i, r, cols):
        Pa[i, r, cols] += PR[i, r, cols]

    def wait_pr(n, cols, sem):
        wait_recv(PR.at[0, pl.ds(0, n), cols], r_p.at[sem])

    def strip31(s):
        wait_ysib(s)
        r = us_(s)
        Pa[1, r, :] = mm(Y[0, r, UALL], W[0, :, :ku]) + mm(Y[1, r, UALL], W[1, :, :ku])

        @pl.when(y == 1)
        def _():
            add(1, r, CA)

        s3(r).start()

    @pl.when(z == 2)
    def _():
        def step_d(t):
            wait_recv(Y.at[k, rs_(t % 2, t // 2), DALL], r_y.at[t])
            d_fwd(t).start()

            @pl.when(t == 1)
            def _():
                wait_recv(X.at[1 - k, :, UALL], r_d.at[NS])

            @pl.when((k == 1) & (t >= 1))
            def _():
                y2(t - 1)

            r = rs_(t % 2, t // 2)
            Qa[1, r, :] = mm(Y[k, r, DALL], X[k, :, DALL])

        each(0, 2 * NS, step_d)
        each(2, 2 * NS, lambda t: z2_d(t).start())

        pl.semaphore_wait(far, n_near)

        @pl.when(k == 1)
        def _():
            y2(NU, XU)

            @pl.when(y == 1)
            def _():
                s2.start()


        def q1(s):
            Qa[1, us_(s), :] += mm(Y[k, us_(s), UALL], X[k, :, UALL])
            q1send(s).start()

        def step_u(s):
            @pl.when((k == 0) & (s >= 1))
            def _():
                y2(2 * s - 1)

            @pl.when(k == 0)
            def _():
                y2(2 * s)

            @pl.when((k == 0) & (s == 4))
            def _():
                each(0, 4, wait_ysib)
                each(0, 7, lambda q: y3(0, q))

            @pl.when((k == 0) & (s >= 4))
            def _():
                y3(0, 2 * s - 1)
                y3(0, 2 * s)

            wait_recv(Y.at[k, us_(s), UALL], r_y.at[2 * NS + s])
            u_sib(s).start()

            @pl.when((k == 1) & (y == 1) & (s == 4))
            def _():
                wait_recv(PR.at[1], r_p.at[0])

            @pl.when((k == 1) & (s >= 4) & (s <= 6))
            def _():
                each(2 * s - 8, 2 * s - 6, strip31)

            @pl.when((k == 1) | (s < NS - 1))
            def _():
                q1(s)

        each(0, NS, step_u)

        @pl.when(k == 1)
        def _():
            each(NS - 2, NS, strip31)

            @pl.when(y == 0)
            def _():
                wait_pr(192, CA, 1)
                for h in range(2):
                    add(0, rs_(h, 0, 6), CA)
                wait_pr(64, CA, 2)
                for h in range(2):
                    add(0, rs_(h, 6, 2), CA)

        @pl.when(k == 0)
        def _():
            y2(NU, XU)

            @pl.when(y == 1)
            def _():
                s2.start()

            y3(0, NU, XU)
            each(NS - 1, NS - y, q1)

            @pl.when(y == 0)
            def _():
                wait_pr(rows, C0, 0)
                add(1, pl.ds(0, half), C0)


            s3(pl.ds(0, half), C0).start()

            each(4, NS, wait_ysib)

            def low(b):
                r = pl.ds(pl.multiple_of(b * half, half), half)
                Pa[1, r, :] = mm(Y[0, r, UALL], W[0, :, :ku]) + mm(Y[1, r, UALL], W[1, :, :ku])

            each(1 + k, 2, low)

            @pl.when(y == 0)
            def _():
                add(1, pl.ds(half, half), C0)

            s3(pl.ds(half, half), C0).start()
            each(NS - 1, NS - 1 + y, q1)

            for u in range(4):
                wait_pr(64, C1, 1 + u)
                for h in range(2):
                    add(1, rs_(h, 2 * u, 2), C1)
                    s3(rs_(h, 2 * u, 2), C1).start()

            @pl.when(y == 0)
            def _():
                wait_pr(192, C0, 5)
                for h in range(2):
                    add(0, rs_(h, 0, 6), C0)
                wait_pr(224, C1, 6)
                for h in range(2):
                    add(0, rs_(h, 0, 7), C1)
                wait_pr(96, C0, 7)
                for h in range(2):
                    add(0, rs_(h, 6, 2), C0)
                    add(0, rs_(h, 7), C1)

    @pl.when((z == 0) | (z == 3))
    def _():
        pl.semaphore_wait(far, n_near)

    @pl.when(c > z)
    def _():
        o_ref[...] = jnp.zeros_like(o_ref)

    @pl.when(c == z)
    def _():
        wait_recv(R.at[pl.ds(0, 3)], r_r.at[0])
        total = Qa[dq] + R[0] + R[1] + R[2]
        diff = lax.broadcasted_iota(jnp.int32, (rows, rows), 0) - lax.broadcasted_iota(jnp.int32, (rows, rows), 1)
        o_ref[...] = jnp.where(diff >= 0, total, 0.0).astype(o_ref.dtype)

    @pl.when((z == 1) & (c == 0))
    def _():
        wait_recv(R.at[pl.ds(0, 3)], r_r.at[0])
        Qa[0] += R[0] + R[1] + R[2]
        wait_recv(R.at[pl.ds(0, 3), pl.ds(0, half)], r_r.at[1])
        for b in range(2):
            PR[0, pl.ds(0, half), COLS[b]] = QD[b]
        o_ref[...] = (Qa[0] + PR[0] + PR[1]).astype(o_ref.dtype)

    @pl.when((z == 2) & (y == 0))
    def _():
        wait_recv(R.at[0], r_r.at[0])
        wait_recv(R.at[1, pl.ds(0, 32)], r_r.at[1])
        for h in range(2):
            Pa[0, rs_(h, 7), :] += R[1, rs_(h, 7), :]
        o_ref[...] = (Pa[0] + R[0]).astype(o_ref.dtype)

    @pl.when((z == 3) & (c == 2))
    def _():
        wait_recv(R, r_r.at[0])
        o_ref[...] = (R[0] + R[1] + R[2] + R[3]).astype(o_ref.dtype)

    @pl.when((z == 3) & (y == 0))
    def _():
        wait_recv(R.at[pl.ds(0, 2)], r_r.at[0])

        o_ref[...] = (R[0] + R[1]).astype(o_ref.dtype)

    @pl.when(c != z)
    def _():
        wait_recv(Qa.at[0], s_z.at[3])

    @pl.when((z == 0) | (z == 3))
    def _():
        wait_recv(X.at[k], s_z.at[0])

    @pl.when(z == 1)
    def _():
        wait_recv(W.at[:, :, pl.ds(0, ku)], s_z.at[0])
        wait_recv(W.at[:, :, pl.ds(0, kd)], s_z.at[1])
        wait_recv(Pa, s_z.at[2])

        @pl.when(c != 0)
        def _():
            wait_recv(R.at[pl.ds(0, 3), pl.ds(0, half)], s_z.at[4])

    @pl.when(z == 2)
    def _():
        wait_recv(W.at[:, :, pl.ds(0, kd)], s_z.at[0])
        wait_recv(W.at[:, :, pl.ds(0, ku)], s_z.at[1])
        wait_recv(Qa.at[1], s_z.at[4])

        @pl.when(y == 0)
        def _():
            wait_recv(Pa.at[0], s_z.at[2])

        @pl.when(y == 1)
        def _():
            wait_recv(Pa, s_z.at[2])


def solution(mesh):
    def local_fn(a_local):
        rows, m = a_local.shape
        kd = m - NU * PW - XU
        f32, bf16 = jnp.float32, jnp.bfloat16
        dma = pltpu.SemaphoreType.DMA
        return pl.pallas_call(
            kernel,
            out_shape=pltpu.VMEM((rows, rows), bf16),
            in_specs=[pl.BlockSpec(memory_space=pl.ANY)],
            out_specs=pl.BlockSpec(memory_space=pltpu.VMEM),
            scratch_shapes=[
                pltpu.VMEM((2, rows, m), bf16),
                pltpu.VMEM((2, rows, m), bf16),
                pltpu.VMEM((2, rows, kd), bf16),
                pltpu.VMEM((2, 2, kd, rows // 2), bf16),
                pltpu.VMEM((2, kd, rows), bf16),
                pltpu.VMEM((2, rows, rows), f32),
                pltpu.VMEM((2, rows, rows // 2), f32),
                pltpu.VMEM((2, rows, rows), f32),
                pltpu.VMEM((2, rows // 2, rows // 2), f32),
                pltpu.VMEM((4, rows, rows), f32),
                pltpu.VMEM((2, rows, rows), f32),
                pltpu.VMEM((rows, rows), f32),
                pltpu.VMEM((2, rows, rows // 2), f32),
                pltpu.SemaphoreType.REGULAR,
                dma((1,)), dma((5,)), dma((3 * NS,)), dma((NS + 1,)), dma((9,)), dma((8,)), dma((2,)), dma((9,)),
            ],
            compiler_params=pltpu.CompilerParams(
                collective_id=0, has_side_effects=True, vmem_limit_bytes=56 * 1024 * 1024),
        )(a_local)

    part_spec = P(("batch", "row"), "col")
    return jax.shard_map(local_fn, mesh=mesh, in_specs=(part_spec,), out_specs=part_spec, check_vma=False)
```
